32 devices in a mesh: dp: 4 (over x, core), seq: 8 (over z, y).
Axes of the slice: x: 2, y: 2, z: 4, core: 2. Of those that a mesh axis runs over, the one named last changes fastest.
Arguments:
- hidden: bfloat16 [8, 1024, 2048], P('dp', 'seq'), may hold values from -6 to 6
- grad_out: bfloat16 [8, 1024, 2048], P('dp', 'seq'), may hold values from -6 to 6
- lengths: int32 [8], P('dp'), may hold values from 256 to 1024, as said below
- norm_gain: bfloat16 [2048], P('seq'), may hold values from 0.25 to 1.75
- input_weight: bfloat16 [2048, 8192], P('seq'), may hold values from -0.125 to 0.125
- conv_weight: bfloat16 [4, 4096], P(None, 'seq'), may hold values from -3 to 3
- conv_bias: bfloat16 [4096], P('seq'), may hold values from -3 to 3
- select_weight: bfloat16 [160, 4096], P(None, 'seq'), may hold values from -0.09375 to 0.09375
- step_weight: bfloat16 [128, 4096], P(None, 'seq'), may hold values from -0.5 to 0.5
- step_bias: bfloat16 [4096], P('seq'), may hold values from -13 to 0
- decay_log: bfloat16 [16, 4096], P(None, 'seq'), may hold values from -0.69921875 to 1.3984375
- skip_weight: bfloat16 [4096], P('seq'), may hold values from 0.5 to 2
- output_weight: bfloat16 [4096, 2048], P('seq'), may hold values from -0.25 to 0.25
Outputs:
- output: bfloat16 [8, 1024, 2048], P('dp', 'seq')
- grad_hidden: float32 [8, 1024, 2048], P('dp', 'seq')
- grad_norm_gain: float32 [2048], P('seq')
- grad_input_weight: float32 [2048, 8192], P('seq')
- grad_conv_weight: float32 [4, 4096], P(None, 'seq')
- grad_conv_bias: float32 [4096], P('seq')
- grad_select_weight: float32 [160, 4096], P(None, 'seq')
- grad_step_weight: float32 [128, 4096], P(None, 'seq')
- grad_step_bias: float32 [4096], P('seq')
- grad_decay_log: float32 [16, 4096], P(None, 'seq')
- grad_skip_weight: float32 [4096], P('seq')
- grad_output_weight: float32 [4096, 2048], P('seq')
The draws below stay inside these ranges and needn't reach their ends.
Inputs may be any that keep to these rules, and one draw needn't show every extreme that they name: Row r holds one sequence in slots 0 to lengths[r] - 1 and padding after it; some row is full.
All inputs are finite; a program needn't handle non-finite values.
Results may differ from the reference program's by a relative error of at most 0.012.
Values may be sent and summed in bfloat16 or wider, within the bound.
A program may use at most 320 MiB of HBM per device.

```python
import math
import jax
import jax.numpy as jnp
from jax import lax

D = 2048
E = 4096
N = 16
R = 128
K = 4
BLOCK = 16
ROWS = 8
SLOTS = 1024


def draw_lengths(key, part):
    length_key, place_key = jax.random.split(key)
    drawn = jax.random.randint(length_key, (ROWS,), SLOTS // 4, SLOTS + 1)
    longest = jax.random.randint(place_key, (), 0, ROWS)
    return jnp.where(jnp.arange(ROWS) == longest, SLOTS, drawn).astype(jnp.int32)


def draw_step_bias(key, part):
    pick_key, fast_key, slow_key = jax.random.split(key, 3)
    slow_share = 0.5
    slow_mask = jax.random.uniform(pick_key, (E,), jnp.float32) < slow_share
    fast_rate = jnp.exp(jax.random.uniform(fast_key, (E,), jnp.float32, math.log(0.02), math.log(0.5)))
    slow_rate = jnp.exp(jax.random.uniform(slow_key, (E,), jnp.float32, math.log(0.1), math.log(0.5))) / SLOTS
    rate_value = jnp.where(slow_mask, slow_rate, fast_rate)
    return jnp.log(jnp.expm1(rate_value)).astype(jnp.bfloat16)


def steps_of(rng, extent, shards, smallest, high):
    def one(axis_at, shards_of):
        heights = jax.random.uniform(jax.random.fold_in(jax.random.fold_in(rng, 6), axis_at), (shards_of,), jnp.float32, smallest / len(shards), high / len(shards))
        return jnp.repeat(jnp.exp(heights), extent[axis_at] // shards_of).reshape((-1,) + (1,) * (len(extent) - axis_at - 1))

    loudness = one(*shards[0])
    for cut in shards[1:]:
        loudness = loudness * one(*cut)
    return loudness


def gaussian(stream_key, extent, deviation, reach, cuts=(), held_as=jnp.bfloat16):
    values = jax.random.normal(stream_key, extent, jnp.float32) * deviation
    if len(cuts) > 0:
        values = steps_of(stream_key, extent, cuts, -0.22, 0.18) * values
    return jnp.clip(values, min=-reach, max=reach).astype(held_as)


def setup_inputs(seed: int = 0) -> dict:
    keys = jax.random.split(jax.random.key(seed), 14)
    return {
        "hidden": gaussian(keys[0], (ROWS, SLOTS, D), 1.0, 6.0, ((0, 4), (1, 8))),
        "grad_out": gaussian(keys[1], (ROWS, SLOTS, D), 1.0, 6.0, ((0, 4), (1, 8))),
        "lengths": draw_lengths(jax.random.fold_in(keys[13], 71), 0),
        "norm_gain": jnp.clip(1.0 + 0.15 * jax.random.normal(keys[3], (D,), jnp.float32), 0.25, 1.75).astype(jnp.bfloat16),
        "input_weight": gaussian(keys[4], (D, 2 * E), D ** -0.5, 0.125, ((0, 8),)),
        "conv_weight": gaussian(keys[5], (K, E), K ** -0.5, 3.0, ((1, 8),)),
        "conv_bias": gaussian(keys[6], (E,), 0.5, 3.0, ((0, 8),)),
        "select_weight": gaussian(keys[7], (R + 2 * N, E), E ** -0.5, 0.09375, ((1, 8),)),
        "step_weight": gaussian(keys[8], (R, E), R ** -0.5, 0.5, ((1, 8),)),
        "step_bias": draw_step_bias(jax.random.fold_in(keys[13], 71), 0),
        "decay_log": jnp.clip(-0.69921875 + 2.0976562 * jax.random.uniform(keys[10], (N, E), jnp.float32) ** steps_of(keys[10], (N, E), ((1, 8),), -0.2, 0.2), -0.69921875, 1.3984375).astype(jnp.bfloat16),
        "skip_weight": jnp.clip(jnp.exp(math.log(2.0) - 1.3862944 * jax.random.uniform(keys[11], (E,), jnp.float32) ** steps_of(keys[11], (E,), ((0, 8),), -0.2, 0.2)), 0.5, 2.0).astype(jnp.bfloat16),
        "output_weight": gaussian(keys[12], (E, D), (E // 8) ** -0.5, 0.25, ((0, 8),)),
    }


@jax.custom_vjp
def low(v):
    return lax.optimization_barrier(v.astype(jnp.bfloat16)).astype(jnp.float32)

@jax.custom_vjp
def low_back(v):
    return v

def low_keep(v):
    return (low(v), None)

def low_pass(kept, grad):
    return (grad,)

def back_keep(v):
    return (v, None)

def back_low(kept, grad):
    return (low(grad),)
low.defvjp(low_keep, low_pass)
low_back.defvjp(back_keep, back_low)
EPSILON = 1e-05
HIGHEST = lax.Precision.HIGHEST

def mixer_row(source, valid_mask, norm_gain, input_weight, conv_weight, conv_bias, select_weight, step_weight, step_bias, decay_log, skip_weight, output_weight):
    inverse = lax.rsqrt(lax.optimization_barrier(jnp.mean(source * source, axis=-1, keepdims=True)) + EPSILON)
    normed = low(source * inverse * norm_gain)
    projected = low_back(jnp.dot(normed, input_weight, precision=HIGHEST))
    conv_input = low(projected[:, :E])
    gate_input = projected[:, E:]
    extended = jnp.concatenate([jnp.zeros((K - 1, E), jnp.float32), conv_input], axis=0)
    conv_sum = conv_bias + sum((conv_weight[tap_index] * extended[tap_index:tap_index + SLOTS] for tap_index in range(K)))
    conv_vals = low(jax.nn.silu(conv_sum))
    selected = low_back(jnp.dot(conv_vals, select_weight.T, precision=HIGHEST))
    step_low = low(selected[:, :R])
    input_coef = selected[:, R:R + N]
    output_coef = selected[:, R + N:]
    step_size = jax.nn.softplus(low_back(jnp.dot(step_low, step_weight, precision=HIGHEST) + step_bias))
    decay_rate = -jnp.exp(decay_log)

    def one_block(state_now, block_items):
        step_block, value_block, input_block, output_block = block_items
        outputs = []
        for offset in range(BLOCK):
            factor = jnp.exp(step_block[offset][None, :] * decay_rate)
            drive_term = (step_block[offset] * value_block[offset])[None, :] * input_block[offset][:, None]
            state_now = factor * state_now + drive_term
            outputs.append(lax.optimization_barrier(jnp.sum(output_block[offset][:, None] * state_now, axis=0)))
        return (state_now, jnp.stack(outputs))
    block_count = SLOTS // BLOCK
    _, produced = lax.scan(jax.checkpoint(one_block), jnp.zeros((N, E), jnp.float32), (step_size.reshape(block_count, BLOCK, E), conv_vals.reshape(block_count, BLOCK, E), input_coef.reshape(block_count, BLOCK, N), output_coef.reshape(block_count, BLOCK, N)))
    ssm_out = produced.reshape(SLOTS, E) + skip_weight * conv_vals
    gated = low(ssm_out * jax.nn.silu(gate_input))
    mixed = low_back(jnp.dot(gated, output_weight, precision=HIGHEST))
    return (source + mixed) * valid_mask[:, None]

def reference(hidden, grad_out, lengths, norm_gain, input_weight, conv_weight, conv_bias, select_weight, step_weight, step_bias, decay_log, skip_weight, output_weight):
    params = tuple((weight_value.astype(jnp.float32) for weight_value in (norm_gain, input_weight, conv_weight, conv_bias, select_weight, step_weight, step_bias, decay_log, skip_weight, output_weight)))
    slot_ids = jnp.arange(SLOTS).astype(jnp.int32)

    def one_row(totals, row_items):
        row_values, row_cot, row_length = row_items
        valid_mask = (slot_ids < row_length).astype(jnp.float32)

        def forward(source, *weights):
            return mixer_row(source, valid_mask, *weights)
        result, backward = jax.vjp(forward, row_values.astype(jnp.float32), *params)
        grads = backward(row_cot.astype(jnp.float32))
        totals = tuple((total_value + grad_value for total_value, grad_value in zip(totals, grads[1:])))
        return (totals, (result.astype(jnp.bfloat16), grads[0]))
    zero_sums = tuple((jnp.zeros(weight_value.shape, jnp.float32) for weight_value in params))
    sums, (output, grad_hidden) = lax.scan(one_row, zero_sums, (hidden, grad_out, lengths))
    return (output, grad_hidden, sums[0], sums[1], sums[2], sums[3], sums[4], sums[5], sums[6], sums[7], sums[8], sums[9])
```

```python
import functools
import jax
import jax.numpy as jnp
from jax import lax
from jax.experimental import pallas as pl
from jax.experimental.pallas import tpu as pltpu

BLOCK = 16
LOG2E = 1.4426950408889634
F32 = jnp.float32
BF16 = jnp.bfloat16


def softplus(v):
    return jnp.maximum(v, 0.0) + jnp.log(1.0 + jnp.exp(-jnp.abs(v)))


def sigmoid(v):
    return 1.0 / (1.0 + jnp.exp(-v))


def nt_dot(a, b):
    return lax.dot_general(a, b, (((1,), (1,)), ((), ())), preferred_element_type=F32)


def tile_matrix(n, wide):
    col = lax.broadcasted_iota(jnp.int32, (n, wide), 1)
    row = lax.broadcasted_iota(jnp.int32, (n, wide), 0)
    return (col % n == row).astype(F32)


def diagonal_mask(rows, n, wide):
    col = lax.broadcasted_iota(jnp.int32, (rows, wide), 1)
    row = lax.broadcasted_iota(jnp.int32, (rows, wide), 0)
    return col // n == row % BLOCK


def scan_forward_kernel(sel_ref, x_ref, gate_ref, stepw_ref, bias_ref, decay_ref, skip_ref,
                        gated_ref, ssm_ref, start_ref,
                        dt_s, u_s, y_s, coef_s, bt_s, hist_s, state_s, *, rank, n):
    chunk = pl.program_id(1)
    length = x_ref.shape[-2]
    wide = BLOCK * n

    @pl.when(chunk == 0)
    def _():
        state_s[...] = jnp.zeros_like(state_s)

    start_ref[...] = state_s[...].reshape(start_ref.shape)
    selected = sel_ref[...].reshape(sel_ref.shape[-2:])
    x = x_ref[...].reshape(x_ref.shape[-2:]).astype(F32)
    low = selected[:, :rank].astype(BF16)
    pre = jnp.dot(low, stepw_ref[...], preferred_element_type=F32) + bias_ref[...]
    dt = softplus(pre)
    dt_s[...] = dt
    u_s[...] = dt * x
    tail = selected[:, rank:]
    bt_s[...] = tail.T
    spread = jnp.dot(tail[:, n:], tile_matrix(n, wide), preferred_element_type=F32)
    coef_s[...] = jnp.where(diagonal_mask(length, n, wide), spread, 0.0).astype(BF16)
    rate = -jnp.exp(decay_ref[...].astype(F32)) * LOG2E

    def block(k, state):
        at = pl.multiple_of(k * BLOCK, BLOCK)
        dts = dt_s[pl.ds(at, BLOCK), :]
        us = u_s[pl.ds(at, BLOCK), :]
        bs = pltpu.roll(bt_s[0:n, :], length - at, 1)
        for i in range(BLOCK):
            factor = jnp.exp2(dts[i:i + 1, :] * rate)
            state = factor * state + us[i:i + 1, :] * bs[:, i:i + 1]
            hist_s[i * n:(i + 1) * n, :] = state.astype(BF16)
        y_s[pl.ds(at, BLOCK), :] = jnp.dot(coef_s[pl.ds(at, BLOCK), :], hist_s[...], preferred_element_type=F32)
        return state

    state_s[...] = lax.fori_loop(0, length // BLOCK, block, state_s[...])
    gate = gate_ref[...].reshape(x.shape)
    ssm = y_s[...] + skip_ref[...] * x
    ssm_ref[...] = ssm.astype(ssm_ref.dtype).reshape(ssm_ref.shape)
    gated_ref[...] = (ssm * gate * sigmoid(gate)).astype(BF16).reshape(gated_ref.shape)


def scan_forward(sel, x, gate, stepw, bias, decay, skip, n):
    chunks, rows, length, width = x.shape
    rank = stepw.shape[0]
    wide = BLOCK * n
    tok = lambda feat: pl.BlockSpec((1, 1, length, feat), lambda r, c: (c, r, 0, 0))
    whole = lambda a: pl.BlockSpec(a.shape, lambda r, c: (0,) * a.ndim)
    return pl.pallas_call(
        functools.partial(scan_forward_kernel, rank=rank, n=n),
        grid=(rows, chunks),
        in_specs=[tok(sel.shape[-1]), tok(width), tok(width), whole(stepw), whole(bias), whole(decay), whole(skip)],
        out_specs=[tok(width), tok(width), pl.BlockSpec((1, 1, n, width), lambda r, c: (c, r, 0, 0))],
        out_shape=[
            jax.ShapeDtypeStruct((chunks, rows, length, width), BF16),
            jax.ShapeDtypeStruct((chunks, rows, length, width), BF16),
            jax.ShapeDtypeStruct((chunks, rows, n, width), F32),
        ],
        scratch_shapes=[
            pltpu.VMEM((length, width), F32), pltpu.VMEM((length, width), F32), pltpu.VMEM((length, width), F32),
            pltpu.VMEM((length, wide), BF16), pltpu.VMEM((2 * n, length), F32),
            pltpu.VMEM((wide, width), BF16), pltpu.VMEM((n, width), F32),
        ],
        name="scan_forward",
    )(sel, x, gate, stepw, bias, decay, skip)


def scan_backward_kernel(sel_ref, x_ref, gate_ref, gg_ref, ssm_ref, start_ref, stepw_ref, bias_ref, decay_ref, skip_ref,
                         ggate_ref, gvals_ref, gpre_ref, gsel_ref, gstepw_ref, gbias_ref, gdecay_ref, gskip_ref,
                         dt_s, u_s, gy_s, gu_s, ah_s, bcoef_s, bt_s, hist_s, adj_s, harm_s, db_s, dc_s, carry_s, gd_s, *, rank, n):
    row, step = pl.program_id(0), pl.program_id(1)
    length = x_ref.shape[-2]
    wide = BLOCK * n
    blocks = length // BLOCK
    flat = lambda ref: ref[...].reshape(ref.shape[-2:])

    @pl.when(step == 0)
    def _():
        carry_s[...] = jnp.zeros_like(carry_s)

    @pl.when((step == 0) & (row == 0))
    def _():
        gstepw_ref[...] = jnp.zeros_like(gstepw_ref)
        gbias_ref[...] = jnp.zeros_like(gbias_ref)
        gskip_ref[...] = jnp.zeros_like(gskip_ref)
        gd_s[...] = jnp.zeros_like(gd_s)

    selected = flat(sel_ref)
    x = flat(x_ref).astype(F32)
    gate = flat(gate_ref)
    gg = flat(gg_ref)
    ssm = flat(ssm_ref).astype(F32)
    sg = sigmoid(gate)
    gy = gg * gate * sg
    ggate_ref[...] = (gg * ssm * sg * (1.0 + gate * (1.0 - sg))).astype(BF16).reshape(ggate_ref.shape)
    gskip_ref[...] += jnp.sum(gy * x, axis=0, keepdims=True)
    gy_s[...] = gy
    low = selected[:, :rank].astype(BF16)
    pre = jnp.dot(low, stepw_ref[...], preferred_element_type=F32) + bias_ref[...]
    dt = softplus(pre)
    dt_s[...] = dt
    u_s[...] = dt * x
    tail = selected[:, rank:]
    bt_s[...] = tail.T
    tiles = tile_matrix(n, wide)
    spread = jnp.dot(tail[:, :n], tiles, preferred_element_type=F32)
    bcoef_s[...] = jnp.where(diagonal_mask(length, n, wide), spread, 0.0).astype(BF16)
    decay = -jnp.exp(decay_ref[...].astype(F32))
    rate = decay * LOG2E
    keep = diagonal_mask(BLOCK, n, wide)
    ones = keep.astype(BF16)
    start = start_ref[...].reshape(carry_s.shape)

    def again(k, state):
        at = pl.multiple_of(k * BLOCK, BLOCK)
        dts = dt_s[pl.ds(at, BLOCK), :]
        us = u_s[pl.ds(at, BLOCK), :]
        bs = pltpu.roll(bt_s[0:n, :], length - at, 1)
        for i in range(BLOCK):
            hist_s[pl.ds(pl.multiple_of((at + i) * n, n), n), :] = state.astype(BF16)
            factor = jnp.exp2(dts[i:i + 1, :] * rate)
            state = factor * state + us[i:i + 1, :] * bs[:, i:i + 1]
        return state

    last = lax.fori_loop(0, blocks, again, start)
    hist_s[pl.ds(length * n, n), :] = last.astype(BF16)

    def back(j, carried):
        carry, gd = carried
        k = blocks - 1 - j
        at = pl.multiple_of(k * BLOCK, BLOCK)
        dts = dt_s[pl.ds(at, BLOCK), :]
        gys = gy_s[pl.ds(at, BLOCK), :]
        cs = pltpu.roll(bt_s[n:2 * n, :], length - at, 1)
        for i in range(BLOCK - 1, -1, -1):
            dt_i = dts[i:i + 1, :]
            g = cs[:, i:i + 1] * gys[i:i + 1, :] + carry
            adj_s[i * n:(i + 1) * n, :] = g.astype(BF16)
            carry = jnp.exp2(dt_i * rate) * g
            h = carry * hist_s[pl.ds(pl.multiple_of((at + i) * n, n), n), :].astype(F32)
            harm_s[i * n:(i + 1) * n, :] = (h * decay).astype(BF16)
            gd = gd + dt_i * h
        adj = adj_s[...]
        rows = pl.ds(at, BLOCK)
        gu_s[rows, :] = jnp.dot(bcoef_s[rows, :], adj, preferred_element_type=F32)
        ah_s[rows, :] = jnp.dot(ones, harm_s[...], preferred_element_type=F32)
        db_s[rows, :] = jnp.where(keep, nt_dot(u_s[rows, :].astype(BF16), adj), 0.0)
        states = hist_s[pl.ds(pl.multiple_of((at + 1) * n, n), wide), :]
        dc_s[rows, :] = jnp.where(keep, nt_dot(gys.astype(BF16), states), 0.0)
        return carry, gd

    carry, gd = lax.fori_loop(0, blocks, back, (carry_s[...], gd_s[...]))
    carry_s[...] = carry
    gd_s[...] = gd
    gu = gu_s[...]
    gpre = ((x * gu + ah_s[...]) * sigmoid(pre)).astype(BF16)
    gpre_ref[...] = gpre.reshape(gpre_ref.shape)
    gvals_ref[...] = (gy * skip_ref[...] + dt * gu).astype(gvals_ref.dtype).reshape(gvals_ref.shape)
    gbias_ref[...] += jnp.sum(gpre.astype(F32), axis=0, keepdims=True)
    gstepw_ref[...] += jnp.dot(selected[:, :rank].T.astype(BF16), gpre, preferred_element_type=F32)
    fold = lambda ref: lax.dot_general(ref[...], tiles, (((1,), (1,)), ((), ())), preferred_element_type=F32, precision=lax.Precision.HIGHEST)
    lead = (0,) * (len(gsel_ref.shape) - 2)
    gsel_ref[lead + (slice(None), slice(0, rank))] = nt_dot(gpre, stepw_ref[...])
    gsel_ref[lead + (slice(None), slice(rank, rank + n))] = fold(db_s)
    gsel_ref[lead + (slice(None), slice(rank + n, rank + 2 * n))] = fold(dc_s)

    @pl.when((row == pl.num_programs(0) - 1) & (step == pl.num_programs(1) - 1))
    def _():
        gdecay_ref[...] = gd * decay


def scan_backward(sel, x, gate, gg, ssm, starts, stepw, bias, decay, skip, n):
    chunks, rows, length, width = x.shape
    rank = stepw.shape[0]
    wide = BLOCK * n
    at = lambda r, c: (chunks - 1 - c, r, 0, 0)
    tok = lambda feat: pl.BlockSpec((1, 1, length, feat), at)
    whole = lambda shape: pl.BlockSpec(shape, lambda r, c: (0,) * len(shape))
    sds = jax.ShapeDtypeStruct
    return pl.pallas_call(
        functools.partial(scan_backward_kernel, rank=rank, n=n),
        grid=(rows, chunks),
        in_specs=[tok(sel.shape[-1]), tok(width), tok(width), tok(width), tok(width), pl.BlockSpec((1, 1, n, width), at),
                  whole(stepw.shape), whole(bias.shape), whole(decay.shape), whole(skip.shape)],
        out_specs=[tok(width), tok(width), tok(width), tok(sel.shape[-1]), whole((rank, width)), whole((1, width)), whole((n, width)), whole((1, width))],
        out_shape=[
            sds(x.shape, BF16), sds(x.shape, F32), sds(x.shape, BF16), sds(sel.shape, F32),
            sds((rank, width), F32), sds((1, width), F32), sds((n, width), F32), sds((1, width), F32),
        ],
        scratch_shapes=[
            pltpu.VMEM((length, width), F32), pltpu.VMEM((length, width), F32), pltpu.VMEM((length, width), F32),
            pltpu.VMEM((length, width), F32), pltpu.VMEM((length, width), F32),
            pltpu.VMEM((length, wide), BF16), pltpu.VMEM((2 * n, length), F32),
            pltpu.VMEM(((length + 1) * n, width), BF16), pltpu.VMEM((wide, width), BF16), pltpu.VMEM((wide, width), BF16),
            pltpu.VMEM((length, wide), F32), pltpu.VMEM((length, wide), F32),
            pltpu.VMEM((n, width), F32), pltpu.VMEM((n, width), F32),
        ],
        name="scan_backward",
    )(sel, x, gate, gg, ssm, starts, stepw, bias, decay, skip)
def conv_forward_kernel(ci_ref, taps_ref, bias_ref, selw_ref, x_ref, sel_ref, ext_s):
    length = ci_ref.shape[-2]
    tap_count = taps_ref.shape[0]

    @pl.when(pl.program_id(1) == 0)
    def _():
        ext_s[0:8, :] = jnp.zeros((8, ext_s.shape[1]), F32)

    ext_s[8:, :] = ci_ref[...].reshape(ci_ref.shape[-2:]).astype(F32)
    total = bias_ref[...].astype(F32)
    for k in range(tap_count):
        total = total + taps_ref[k:k + 1, :].astype(F32) * ext_s[pl.ds(8 - tap_count + 1 + k, length), :]
    ext_s[0:8, :] = ext_s[length:length + 8, :]
    x = (total * sigmoid(total)).astype(BF16)
    x_ref[...] = x.reshape(x_ref.shape)
    sel_ref[...] = nt_dot(x, selw_ref[...]).reshape(sel_ref.shape)


def conv_forward(ci, taps, bias, selw):
    chunks, rows, length, width = ci.shape
    tok = lambda feat: pl.BlockSpec((1, 1, length, feat), lambda r, c: (c, r, 0, 0))
    whole = lambda a: pl.BlockSpec(a.shape, lambda r, c: (0,) * a.ndim)
    return pl.pallas_call(
        conv_forward_kernel,
        grid=(rows, chunks),
        in_specs=[tok(width), whole(taps), whole(bias), whole(selw)],
        out_specs=[tok(width), tok(selw.shape[0])],
        out_shape=[jax.ShapeDtypeStruct(ci.shape, BF16), jax.ShapeDtypeStruct((chunks, rows, length, selw.shape[0]), F32)],
        scratch_shapes=[pltpu.VMEM((length + 8, width), F32)],
        name="conv_forward",
    )(ci, taps, bias, selw)


def conv_backward_kernel(ci_ref, prev_ref, gvals_ref, gsel_ref, taps_ref, bias_ref, selw_ref,
                         gci_ref, gtaps_ref, gbias_ref, gselw_ref, ext_s, gext_s):
    row, step = pl.program_id(0), pl.program_id(1)
    length = ci_ref.shape[-2]
    tap_count = taps_ref.shape[0]
    flat = lambda ref: ref[...].reshape(ref.shape[-2:])

    @pl.when(step == 0)
    def _():
        gext_s[length:, :] = jnp.zeros((8, gext_s.shape[1]), F32)

    @pl.when((step == 0) & (row == 0))
    def _():
        gtaps_ref[...] = jnp.zeros_like(gtaps_ref)
        gbias_ref[...] = jnp.zeros_like(gbias_ref)
        gselw_ref[...] = jnp.zeros_like(gselw_ref)

    first = step == pl.num_programs(1) - 1
    ext_s[8:, :] = flat(ci_ref).astype(F32)
    before = flat(prev_ref)[length - 16:, :].astype(F32)[8:, :]
    ext_s[0:8, :] = jnp.where(first, 0.0, before)
    total = bias_ref[...].astype(F32)
    for k in range(tap_count):
        total = total + taps_ref[k:k + 1, :].astype(F32) * ext_s[pl.ds(8 - tap_count + 1 + k, length), :]
    sg = sigmoid(total)
    x = (total * sg).astype(BF16)
    gsel = flat(gsel_ref).astype(BF16)
    gvals = flat(gvals_ref) + jnp.dot(gsel, selw_ref[...], preferred_element_type=F32)
    gconv = gvals * sg * (1.0 + total * (1.0 - sg))
    gbias_ref[...] += jnp.sum(gconv, axis=0, keepdims=True)
    for k in range(tap_count):
        gtaps_ref[k:k + 1, :] += jnp.sum(gconv * ext_s[pl.ds(8 - tap_count + 1 + k, length), :], axis=0, keepdims=True)
    gselw_ref[...] += jnp.dot(flat(gsel_ref).T.astype(BF16), x, preferred_element_type=F32)
    gext_s[0:length, :] = gconv
    gci = jnp.zeros_like(gconv)
    for k in range(tap_count):
        gci = gci + taps_ref[k:k + 1, :].astype(F32) * gext_s[pl.ds(tap_count - 1 - k, length), :]
    gci_ref[...] = gci.astype(BF16).reshape(gci_ref.shape)
    gext_s[length:, :] = gconv[0:8, :]


def conv_backward(ci, gvals, gsel, taps, bias, selw):
    chunks, rows, length, width = ci.shape
    at = lambda r, c: (chunks - 1 - c, r, 0, 0)
    before = lambda r, c: (jnp.maximum(chunks - 2 - c, 0), r, 0, 0)
    tok = lambda feat, where: pl.BlockSpec((1, 1, length, feat), where)
    whole = lambda shape: pl.BlockSpec(shape, lambda r, c: (0,) * len(shape))
    sds = jax.ShapeDtypeStruct
    return pl.pallas_call(
        conv_backward_kernel,
        grid=(rows, chunks),
        in_specs=[tok(width, at), tok(width, before), tok(width, at), tok(gsel.shape[-1], at), whole(taps.shape), whole(bias.shape), whole(selw.shape)],
        out_specs=[tok(width, at), whole(taps.shape), whole(bias.shape), whole(selw.shape)],
        out_shape=[sds(ci.shape, BF16), sds(taps.shape, F32), sds(bias.shape, F32), sds(selw.shape, F32)],
        scratch_shapes=[pltpu.VMEM((length + 8, width), F32), pltpu.VMEM((length + 8, width), F32)],
        name="conv_backward",
    )(ci, ci, gvals, gsel, taps, bias, selw)
from jax.sharding import PartitionSpec as P

EPSILON = 1e-05


def local(hidden, grad_out, lengths, norm_gain, input_weight, conv_weight, conv_bias, select_weight,
          step_weight, step_bias, decay_log, skip_weight, output_weight):
    rows, length, model = hidden.shape
    chunks = lax.axis_size("seq")
    copies = lax.axis_size("dp")
    width = output_weight.shape[0]
    share = input_weight.shape[0]
    rank = step_weight.shape[0]
    n = decay_log.shape[0]
    tokens = chunks * rows * length
    here = lax.axis_index("seq")

    hidden_all = lax.all_gather(hidden, "seq", axis=0)
    gain_all = lax.all_gather(norm_gain, "seq", axis=0, tiled=True).astype(F32)
    blocks = input_weight.reshape(share, 2, chunks, width)
    blocks = lax.all_to_all(blocks, "seq", split_axis=2, concat_axis=0, tiled=False)
    w_conv = blocks[:, :, 0].reshape(model, width)
    w_gate = blocks[:, :, 1].reshape(model, width)
    slots = here * length + lax.broadcasted_iota(jnp.int32, (rows, length), 1)
    valid = (slots < lengths[:, None]).astype(F32)[..., None]
    cotangent = grad_out.astype(F32) * valid
    gm = lax.all_gather(cotangent.astype(BF16), "seq", axis=0).reshape(tokens, model)

    source_all = hidden_all.reshape(tokens, model).astype(F32)
    inverse_all = lax.rsqrt(jnp.mean(source_all * source_all, axis=-1, keepdims=True) + EPSILON)
    normed = (source_all * inverse_all * gain_all).astype(BF16)
    shaped = lambda a: a.reshape(chunks, rows, length, a.shape[-1])
    ci = shaped(jnp.dot(normed, w_conv, preferred_element_type=F32).astype(BF16))
    gate = shaped(jnp.dot(normed, w_gate, preferred_element_type=F32))
    bias_row = conv_bias.reshape(1, width)
    x, partial = conv_forward(ci, conv_weight, bias_row, select_weight)
    sel = lax.psum(partial, "seq")
    step_row = step_bias.reshape(1, width)
    skip_row = skip_weight.reshape(1, width)
    gated, ssm, starts = scan_forward(sel, x, gate, step_weight, step_row, decay_log, skip_row, n)
    gated2 = gated.reshape(tokens, width)
    mixed = jnp.dot(gated2, output_weight, preferred_element_type=F32).astype(BF16)
    mixed = lax.psum_scatter(shaped(mixed), "seq", scatter_dimension=0, tiled=False)
    source = hidden.astype(F32)
    output = ((source + mixed.astype(F32)) * valid).astype(BF16)

    gg = shaped(lax.dot_general(gm, output_weight, (((1,), (1,)), ((), ())), preferred_element_type=F32))
    ggate, gvals, gpre, gpart, gstepw, gstepb, gdecay, gskip = scan_backward(
        sel, x, gate, gg, ssm, starts, step_weight, step_row, decay_log, skip_row, n)
    gsel = lax.psum(gpart, "seq")
    tn = lambda a, b: lax.dot_general(a, b, (((0,), (0,)), ((), ())), preferred_element_type=F32)
    gout = tn(gated2, gm)
    gci, gtaps, gconvb, gselw = conv_backward(ci, gvals, gsel, conv_weight, bias_row, select_weight)
    gci2 = gci.reshape(tokens, width)
    ggate2 = ggate.reshape(tokens, width)
    gin = jnp.stack([tn(normed, gci2).astype(BF16), tn(normed, ggate2).astype(BF16)], axis=1)
    gin = gin.reshape(chunks, copies, share // copies, 2, width)
    gin = lax.psum_scatter(gin, "dp", scatter_dimension=1, tiled=False)
    gin = lax.all_to_all(gin, "seq", split_axis=0, concat_axis=2, tiled=False)
    gin = lax.all_gather(gin.reshape(share // copies, 2 * chunks * width), "dp", axis=0, tiled=True).astype(F32)
    both = lambda g, w: lax.dot_general(g, w, (((1,), (1,)), ((), ())), preferred_element_type=F32)
    gnormed = (both(gci2, w_conv) + both(ggate2, w_gate)).astype(BF16)
    gnormed = lax.psum_scatter(shaped(gnormed), "seq", scatter_dimension=0, tiled=False).astype(F32)
    inverse = lax.rsqrt(jnp.mean(source * source, axis=-1, keepdims=True) + EPSILON)
    scaled = gnormed * gain_all
    ghidden = inverse * scaled - source * inverse ** 3 * jnp.mean(scaled * source, axis=-1, keepdims=True) + cotangent
    ggain = jnp.sum(gnormed * source * inverse, axis=(0, 1))
    ggain = lax.psum(ggain, ("dp", "seq"))
    ggain = lax.dynamic_slice(ggain, (here * share,), (share,))
    gtaps, gconvb, gselw, gstepw, gstepb, gdecay, gskip, gout = lax.psum(
        (gtaps, gconvb, gselw, gstepw, gstepb, gdecay, gskip, gout), "dp")
    return (output, ghidden, ggain, gin, gtaps, gconvb.reshape(width), gselw, gstepw, gstepb.reshape(width),
            gdecay, gskip.reshape(width), gout)


def solution(mesh):
    tok, vec, col, row = P("dp", "seq", None), P("seq"), P(None, "seq"), P("seq", None)
    return jax.shard_map(
        local,
        mesh=mesh,
        in_specs=(tok, tok, P("dp"), vec, row, col, vec, col, col, vec, col, vec, row),
        out_specs=(tok, tok, vec, row, col, vec, col, col, vec, col, vec, row),
        check_vma=False,
    )
```

```python
import functools
import jax
import jax.numpy as jnp
from jax import lax
from jax.experimental import pallas as pl
from jax.experimental.pallas import tpu as pltpu

BLOCK = 16
EPSILON = 1e-05
LOG2E = 1.4426950408889634
F32 = jnp.float32
BF16 = jnp.bfloat16


def softplus(v):
    return jnp.maximum(v, 0.0) + jnp.log(1.0 + jnp.exp(-jnp.abs(v)))


def sigmoid(v):
    return 1.0 / (1.0 + jnp.exp(-v))


def nt_dot(a, b):
    return lax.dot_general(a, b, (((1,), (1,)), ((), ())), preferred_element_type=F32)


def tile_matrix(n, wide):
    col = lax.broadcasted_iota(jnp.int32, (n, wide), 1)
    row = lax.broadcasted_iota(jnp.int32, (n, wide), 0)
    return (col % n == row).astype(F32)


def diagonal_mask(rows, n, wide):
    col = lax.broadcasted_iota(jnp.int32, (rows, wide), 1)
    row = lax.broadcasted_iota(jnp.int32, (rows, wide), 0)
    return col // n == row % BLOCK


def scan_forward_kernel(sel_ref, x_ref, gate_ref, stepw_ref, bias_ref, decay_ref, skip_ref,
                        gated_ref, ssm_ref, start_ref,
                        dt_s, u_s, y_s, coef_s, bt_s, hist_s, state_s, *, rank, n):
    chunk = pl.program_id(1)
    length = x_ref.shape[-2]
    wide = BLOCK * n

    @pl.when(chunk == 0)
    def _():
        state_s[...] = jnp.zeros_like(state_s)

    start_ref[...] = state_s[...].reshape(start_ref.shape)
    selected = sel_ref[...].reshape(sel_ref.shape[-2:]).astype(F32)
    x = x_ref[...].reshape(x_ref.shape[-2:]).astype(F32)
    low = selected[:rank].T.astype(BF16)
    pre = jnp.dot(low, stepw_ref[...], preferred_element_type=F32) + bias_ref[...]
    dt = softplus(pre)
    dt_s[...] = dt
    u_s[...] = dt * x
    bt_s[...] = selected[rank:]
    spread = jnp.dot(selected[rank:].T[:, n:], tile_matrix(n, wide), preferred_element_type=F32)
    coef_s[...] = jnp.where(diagonal_mask(length, n, wide), spread, 0.0).astype(BF16)
    rate = -jnp.exp(decay_ref[...].astype(F32)) * LOG2E

    def block(k, state):
        at = pl.multiple_of(k * BLOCK, BLOCK)
        dts = dt_s[pl.ds(at, BLOCK), :]
        us = u_s[pl.ds(at, BLOCK), :]
        bs = pltpu.roll(bt_s[0:n, :], length - at, 1)
        for i in range(BLOCK):
            factor = jnp.exp2(dts[i:i + 1, :] * rate)
            state = factor * state + us[i:i + 1, :] * bs[:, i:i + 1]
            hist_s[i * n:(i + 1) * n, :] = state.astype(BF16)
        y_s[pl.ds(at, BLOCK), :] = jnp.dot(coef_s[pl.ds(at, BLOCK), :], hist_s[...], preferred_element_type=F32)
        return state

    state_s[...] = lax.fori_loop(0, length // BLOCK, block, state_s[...])
    gate = gate_ref[...].reshape(x.shape)
    ssm = y_s[...] + skip_ref[...] * x
    ssm_ref[...] = ssm.astype(ssm_ref.dtype).reshape(ssm_ref.shape)
    gated_ref[...] = (ssm * gate * sigmoid(gate)).astype(BF16).reshape(gated_ref.shape)


def scan_forward(sel, x, gate, stepw, bias, decay, skip, n):
    chunks, rows, length, width = x.shape
    rank = stepw.shape[0]
    wide = BLOCK * n
    tok = lambda feat: pl.BlockSpec((1, 1, length, feat), lambda r, c: (c, r, 0, 0))
    whole = lambda a: pl.BlockSpec(a.shape, lambda r, c: (0,) * a.ndim)
    return pl.pallas_call(
        functools.partial(scan_forward_kernel, rank=rank, n=n),
        grid=(rows, chunks),
        in_specs=[pl.BlockSpec((1, 1) + sel.shape[2:], lambda r, c: (c, r, 0, 0)), tok(width), tok(width), whole(stepw), whole(bias), whole(decay), whole(skip)],
        out_specs=[tok(width), tok(width), pl.BlockSpec((1, 1, n, width), lambda r, c: (c, r, 0, 0))],
        out_shape=[
            jax.ShapeDtypeStruct((chunks, rows, length, width), BF16),
            jax.ShapeDtypeStruct((chunks, rows, length, width), BF16),
            jax.ShapeDtypeStruct((chunks, rows, n, width), F32),
        ],
        scratch_shapes=[
            pltpu.VMEM((length, width), F32), pltpu.VMEM((length, width), F32), pltpu.VMEM((length, width), F32),
            pltpu.VMEM((length, wide), BF16), pltpu.VMEM((2 * n, length), F32),
            pltpu.VMEM((wide, width), BF16), pltpu.VMEM((n, width), F32),
        ],
        name="scan_forward",
    )(sel, x, gate, stepw, bias, decay, skip)


def scan_backward_kernel(sel_ref, x_ref, gate_ref, gg_ref, ssm_ref, start_ref, stepw_ref, bias_ref, decay_ref, skip_ref,
                         ggate_ref, gvals_ref, gpre_ref, gsel_ref, gstepw_ref, gbias_ref, gdecay_ref, gskip_ref,
                         dt_s, u_s, gy_s, gu_s, ah_s, bcoef_s, bt_s, hist_s, adj_s, harm_s, db_s, dc_s, carry_s, gd_s, *, rank, n):
    row, step = pl.program_id(0), pl.program_id(1)
    length = x_ref.shape[-2]
    wide = BLOCK * n
    blocks = length // BLOCK
    flat = lambda ref: ref[...].reshape(ref.shape[-2:])

    @pl.when(step == 0)
    def _():
        carry_s[...] = jnp.zeros_like(carry_s)

    @pl.when((step == 0) & (row == 0))
    def _():
        gstepw_ref[...] = jnp.zeros_like(gstepw_ref)
        gbias_ref[...] = jnp.zeros_like(gbias_ref)
        gskip_ref[...] = jnp.zeros_like(gskip_ref)
        gd_s[...] = jnp.zeros_like(gd_s)

    selected = flat(sel_ref).astype(F32)
    x = flat(x_ref).astype(F32)
    gate = flat(gate_ref)
    gg = flat(gg_ref)
    ssm = flat(ssm_ref).astype(F32)
    sg = sigmoid(gate)
    gy = gg * gate * sg
    ggate_ref[...] = (gg * ssm * sg * (1.0 + gate * (1.0 - sg))).astype(BF16).reshape(ggate_ref.shape)
    gskip_ref[...] += jnp.sum(gy * x, axis=0, keepdims=True)
    gy_s[...] = gy
    low = selected[:rank].T.astype(BF16)
    pre = jnp.dot(low, stepw_ref[...], preferred_element_type=F32) + bias_ref[...]
    dt = softplus(pre)
    dt_s[...] = dt
    u_s[...] = dt * x
    bt_s[...] = selected[rank:]
    tiles = tile_matrix(n, wide)
    spread = jnp.dot(selected[rank:].T[:, :n], tiles, preferred_element_type=F32)
    bcoef_s[...] = jnp.where(diagonal_mask(length, n, wide), spread, 0.0).astype(BF16)
    decay = -jnp.exp(decay_ref[...].astype(F32))
    rate = decay * LOG2E
    keep = diagonal_mask(BLOCK, n, wide)
    ones = keep.astype(BF16)
    start = start_ref[...].reshape(carry_s.shape)

    def again(k, state):
        at = pl.multiple_of(k * BLOCK, BLOCK)
        dts = dt_s[pl.ds(at, BLOCK), :]
        us = u_s[pl.ds(at, BLOCK), :]
        bs = pltpu.roll(bt_s[0:n, :], length - at, 1)
        for i in range(BLOCK):
            hist_s[pl.ds(pl.multiple_of((at + i) * n, n), n), :] = state.astype(BF16)
            factor = jnp.exp2(dts[i:i + 1, :] * rate)
            state = factor * state + us[i:i + 1, :] * bs[:, i:i + 1]
        return state

    last = lax.fori_loop(0, blocks, again, start)
    hist_s[pl.ds(length * n, n), :] = last.astype(BF16)

    def back(j, carried):
        carry, gd = carried
        k = blocks - 1 - j
        at = pl.multiple_of(k * BLOCK, BLOCK)
        dts = dt_s[pl.ds(at, BLOCK), :]
        gys = gy_s[pl.ds(at, BLOCK), :]
        cs = pltpu.roll(bt_s[n:2 * n, :], length - at, 1)
        for i in range(BLOCK - 1, -1, -1):
            dt_i = dts[i:i + 1, :]
            g = cs[:, i:i + 1] * gys[i:i + 1, :] + carry
            adj_s[i * n:(i + 1) * n, :] = g.astype(BF16)
            carry = jnp.exp2(dt_i * rate) * g
            h = carry * hist_s[pl.ds(pl.multiple_of((at + i) * n, n), n), :].astype(F32)
            harm_s[i * n:(i + 1) * n, :] = (h * decay).astype(BF16)
            gd = gd + dt_i * h
        adj = adj_s[...]
        rows = pl.ds(at, BLOCK)
        gu_s[rows, :] = jnp.dot(bcoef_s[rows, :], adj, preferred_element_type=F32)
        ah_s[rows, :] = jnp.dot(ones, harm_s[...], preferred_element_type=F32)
        db_s[rows, :] = jnp.where(keep, nt_dot(u_s[rows, :].astype(BF16), adj), 0.0)
        states = hist_s[pl.ds(pl.multiple_of((at + 1) * n, n), wide), :]
        dc_s[rows, :] = jnp.where(keep, nt_dot(gys.astype(BF16), states), 0.0)
        return carry, gd

    carry, gd = lax.fori_loop(0, blocks, back, (carry_s[...], gd_s[...]))
    carry_s[...] = carry
    gd_s[...] = gd
    gu = gu_s[...]
    gpre = ((x * gu + ah_s[...]) * sigmoid(pre)).astype(BF16)
    gpre_ref[...] = gpre.reshape(gpre_ref.shape)
    gvals_ref[...] = (gy * skip_ref[...] + dt * gu).astype(gvals_ref.dtype).reshape(gvals_ref.shape)
    gbias_ref[...] += jnp.sum(gpre.astype(F32), axis=0, keepdims=True)
    gstepw_ref[...] += jnp.dot(selected[:rank].astype(BF16), gpre, preferred_element_type=F32)
    fold = lambda ref: lax.dot_general(tiles, ref[...], (((1,), (1,)), ((), ())), preferred_element_type=F32, precision=lax.Precision.HIGHEST)
    gsel_ref[0, 0, 0:rank, :] = nt_dot(stepw_ref[...], gpre).astype(BF16)
    gsel_ref[0, 0, rank:rank + n, :] = fold(db_s).astype(BF16)
    gsel_ref[0, 0, rank + n:rank + 2 * n, :] = fold(dc_s).astype(BF16)

    @pl.when((row == pl.num_programs(0) - 1) & (step == pl.num_programs(1) - 1))
    def _():
        gdecay_ref[...] = gd * decay


def scan_backward(sel, x, gate, gg, ssm, starts, stepw, bias, decay, skip, n):
    chunks, rows, length, width = x.shape
    rank = stepw.shape[0]
    wide = BLOCK * n
    at = lambda r, c: (chunks - 1 - c, r, 0, 0)
    tok = lambda feat: pl.BlockSpec((1, 1, length, feat), at)
    whole = lambda shape: pl.BlockSpec(shape, lambda r, c: (0,) * len(shape))
    sds = jax.ShapeDtypeStruct
    return pl.pallas_call(
        functools.partial(scan_backward_kernel, rank=rank, n=n),
        grid=(rows, chunks),
        in_specs=[pl.BlockSpec((1, 1) + sel.shape[2:], at), tok(width), tok(width), tok(width), tok(width), pl.BlockSpec((1, 1, n, width), at),
                  whole(stepw.shape), whole(bias.shape), whole(decay.shape), whole(skip.shape)],
        out_specs=[tok(width), tok(width), tok(width), pl.BlockSpec((1, 1) + sel.shape[2:], at), whole((rank, width)), whole((1, width)), whole((n, width)), whole((1, width))],
        out_shape=[
            sds(x.shape, BF16), sds(x.shape, F32), sds(x.shape, BF16), sds(sel.shape, BF16),
            sds((rank, width), F32), sds((1, width), F32), sds((n, width), F32), sds((1, width), F32),
        ],
        scratch_shapes=[
            pltpu.VMEM((length, width), F32), pltpu.VMEM((length, width), F32), pltpu.VMEM((length, width), F32),
            pltpu.VMEM((length, width), F32), pltpu.VMEM((length, width), F32),
            pltpu.VMEM((length, wide), BF16), pltpu.VMEM((2 * n, length), F32),
            pltpu.VMEM(((length + 1) * n, width), BF16), pltpu.VMEM((wide, width), BF16), pltpu.VMEM((wide, width), BF16),
            pltpu.VMEM((length, wide), F32), pltpu.VMEM((length, wide), F32),
            pltpu.VMEM((n, width), F32), pltpu.VMEM((n, width), F32),
        ],
        name="scan_backward",
    )(sel, x, gate, gg, ssm, starts, stepw, bias, decay, skip)
def conv_forward_kernel(ci_ref, taps_ref, bias_ref, selw_ref, x_ref, sel_ref, ext_s):
    length = ci_ref.shape[-2]
    tap_count = taps_ref.shape[0]

    @pl.when(pl.program_id(1) == 0)
    def _():
        ext_s[0:8, :] = jnp.zeros((8, ext_s.shape[1]), F32)

    ext_s[8:, :] = ci_ref[...].reshape(ci_ref.shape[-2:]).astype(F32)
    total = bias_ref[...].astype(F32)
    for k in range(tap_count):
        total = total + taps_ref[k:k + 1, :].astype(F32) * ext_s[pl.ds(8 - tap_count + 1 + k, length), :]
    ext_s[0:8, :] = ext_s[length:length + 8, :]
    x = (total * sigmoid(total)).astype(BF16)
    x_ref[...] = x.reshape(x_ref.shape)
    sel_ref[...] = nt_dot(selw_ref[...], x).astype(BF16).reshape(sel_ref.shape)


def conv_forward(ci, taps, bias, selw):
    chunks, rows, length, width = ci.shape
    tok = lambda feat: pl.BlockSpec((1, 1, length, feat), lambda r, c: (c, r, 0, 0))
    whole = lambda a: pl.BlockSpec(a.shape, lambda r, c: (0,) * a.ndim)
    coef = (selw.shape[0], length)
    return pl.pallas_call(
        conv_forward_kernel,
        grid=(rows, chunks),
        in_specs=[tok(width), whole(taps), whole(bias), whole(selw)],
        out_specs=[tok(width), pl.BlockSpec((1, 1) + coef, lambda r, c: (c, r, 0, 0))],
        out_shape=[jax.ShapeDtypeStruct(ci.shape, BF16), jax.ShapeDtypeStruct((chunks, rows) + coef, BF16)],
        scratch_shapes=[pltpu.VMEM((length + 8, width), F32)],
        name="conv_forward",
    )(ci, taps, bias, selw)


def conv_backward_kernel(ci_ref, prev_ref, gvals_ref, gsel_ref, taps_ref, bias_ref, selw_ref,
                         gci_ref, gtaps_ref, gbias_ref, gselw_ref, ext_s, gext_s):
    row, step = pl.program_id(0), pl.program_id(1)
    length = ci_ref.shape[-2]
    tap_count = taps_ref.shape[0]
    flat = lambda ref: ref[...].reshape(ref.shape[-2:])

    @pl.when(step == 0)
    def _():
        gext_s[length:, :] = jnp.zeros((8, gext_s.shape[1]), F32)

    @pl.when((step == 0) & (row == 0))
    def _():
        gtaps_ref[...] = jnp.zeros_like(gtaps_ref)
        gbias_ref[...] = jnp.zeros_like(gbias_ref)
        gselw_ref[...] = jnp.zeros_like(gselw_ref)

    first = step == pl.num_programs(1) - 1
    ext_s[8:, :] = flat(ci_ref).astype(F32)
    before = flat(prev_ref)[length - 16:, :].astype(F32)[8:, :]
    ext_s[0:8, :] = jnp.where(first, 0.0, before)
    total = bias_ref[...].astype(F32)
    for k in range(tap_count):
        total = total + taps_ref[k:k + 1, :].astype(F32) * ext_s[pl.ds(8 - tap_count + 1 + k, length), :]
    sg = sigmoid(total)
    x = (total * sg).astype(BF16)
    gsel = flat(gsel_ref)
    gvals = flat(gvals_ref) + jnp.dot(gsel.astype(F32).T.astype(BF16), selw_ref[...], preferred_element_type=F32)
    gconv = gvals * sg * (1.0 + total * (1.0 - sg))
    gbias_ref[...] += jnp.sum(gconv, axis=0, keepdims=True)
    for k in range(tap_count):
        gtaps_ref[k:k + 1, :] += jnp.sum(gconv * ext_s[pl.ds(8 - tap_count + 1 + k, length), :], axis=0, keepdims=True)
    gselw_ref[...] += jnp.dot(gsel, x, preferred_element_type=F32)
    gext_s[0:length, :] = gconv
    gci = jnp.zeros_like(gconv)
    for k in range(tap_count):
        gci = gci + taps_ref[k:k + 1, :].astype(F32) * gext_s[pl.ds(tap_count - 1 - k, length), :]
    gci_ref[...] = gci.astype(BF16).reshape(gci_ref.shape)
    gext_s[length:, :] = gconv[0:8, :]


def conv_backward(ci, gvals, gsel, taps, bias, selw):
    chunks, rows, length, width = ci.shape
    at = lambda r, c: (chunks - 1 - c, r, 0, 0)
    before = lambda r, c: (jnp.maximum(chunks - 2 - c, 0), r, 0, 0)
    tok = lambda feat, where: pl.BlockSpec((1, 1, length, feat), where)
    whole = lambda shape: pl.BlockSpec(shape, lambda r, c: (0,) * len(shape))
    sds = jax.ShapeDtypeStruct
    return pl.pallas_call(
        conv_backward_kernel,
        grid=(rows, chunks),
        in_specs=[tok(width, at), tok(width, before), tok(width, at), pl.BlockSpec((1, 1) + gsel.shape[2:], at), whole(taps.shape), whole(bias.shape), whole(selw.shape)],
        out_specs=[tok(width, at), whole(taps.shape), whole(bias.shape), whole(selw.shape)],
        out_shape=[sds(ci.shape, BF16), sds(taps.shape, F32), sds(bias.shape, F32), sds(selw.shape, F32)],
        scratch_shapes=[pltpu.VMEM((length + 8, width), F32), pltpu.VMEM((length + 8, width), F32)],
        name="conv_backward",
    )(ci, ci, gvals, gsel, taps, bias, selw)
MESH = pl.DeviceIdType.MESH


def remote(src, dst, send, recv, device):
    return pltpu.make_async_remote_copy(src_ref=src, dst_ref=dst, send_sem=send, recv_sem=recv, device_id=device, device_id_type=MESH)


def grid_of(chunks, copies):
    deep = max(1, copies // 2)
    return (chunks // deep, deep) if chunks % deep == 0 else (chunks, 1)


def meet(chunks, copies):
    me, mine = lax.axis_index("seq"), lax.axis_index("dp")
    barrier = pltpu.get_barrier_semaphore()

    def greet(k, _):
        pl.semaphore_signal(barrier, inc=1, device_id={"seq": lax.rem(me + k, chunks)}, device_id_type=MESH)
        return 0

    def greet_copy(k, _):
        pl.semaphore_signal(barrier, inc=1, device_id={"dp": lax.rem(mine + k, copies)}, device_id_type=MESH)
        return 0

    lax.fori_loop(1, chunks, greet, 0)
    if copies > 1:
        lax.fori_loop(1, copies, greet_copy, 0)
    pl.semaphore_wait(barrier, chunks - 1 + max(copies - 1, 0))


def gather_project_kernel(hid_ref, wq_ref, gain_ref, n_ref, ci_ref, gate_ref, w_ref, row_ref,
                          hid_v, gain_v, w_v, n_v, ci_v, gate_v,
                          load_sem, out_sem, hrecv, hside, hup, hdown,
                          w1send, w1recv, w2recv, w2send, w3send, gsend, grecv, *, chunks, copies, share, split):
    zs, ys = grid_of(chunks, copies)
    xs = copies // 2
    me, mine = lax.axis_index("seq"), lax.axis_index("dp")
    z, y = me // ys, me % ys
    x, c = mine // 2, mine % 2
    tokens, model = hid_v.shape[1:]
    width = ci_v.shape[1]
    inner = chunks * width
    half = tokens // 2
    piece = share // (copies if split else 1)
    spot = mine if split else 0
    load = pltpu.make_async_copy(hid_ref, hid_v.at[me], load_sem)
    load.start()
    meet(chunks, copies)
    load.wait()

    def w_rows(s, d):
        return pl.ds(pl.multiple_of(s * share + d * piece, piece), piece)

    def w_first(s, part):
        src = wq_ref.at[pl.ds(pl.multiple_of(spot * piece, piece), piece), pl.ds(pl.multiple_of(part * inner + s * width, width), width)]
        return remote(src, w_v.at[w_rows(me, spot), pl.ds(part * width, width)], w1send.at[s, part], w1recv.at[me, part], {"seq": s})

    def w_landed(s, part):
        dst = w_v.at[w_rows(s, spot), pl.ds(part * width, width)]
        return remote(dst, dst, w1send.at[s, part], w1recv.at[s, part], {"seq": s})

    def w_own(part):
        src = wq_ref.at[pl.ds(pl.multiple_of(spot * piece, piece), piece), pl.ds(pl.multiple_of(part * inner + me * width, width), width)]
        return pltpu.make_async_copy(src, w_v.at[w_rows(me, spot), pl.ds(part * width, width)], out_sem.at[part])

    def every_other(fn):
        def one(k, _):
            fn(lax.rem(me + k, chunks))
            return 0
        lax.fori_loop(1, chunks, one, 0)

    def gain_to(s):
        return remote(gain_ref, gain_v.at[me], gsend.at[s], grecv.at[me], {"seq": s})

    def gain_from(s):
        return remote(gain_v.at[s], gain_v.at[s], gsend.at[s], grecv.at[s], {"seq": s})

    def send_first(s):
        gain_to(s).start()
        w_first(s, 0).start()
        w_first(s, 1).start()

    def block(o, yy, h):
        return hid_v.at[o * ys + yy, pl.ds(h * half, half)]

    def up(o, h):
        return remote(block(o, y, h), block(o, y, h), hup.at[o, h], hrecv.at[o * ys + y, h], {"seq": (z + 1) * ys + y})

    def down(o, h):
        return remote(block(o, y, h), block(o, y, h), hdown.at[o, h], hrecv.at[o * ys + y, h], {"seq": (z - 1) * ys + y})

    def side(o, j, h):
        other = lax.rem(y + j, ys)
        return remote(block(o, y, h), block(o, y, h), hside.at[o, j - 1, h], hrecv.at[o * ys + y, h], {"seq": z * ys + other})

    def landed(o, yy, h):
        return remote(block(o, yy, h), block(o, yy, h), hside.at[o, 0, h], hrecv.at[o * ys + yy, h], {"seq": lax.rem(me + 1, chunks)})

    def when(cond, fn):
        pl.when(cond)(fn)

    gain_own = pltpu.make_async_copy(gain_ref, gain_v.at[me], out_sem.at[2])
    gain_own.start()
    for part in range(2):
        w_own(part).start()
    for h in range(2):
        when(z + 1 < zs, lambda: up(z, h).start())
        when(z > 0, lambda: down(z, h).start())
        for j in range(1, ys):
            side(z, j, h).start()
    every_other(send_first)

    def relay(k):
        for h in range(2):
            @pl.when(z - k >= 0)
            def _():
                landed(z - k, y, h).wait_recv()
                when(z + 1 < zs, lambda: up(z - k, h).start())
                for j in range(1, ys):
                    side(z - k, j, h).start()

            @pl.when(z + k < zs)
            def _():
                landed(z + k, y, h).wait_recv()
                when(z > 0, lambda: down(z + k, h).start())
                for j in range(1, ys):
                    side(z + k, j, h).start()

    def shared(s, d, sems, k, device):
        return remote(w_v.at[w_rows(s, d)], w_v.at[w_rows(s, d)], sems.at[s, k], w2recv.at[s, d], device)

    def spread(s):
        for j in range(1, xs):
            shared(s, mine, w2send, j - 1, {"dp": lax.rem(x + j, xs) * 2 + c}).start()
        shared(s, mine, w3send, 0, {"dp": x * 2 + 1 - c}).start()

    gain_own.wait()
    for part in range(2):
        w_own(part).wait()
    if split:
        spread(me)

    def take_first(s):
        gain_from(s).wait_recv()
        for part in range(2):
            w_landed(s, part).wait_recv()
        if split:
            spread(s)

    every_other(take_first)
    if zs > 1:
        relay(1)

    def take_second(s, _):
        for j in range(1, xs):
            d = lax.rem(x + j, xs) * 2 + c
            shared(s, d, w2send, j - 1, {"dp": d}).wait_recv()
            shared(s, d, w3send, j, {"dp": x * 2 + 1 - c}).start()
        return 0

    def take_third(s, _):
        for j in range(xs):
            d = lax.rem(x + j, xs) * 2 + 1 - c
            shared(s, d, w2send, 0, {"dp": d}).wait_recv()
        return 0

    if split:
        lax.fori_loop(0, chunks, take_second, 0)
    if zs > 2:
        relay(2)
    if split:
        lax.fori_loop(0, chunks, take_third, 0)

    row_ref[...] = jnp.concatenate([gain_v[s] for s in range(chunks)], axis=-1)
    w_out = pltpu.make_async_copy(w_v, w_ref, load_sem)
    w_out.start()
    steps = 4 if width >= 512 else 1
    tile = 2 * width // steps

    def project(at):
        def rows(i, _):
            sl = pl.ds(pl.multiple_of(i * 32, 32), 32)
            h = hid_v[at, sl, :].astype(F32)
            inverse = lax.rsqrt(jnp.mean(h * h, axis=-1, keepdims=True) + EPSILON)
            n_v[sl, :] = (h * inverse * row_ref[...]).astype(BF16)
            return 0
        lax.fori_loop(0, tokens // 32, rows, 0)
        n_out = pltpu.make_async_copy(n_v, n_ref.at[at], out_sem.at[0])
        n_out.start()

        def columns(i, _):
            sl = pl.ds(pl.multiple_of(i * tile, tile), tile)
            got = jnp.dot(n_v[...], w_v[:, sl], preferred_element_type=F32)
            if steps == 1:
                ci_v[...] = got[:, :width].astype(BF16)
                gate_v[...] = got[:, width:]
            else:
                @pl.when(i < steps // 2)
                def _():
                    ci_v[:, sl] = got.astype(BF16)

                @pl.when(i >= steps // 2)
                def _():
                    gate_v[:, pl.ds(pl.multiple_of(i * tile - width, tile), tile)] = got
            return 0
        lax.fori_loop(0, steps, columns, 0)
        ci_out = pltpu.make_async_copy(ci_v, ci_ref.at[at], out_sem.at[1])
        gate_out = pltpu.make_async_copy(gate_v, gate_ref.at[at], out_sem.at[2])
        ci_out.start()
        gate_out.start()
        n_out.wait()
        ci_out.wait()
        gate_out.wait()

    def work(first, last):
        def one(i, _):
            k0, j = i // (2 * ys), i % (2 * ys)
            lower, yy = j // ys, j % ys
            own = yy == y
            k = k0 - jnp.where(own, 0, 1)
            o = z + k * (2 * lower - 1)
            ok = (k >= 0) & (k < zs) & (o >= 0) & (o < zs) & ((lower == 0) | (k > 0))

            @pl.when(ok & jnp.logical_not(own))
            def _():
                for h in range(2):
                    landed(o, yy, h).wait_recv()

            @pl.when(ok)
            def _():
                project(o * ys + yy)
            return 0
        lax.fori_loop(first * 2 * ys, last * 2 * ys, one, 0)

    work(0, min(3, zs))

    def later(k, _):
        relay(k)
        work(k, k + 1)
        return 0

    lax.fori_loop(3, zs, later, 0)
    work(zs, zs + 1)
    w_out.wait()

    def drain_first(s):
        gain_to(s).wait_send()
        for part in range(2):
            w_first(s, part).wait_send()

    every_other(drain_first)

    def drain_second(s, _):
        for j in range(1, xs):
            shared(s, mine, w2send, j - 1, {"dp": mine}).wait_send()
        for j in range(xs):
            shared(s, mine, w3send, j, {"dp": mine}).wait_send()
        return 0

    if split:
        lax.fori_loop(0, chunks, drain_second, 0)

    def drain(k, _):
        for h in range(2):
            @pl.when(z - k >= 0)
            def _():
                when(z + 1 < zs, lambda: up(z - k, h).wait_send())
                for j in range(1, ys):
                    side(z - k, j, h).wait_send()

            @pl.when((z + k < zs) & (k > 0))
            def _():
                when(z > 0, lambda: down(z + k, h).wait_send())
                for j in range(1, ys):
                    side(z + k, j, h).wait_send()
        return 0

    lax.fori_loop(0, zs, drain, 0)
    for h in range(2):
        when(z > 0, lambda: down(z, h).wait_send())


def gather_project(hidden, wq, gain, chunks, copies, share, split):
    tokens, model = hidden.shape
    width = wq.shape[1] // 2 // chunks
    zs, ys = grid_of(chunks, copies)
    any_spec = pl.BlockSpec(memory_space=pl.ANY)
    sds = jax.ShapeDtypeStruct
    dma = pltpu.SemaphoreType.DMA
    return pl.pallas_call(
        functools.partial(gather_project_kernel, chunks=chunks, copies=copies, share=share, split=split),
        in_specs=[any_spec] * 3,
        out_specs=[any_spec] * 4 + [pl.BlockSpec(memory_space=pltpu.VMEM)],
        out_shape=[sds((chunks, tokens, model), BF16), sds((chunks, tokens, width), BF16),
                   sds((chunks, tokens, width), F32), sds((model, 2 * width), BF16), sds((1, model), F32)],
        scratch_shapes=[
            pltpu.VMEM((chunks, tokens, model), BF16), pltpu.VMEM((chunks, 1, share), F32), pltpu.VMEM((model, 2 * width), BF16),
            pltpu.VMEM((tokens, model), BF16), pltpu.VMEM((tokens, width), BF16), pltpu.VMEM((tokens, width), F32),
            dma(()), dma((3,)), dma((chunks, 2)), dma((zs, max(1, ys - 1), 2)), dma((zs, 2)), dma((zs, 2)),
            dma((chunks, 2)), dma((chunks, 2)), dma((chunks, copies)), dma((chunks, max(1, copies // 2))), dma((chunks, max(1, copies // 2))),
            dma((chunks,)), dma((chunks,)),
        ],
        compiler_params=pltpu.CompilerParams(collective_id=0, has_side_effects=True, vmem_limit_bytes=60 * 1024 * 1024),
        name="gather_project",
    )(hidden, wq, gain)


def total_kernel(part_ref, out_ref, recv_v, send1, recv1, send2, recv2, own_sem, *, chunks):
    me = lax.axis_index("seq")
    meet(chunks, 1)

    def first(s):
        return remote(part_ref.at[s], recv_v.at[me], send1.at[s], recv1.at[me], {"seq": s})

    def landed_first(s):
        return remote(part_ref.at[s], recv_v.at[s], send1.at[s], recv1.at[s], {"seq": s})

    def second(s):
        return remote(out_ref.at[me], out_ref.at[me], send2.at[s], recv2.at[me], {"seq": s})

    def landed_second(s):
        return remote(out_ref.at[s], out_ref.at[s], send2.at[s], recv2.at[s], {"seq": s})

    def every_other(fn):
        def one(k, _):
            fn(lax.rem(me + k, chunks))
            return 0
        lax.fori_loop(1, chunks, one, 0)

    every_other(lambda s: first(s).start())
    recv_v[me] = part_ref[me]
    every_other(lambda s: landed_first(s).wait_recv())
    total = recv_v[0].astype(F32)
    for s in range(1, chunks):
        total = total + recv_v[s].astype(F32)
    out_ref[me] = total.astype(BF16)
    every_other(lambda s: second(s).start())
    every_other(lambda s: landed_second(s).wait_recv())
    every_other(lambda s: first(s).wait_send())
    every_other(lambda s: second(s).wait_send())


def total_over_seq(part, chunks, key):
    vmem = pl.BlockSpec(memory_space=pltpu.VMEM)
    dma = pltpu.SemaphoreType.DMA
    return pl.pallas_call(
        functools.partial(total_kernel, chunks=chunks),
        in_specs=[vmem],
        out_specs=vmem,
        out_shape=jax.ShapeDtypeStruct(part.shape, BF16),
        scratch_shapes=[pltpu.VMEM(part.shape, BF16),
                        dma((chunks,)), dma((chunks,)), dma((chunks,)), dma((chunks,)), dma(())],
        compiler_params=pltpu.CompilerParams(collective_id=key, has_side_effects=True, vmem_limit_bytes=60 * 1024 * 1024),
        name=f"total_over_seq_{key}",
    )(part)
def order_of(zs):
    return [sorted(range(zs), key=lambda t: (-abs(t - z), t)) for z in range(zs)]


def scatter_kernel(*refs, chunks, copies, split):
    if split:
        (gc_ref, gg_ref, w_ref, late_ref, gin_ref, red_ref, sum_ref, all_ref,
         ysend_v, yrecv_v, own_v, zrecv_v, late_v, w_v, g1_v, mine_v, g2_v, t_v, fin_v, load_sem,
         ysend, yrecv, zup, zdown, zrecv, lsend, lrecv,
         g1send, g1recv, g2send, g2recv, g3send, g3recv, g4send, g4recv) = refs
    else:
        (gc_ref, gg_ref, w_ref, late_ref, red_ref, sum_ref,
         ysend_v, yrecv_v, own_v, zrecv_v, late_v, w_v, load_sem,
         ysend, yrecv, zup, zdown, zrecv, lsend, lrecv) = refs
    zs, ys = grid_of(chunks, copies)
    xs = copies // 2
    me, mine = lax.axis_index("seq"), lax.axis_index("dp")
    z, y = me // ys, me % ys
    x, c = mine // 2, mine % 2
    tokens, width = gc_ref.shape[1:]
    model = w_ref.shape[0]
    half = tokens // 2
    tile = min(256, model)
    tables = order_of(zs)

    def dest(i):
        got = 0
        for k in range(zs):
            got = got + jnp.where(z == k, tables[k][i], 0)
        return got

    w_in = pltpu.make_async_copy(w_ref, w_v, load_sem.at[0])
    w_in.start()
    if split:
        piece, inner2 = fin_v.shape
        inner = inner2 // 2
        loads = [pltpu.make_async_copy(gin_ref.at[:, q * 2 + c], mine_v.at[q], load_sem.at[1 + q]) for q in range(xs)]
        for one in loads:
            one.start()
    meet(chunks, copies)

    def late_to(d):
        return remote(late_ref, late_v.at[mine], lsend.at[d], lrecv.at[mine], {"dp": d})

    def late_from(d):
        return remote(late_v.at[d], late_v.at[d], lsend.at[d], lrecv.at[d], {"dp": d})

    def every_copy(fn):
        def one(k, _):
            fn(lax.rem(mine + k, copies))
            return 0
        lax.fori_loop(1, copies, one, 0)

    if split:
        def g1(q):
            return remote(gin_ref.at[:, q * 2 + 1 - c], g1_v.at[q], g1send.at[q], g1recv.at[q], {"dp": x * 2 + 1 - c})

        for q in range(xs):
            g1(q).start()
    every_copy(lambda d: late_to(d).start())
    w_in.wait()

    def partial(s, out, at):
        def one(i, _):
            sl = pl.ds(pl.multiple_of(i * tile, tile), tile)
            got = nt_dot(gc_ref[s], w_v[sl, :width]) + nt_dot(gg_ref[s], w_v[sl, width:])
            out[at, :, sl] = got.astype(BF16)
            return 0
        lax.fori_loop(0, model // tile, one, 0)

    def to_side(i, j, h):
        rows = pl.ds(h * half, half)
        k = i * (ys - 1) + j - 1
        return remote(ysend_v.at[k % ysend_v.shape[0], rows], yrecv_v.at[k, rows], ysend.at[k, h], yrecv.at[k, h], {"seq": z * ys + lax.rem(y + j, ys)})

    slots = ysend_v.shape[0]
    for i in range(zs):
        for j in range(1, ys):
            k = i * (ys - 1) + j - 1
            if k >= slots:
                for h in range(2):
                    to_side((k - slots) // (ys - 1), (k - slots) % (ys - 1) + 1, h).wait_send()
            partial(dest(i) * ys + lax.rem(y + j, ys), ysend_v, k % slots)
            for h in range(2):
                to_side(i, j, h).start()

    def add_into(total, terms):
        def one(r, _):
            sl = pl.ds(pl.multiple_of(r * 32, 32), 32)
            total(sl, terms)
            return 0
        return one

    if split:
        def g2(q):
            return remote(mine_v.at[q], g2_v.at[x], g2send.at[q], g2recv.at[x], {"dp": q * 2 + c})

        def g2_from(q):
            return remote(g2_v.at[q], g2_v.at[q], g2send.at[q], g2recv.at[q], {"dp": q * 2 + c})

        for q in range(xs):
            loads[q].wait()
            g1(q).wait_recv()

            def fold(s, _):
                mine_v[q, s] = (mine_v[q, s].astype(F32) + g1_v[q, s].astype(F32)).astype(BF16)
                return 0
            lax.fori_loop(0, chunks, fold, 0)

            @pl.when(q != x)
            def _():
                g2(q).start()

        def columns(part, s):
            return pl.ds(pl.multiple_of(part * inner + s * width, width), width)

        def g3(s, part):
            return remote(t_v.at[s, :, pl.ds(part * width, width)], fin_v.at[:, columns(part, me)], g3send.at[s, part], g3recv.at[me, part], {"seq": s})

        def g3_from(s, part):
            return remote(fin_v.at[:, columns(part, s)], fin_v.at[:, columns(part, s)], g3send.at[s, part], g3recv.at[s, part], {"seq": s})

        def every_other(fn):
            def one(k, _):
                fn(lax.rem(me + k, chunks))
                return 0
            lax.fori_loop(1, chunks, one, 0)

        def third():
            for q in range(xs):
                @pl.when(q != x)
                def _():
                    g2_from(q).wait_recv()

            def fold(s, _):
                total = mine_v[x, s].astype(F32)
                for q in range(1, xs):
                    total = total + g2_v[lax.rem(x + q, xs), s].astype(F32)
                t_v[s] = total.astype(BF16)
                return 0
            lax.fori_loop(0, chunks, fold, 0)
            for part in range(2):
                every_other(lambda s: g3(s, part).start())
                fin_v[:, columns(part, me)] = t_v[me, :, part * width:(part + 1) * width]

        def rows_of(d):
            return pl.ds(pl.multiple_of(d * piece, piece), piece)

        def g4(d_src, k, d):
            src = fin_v if d_src is None else all_ref.at[rows_of(d_src)]
            row = mine if d_src is None else d_src
            return remote(src, all_ref.at[rows_of(row)], g4send.at[k], g4recv.at[row], {"dp": d})

        def g4_from(d):
            return remote(all_ref.at[rows_of(d)], all_ref.at[rows_of(d)], g4send.at[0], g4recv.at[d], {"dp": d})

        keep = pltpu.make_async_copy(fin_v, all_ref.at[rows_of(mine)], load_sem.at[0])

        def fourth():
            for part in range(2):
                every_other(lambda s: g3_from(s, part).wait_recv())
            for j in range(1, xs):
                g4(None, j, lax.rem(x + j, xs) * 2 + c).start()
            g4(None, 0, x * 2 + 1 - c).start()
            keep.start()

    def arrived(i, j, h):
        rows = pl.ds(h * half, half)
        k = i * (ys - 1) + j - 1
        return remote(yrecv_v.at[k, rows], yrecv_v.at[k, rows], ysend.at[k, h], yrecv.at[k, h], {"seq": z * ys + lax.rem(y + j, ys)})

    def climb(t, h):
        rows = pl.ds(h * half, half)
        return remote(own_v.at[t, rows], zrecv_v.at[t, rows], zup.at[t, h], zrecv.at[t, h], {"seq": (z + 1) * ys + y})

    def sink(t, h):
        rows = pl.ds(h * half, half)
        slot = jnp.where(t == z - 1, zs, t)
        return remote(own_v.at[t, rows], zrecv_v.at[slot, rows], zdown.at[t, h], zrecv.at[slot, h], {"seq": (z - 1) * ys + y})

    def from_z(slot, h):
        rows = pl.ds(h * half, half)
        return remote(zrecv_v.at[slot, rows], zrecv_v.at[slot, rows], zup.at[0, h], zrecv.at[slot, h], {"seq": lax.rem(me + 1, chunks)})

    def accumulate(t, h, read):
        def one(r, _):
            sl = pl.ds(pl.multiple_of(h * half + r * 32, 32), 32)
            own_v[t, sl, :] = (own_v[t, sl, :].astype(F32) + read(sl)).astype(BF16)
            return 0
        lax.fori_loop(0, half // 32, one, 0)

    for i in range(zs):
        t = dest(i)
        partial(t * ys + y, own_v, t)
        for h in range(2):
            for j in range(1, ys):
                arrived(i, ys - j, h).wait_recv()

            def side_sum(sl):
                total = yrecv_v[i * (ys - 1), sl, :].astype(F32)
                for j in range(2, ys):
                    total = total + yrecv_v[i * (ys - 1) + j - 1, sl, :].astype(F32)
                return total

            if ys > 1:
                accumulate(t, h, side_sum)

            @pl.when(((t > z) & (z > 0)) | ((t == z) & (z > 0)))
            def _():
                from_z(t, h).wait_recv()
                accumulate(t, h, lambda sl: zrecv_v[t, sl, :].astype(F32))

            @pl.when((t < z) & (z + 1 < zs))
            def _():
                from_z(t, h).wait_recv()
                accumulate(t, h, lambda sl: zrecv_v[t, sl, :].astype(F32))

            @pl.when((t == z) & (z + 1 < zs))
            def _():
                from_z(zs, h).wait_recv()
                accumulate(t, h, lambda sl: zrecv_v[zs, sl, :].astype(F32))

            @pl.when(t > z)
            def _():
                climb(t, h).start()

            @pl.when(t < z)
            def _():
                sink(t, h).start()
        if split and i == 0:
            third()
        if split and i == max(0, zs - 2):
            fourth()

    red_ref[...] = own_v[z]
    every_copy(lambda d: late_from(d).wait_recv())
    total = late_ref[...]
    for k in range(1, copies):
        total = total + late_v[lax.rem(mine + k, copies)]
    sum_ref[...] = total
    if split:
        for j in range(1, xs):
            d = lax.rem(x + j, xs) * 2 + c
            g4_from(d).wait_recv()
            g4(d, xs - 1 + j, x * 2 + 1 - c).start()
        keep.wait()
        for j in range(xs):
            g4_from(lax.rem(x + j, xs) * 2 + 1 - c).wait_recv()

    every_copy(lambda d: late_to(d).wait_send())
    count = zs * (ys - 1)
    for k in range(max(0, count - slots), count):
        for h in range(2):
            to_side(k // (ys - 1), k % (ys - 1) + 1, h).wait_send()
    for i in range(zs):
        t = dest(i)
        for h in range(2):
            @pl.when(t > z)
            def _():
                climb(t, h).wait_send()

            @pl.when(t < z)
            def _():
                sink(t, h).wait_send()
    if split:
        for q in range(xs):
            g1(q).wait_send()

            @pl.when(q != x)
            def _():
                g2(q).wait_send()
        for part in range(2):
            every_other(lambda s: g3(s, part).wait_send())
        for j in range(xs):
            g4(None, j, mine).wait_send()
        for j in range(1, xs):
            g4(lax.rem(x + j, xs) * 2 + c, xs - 1 + j, mine).wait_send()


def scatter_sums(gc, gg, w_all, late, gin, chunks, copies, split):
    tokens, width = gc.shape[1:]
    model = w_all.shape[0]
    zs, ys = grid_of(chunks, copies)
    xs = max(1, copies // 2)
    others = max(1, zs * (ys - 1))
    slots = min(others, 4)
    any_spec = pl.BlockSpec(memory_space=pl.ANY)
    vmem = pl.BlockSpec(memory_space=pltpu.VMEM)
    sds = jax.ShapeDtypeStruct
    dma = pltpu.SemaphoreType.DMA
    args = [gc, gg, w_all, late]
    in_specs = [vmem, vmem, any_spec, vmem]
    out_specs = [vmem, vmem]
    out_shape = [sds((tokens, model), BF16), sds(late.shape, F32)]
    scratch = [pltpu.VMEM((slots, tokens, model), BF16), pltpu.VMEM((others, tokens, model), BF16),
               pltpu.VMEM((zs, tokens, model), BF16), pltpu.VMEM((zs + 1, tokens, model), BF16),
               pltpu.VMEM((copies,) + late.shape, F32), pltpu.VMEM(w_all.shape, BF16)]
    sems = [dma((1 + xs,)), dma((others, 2)), dma((others, 2)), dma((zs, 2)), dma((zs, 2)), dma((zs + 1, 2)), dma((copies,)), dma((copies,))]
    if split:
        piece = gin.shape[2]
        slab = (xs, chunks, piece, 2 * width)
        args.append(gin)
        in_specs.append(any_spec)
        out_specs.append(any_spec)
        out_shape.append(sds((copies * piece, 2 * chunks * width), BF16))
        scratch += [pltpu.VMEM(slab, BF16), pltpu.VMEM(slab, BF16), pltpu.VMEM(slab, BF16), pltpu.VMEM(slab[1:], BF16),
                    pltpu.VMEM((piece, 2 * chunks * width), BF16)]
        sems += [dma((xs,)), dma((xs,)), dma((xs,)), dma((xs,)), dma((chunks, 2)), dma((chunks, 2)), dma((2 * xs,)), dma((copies,))]
    return pl.pallas_call(
        functools.partial(scatter_kernel, chunks=chunks, copies=copies, split=split),
        in_specs=in_specs,
        out_specs=out_specs,
        out_shape=out_shape,
        scratch_shapes=scratch + sems,
        compiler_params=pltpu.CompilerParams(collective_id=3, has_side_effects=True, vmem_limit_bytes=62 * 1024 * 1024),
        name="scatter_sums",
    )(*args)
from jax.sharding import PartitionSpec as P


def local(hidden, grad_out, lengths, norm_gain, input_weight, conv_weight, conv_bias, select_weight,
          step_weight, step_bias, decay_log, skip_weight, output_weight):
    rows, length, model = hidden.shape
    chunks = lax.axis_size("seq")
    copies = lax.axis_size("dp")
    width = output_weight.shape[0]
    share = input_weight.shape[0]
    rank = step_weight.shape[0]
    n = decay_log.shape[0]
    tokens = chunks * rows * length
    here = lax.axis_index("seq")

    split = (share // copies) % 16 == 0 and copies % 2 == 0
    normed, ci, gate, w_all, gain_row = gather_project(
        hidden.reshape(rows * length, model), input_weight, norm_gain.astype(F32).reshape(1, share), chunks, copies, share, split)
    normed = normed.reshape(tokens, model)
    slots = here * length + lax.broadcasted_iota(jnp.int32, (rows, length), 1)
    valid = (slots < lengths[:, None]).astype(F32)[..., None]
    cotangent = grad_out.astype(F32) * valid
    behind, gain_row = lax.optimization_barrier((cotangent.astype(BF16), gain_row))
    gm = lax.all_gather(behind, "seq", axis=0).reshape(tokens, model)

    shaped = lambda a: a.reshape(chunks, rows, length, a.shape[-1])
    ci, gate = shaped(ci), shaped(gate)
    bias_row = conv_bias.reshape(1, width)
    x, partial = conv_forward(ci, conv_weight, bias_row, select_weight)
    sel = total_over_seq(partial, chunks, 1)
    step_row = step_bias.reshape(1, width)
    skip_row = skip_weight.reshape(1, width)
    gated, ssm, starts = scan_forward(sel, x, gate, step_weight, step_row, decay_log, skip_row, n)
    gated2 = gated.reshape(tokens, width)
    mixed = jnp.dot(gated2, output_weight, preferred_element_type=F32).astype(BF16)
    mixed = lax.psum_scatter(shaped(mixed), "seq", scatter_dimension=0, tiled=False)
    source = hidden.astype(F32)
    output = ((source + mixed.astype(F32)) * valid).astype(BF16)

    gg = shaped(lax.dot_general(gm, output_weight, (((1,), (1,)), ((), ())), preferred_element_type=F32))
    ggate, gvals, gpre, gpart, gstepw, gstepb, gdecay, gskip = scan_backward(
        sel, x, gate, gg, ssm, starts, step_weight, step_row, decay_log, skip_row, n)
    gsel = total_over_seq(gpart, chunks, 2)
    tn = lambda a, b: lax.dot_general(a, b, (((0,), (0,)), ((), ())), preferred_element_type=F32)
    gout = tn(gated2, gm)
    gstepw, gstepb, gdecay, gskip, gout = lax.psum((gstepw, gstepb, gdecay, gskip, gout), "dp")
    gci, gtaps, gconvb, gselw = conv_backward(ci, gvals, gsel, conv_weight, bias_row, select_weight)
    tap_count = gtaps.shape[0]
    gci2 = gci.reshape(tokens, width)
    ggate2 = ggate.reshape(tokens, width)
    gin = jnp.concatenate([tn(normed, gci2).astype(BF16), tn(normed, ggate2).astype(BF16)], axis=1)
    gin = gin.reshape(chunks, copies, share // copies, 2 * width)
    late = jnp.concatenate([gselw, gtaps, gconvb], axis=0)
    late = jnp.pad(late, ((0, -late.shape[0] % 8), (0, 0)))
    flat = lambda a: a.reshape(chunks, rows * length, width)
    got = scatter_sums(flat(gci), flat(ggate), w_all, late, gin, chunks, copies, split)
    scaled, late = got[:2]
    if split:
        gin = got[2].astype(F32)
    else:
        gin = gin.reshape(chunks, copies, share // copies, 2, width)
        gin = lax.psum_scatter(gin, "dp", scatter_dimension=1, tiled=False)
        gin = lax.all_to_all(gin, "seq", split_axis=0, concat_axis=2, tiled=False)
        gin = lax.all_gather(gin.reshape(share // copies, 2 * chunks * width), "dp", axis=0, tiled=True).astype(F32)
    ggain = jnp.sum(gin * input_weight.astype(F32), axis=1) / norm_gain.astype(F32)
    scaled = scaled.reshape(rows, length, model).astype(F32) * gain_row
    inverse = lax.rsqrt(jnp.mean(source * source, axis=-1, keepdims=True) + EPSILON)
    ghidden = inverse * scaled - source * inverse ** 3 * jnp.mean(scaled * source, axis=-1, keepdims=True) + cotangent
    picked = gselw.shape[0]
    gselw, gtaps, gconvb = late[:picked], late[picked:picked + tap_count], late[picked + tap_count]
    return (output, ghidden, ggain, gin, gtaps, gconvb, gselw, gstepw, gstepb.reshape(width),
            gdecay, gskip.reshape(width), gout)


def solution(mesh):
    tok, vec, col, row = P("dp", "seq", None), P("seq"), P(None, "seq"), P("seq", None)
    return jax.shard_map(
        local,
        mesh=mesh,
        in_specs=(tok, tok, P("dp"), vec, row, col, vec, col, col, vec, col, vec, row),
        out_specs=(tok, tok, vec, row, col, vec, col, col, vec, col, vec, row),
        check_vma=False,
    )
```

```python
import functools
import jax
import jax.numpy as jnp
from jax import lax
from jax.experimental import pallas as pl
from jax.experimental.pallas import tpu as pltpu

BLOCK = 16
EPSILON = 1e-05
LOG2E = 1.4426950408889634
F32 = jnp.float32
BF16 = jnp.bfloat16


def inverse_of(whole):
    guess = pl.reciprocal(whole, approx=True)
    return guess * (2.0 - whole * guess)


def gates_of(pre):
    small = jnp.exp2(jnp.abs(pre) * -LOG2E)
    whole = 1.0 + small
    log_part = jnp.where(small < 1e-3, small * (1.0 - small * (0.5 - small * (1.0 / 3.0))), jnp.log(whole))
    return jnp.maximum(pre, 0.0) + log_part, jnp.where(pre >= 0.0, 1.0, small) * inverse_of(whole)


def sigmoid(v):
    return 0.5 + 0.5 * jnp.tanh(0.5 * v)


def nt_dot(a, b):
    return lax.dot_general(a, b, (((1,), (1,)), ((), ())), preferred_element_type=F32)


def lane_tiles(width):
    step = min(width, 512)
    return [slice(k, k + step) for k in range(0, width, step)]


def tile_matrix(n, wide):
    col = lax.broadcasted_iota(jnp.int32, (n, wide), 1)
    row = lax.broadcasted_iota(jnp.int32, (n, wide), 0)
    return (col % n == row).astype(F32)


def diagonal_mask(rows, n, wide):
    col = lax.broadcasted_iota(jnp.int32, (rows, wide), 1)
    row = lax.broadcasted_iota(jnp.int32, (rows, wide), 0)
    return col // n == row % BLOCK


def scan_step(selected, x, gate, fresh, stepw_ref, bias_ref, skip_ref, gated_ref, gact_ref, tail_ref, dt_ref, slope_ref,
              u_s, y_s, coef_s, bt_s, hist_a, hist_b, state_s, rate_s, rank, n):
    length = x.shape[0]
    wide = BLOCK * n
    state_s[...] = jnp.where(fresh, 0.0, state_s[...])
    low = selected[:rank].T.astype(BF16)
    pre = jnp.dot(low, stepw_ref[...], preferred_element_type=F32) + bias_ref[...]
    dt, slope = gates_of(pre)
    dt_ref[...] = dt
    slope_ref[...] = slope
    u_s[...] = dt * x
    bt_s[...] = selected[rank:]
    spread = jnp.dot(selected[rank:].T[:, n:], tile_matrix(n, wide), preferred_element_type=F32)
    coef_s[...] = jnp.where(diagonal_mask(length, n, wide), spread, 0.0).astype(BF16)
    blocks = length // BLOCK

    def finish(k, hist):
        rows = pl.ds(pl.multiple_of(k * BLOCK, BLOCK), BLOCK)
        y_s[rows, :] = jnp.dot(coef_s[rows, :], hist[...], preferred_element_type=F32)

    def block(k, state, hist):
        at = pl.multiple_of(k * BLOCK, BLOCK)
        bs = pltpu.roll(bt_s[0:n, :], length - at, 1)
        dts = dt_ref[pl.ds(at, BLOCK), :]
        us = u_s[pl.ds(at, BLOCK), :]
        rate = rate_s[...]
        for i in range(BLOCK):
            factor = jnp.exp2(dts[i:i + 1, :] * rate)
            state = factor * state + us[i:i + 1, :] * bs[:, i:i + 1]
            hist[i * n:(i + 1) * n, :] = state.astype(BF16)
        return state

    def pair(j, state):
        finish(jnp.maximum(2 * j - 1, 0), hist_b)
        state = block(2 * j, state, hist_a)
        finish(2 * j, hist_a)
        return block(2 * j + 1, state, hist_b)

    state_s[...] = lax.fori_loop(0, blocks // 2, pair, state_s[...])
    finish(blocks - 1, hist_b)
    ssm = y_s[...] + skip_ref[...] * x
    sg = sigmoid(gate)
    gact = gate * sg
    gact_ref[...] = gact
    tail_ref[...] = (ssm * sg * (1.0 + gate * (1.0 - sg))).astype(BF16)
    gated_ref[...] = (ssm * gact).astype(BF16)


def scan_backward_kernel(sel_ref, x_ref, gact_ref, gg_ref, tail_ref, start_ref, dt_ref, slope_ref, stepw_ref, decay_ref, skip_ref,
                         ggate_ref, gvals_ref, gpre_ref, gsel_ref, gstepw_ref, gbias_ref, gdecay_ref, gskip_ref,
                         dt_s, u_s, gy_s, gu_s, ah_s, bcoef_s, bt_s, hist_s, adj_a, harm_a, adj_b, harm_b, db_s, dc_s, carry_s, gd_s, rate_s, factor_s, kept_s, *, rank, n):
    row, step = pl.program_id(0), pl.program_id(1)
    length = x_ref.shape[-2]
    wide = BLOCK * n
    blocks = length // BLOCK
    flat = lambda ref: ref[...].reshape(ref.shape[-2:])

    @pl.when(step == 0)
    def _():
        carry_s[...] = jnp.zeros_like(carry_s)

    @pl.when((step == 0) & (row == 0))
    def _():
        gstepw_ref[...] = jnp.zeros_like(gstepw_ref)
        gbias_ref[...] = jnp.zeros_like(gbias_ref)
        gskip_ref[...] = jnp.zeros_like(gskip_ref)
        gd_s[...] = jnp.zeros_like(gd_s)

    selected = flat(sel_ref).astype(F32)
    x = flat(x_ref).astype(F32)
    gg = flat(gg_ref)
    gy = gg * flat(gact_ref)
    ggate_ref[...] = (gg * flat(tail_ref).astype(F32)).astype(BF16).reshape(ggate_ref.shape)
    gskip_ref[...] += jnp.sum(gy * x, axis=0, keepdims=True)
    gy_s[...] = gy
    dt = flat(dt_ref)
    dt_s[...] = dt
    u_s[...] = dt * x
    bt_s[...] = selected[rank:]
    tiles = tile_matrix(n, wide)
    spread = jnp.dot(selected[rank:].T[:, :n], tiles, preferred_element_type=F32)
    bcoef_s[...] = jnp.where(diagonal_mask(length, n, wide), spread, 0.0).astype(BF16)
    rate_s[...] = -jnp.exp(decay_ref[...].astype(F32)) * LOG2E
    keep = diagonal_mask(BLOCK, n, wide)
    ones = keep.astype(BF16)
    lanes = lane_tiles(x.shape[1])
    state_s = start_ref.at[0, 0]

    def steps(lane):
        def again(k, state):
            at = pl.multiple_of(k * BLOCK, BLOCK)
            bs = pltpu.roll(bt_s[0:n, :], length - at, 1)
            dts = dt_s[pl.ds(at, BLOCK), lane]
            us = u_s[pl.ds(at, BLOCK), lane]
            rate = rate_s[:, lane]
            for i in range(BLOCK):
                here = pl.ds(pl.multiple_of((at + i) * n, n), n)
                factor = jnp.exp2(dts[i:i + 1, :] * rate)
                factor_s[here, lane] = factor
                old = factor * state
                kept_s[here, lane] = old
                state = old + us[i:i + 1, :] * bs[:, i:i + 1]
                hist_s[here, lane] = state.astype(BF16)
            return state

        lax.fori_loop(0, blocks, again, state_s[:, lane])

        def products(k, adj_s, harm_s):
            at = pl.multiple_of(k * BLOCK, BLOCK)
            rows = pl.ds(at, BLOCK)
            adj = adj_s[:, lane]
            gu_s[rows, lane] = jnp.dot(bcoef_s[rows, :], adj, preferred_element_type=F32)
            ah_s[rows, lane] = jnp.dot(ones, harm_s[:, lane], preferred_element_type=F32)
            db = jnp.where(keep, nt_dot(u_s[rows, lane].astype(BF16), adj), 0.0)
            states = hist_s[pl.ds(pl.multiple_of(at * n, n), wide), lane]
            dc = jnp.where(keep, nt_dot(gy_s[rows, lane].astype(BF16), states), 0.0)
            if lane.start == 0:
                db_s[rows, :] = db
                dc_s[rows, :] = dc
            else:
                db_s[rows, :] += db
                dc_s[rows, :] += dc

        def block(k, carry, adj_s, harm_s):
            at = pl.multiple_of(k * BLOCK, BLOCK)
            cs = pltpu.roll(bt_s[n:2 * n, :], length - at, 1)
            dts = dt_s[pl.ds(at, BLOCK), lane]
            gys = gy_s[pl.ds(at, BLOCK), lane]
            rate = rate_s[:, lane]
            gd = gd_s[:, lane]
            for i in range(BLOCK - 1, -1, -1):
                here = pl.ds(pl.multiple_of((at + i) * n, n), n)
                g = cs[:, i:i + 1] * gys[i:i + 1, :] + carry
                adj_s[i * n:(i + 1) * n, lane] = g.astype(BF16)
                carry = factor_s[here, lane] * g
                h = g * kept_s[here, lane]
                harm_s[i * n:(i + 1) * n, lane] = (h * rate).astype(BF16)
                gd = gd + dts[i:i + 1, :] * h
            gd_s[:, lane] = gd
            return carry

        def pair(j, carry):
            k = blocks - 1 - 2 * j
            if lane.start == 0:
                products(jnp.minimum(k + 1, blocks - 1), adj_b, harm_b)
            else:
                @pl.when(j > 0)
                def _():
                    products(k + 1, adj_b, harm_b)
            carry = block(k, carry, adj_a, harm_a)
            products(k, adj_a, harm_a)
            return block(k - 1, carry, adj_b, harm_b)

        carry_s[:, lane] = lax.fori_loop(0, blocks // 2, pair, carry_s[:, lane])
        products(0, adj_b, harm_b)

    for lane in lanes:
        steps(lane)
    gu = gu_s[...]
    gpre = ((x * gu + ah_s[...] * (1.0 / LOG2E)) * flat(slope_ref)).astype(BF16)
    gpre_ref[...] = gpre.reshape(gpre_ref.shape)
    gvals_ref[...] = (gy * skip_ref[...] + dt * gu).astype(gvals_ref.dtype).reshape(gvals_ref.shape)
    gbias_ref[...] += jnp.sum(gpre.astype(F32), axis=0, keepdims=True)
    gstepw_ref[...] += jnp.dot(selected[:rank].astype(BF16), gpre, preferred_element_type=F32)
    fold = lambda ref: nt_dot(tiles.astype(BF16), ref[...].astype(BF16))
    gsel_ref[0, 0, 0:rank, :] = nt_dot(stepw_ref[...], gpre).astype(BF16)
    gsel_ref[0, 0, rank:rank + n, :] = fold(db_s).astype(BF16)
    gsel_ref[0, 0, rank + n:rank + 2 * n, :] = fold(dc_s).astype(BF16)

    @pl.when((row == pl.num_programs(0) - 1) & (step == pl.num_programs(1) - 1))
    def _():
        gdecay_ref[...] = gd_s[...] * rate_s[...] * (1.0 / LOG2E)


def scan_backward(sel, x, gact, gg, tail, starts, dt, slope, stepw, decay, skip, n):
    chunks, rows, length, width = x.shape
    rank = stepw.shape[0]
    wide = BLOCK * n
    at = lambda r, c: (chunks - 1 - c, r, 0, 0)
    tok = lambda feat: pl.BlockSpec((1, 1, length, feat), at)
    whole = lambda shape: pl.BlockSpec(shape, lambda r, c: (0,) * len(shape))
    sds = jax.ShapeDtypeStruct
    return pl.pallas_call(
        functools.partial(scan_backward_kernel, rank=rank, n=n),
        grid=(rows, chunks),
        in_specs=[pl.BlockSpec((1, 1) + sel.shape[2:], at), tok(width), tok(width), tok(width), tok(width), pl.BlockSpec((1, 1, n, width), at), tok(width), tok(width),
                  whole(stepw.shape), whole(decay.shape), whole(skip.shape)],
        out_specs=[tok(width), tok(width), tok(width), pl.BlockSpec((1, 1) + sel.shape[2:], at), whole((rank, width)), whole((1, width)), whole((n, width)), whole((1, width))],
        out_shape=[
            sds(x.shape, BF16), sds(x.shape, F32), sds(x.shape, BF16), sds(sel.shape, BF16),
            sds((rank, width), F32), sds((1, width), F32), sds((n, width), F32), sds((1, width), F32),
        ],
        scratch_shapes=[
            pltpu.VMEM((length, width), F32), pltpu.VMEM((length, width), F32), pltpu.VMEM((length, width), F32),
            pltpu.VMEM((length, width), F32), pltpu.VMEM((length, width), F32),
            pltpu.VMEM((length, wide), BF16), pltpu.VMEM((2 * n, length), F32),
            pltpu.VMEM((length * n, width), BF16), pltpu.VMEM((wide, width), BF16), pltpu.VMEM((wide, width), BF16),
            pltpu.VMEM((wide, width), BF16), pltpu.VMEM((wide, width), BF16),
            pltpu.VMEM((length, wide), F32), pltpu.VMEM((length, wide), F32),
            pltpu.VMEM((n, width), F32), pltpu.VMEM((n, width), F32), pltpu.VMEM((n, width), F32),
            pltpu.VMEM((length * n, width), F32), pltpu.VMEM((length * n, width), F32),
        ],
        name="scan_backward",
    )(sel, x, gact, gg, tail, starts, dt, slope, stepw, decay, skip)
def conv_step(ci, fresh, taps_ref, bias_ref, selw_ref, ext_s):
    length = ci.shape[0]
    tap_count = taps_ref.shape[0]
    ext_s[0:8, :] = jnp.where(fresh, 0.0, ext_s[length:length + 8, :])
    ext_s[8:, :] = ci.astype(F32)
    total = bias_ref[...].astype(F32)
    for k in range(tap_count):
        total = total + taps_ref[k:k + 1, :].astype(F32) * ext_s[pl.ds(8 - tap_count + 1 + k, length), :]
    x = (total * sigmoid(total)).astype(BF16)
    return x, nt_dot(selw_ref[...], x).astype(BF16)


def conv_backward_kernel(ci_ref, prev_ref, gvals_ref, gsel_ref, taps_ref, bias_ref, selw_ref,
                         gci_ref, gtaps_ref, gbias_ref, gselw_ref, ext_s, gext_s):
    row, step = pl.program_id(0), pl.program_id(1)
    length = ci_ref.shape[-2]
    tap_count = taps_ref.shape[0]
    flat = lambda ref: ref[...].reshape(ref.shape[-2:])

    @pl.when(step == 0)
    def _():
        gext_s[length:, :] = jnp.zeros((8, gext_s.shape[1]), F32)

    @pl.when((step == 0) & (row == 0))
    def _():
        gtaps_ref[...] = jnp.zeros_like(gtaps_ref)
        gbias_ref[...] = jnp.zeros_like(gbias_ref)
        gselw_ref[...] = jnp.zeros_like(gselw_ref)

    first = step == pl.num_programs(1) - 1
    ext_s[8:, :] = flat(ci_ref).astype(F32)
    before = flat(prev_ref)[length - 16:, :].astype(F32)[8:, :]
    ext_s[0:8, :] = jnp.where(first, 0.0, before)
    total = bias_ref[...].astype(F32)
    for k in range(tap_count):
        total = total + taps_ref[k:k + 1, :].astype(F32) * ext_s[pl.ds(8 - tap_count + 1 + k, length), :]
    sg = sigmoid(total)
    x = (total * sg).astype(BF16)
    gsel = flat(gsel_ref)
    gvals = flat(gvals_ref) + jnp.dot(gsel.astype(F32).T.astype(BF16), selw_ref[...], preferred_element_type=F32)
    gconv = gvals * sg * (1.0 + total * (1.0 - sg))
    gbias_ref[...] += jnp.sum(gconv, axis=0, keepdims=True)
    for k in range(tap_count):
        gtaps_ref[k:k + 1, :] += jnp.sum(gconv * ext_s[pl.ds(8 - tap_count + 1 + k, length), :], axis=0, keepdims=True)
    gselw_ref[...] += jnp.dot(gsel, x, preferred_element_type=F32)
    gext_s[0:length, :] = gconv
    gci = jnp.zeros_like(gconv)
    for k in range(tap_count):
        gci = gci + taps_ref[k:k + 1, :].astype(F32) * gext_s[pl.ds(tap_count - 1 - k, length), :]
    gci_ref[...] = gci.astype(BF16).reshape(gci_ref.shape)
    gext_s[length:, :] = gconv[0:8, :]


def conv_backward(ci, gvals, gsel, taps, bias, selw):
    chunks, rows, length, width = ci.shape
    at = lambda r, c: (chunks - 1 - c, r, 0, 0)
    before = lambda r, c: (jnp.maximum(chunks - 2 - c, 0), r, 0, 0)
    tok = lambda feat, where: pl.BlockSpec((1, 1, length, feat), where)
    whole = lambda shape: pl.BlockSpec(shape, lambda r, c: (0,) * len(shape))
    sds = jax.ShapeDtypeStruct
    return pl.pallas_call(
        conv_backward_kernel,
        grid=(rows, chunks),
        in_specs=[tok(width, at), tok(width, before), tok(width, at), pl.BlockSpec((1, 1) + gsel.shape[2:], at), whole(taps.shape), whole(bias.shape), whole(selw.shape)],
        out_specs=[tok(width, at), whole(taps.shape), whole(bias.shape), whole(selw.shape)],
        out_shape=[sds(ci.shape, BF16), sds(taps.shape, F32), sds(bias.shape, F32), sds(selw.shape, F32)],
        scratch_shapes=[pltpu.VMEM((length + 8, width), F32), pltpu.VMEM((length + 8, width), F32)],
        name="conv_backward",
    )(ci, ci, gvals, gsel, taps, bias, selw)
MESH = pl.DeviceIdType.MESH


def remote(src, dst, send, recv, device):
    return pltpu.make_async_remote_copy(src_ref=src, dst_ref=dst, send_sem=send, recv_sem=recv, device_id=device, device_id_type=MESH)


def grid_of(chunks, copies):
    deep = max(1, copies // 2)
    return (chunks // deep, deep) if chunks % deep == 0 else (chunks, 1)


def meet(chunks, copies):
    me, mine = lax.axis_index("seq"), lax.axis_index("dp")
    barrier = pltpu.get_barrier_semaphore()

    def greet(k, _):
        pl.semaphore_signal(barrier, inc=1, device_id={"seq": lax.rem(me + k, chunks)}, device_id_type=MESH)
        return 0

    def greet_copy(k, _):
        pl.semaphore_signal(barrier, inc=1, device_id={"dp": lax.rem(mine + k, copies)}, device_id_type=MESH)
        return 0

    lax.fori_loop(1, chunks, greet, 0)
    if copies > 1:
        lax.fori_loop(1, copies, greet_copy, 0)
    pl.semaphore_wait(barrier, chunks - 1 + max(copies - 1, 0))


def gather_project_kernel(hid_ref, wq_ref, gain_ref, n_ref, ci_ref, gate_ref, w_ref, row_ref,
                          hid_v, gain_v, w_v, n_v, ci_v, gate_v,
                          load_sem, out_sem, hrecv, hside, hup, hdown,
                          w1send, w1recv, w2recv, w2send, w3send, gsend, grecv, *, chunks, copies, share, split):
    zs, ys = grid_of(chunks, copies)
    xs = copies // 2
    me, mine = lax.axis_index("seq"), lax.axis_index("dp")
    z, y = me // ys, me % ys
    x, c = mine // 2, mine % 2
    tokens, model = hid_v.shape[1:]
    width = ci_v.shape[1]
    inner = chunks * width
    half = tokens // 2
    piece = share // (copies if split else 1)
    spot = mine if split else 0
    load = pltpu.make_async_copy(hid_ref, hid_v.at[me], load_sem)
    load.start()
    meet(chunks, copies)
    load.wait()

    def w_rows(s, d):
        return pl.ds(pl.multiple_of(s * share + d * piece, piece), piece)

    def w_first(s, part):
        src = wq_ref.at[pl.ds(pl.multiple_of(spot * piece, piece), piece), pl.ds(pl.multiple_of(part * inner + s * width, width), width)]
        return remote(src, w_v.at[w_rows(me, spot), pl.ds(part * width, width)], w1send.at[s, part], w1recv.at[me, part], {"seq": s})

    def w_landed(s, part):
        dst = w_v.at[w_rows(s, spot), pl.ds(part * width, width)]
        return remote(dst, dst, w1send.at[s, part], w1recv.at[s, part], {"seq": s})

    def w_own(part):
        src = wq_ref.at[pl.ds(pl.multiple_of(spot * piece, piece), piece), pl.ds(pl.multiple_of(part * inner + me * width, width), width)]
        return pltpu.make_async_copy(src, w_v.at[w_rows(me, spot), pl.ds(part * width, width)], out_sem.at[part])

    def every_other(fn):
        def one(k, _):
            fn(lax.rem(me + k, chunks))
            return 0
        lax.fori_loop(1, chunks, one, 0)

    def gain_to(s):
        return remote(gain_ref, gain_v.at[me], gsend.at[s], grecv.at[me], {"seq": s})

    def gain_from(s):
        return remote(gain_v.at[s], gain_v.at[s], gsend.at[s], grecv.at[s], {"seq": s})

    def send_first(s):
        gain_to(s).start()
        w_first(s, 0).start()
        w_first(s, 1).start()

    def block(o, yy, h):
        return hid_v.at[o * ys + yy, pl.ds(h * half, half)]

    def up(o, h):
        return remote(block(o, y, h), block(o, y, h), hup.at[o, h], hrecv.at[o * ys + y, h], {"seq": (z + 1) * ys + y})

    def down(o, h):
        return remote(block(o, y, h), block(o, y, h), hdown.at[o, h], hrecv.at[o * ys + y, h], {"seq": (z - 1) * ys + y})

    def side(o, j, h):
        other = lax.rem(y + j, ys)
        return remote(block(o, y, h), block(o, y, h), hside.at[o, j - 1, h], hrecv.at[o * ys + y, h], {"seq": z * ys + other})

    def landed(o, yy, h):
        return remote(block(o, yy, h), block(o, yy, h), hside.at[o, 0, h], hrecv.at[o * ys + yy, h], {"seq": lax.rem(me + 1, chunks)})

    def when(cond, fn):
        pl.when(cond)(fn)

    gain_own = pltpu.make_async_copy(gain_ref, gain_v.at[me], out_sem.at[2])
    gain_own.start()
    for part in range(2):
        w_own(part).start()
    for h in range(2):
        when(z + 1 < zs, lambda: up(z, h).start())
        when(z > 0, lambda: down(z, h).start())
        for j in range(1, ys):
            side(z, j, h).start()
    every_other(send_first)

    def relay(k):
        for h in range(2):
            @pl.when(z - k >= 0)
            def _():
                landed(z - k, y, h).wait_recv()
                when(z + 1 < zs, lambda: up(z - k, h).start())
                for j in range(1, ys):
                    side(z - k, j, h).start()

            @pl.when(z + k < zs)
            def _():
                landed(z + k, y, h).wait_recv()
                when(z > 0, lambda: down(z + k, h).start())
                for j in range(1, ys):
                    side(z + k, j, h).start()

    def shared(s, d, sems, k, device):
        return remote(w_v.at[w_rows(s, d)], w_v.at[w_rows(s, d)], sems.at[s, k], w2recv.at[s, d], device)

    def spread(s):
        for j in range(1, xs):
            shared(s, mine, w2send, j - 1, {"dp": lax.rem(x + j, xs) * 2 + c}).start()
        shared(s, mine, w3send, 0, {"dp": x * 2 + 1 - c}).start()

    gain_own.wait()
    for part in range(2):
        w_own(part).wait()
    if split:
        spread(me)

    def take_first(s):
        gain_from(s).wait_recv()
        for part in range(2):
            w_landed(s, part).wait_recv()
        if split:
            spread(s)

    if zs > 1:
        relay(1)
    every_other(take_first)

    def take_second(s, _):
        for j in range(1, xs):
            d = lax.rem(x + j, xs) * 2 + c
            shared(s, d, w2send, j - 1, {"dp": d}).wait_recv()
            shared(s, d, w3send, j, {"dp": x * 2 + 1 - c}).start()
        return 0

    def take_third(s, _):
        for j in range(xs):
            d = lax.rem(x + j, xs) * 2 + 1 - c
            shared(s, d, w2send, 0, {"dp": d}).wait_recv()
        return 0

    if zs > 2:
        relay(2)
    if split:
        lax.fori_loop(0, chunks, take_second, 0)
    if split:
        lax.fori_loop(0, chunks, take_third, 0)

    row_ref[...] = jnp.concatenate([gain_v[s] for s in range(chunks)], axis=-1)
    w_out = pltpu.make_async_copy(w_v, w_ref, load_sem)
    w_out.start()
    steps = 4 if width >= 512 else 1
    tile = 2 * width // steps

    def project(at):
        def rows(i, _):
            sl = pl.ds(pl.multiple_of(i * 32, 32), 32)
            h = hid_v[at, sl, :].astype(F32)
            inverse = lax.rsqrt(jnp.mean(h * h, axis=-1, keepdims=True) + EPSILON)
            n_v[sl, :] = (h * inverse * row_ref[...]).astype(BF16)
            return 0
        lax.fori_loop(0, tokens // 32, rows, 0)
        n_out = pltpu.make_async_copy(n_v, n_ref.at[at], out_sem.at[0])
        n_out.start()

        def columns(i, _):
            sl = pl.ds(pl.multiple_of(i * tile, tile), tile)
            got = jnp.dot(n_v[...], w_v[:, sl], preferred_element_type=F32)
            if steps == 1:
                ci_v[...] = got[:, :width].astype(BF16)
                gate_v[...] = got[:, width:]
            else:
                @pl.when(i < steps // 2)
                def _():
                    ci_v[:, sl] = got.astype(BF16)

                @pl.when(i >= steps // 2)
                def _():
                    gate_v[:, pl.ds(pl.multiple_of(i * tile - width, tile), tile)] = got
            return 0
        lax.fori_loop(0, steps, columns, 0)
        ci_out = pltpu.make_async_copy(ci_v, ci_ref.at[at], out_sem.at[1])
        gate_out = pltpu.make_async_copy(gate_v, gate_ref.at[at], out_sem.at[2])
        ci_out.start()
        gate_out.start()
        n_out.wait()
        ci_out.wait()
        gate_out.wait()

    def work(first, last):
        def one(i, _):
            k0, j = i // (2 * ys), i % (2 * ys)
            lower, yy = j // ys, j % ys
            own = yy == y
            k = k0 - jnp.where(own, 0, 1)
            o = z + k * (2 * lower - 1)
            ok = (k >= 0) & (k < zs) & (o >= 0) & (o < zs) & ((lower == 0) | (k > 0))

            @pl.when(ok & jnp.logical_not(own))
            def _():
                for h in range(2):
                    landed(o, yy, h).wait_recv()

            @pl.when(ok)
            def _():
                project(o * ys + yy)
            return 0
        lax.fori_loop(first * 2 * ys, last * 2 * ys, one, 0)

    work(0, min(3, zs))

    def later(k, _):
        relay(k)
        work(k, k + 1)
        return 0

    lax.fori_loop(3, zs, later, 0)
    work(zs, zs + 1)
    w_out.wait()

    def drain_first(s):
        gain_to(s).wait_send()
        for part in range(2):
            w_first(s, part).wait_send()

    every_other(drain_first)

    def drain_second(s, _):
        for j in range(1, xs):
            shared(s, mine, w2send, j - 1, {"dp": mine}).wait_send()
        for j in range(xs):
            shared(s, mine, w3send, j, {"dp": mine}).wait_send()
        return 0

    if split:
        lax.fori_loop(0, chunks, drain_second, 0)

    def drain(k, _):
        for h in range(2):
            @pl.when(z - k >= 0)
            def _():
                when(z + 1 < zs, lambda: up(z - k, h).wait_send())
                for j in range(1, ys):
                    side(z - k, j, h).wait_send()

            @pl.when((z + k < zs) & (k > 0))
            def _():
                when(z > 0, lambda: down(z + k, h).wait_send())
                for j in range(1, ys):
                    side(z + k, j, h).wait_send()
        return 0

    lax.fori_loop(0, zs, drain, 0)
    for h in range(2):
        when(z > 0, lambda: down(z, h).wait_send())


def gather_project(hidden, wq, gain, chunks, copies, share, split):
    tokens, model = hidden.shape
    width = wq.shape[1] // 2 // chunks
    zs, ys = grid_of(chunks, copies)
    any_spec = pl.BlockSpec(memory_space=pl.ANY)
    sds = jax.ShapeDtypeStruct
    dma = pltpu.SemaphoreType.DMA
    return pl.pallas_call(
        functools.partial(gather_project_kernel, chunks=chunks, copies=copies, share=share, split=split),
        in_specs=[any_spec] * 3,
        out_specs=[any_spec] * 4 + [pl.BlockSpec(memory_space=pltpu.VMEM)],
        out_shape=[sds((chunks, tokens, model), BF16), sds((chunks, tokens, width), BF16),
                   sds((chunks, tokens, width), F32), sds((model, 2 * width), BF16), sds((1, model), F32)],
        scratch_shapes=[
            pltpu.VMEM((chunks, tokens, model), BF16), pltpu.VMEM((chunks, 1, share), F32), pltpu.VMEM((model, 2 * width), BF16),
            pltpu.VMEM((tokens, model), BF16), pltpu.VMEM((tokens, width), BF16), pltpu.VMEM((tokens, width), F32),
            dma(()), dma((3,)), dma((chunks, 2)), dma((zs, max(1, ys - 1), 2)), dma((zs, 2)), dma((zs, 2)),
            dma((chunks, 2)), dma((chunks, 2)), dma((chunks, copies)), dma((chunks, max(1, copies // 2))), dma((chunks, max(1, copies // 2))),
            dma((chunks,)), dma((chunks,)),
        ],
        compiler_params=pltpu.CompilerParams(collective_id=0, has_side_effects=True, vmem_limit_bytes=60 * 1024 * 1024),
        name="gather_project",
    )(hidden, wq, gain)


def total_kernel(*refs, chunks, copies, extra):
    part_ref, out_ref = refs[0], refs[1 + extra]
    early, early_out = refs[1:1 + extra], refs[2 + extra:2 + 2 * extra]
    refs = refs[2 + 2 * extra:]
    recv_v, send1, recv1, send2, recv2 = refs[:5]
    bufs, sems = refs[5:5 + 3 * extra], refs[5 + 3 * extra:]
    me, mine = lax.axis_index("seq"), lax.axis_index("dp")
    x, c = mine // 2, mine % 2
    xs = copies // 2
    meet(chunks, copies if extra else 1)

    def first(s):
        return remote(part_ref.at[s], recv_v.at[me], send1.at[s], recv1.at[me], {"seq": s})

    def landed_first(s):
        return remote(part_ref.at[s], recv_v.at[s], send1.at[s], recv1.at[s], {"seq": s})

    def second(s):
        return remote(out_ref.at[me], out_ref.at[me], send2.at[s], recv2.at[me], {"seq": s})

    def landed_second(s):
        return remote(out_ref.at[s], out_ref.at[s], send2.at[s], recv2.at[s], {"seq": s})

    def every_other(fn):
        def one(k, _):
            fn(lax.rem(me + k, chunks))
            return 0
        lax.fori_loop(1, chunks, one, 0)

    def part_of(e, core):
        rows = early[e].shape[0] // 2
        return pl.ds(pl.multiple_of(core * rows, rows), rows)

    def to_core(e):
        return remote(early[e].at[part_of(e, 1 - c)], bufs[3 * e], sems[0].at[e], sems[1].at[e], {"dp": x * 2 + 1 - c})

    def across(e, j):
        return remote(bufs[3 * e + 1], bufs[3 * e + 2].at[x], sems[2].at[e, j], sems[3].at[e, x], {"dp": lax.rem(x + j, xs) * 2 + c})

    def from_across(e, j):
        q = lax.rem(x + j, xs)
        return remote(bufs[3 * e + 2].at[q], bufs[3 * e + 2].at[q], sems[2].at[e, j], sems[3].at[e, q], {"dp": q * 2 + c})

    def back(e):
        return remote(early_out[e].at[part_of(e, c)], early_out[e].at[part_of(e, c)], sems[4].at[e], sems[5].at[e], {"dp": x * 2 + 1 - c})

    def from_back(e):
        return remote(early_out[e].at[part_of(e, 1 - c)], early_out[e].at[part_of(e, 1 - c)], sems[4].at[e], sems[5].at[e], {"dp": x * 2 + 1 - c})

    def by_rows(e, fn):
        count = early[e].shape[0] // 2
        step = 16

        def one(i, _):
            fn(pl.multiple_of(i * step, step), step, pl.multiple_of(c * count, count) + i * step)
            return 0
        lax.fori_loop(0, count // step, one, 0)

    every_other(lambda s: first(s).start())
    for e in range(extra):
        to_core(e).start()
    recv_v[me] = part_ref[me]
    for e in range(extra):
        to_core(e).wait_recv()

        def fold(at, step, full):
            mine_rows = early[e][pl.ds(pl.multiple_of(full, step), step), :].astype(F32)
            bufs[3 * e + 1][pl.ds(at, step), :] = (mine_rows + bufs[3 * e][pl.ds(at, step), :].astype(F32)).astype(BF16)

        by_rows(e, fold)
        for j in range(1, xs):
            across(e, j).start()
    every_other(lambda s: landed_first(s).wait_recv())
    total = recv_v[0].astype(F32)
    for s in range(1, chunks):
        total = total + recv_v[s].astype(F32)
    out_ref[me] = total.astype(BF16)
    every_other(lambda s: second(s).start())
    for e in range(extra):
        for j in range(1, xs):
            from_across(e, j).wait_recv()

        def finish(at, step, full):
            total = bufs[3 * e + 1][pl.ds(at, step), :].astype(F32)
            for j in range(1, xs):
                total = total + bufs[3 * e + 2][lax.rem(x + j, xs), pl.ds(at, step), :].astype(F32)
            early_out[e][pl.ds(pl.multiple_of(full, step), step), :] = total.astype(BF16)

        by_rows(e, finish)
        back(e).start()
    every_other(lambda s: landed_second(s).wait_recv())
    every_other(lambda s: first(s).wait_send())
    every_other(lambda s: second(s).wait_send())
    for e in range(extra):
        from_back(e).wait_recv()
        to_core(e).wait_send()
        for j in range(1, xs):
            across(e, j).wait_send()
        back(e).wait_send()


def total_over_seq(part, chunks, copies, key, early=()):
    vmem = pl.BlockSpec(memory_space=pltpu.VMEM)
    dma = pltpu.SemaphoreType.DMA
    extra = len(early)
    xs = max(1, copies // 2)
    scratch = [pltpu.VMEM(part.shape, BF16), dma((chunks,)), dma((chunks,)), dma((chunks,)), dma((chunks,))]
    for a in early:
        rows = a.shape[0] // 2
        scratch += [pltpu.VMEM((rows, a.shape[1]), BF16), pltpu.VMEM((rows, a.shape[1]), BF16), pltpu.VMEM((xs, rows, a.shape[1]), BF16)]
    if extra:
        scratch += [dma((extra,)), dma((extra,)), dma((extra, xs)), dma((extra, xs)), dma((extra,)), dma((extra,))]
    sds = jax.ShapeDtypeStruct
    got = pl.pallas_call(
        functools.partial(total_kernel, chunks=chunks, copies=copies, extra=extra),
        in_specs=[vmem] * (1 + extra),
        out_specs=[vmem] * (1 + extra),
        out_shape=[sds(part.shape, BF16)] + [sds(a.shape, BF16) for a in early],
        scratch_shapes=scratch,
        compiler_params=pltpu.CompilerParams(collective_id=key, has_side_effects=True, vmem_limit_bytes=60 * 1024 * 1024),
        name=f"total_over_seq_{key}",
    )(part, *early)
    return got if extra else got[0]
def forward_kernel(ci_ref, gate_ref, gm_ref, taps_ref, cbias_ref, selw_ref, stepw_ref, sbias_ref, decay_ref, skip_ref,
                   gmall_ref, sel_ref, x_ref, gated_ref, gact_ref, tail_ref, dt_ref, slope_ref, start_ref,
                   gate_v, part_v, recv_v, x_v, gated_v, gact_v, tail_v, dt_v, slope_v, start_v,
                   ext_s, u_s, y_s, coef_s, bt_s, hist_a, hist_b, state_s, rate_s,
                   load_sem, own_sem, out_sem, grecv, gside, gup, gdown, send1, recv1, send2, recv2, *, chunks, copies, n):
    zs, ys = grid_of(chunks, copies)
    me = lax.axis_index("seq")
    z, y = me // ys, me % ys
    tokens, model = gm_ref.shape
    rows, length, width = ci_ref.shape[1:]
    rank = stepw_ref.shape[0]
    half = tokens // 2
    load = pltpu.make_async_copy(gate_ref, gate_v, load_sem)
    load.start()
    own = pltpu.make_async_copy(gm_ref, gmall_ref.at[me], own_sem)
    own.start()
    meet(chunks, 1)

    def block(o, yy, h):
        return gmall_ref.at[o * ys + yy, pl.ds(h * half, half)]

    def source(o, h, k):
        return gm_ref.at[pl.ds(h * half, half)] if k is None else block(o, y, h)

    def up(o, h, k=0):
        return remote(source(o, h, k), block(o, y, h), gup.at[o, h], grecv.at[o * ys + y, h], {"seq": (z + 1) * ys + y})

    def down(o, h, k=0):
        return remote(source(o, h, k), block(o, y, h), gdown.at[o, h], grecv.at[o * ys + y, h], {"seq": (z - 1) * ys + y})

    def side(o, j, h, k=0):
        return remote(source(o, h, k), block(o, y, h), gside.at[o, j - 1, h], grecv.at[o * ys + y, h], {"seq": z * ys + lax.rem(y + j, ys)})

    def landed(o, yy, h):
        return remote(block(o, yy, h), block(o, yy, h), gside.at[o, 0, h], grecv.at[o * ys + yy, h], {"seq": lax.rem(me + 1, chunks)})

    def when(cond, fn):
        pl.when(cond)(fn)

    for h in range(2):
        when(z + 1 < zs, lambda: up(z, h, None).start())
        when(z > 0, lambda: down(z, h, None).start())
        for j in range(1, ys):
            side(z, j, h, None).start()

    def relay(k):
        for h in range(2):
            @pl.when(z - k >= 0)
            def _():
                landed(z - k, y, h).wait_recv()
                when(z + 1 < zs, lambda: up(z - k, h).start())
                for j in range(1, ys):
                    side(z - k, j, h).start()

            @pl.when(z + k < zs)
            def _():
                landed(z + k, y, h).wait_recv()
                when(z > 0, lambda: down(z + k, h).start())
                for j in range(1, ys):
                    side(z + k, j, h).start()

    rate_s[...] = -jnp.exp(decay_ref[...].astype(F32)) * LOG2E

    def conv(i, _):
        r, c = i // chunks, i % chunks
        x, part = conv_step(ci_ref[c, r], c == 0, taps_ref, cbias_ref, selw_ref, ext_s)
        x_v[c, r] = x
        part_v[c, r] = part
        return 0

    lax.fori_loop(0, rows * chunks, conv, 0)
    x_out = pltpu.make_async_copy(x_v, x_ref, out_sem.at[0, 0])
    x_out.start()

    def first(s):
        return remote(part_v.at[s], recv_v.at[me], send1.at[s], recv1.at[me], {"seq": s})

    def landed_first(s):
        return remote(part_v.at[s], recv_v.at[s], send1.at[s], recv1.at[s], {"seq": s})

    def second(s):
        return remote(sel_ref.at[me], sel_ref.at[me], send2.at[s], recv2.at[me], {"seq": s})

    def landed_second(s):
        return remote(sel_ref.at[s], sel_ref.at[s], send2.at[s], recv2.at[s], {"seq": s})

    def every_other(fn):
        def one(k, _):
            fn(lax.rem(me + k, chunks))
            return 0
        lax.fori_loop(1, chunks, one, 0)

    every_other(lambda s: first(s).start())
    recv_v[me] = part_v[me]
    every_other(lambda s: landed_first(s).wait_recv())
    total = recv_v[0].astype(F32)
    for s in range(1, chunks):
        total = total + recv_v[s].astype(F32)
    sel_ref[me] = total.astype(BF16)
    every_other(lambda s: second(s).start())
    if zs > 1:
        relay(1)
    every_other(lambda s: landed_second(s).wait_recv())
    load.wait()
    pairs = ((gated_v, gated_ref), (gact_v, gact_ref), (tail_v, tail_ref), (dt_v, dt_ref), (slope_v, slope_ref), (start_v, start_ref))

    def outs(c, r):
        return [pltpu.make_async_copy(src.at[c, r], dst.at[c, r], out_sem.at[1 + k, c * rows + r]) for k, (src, dst) in enumerate(pairs)]

    def scan(i, _):
        r, c = i // chunks, i % chunks
        start_v[c, r] = jnp.where(c == 0, 0.0, state_s[...])
        scan_step(sel_ref[c, r].astype(F32), x_v[c, r].astype(F32), gate_v[c, r], c == 0, stepw_ref, sbias_ref, skip_ref,
                  gated_v.at[c, r], gact_v.at[c, r], tail_v.at[c, r], dt_v.at[c, r], slope_v.at[c, r],
                  u_s, y_s, coef_s, bt_s, hist_a, hist_b, state_s, rate_s, rank, n)
        for one in outs(c, r):
            one.start()
        return 0

    count = rows * chunks
    parts = max(1, zs - 2)
    for k in range(parts):
        lax.fori_loop(count * k // parts, count * (k + 1) // parts, scan, 0)
        if 2 + k < zs:
            relay(2 + k)

    def others(o, _):
        for j in range(1, ys):
            for h in range(2):
                landed(o, lax.rem(y + j, ys), h).wait_recv()
        return 0

    lax.fori_loop(0, zs, others, 0)
    own.wait()
    x_out.wait()

    def settle(i, _):
        for one in outs(i // rows, i % rows):
            one.wait()
        return 0

    lax.fori_loop(0, count, settle, 0)
    every_other(lambda s: first(s).wait_send())
    every_other(lambda s: second(s).wait_send())

    def drain(k, _):
        for h in range(2):
            @pl.when(z - k >= 0)
            def _():
                when(z + 1 < zs, lambda: up(z - k, h).wait_send())
                for j in range(1, ys):
                    side(z - k, j, h).wait_send()

            @pl.when((z + k < zs) & (k > 0))
            def _():
                when(z > 0, lambda: down(z + k, h).wait_send())
                for j in range(1, ys):
                    side(z + k, j, h).wait_send()
        return 0

    lax.fori_loop(0, zs, drain, 0)
    for h in range(2):
        when(z > 0, lambda: down(z, h).wait_send())


def forward(ci, gate, gm, taps, cbias, selw, stepw, sbias, decay, skip, copies, n):
    chunks, rows, length, width = ci.shape
    tokens, model = gm.shape
    zs, ys = grid_of(chunks, copies)
    wide = BLOCK * n
    sds = jax.ShapeDtypeStruct
    dma = pltpu.SemaphoreType.DMA
    vmem = pl.BlockSpec(memory_space=pltpu.VMEM)
    hbm = pl.BlockSpec(memory_space=pl.ANY)
    coef = (chunks, rows, selw.shape[0], length)
    starts = (chunks, rows, n, width)
    full = ci.shape
    return pl.pallas_call(
        functools.partial(forward_kernel, chunks=chunks, copies=copies, n=n),
        in_specs=[vmem, hbm] + [vmem] * 8,
        out_specs=[hbm, vmem] + [hbm] * 7,
        out_shape=[sds((chunks, tokens, model), BF16), sds(coef, BF16), sds(full, BF16), sds(full, BF16), sds(full, F32), sds(full, BF16),
                   sds(full, F32), sds(full, F32), sds(starts, F32)],
        scratch_shapes=[
            pltpu.VMEM(full, F32), pltpu.VMEM(coef, BF16), pltpu.VMEM(coef, BF16), pltpu.VMEM(full, BF16), pltpu.VMEM(full, BF16),
            pltpu.VMEM(full, F32), pltpu.VMEM(full, BF16), pltpu.VMEM(full, F32), pltpu.VMEM(full, F32), pltpu.VMEM(starts, F32),
            pltpu.VMEM((length + 8, width), F32), pltpu.VMEM((length, width), F32), pltpu.VMEM((length, width), F32),
            pltpu.VMEM((length, wide), BF16), pltpu.VMEM((2 * n, length), F32), pltpu.VMEM((wide, width), BF16), pltpu.VMEM((wide, width), BF16),
            pltpu.VMEM((n, width), F32), pltpu.VMEM((n, width), F32),
            dma(()), dma(()), dma((7, rows * chunks)), dma((chunks, 2)), dma((zs, max(1, ys - 1), 2)), dma((zs, 2)), dma((zs, 2)),
            dma((chunks,)), dma((chunks,)), dma((chunks,)), dma((chunks,)),
        ],
        compiler_params=pltpu.CompilerParams(collective_id=1, has_side_effects=True, vmem_limit_bytes=60 * 1024 * 1024),
        name="forward",
    )(ci, gate, gm, taps, cbias, selw, stepw, sbias, decay, skip)


def order_of(zs):
    return [sorted(range(zs), key=lambda t: (-abs(t - z), t)) for z in range(zs)]


def scatter_kernel(*refs, chunks, copies, split):
    if split:
        (gc_ref, gg_ref, w_ref, late_ref, ginc_ref, ging_ref, red_ref, sum_ref, all_ref,
         ysend_v, yrecv_v, own_v, zrecv_v, late_v, w_v, g1_v, mine_v, g2_v, t_v, fin_v, load_sem,
         ysend, yrecv, zup, zdown, zrecv, lsend, lrecv,
         g1send, g1recv, g2send, g2recv, g3send, g3recv, g4send, g4recv) = refs
    else:
        (gc_ref, gg_ref, w_ref, late_ref, red_ref, sum_ref,
         ysend_v, yrecv_v, own_v, zrecv_v, late_v, w_v, load_sem,
         ysend, yrecv, zup, zdown, zrecv, lsend, lrecv) = refs
    zs, ys = grid_of(chunks, copies)
    xs = copies // 2
    me, mine = lax.axis_index("seq"), lax.axis_index("dp")
    z, y = me // ys, me % ys
    x, c = mine // 2, mine % 2
    tokens, width = gc_ref.shape[1:]
    model = w_ref.shape[0]
    half = tokens // 2
    tile = min(256, model)
    tables = order_of(zs)

    def dest(i):
        got = 0
        for k in range(zs):
            got = got + jnp.where(z == k, tables[k][i], 0)
        return got

    w_in = pltpu.make_async_copy(w_ref, w_v, load_sem.at[0])
    w_in.start()
    if split:
        piece, inner2 = fin_v.shape
        inner = inner2 // 2
        sides = (ginc_ref, ging_ref)
        cols = [pl.ds(part * width, width) for part in range(2)]
        loads = [[pltpu.make_async_copy(sides[part].at[:, q * 2 + c], mine_v.at[q, :, :, cols[part]], load_sem.at[1 + q * 2 + part]) for part in range(2)]
                 for q in range(xs)]
        for q in range(xs):
            for part in range(2):
                loads[q][part].start()
    meet(chunks, copies)

    def late_to(d):
        return remote(late_ref, late_v.at[mine], lsend.at[d], lrecv.at[mine], {"dp": d})

    def late_from(d):
        return remote(late_v.at[d], late_v.at[d], lsend.at[d], lrecv.at[d], {"dp": d})

    def every_copy(fn):
        def one(k, _):
            fn(lax.rem(mine + k, copies))
            return 0
        lax.fori_loop(1, copies, one, 0)

    if split:
        def g1(q, part):
            return remote(sides[part].at[:, q * 2 + 1 - c], g1_v.at[q, :, :, cols[part]], g1send.at[q, part], g1recv.at[q, part], {"dp": x * 2 + 1 - c})

        for q in range(xs):
            for part in range(2):
                g1(q, part).start()
    every_copy(lambda d: late_to(d).start())
    w_in.wait()

    def partial(s, out, at):
        def one(i, _):
            sl = pl.ds(pl.multiple_of(i * tile, tile), tile)
            got = nt_dot(gc_ref[s], w_v[sl, :width]) + nt_dot(gg_ref[s], w_v[sl, width:])
            out[at, :, sl] = got.astype(BF16)
            return 0
        lax.fori_loop(0, model // tile, one, 0)

    def to_side(i, j, h):
        rows = pl.ds(h * half, half)
        k = i * (ys - 1) + j - 1
        return remote(ysend_v.at[k % ysend_v.shape[0], rows], yrecv_v.at[k, rows], ysend.at[k, h], yrecv.at[k, h], {"seq": z * ys + lax.rem(y + j, ys)})

    slots = ysend_v.shape[0]
    ahead = 2 if slots == zs * (ys - 1) else zs
    for i in range(zs):
        for j in range(1, ys):
            k = i * (ys - 1) + j - 1
            if k >= slots:
                for h in range(2):
                    to_side((k - slots) // (ys - 1), (k - slots) % (ys - 1) + 1, h).wait_send()
            partial(dest(i) * ys + lax.rem(y + j, ys), ysend_v, k % slots)
            if i < ahead:
                for h in range(2):
                    to_side(i, j, h).start()

    def add_into(total, terms):
        def one(r, _):
            sl = pl.ds(pl.multiple_of(r * 32, 32), 32)
            total(sl, terms)
            return 0
        return one

    if split:
        def g2(q):
            return remote(mine_v.at[q], g2_v.at[x], g2send.at[q], g2recv.at[x], {"dp": q * 2 + c})

        def g2_from(q):
            return remote(g2_v.at[q], g2_v.at[q], g2send.at[q], g2recv.at[q], {"dp": q * 2 + c})

        for q in range(xs):
            for part in range(2):
                loads[q][part].wait()
                g1(q, part).wait_recv()

            def fold(s, _):
                mine_v[q, s] = (mine_v[q, s].astype(F32) + g1_v[q, s].astype(F32)).astype(BF16)
                return 0
            lax.fori_loop(0, chunks, fold, 0)

            @pl.when(q != x)
            def _():
                g2(q).start()

        def columns(part, s):
            return pl.ds(pl.multiple_of(part * inner + s * width, width), width)

        def g3(s, part):
            return remote(t_v.at[s, :, pl.ds(part * width, width)], fin_v.at[:, columns(part, me)], g3send.at[s, part], g3recv.at[me, part], {"seq": s})

        def g3_from(s, part):
            return remote(fin_v.at[:, columns(part, s)], fin_v.at[:, columns(part, s)], g3send.at[s, part], g3recv.at[s, part], {"seq": s})

        def every_other(fn):
            def one(k, _):
                fn(lax.rem(me + k, chunks))
                return 0
            lax.fori_loop(1, chunks, one, 0)

        def third():
            for q in range(xs):
                @pl.when(q != x)
                def _():
                    g2_from(q).wait_recv()

            def fold(s, _):
                total = mine_v[x, s].astype(F32)
                for q in range(1, xs):
                    total = total + g2_v[lax.rem(x + q, xs), s].astype(F32)
                t_v[s] = total.astype(BF16)
                return 0
            lax.fori_loop(0, chunks, fold, 0)
            for part in range(2):
                every_other(lambda s: g3(s, part).start())
                fin_v[:, columns(part, me)] = t_v[me, :, part * width:(part + 1) * width]

        def rows_of(d):
            return pl.ds(pl.multiple_of(d * piece, piece), piece)

        def g4(d_src, k, d):
            src = fin_v if d_src is None else all_ref.at[rows_of(d_src)]
            row = mine if d_src is None else d_src
            return remote(src, all_ref.at[rows_of(row)], g4send.at[k], g4recv.at[row], {"dp": d})

        def g4_from(d):
            return remote(all_ref.at[rows_of(d)], all_ref.at[rows_of(d)], g4send.at[0], g4recv.at[d], {"dp": d})

        keep = pltpu.make_async_copy(fin_v, all_ref.at[rows_of(mine)], load_sem.at[0])

        def fourth():
            for part in range(2):
                every_other(lambda s: g3_from(s, part).wait_recv())
            for j in range(1, xs):
                g4(None, j, lax.rem(x + j, xs) * 2 + c).start()
            g4(None, 0, x * 2 + 1 - c).start()
            keep.start()

    def arrived(i, j, h):
        rows = pl.ds(h * half, half)
        k = i * (ys - 1) + j - 1
        return remote(yrecv_v.at[k, rows], yrecv_v.at[k, rows], ysend.at[k, h], yrecv.at[k, h], {"seq": z * ys + lax.rem(y + j, ys)})

    def climb(t, h):
        rows = pl.ds(h * half, half)
        return remote(own_v.at[t, rows], zrecv_v.at[t, rows], zup.at[t, h], zrecv.at[t, h], {"seq": (z + 1) * ys + y})

    def sink(t, h):
        rows = pl.ds(h * half, half)
        slot = jnp.where(t == z - 1, zs, t)
        return remote(own_v.at[t, rows], zrecv_v.at[slot, rows], zdown.at[t, h], zrecv.at[slot, h], {"seq": (z - 1) * ys + y})

    def from_z(slot, h):
        rows = pl.ds(h * half, half)
        return remote(zrecv_v.at[slot, rows], zrecv_v.at[slot, rows], zup.at[0, h], zrecv.at[slot, h], {"seq": lax.rem(me + 1, chunks)})

    def accumulate(t, h, read):
        def one(r, _):
            sl = pl.ds(pl.multiple_of(h * half + r * 32, 32), 32)
            own_v[t, sl, :] = (own_v[t, sl, :].astype(F32) + read(sl)).astype(BF16)
            return 0
        lax.fori_loop(0, half // 32, one, 0)

    for i in range(zs):
        t = dest(i)
        partial(t * ys + y, own_v, t)
        for h in range(2):
            for j in range(1, ys):
                arrived(i, ys - j, h).wait_recv()

            def side_sum(sl):
                total = yrecv_v[i * (ys - 1), sl, :].astype(F32)
                for j in range(2, ys):
                    total = total + yrecv_v[i * (ys - 1) + j - 1, sl, :].astype(F32)
                return total

            if h == 0 and i + ahead < zs:
                for j in range(1, ys):
                    for g in range(2):
                        to_side(i + ahead, j, g).start()
            if ys > 1:
                accumulate(t, h, side_sum)

            @pl.when(((t > z) & (z > 0)) | ((t == z) & (z > 0)))
            def _():
                from_z(t, h).wait_recv()
                accumulate(t, h, lambda sl: zrecv_v[t, sl, :].astype(F32))

            @pl.when((t < z) & (z + 1 < zs))
            def _():
                from_z(t, h).wait_recv()
                accumulate(t, h, lambda sl: zrecv_v[t, sl, :].astype(F32))

            @pl.when((t == z) & (z + 1 < zs))
            def _():
                from_z(zs, h).wait_recv()
                accumulate(t, h, lambda sl: zrecv_v[zs, sl, :].astype(F32))

            @pl.when(t > z)
            def _():
                climb(t, h).start()

            @pl.when(t < z)
            def _():
                sink(t, h).start()
        if split and i == 0:
            third()
        if split and i == max(0, zs - 2):
            fourth()

    red_ref[...] = own_v[z]
    every_copy(lambda d: late_from(d).wait_recv())
    total = late_ref[...]
    for k in range(1, copies):
        total = total + late_v[lax.rem(mine + k, copies)]
    sum_ref[...] = total
    if split:
        for j in range(1, xs):
            d = lax.rem(x + j, xs) * 2 + c
            g4_from(d).wait_recv()
            g4(d, xs - 1 + j, x * 2 + 1 - c).start()
        keep.wait()
        for j in range(xs):
            g4_from(lax.rem(x + j, xs) * 2 + 1 - c).wait_recv()

    every_copy(lambda d: late_to(d).wait_send())
    count = zs * (ys - 1)
    for k in range(max(0, count - slots), count):
        for h in range(2):
            to_side(k // (ys - 1), k % (ys - 1) + 1, h).wait_send()
    for i in range(zs):
        t = dest(i)
        for h in range(2):
            @pl.when(t > z)
            def _():
                climb(t, h).wait_send()

            @pl.when(t < z)
            def _():
                sink(t, h).wait_send()
    if split:
        for q in range(xs):
            for part in range(2):
                g1(q, part).wait_send()

            @pl.when(q != x)
            def _():
                g2(q).wait_send()
        for part in range(2):
            every_other(lambda s: g3(s, part).wait_send())
        for j in range(xs):
            g4(None, j, mine).wait_send()
        for j in range(1, xs):
            g4(lax.rem(x + j, xs) * 2 + c, xs - 1 + j, mine).wait_send()


def scatter_sums(gc, gg, w_all, late, ginc, ging, chunks, copies, split):
    tokens, width = gc.shape[1:]
    model = w_all.shape[0]
    zs, ys = grid_of(chunks, copies)
    xs = max(1, copies // 2)
    others = max(1, zs * (ys - 1))
    slots = min(others, 4)
    any_spec = pl.BlockSpec(memory_space=pl.ANY)
    vmem = pl.BlockSpec(memory_space=pltpu.VMEM)
    sds = jax.ShapeDtypeStruct
    dma = pltpu.SemaphoreType.DMA
    args = [gc, gg, w_all, late]
    in_specs = [vmem, vmem, any_spec, vmem]
    out_specs = [vmem, vmem]
    out_shape = [sds((tokens, model), BF16), sds(late.shape, F32)]
    scratch = [pltpu.VMEM((slots, tokens, model), BF16), pltpu.VMEM((others, tokens, model), BF16),
               pltpu.VMEM((zs, tokens, model), BF16), pltpu.VMEM((zs + 1, tokens, model), BF16),
               pltpu.VMEM((copies,) + late.shape, F32), pltpu.VMEM(w_all.shape, BF16)]
    sems = [dma((1 + 2 * xs,)), dma((others, 2)), dma((others, 2)), dma((zs, 2)), dma((zs, 2)), dma((zs + 1, 2)), dma((copies,)), dma((copies,))]
    if split:
        piece = ginc.shape[2]
        slab = (xs, chunks, piece, 2 * width)
        args += [ginc, ging]
        in_specs += [any_spec] * 2
        out_specs.append(any_spec)
        out_shape.append(sds((copies * piece, 2 * chunks * width), BF16))
        scratch += [pltpu.VMEM(slab, BF16), pltpu.VMEM(slab, BF16), pltpu.VMEM(slab, BF16), pltpu.VMEM(slab[1:], BF16),
                    pltpu.VMEM((piece, 2 * chunks * width), BF16)]
        sems += [dma((xs, 2)), dma((xs, 2)), dma((xs,)), dma((xs,)), dma((chunks, 2)), dma((chunks, 2)), dma((2 * xs,)), dma((copies,))]
    return pl.pallas_call(
        functools.partial(scatter_kernel, chunks=chunks, copies=copies, split=split),
        in_specs=in_specs,
        out_specs=out_specs,
        out_shape=out_shape,
        scratch_shapes=scratch + sems,
        compiler_params=pltpu.CompilerParams(collective_id=3, has_side_effects=True, vmem_limit_bytes=62 * 1024 * 1024),
        name="scatter_sums",
    )(*args)
from jax.sharding import PartitionSpec as P


def local(hidden, grad_out, lengths, norm_gain, input_weight, conv_weight, conv_bias, select_weight,
          step_weight, step_bias, decay_log, skip_weight, output_weight):
    rows, length, model = hidden.shape
    chunks = lax.axis_size("seq")
    copies = lax.axis_size("dp")
    width = output_weight.shape[0]
    share = input_weight.shape[0]
    rank = step_weight.shape[0]
    n = decay_log.shape[0]
    tokens = chunks * rows * length
    here = lax.axis_index("seq")

    split = (share // copies) % 16 == 0 and copies % 2 == 0
    normed, ci, gate, w_all, gain_row = gather_project(
        hidden.reshape(rows * length, model), input_weight, norm_gain.astype(F32).reshape(1, share), chunks, copies, share, split)
    normed = normed.reshape(tokens, model)
    slots = here * length + lax.broadcasted_iota(jnp.int32, (rows, length), 1)
    valid = (slots < lengths[:, None]).astype(F32)[..., None]
    cotangent = grad_out.astype(F32) * valid
    shaped = lambda a: a.reshape(chunks, rows, length, a.shape[-1])
    ci, gate = shaped(ci), shaped(gate)
    bias_row = conv_bias.reshape(1, width)
    step_row = step_bias.reshape(1, width)
    skip_row = skip_weight.reshape(1, width)
    gm, sel, x, gated, gact, tail, dt, slope, starts = forward(
        ci, gate, cotangent.astype(BF16).reshape(rows * length, model), conv_weight, bias_row, select_weight,
        step_weight, step_row, decay_log, skip_row, copies, n)
    gm = gm.reshape(tokens, model)
    gated2 = gated.reshape(tokens, width)
    mixed = jnp.dot(gated2, output_weight, preferred_element_type=F32).astype(BF16)
    mixed = lax.psum_scatter(shaped(mixed), "seq", scatter_dimension=0, tiled=False)
    source = hidden.astype(F32)
    output = ((source + mixed.astype(F32)) * valid).astype(BF16)

    gg = shaped(lax.dot_general(gm, output_weight, (((1,), (1,)), ((), ())), preferred_element_type=F32))
    ggate, gvals, gpre, gpart, gstepw, gstepb, gdecay, gskip = scan_backward(
        sel, x, gact, gg, tail, starts, dt, slope, step_weight, decay_log, skip_row, n)
    tn = lambda a, b: lax.dot_general(a, b, (((0,), (0,)), ((), ())), preferred_element_type=F32)
    gout = tn(gated2, gm).astype(BF16)
    small = jnp.concatenate([gstepw, gdecay, gstepb, gskip], axis=0).astype(BF16)
    small = jnp.pad(small, ((0, -small.shape[0] % 32), (0, 0)))
    gsel, gout, small = total_over_seq(gpart, chunks, copies, 2, (gout, small))
    gout, small = gout.astype(F32), small.astype(F32)
    gstepw, gdecay, gstepb, gskip = small[:rank], small[rank:rank + n], small[rank + n], small[rank + n + 1]
    gci, gtaps, gconvb, gselw = conv_backward(ci, gvals, gsel, conv_weight, bias_row, select_weight)
    tap_count = gtaps.shape[0]
    gci2 = gci.reshape(tokens, width)
    ggate2 = ggate.reshape(tokens, width)
    ginc, ging = (tn(normed, g).astype(BF16).reshape(chunks, copies, share // copies, width) for g in (gci2, ggate2))
    late = jnp.concatenate([gselw, gtaps, gconvb], axis=0)
    late = jnp.pad(late, ((0, -late.shape[0] % 8), (0, 0)))
    flat = lambda a: a.reshape(chunks, rows * length, width)
    got = scatter_sums(flat(gci), flat(ggate), w_all, late, ginc, ging, chunks, copies, split)
    scaled, late = got[:2]
    if split:
        gin = got[2].astype(F32)
    else:
        gin = jnp.stack([ginc, ging], axis=3)
        gin = lax.psum_scatter(gin, "dp", scatter_dimension=1, tiled=False)
        gin = lax.all_to_all(gin, "seq", split_axis=0, concat_axis=2, tiled=False)
        gin = lax.all_gather(gin.reshape(share // copies, 2 * chunks * width), "dp", axis=0, tiled=True).astype(F32)
    ggain = jnp.sum(gin * input_weight.astype(F32), axis=1) / norm_gain.astype(F32)
    scaled = scaled.reshape(rows, length, model).astype(F32) * gain_row
    inverse = lax.rsqrt(jnp.mean(source * source, axis=-1, keepdims=True) + EPSILON)
    ghidden = inverse * scaled - source * inverse ** 3 * jnp.mean(scaled * source, axis=-1, keepdims=True) + cotangent
    picked = gselw.shape[0]
    gselw, gtaps, gconvb = late[:picked], late[picked:picked + tap_count], late[picked + tap_count]
    return (output, ghidden, ggain, gin, gtaps, gconvb, gselw, gstepw, gstepb,
            gdecay, gskip, gout)


def solution(mesh):
    tok, vec, col, row = P("dp", "seq", None), P("seq"), P(None, "seq"), P("seq", None)
    return jax.shard_map(
        local,
        mesh=mesh,
        in_specs=(tok, tok, P("dp"), vec, row, col, vec, col, col, vec, col, vec, row),
        out_specs=(tok, tok, vec, row, col, vec, col, col, vec, col, vec, row),
        check_vma=False,
    )
```

```python
import functools
import jax
import jax.numpy as jnp
from jax import lax
from jax.experimental import pallas as pl
from jax.experimental.pallas import tpu as pltpu

BLOCK = 16
EPSILON = 1e-05
LOG2E = 1.4426950408889634
F32 = jnp.float32
BF16 = jnp.bfloat16


def inverse_of(whole):
    guess = pl.reciprocal(whole, approx=True)
    return guess * (2.0 - whole * guess)


def gates_of(pre):
    small = jnp.exp2(jnp.abs(pre) * -LOG2E)
    whole = 1.0 + small
    log_part = jnp.where(small < 1e-3, small * (1.0 - small * (0.5 - small * (1.0 / 3.0))), jnp.log(whole))
    return jnp.maximum(pre, 0.0) + log_part, jnp.where(pre >= 0.0, 1.0, small) * inverse_of(whole)


def sigmoid(v):
    return 0.5 + 0.5 * jnp.tanh(0.5 * v)


def nt_dot(a, b):
    return lax.dot_general(a, b, (((1,), (1,)), ((), ())), preferred_element_type=F32)


def lane_tiles(width):
    step = min(width, 512)
    return [slice(k, k + step) for k in range(0, width, step)]


def tile_matrix(n, wide):
    col = lax.broadcasted_iota(jnp.int32, (n, wide), 1)
    row = lax.broadcasted_iota(jnp.int32, (n, wide), 0)
    return (col % n == row).astype(F32)


def diagonal_mask(rows, n, wide):
    col = lax.broadcasted_iota(jnp.int32, (rows, wide), 1)
    row = lax.broadcasted_iota(jnp.int32, (rows, wide), 0)
    return col // n == row % BLOCK


def scan_step(selected, x, gate, fresh, stepw_ref, bias_ref, skip_ref, gated_ref, gact_ref, tail_ref, dt_ref, slope_ref,
              u_s, y_s, coef_s, bt_s, hist_a, hist_b, state_s, rate_s, rank, n):
    length = x.shape[0]
    wide = BLOCK * n
    state_s[...] = jnp.where(fresh, 0.0, state_s[...])
    low = selected[:rank].T.astype(BF16)
    pre = jnp.dot(low, stepw_ref[...], preferred_element_type=F32) + bias_ref[...]
    dt, slope = gates_of(pre)
    dt_ref[...] = dt
    slope_ref[...] = slope
    u_s[...] = dt * x
    bt_s[...] = selected[rank:]
    spread = jnp.dot(selected[rank:].T[:, n:], tile_matrix(n, wide), preferred_element_type=F32)
    coef_s[...] = jnp.where(diagonal_mask(length, n, wide), spread, 0.0).astype(BF16)
    blocks = length // BLOCK

    def finish(k, hist):
        rows = pl.ds(pl.multiple_of(k * BLOCK, BLOCK), BLOCK)
        y_s[rows, :] = jnp.dot(coef_s[rows, :], hist[...], preferred_element_type=F32)

    def block(k, state, hist):
        at = pl.multiple_of(k * BLOCK, BLOCK)
        bs = pltpu.roll(bt_s[0:n, :], length - at, 1)
        dts = dt_ref[pl.ds(at, BLOCK), :]
        us = u_s[pl.ds(at, BLOCK), :]
        rate = rate_s[...]
        for i in range(BLOCK):
            factor = jnp.exp2(dts[i:i + 1, :] * rate)
            state = factor * state + us[i:i + 1, :] * bs[:, i:i + 1]
            hist[i * n:(i + 1) * n, :] = state.astype(BF16)
        return state

    def pair(j, state):
        finish(jnp.maximum(2 * j - 1, 0), hist_b)
        state = block(2 * j, state, hist_a)
        finish(2 * j, hist_a)
        return block(2 * j + 1, state, hist_b)

    state_s[...] = lax.fori_loop(0, blocks // 2, pair, state_s[...])
    finish(blocks - 1, hist_b)
    ssm = y_s[...] + skip_ref[...] * x
    sg = sigmoid(gate)
    gact = gate * sg
    gact_ref[...] = gact
    tail_ref[...] = (ssm * sg * (1.0 + gate * (1.0 - sg))).astype(BF16)
    gated_ref[...] = (ssm * gact).astype(BF16)


def back_step(selected, x, fresh, gact_ref, gg_ref, tail_ref, start_ref, dt_ref, slope_ref, stepw_ref, skip_ref,
              ggate_ref, gvals_ref, gsel_ref, gstepw_ref, gbias_ref, gskip_ref,
              u_s, gy_s, gu_s, ah_s, bcoef_s, bt_s, hist_s, adj_a, harm_a, adj_b, harm_b, db_s, dc_s, carry_s, gd_s, rate_s, factor_s, kept_s, rank, n):
    length = x.shape[0]
    wide = BLOCK * n
    blocks = length // BLOCK
    carry_s[...] = jnp.where(fresh, 0.0, carry_s[...])
    gg = gg_ref[...]
    gy = gg * gact_ref[...]
    ggate_ref[...] = (gg * tail_ref[...].astype(F32)).astype(BF16)
    gskip_ref[...] += jnp.sum(gy * x, axis=0, keepdims=True)
    gy_s[...] = gy
    dt = dt_ref[...]
    u_s[...] = dt * x
    bt_s[...] = selected[rank:]
    tiles = tile_matrix(n, wide)
    spread = jnp.dot(selected[rank:].T[:, :n], tiles, preferred_element_type=F32)
    bcoef_s[...] = jnp.where(diagonal_mask(length, n, wide), spread, 0.0).astype(BF16)
    keep = diagonal_mask(BLOCK, n, wide)
    ones = keep.astype(BF16)
    lanes = lane_tiles(x.shape[1])
    state_s = start_ref

    def steps(lane):
        def again(k, state):
            at = pl.multiple_of(k * BLOCK, BLOCK)
            bs = pltpu.roll(bt_s[0:n, :], length - at, 1)
            dts = dt_ref[pl.ds(at, BLOCK), lane]
            us = u_s[pl.ds(at, BLOCK), lane]
            rate = rate_s[:, lane]
            for i in range(BLOCK):
                here = pl.ds(pl.multiple_of((at + i) * n, n), n)
                factor = jnp.exp2(dts[i:i + 1, :] * rate)
                factor_s[here, lane] = factor
                old = factor * state
                kept_s[here, lane] = old
                state = old + us[i:i + 1, :] * bs[:, i:i + 1]
                hist_s[here, lane] = state.astype(BF16)
            return state

        lax.fori_loop(0, blocks, again, state_s[:, lane])

        def products(k, adj_s, harm_s):
            at = pl.multiple_of(k * BLOCK, BLOCK)
            rows = pl.ds(at, BLOCK)
            adj = adj_s[:, lane]
            gu_s[rows, lane] = jnp.dot(bcoef_s[rows, :], adj, preferred_element_type=F32)
            ah_s[rows, lane] = jnp.dot(ones, harm_s[:, lane], preferred_element_type=F32)
            db = jnp.where(keep, nt_dot(u_s[rows, lane].astype(BF16), adj), 0.0)
            states = hist_s[pl.ds(pl.multiple_of(at * n, n), wide), lane]
            dc = jnp.where(keep, nt_dot(gy_s[rows, lane].astype(BF16), states), 0.0)
            if lane.start == 0:
                db_s[rows, :] = db
                dc_s[rows, :] = dc
            else:
                db_s[rows, :] += db
                dc_s[rows, :] += dc

        def block(k, carry, adj_s, harm_s):
            at = pl.multiple_of(k * BLOCK, BLOCK)
            cs = pltpu.roll(bt_s[n:2 * n, :], length - at, 1)
            dts = dt_ref[pl.ds(at, BLOCK), lane]
            gys = gy_s[pl.ds(at, BLOCK), lane]
            rate = rate_s[:, lane]
            gd = gd_s[:, lane]
            for i in range(BLOCK - 1, -1, -1):
                here = pl.ds(pl.multiple_of((at + i) * n, n), n)
                g = cs[:, i:i + 1] * gys[i:i + 1, :] + carry
                adj_s[i * n:(i + 1) * n, lane] = g.astype(BF16)
                carry = factor_s[here, lane] * g
                h = g * kept_s[here, lane]
                harm_s[i * n:(i + 1) * n, lane] = (h * rate).astype(BF16)
                gd = gd + dts[i:i + 1, :] * h
            gd_s[:, lane] = gd
            return carry

        def pair(j, carry):
            k = blocks - 1 - 2 * j
            if lane.start == 0:
                products(jnp.minimum(k + 1, blocks - 1), adj_b, harm_b)
            else:
                @pl.when(j > 0)
                def _():
                    products(k + 1, adj_b, harm_b)
            carry = block(k, carry, adj_a, harm_a)
            products(k, adj_a, harm_a)
            return block(k - 1, carry, adj_b, harm_b)

        carry_s[:, lane] = lax.fori_loop(0, blocks // 2, pair, carry_s[:, lane])
        products(0, adj_b, harm_b)

    for lane in lanes:
        steps(lane)
    gu = gu_s[...]
    gpre = ((x * gu + ah_s[...] * (1.0 / LOG2E)) * slope_ref[...]).astype(BF16)
    gvals_ref[...] = (gy * skip_ref[...] + dt * gu).astype(gvals_ref.dtype)
    gbias_ref[...] += jnp.sum(gpre.astype(F32), axis=0, keepdims=True)
    gstepw_ref[...] += jnp.dot(selected[:rank].astype(BF16), gpre, preferred_element_type=F32)
    fold = lambda ref: nt_dot(tiles.astype(BF16), ref[...].astype(BF16))
    gsel_ref[0:rank, :] = nt_dot(stepw_ref[...], gpre).astype(BF16)
    gsel_ref[rank:rank + n, :] = fold(db_s).astype(BF16)
    gsel_ref[rank + n:rank + 2 * n, :] = fold(dc_s).astype(BF16)


def conv_step(ci, fresh, taps_ref, bias_ref, selw_ref, ext_s):
    length = ci.shape[0]
    tap_count = taps_ref.shape[0]
    ext_s[0:8, :] = jnp.where(fresh, 0.0, ext_s[length:length + 8, :])
    ext_s[8:, :] = ci.astype(F32)
    total = bias_ref[...].astype(F32)
    for k in range(tap_count):
        total = total + taps_ref[k:k + 1, :].astype(F32) * ext_s[pl.ds(8 - tap_count + 1 + k, length), :]
    x = (total * sigmoid(total)).astype(BF16)
    return x, nt_dot(selw_ref[...], x).astype(BF16)


def conv_back_step(ci_ref, prev_ref, first, fresh, gvals_ref, gsel_ref, taps_ref, bias_ref, selw_ref,
                   gci_ref, gtaps_ref, gbias_ref, gselw_ref, ext_s, gext_s):
    length = ci_ref.shape[0]
    tap_count = taps_ref.shape[0]
    gext_s[length:, :] = jnp.where(fresh, 0.0, gext_s[length:, :])
    ext_s[8:, :] = ci_ref[...].astype(F32)
    before = prev_ref[...][length - 16:, :].astype(F32)[8:, :]
    ext_s[0:8, :] = jnp.where(first, 0.0, before)
    total = bias_ref[...].astype(F32)
    for k in range(tap_count):
        total = total + taps_ref[k:k + 1, :].astype(F32) * ext_s[pl.ds(8 - tap_count + 1 + k, length), :]
    sg = sigmoid(total)
    x = (total * sg).astype(BF16)
    gsel = gsel_ref[...]
    gvals = gvals_ref[...] + jnp.dot(gsel.astype(F32).T.astype(BF16), selw_ref[...], preferred_element_type=F32)
    gconv = gvals * sg * (1.0 + total * (1.0 - sg))
    gbias_ref[...] += jnp.sum(gconv, axis=0, keepdims=True)
    for k in range(tap_count):
        gtaps_ref[k:k + 1, :] += jnp.sum(gconv * ext_s[pl.ds(8 - tap_count + 1 + k, length), :], axis=0, keepdims=True)
    gselw_ref[...] += jnp.dot(gsel, x, preferred_element_type=F32)
    gext_s[0:length, :] = gconv
    gci = jnp.zeros_like(gconv)
    for k in range(tap_count):
        gci = gci + taps_ref[k:k + 1, :].astype(F32) * gext_s[pl.ds(tap_count - 1 - k, length), :]
    gci_ref[...] = gci.astype(BF16)
    gext_s[length:, :] = gconv[0:8, :]


MESH = pl.DeviceIdType.MESH


def remote(src, dst, send, recv, device):
    return pltpu.make_async_remote_copy(src_ref=src, dst_ref=dst, send_sem=send, recv_sem=recv, device_id=device, device_id_type=MESH)


def grid_of(chunks, copies):
    deep = max(1, copies // 2)
    return (chunks // deep, deep) if chunks % deep == 0 else (chunks, 1)


def meet(chunks, copies):
    me, mine = lax.axis_index("seq"), lax.axis_index("dp")
    barrier = pltpu.get_barrier_semaphore()

    def greet(k, _):
        pl.semaphore_signal(barrier, inc=1, device_id={"seq": lax.rem(me + k, chunks)}, device_id_type=MESH)
        return 0

    def greet_copy(k, _):
        pl.semaphore_signal(barrier, inc=1, device_id={"dp": lax.rem(mine + k, copies)}, device_id_type=MESH)
        return 0

    lax.fori_loop(1, chunks, greet, 0)
    if copies > 1:
        lax.fori_loop(1, copies, greet_copy, 0)
    pl.semaphore_wait(barrier, chunks - 1 + max(copies - 1, 0))


def gather_project_kernel(hid_ref, wq_ref, gain_ref, n_ref, ci_ref, gate_ref, w_ref, row_ref,
                          hid_v, gain_v, w_v, n_v, ci_v, gate_v,
                          load_sem, out_sem, hrecv, hside, hup, hdown, hlend,
                          w1send, w1recv, w2recv, w2send, w3send, gsend, grecv, *, chunks, copies, share, split):
    zs, ys = grid_of(chunks, copies)
    xs = copies // 2
    me, mine = lax.axis_index("seq"), lax.axis_index("dp")
    z, y = me // ys, me % ys
    x, c = mine // 2, mine % 2
    tokens, model = hid_v.shape[1:]
    width = ci_v.shape[1]
    inner = chunks * width
    half = tokens // 2
    even = ys == 2 and zs % 2 == 0
    piece = share // (copies if split else 1)
    spot = mine if split else 0
    load = pltpu.make_async_copy(hid_ref, hid_v.at[me], load_sem)
    load.start()
    meet(chunks, copies)
    load.wait()

    def w_rows(s, d):
        return pl.ds(pl.multiple_of(s * share + d * piece, piece), piece)

    def w_first(s, part):
        src = wq_ref.at[pl.ds(pl.multiple_of(spot * piece, piece), piece), pl.ds(pl.multiple_of(part * inner + s * width, width), width)]
        return remote(src, w_v.at[w_rows(me, spot), pl.ds(part * width, width)], w1send.at[s, part], w1recv.at[me, part], {"seq": s})

    def w_landed(s, part):
        dst = w_v.at[w_rows(s, spot), pl.ds(part * width, width)]
        return remote(dst, dst, w1send.at[s, part], w1recv.at[s, part], {"seq": s})

    def w_own(part):
        src = wq_ref.at[pl.ds(pl.multiple_of(spot * piece, piece), piece), pl.ds(pl.multiple_of(part * inner + me * width, width), width)]
        return pltpu.make_async_copy(src, w_v.at[w_rows(me, spot), pl.ds(part * width, width)], out_sem.at[part])

    def every_other(fn):
        def one(k, _):
            fn(lax.rem(me + k, chunks))
            return 0
        lax.fori_loop(1, chunks, one, 0)

    def gain_to(s):
        return remote(gain_ref, gain_v.at[me], gsend.at[s], grecv.at[me], {"seq": s})

    def gain_from(s):
        return remote(gain_v.at[s], gain_v.at[s], gsend.at[s], grecv.at[s], {"seq": s})

    def send_first(s):
        gain_to(s).start()
        w_first(s, 0).start()
        w_first(s, 1).start()

    def block(o, yy, h):
        return hid_v.at[o * ys + yy, pl.ds(h * half, half)]

    def up(o, h):
        return remote(block(o, y, h), block(o, y, h), hup.at[o, h], hrecv.at[o * ys + y, h], {"seq": (z + 1) * ys + y})

    def down(o, h):
        return remote(block(o, y, h), block(o, y, h), hdown.at[o, h], hrecv.at[o * ys + y, h], {"seq": (z - 1) * ys + y})

    def side(o, j, h):
        other = lax.rem(y + j, ys)
        return remote(block(o, y, h), block(o, y, h), hside.at[o, j - 1, h], hrecv.at[o * ys + y, h], {"seq": z * ys + other})

    def landed(o, yy, h):
        return remote(block(o, yy, h), block(o, yy, h), hside.at[o, 0, h], hrecv.at[o * ys + yy, h], {"seq": lax.rem(me + 1, chunks)})

    def when(cond, fn):
        pl.when(cond)(fn)

    gain_own = pltpu.make_async_copy(gain_ref, gain_v.at[me], out_sem.at[2])
    gain_own.start()
    for part in range(2):
        w_own(part).start()
    for h in range(2):
        when(z + 1 < zs, lambda: up(z, h).start())
        when(z > 0, lambda: down(z, h).start())
        for j in range(1, ys):
            side(z, j, h).start()
    every_other(send_first)

    partner = z + 1 - 2 * (z % 2)

    def sides(o, h, act):
        if even and h == 1:
            when(o != partner, lambda: act(side(o, 1, h)))
        else:
            for j in range(1, ys):
                act(side(o, j, h))

    def lend():
        return remote(block(z, 1 - y, 1), block(z, 1 - y, 1), hlend, hrecv.at[z * ys + 1 - y, 1], {"seq": partner * ys + y})

    def lend_on():
        if even:
            landed(z, 1 - y, 1).wait_recv()
            lend().start()

    def relay(k):
        for h in range(2):
            @pl.when(z - k >= 0)
            def _():
                landed(z - k, y, h).wait_recv()
                when(z + 1 < zs, lambda: up(z - k, h).start())
                sides(z - k, h, lambda one: one.start())

            @pl.when(z + k < zs)
            def _():
                landed(z + k, y, h).wait_recv()
                when(z > 0, lambda: down(z + k, h).start())
                sides(z + k, h, lambda one: one.start())

    def shared(s, d, sems, k, device):
        return remote(w_v.at[w_rows(s, d)], w_v.at[w_rows(s, d)], sems.at[s, k], w2recv.at[s, d], device)

    def spread(s):
        for j in range(1, xs):
            shared(s, mine, w2send, j - 1, {"dp": lax.rem(x + j, xs) * 2 + c}).start()
        shared(s, mine, w3send, 0, {"dp": x * 2 + 1 - c}).start()

    gain_own.wait()
    for part in range(2):
        w_own(part).wait()
    if split:
        spread(me)

    def take_first(s):
        gain_from(s).wait_recv()
        for part in range(2):
            w_landed(s, part).wait_recv()
        if split:
            spread(s)

    if zs > 1:
        relay(1)
    every_other(take_first)

    def take_second(s, _):
        for j in range(1, xs):
            d = lax.rem(x + j, xs) * 2 + c
            shared(s, d, w2send, j - 1, {"dp": d}).wait_recv()
            shared(s, d, w3send, j, {"dp": x * 2 + 1 - c}).start()
        return 0

    def take_third(s, _):
        for j in range(xs):
            d = lax.rem(x + j, xs) * 2 + 1 - c
            shared(s, d, w2send, 0, {"dp": d}).wait_recv()
        return 0

    if zs > 2:
        relay(2)
    lend_on()
    if split:
        lax.fori_loop(0, chunks, take_second, 0)
    if split:
        lax.fori_loop(0, chunks, take_third, 0)

    row_ref[...] = jnp.concatenate([gain_v[s] for s in range(chunks)], axis=-1)
    w_out = pltpu.make_async_copy(w_v, w_ref, load_sem)
    w_out.start()
    steps = 4 if width >= 512 else 1
    tile = 2 * width // steps

    def project(at):
        def rows(i, _):
            sl = pl.ds(pl.multiple_of(i * 32, 32), 32)
            h = hid_v[at, sl, :].astype(F32)
            inverse = lax.rsqrt(jnp.mean(h * h, axis=-1, keepdims=True) + EPSILON)
            n_v[sl, :] = (h * inverse * row_ref[...]).astype(BF16)
            return 0
        lax.fori_loop(0, tokens // 32, rows, 0)
        n_out = pltpu.make_async_copy(n_v, n_ref.at[at], out_sem.at[0])
        n_out.start()

        def columns(i, _):
            sl = pl.ds(pl.multiple_of(i * tile, tile), tile)
            got = jnp.dot(n_v[...], w_v[:, sl], preferred_element_type=F32)
            if steps == 1:
                ci_v[...] = got[:, :width].astype(BF16)
                gate_v[...] = got[:, width:]
            else:
                @pl.when(i < steps // 2)
                def _():
                    ci_v[:, sl] = got.astype(BF16)

                @pl.when(i >= steps // 2)
                def _():
                    gate_v[:, pl.ds(pl.multiple_of(i * tile - width, tile), tile)] = got
            return 0
        lax.fori_loop(0, steps, columns, 0)
        ci_out = pltpu.make_async_copy(ci_v, ci_ref.at[at], out_sem.at[1])
        gate_out = pltpu.make_async_copy(gate_v, gate_ref.at[at], out_sem.at[2])
        ci_out.start()
        gate_out.start()
        n_out.wait()
        ci_out.wait()
        gate_out.wait()

    def work(first, last):
        def one(i, _):
            k0, j = i // (2 * ys), i % (2 * ys)
            lower, yy = j // ys, j % ys
            own = yy == y
            k = k0 - jnp.where(own, 0, 1)
            o = z + k * (2 * lower - 1)
            ok = (k >= 0) & (k < zs) & (o >= 0) & (o < zs) & ((lower == 0) | (k > 0))

            @pl.when(ok & jnp.logical_not(own))
            def _():
                landed(o, yy, 0).wait_recv()
                if even:
                    when(o != z, lambda: landed(o, yy, 1).wait_recv())
                else:
                    landed(o, yy, 1).wait_recv()

            @pl.when(ok)
            def _():
                project(o * ys + yy)
            return 0
        lax.fori_loop(first * 2 * ys, last * 2 * ys, one, 0)

    work(0, min(3, zs))

    def later(k, _):
        relay(k)
        work(k, k + 1)
        return 0

    lax.fori_loop(3, zs, later, 0)
    work(zs, zs + 1)
    w_out.wait()

    def drain_first(s):
        gain_to(s).wait_send()
        for part in range(2):
            w_first(s, part).wait_send()

    every_other(drain_first)

    def drain_second(s, _):
        for j in range(1, xs):
            shared(s, mine, w2send, j - 1, {"dp": mine}).wait_send()
        for j in range(xs):
            shared(s, mine, w3send, j, {"dp": mine}).wait_send()
        return 0

    if split:
        lax.fori_loop(0, chunks, drain_second, 0)

    def drain(k, _):
        for h in range(2):
            @pl.when(z - k >= 0)
            def _():
                when(z + 1 < zs, lambda: up(z - k, h).wait_send())
                sides(z - k, h, lambda one: one.wait_send())

            @pl.when((z + k < zs) & (k > 0))
            def _():
                when(z > 0, lambda: down(z + k, h).wait_send())
                sides(z + k, h, lambda one: one.wait_send())
        return 0

    lax.fori_loop(0, zs, drain, 0)
    for h in range(2):
        when(z > 0, lambda: down(z, h).wait_send())
    if even:
        lend().wait_send()


def gather_project(hidden, wq, gain, chunks, copies, share, split):
    tokens, model = hidden.shape
    width = wq.shape[1] // 2 // chunks
    zs, ys = grid_of(chunks, copies)
    any_spec = pl.BlockSpec(memory_space=pl.ANY)
    sds = jax.ShapeDtypeStruct
    dma = pltpu.SemaphoreType.DMA
    return pl.pallas_call(
        functools.partial(gather_project_kernel, chunks=chunks, copies=copies, share=share, split=split),
        in_specs=[any_spec] * 3,
        out_specs=[any_spec] * 4 + [pl.BlockSpec(memory_space=pltpu.VMEM)],
        out_shape=[sds((chunks, tokens, model), BF16), sds((chunks, tokens, width), BF16),
                   sds((chunks, tokens, width), F32), sds((model, 2 * width), BF16), sds((1, model), F32)],
        scratch_shapes=[
            pltpu.VMEM((chunks, tokens, model), BF16), pltpu.VMEM((chunks, 1, share), F32), pltpu.VMEM((model, 2 * width), BF16),
            pltpu.VMEM((tokens, model), BF16), pltpu.VMEM((tokens, width), BF16), pltpu.VMEM((tokens, width), F32),
            dma(()), dma((3,)), dma((chunks, 2)), dma((zs, max(1, ys - 1), 2)), dma((zs, 2)), dma((zs, 2)), dma(()),
            dma((chunks, 2)), dma((chunks, 2)), dma((chunks, copies)), dma((chunks, max(1, copies // 2))), dma((chunks, max(1, copies // 2))),
            dma((chunks,)), dma((chunks,)),
        ],
        compiler_params=pltpu.CompilerParams(collective_id=0, has_side_effects=True, vmem_limit_bytes=60 * 1024 * 1024),
        name="gather_project",
    )(hidden, wq, gain)


def forward_kernel(ci_ref, gate_ref, gm_ref, taps_ref, cbias_ref, selw_ref, stepw_ref, sbias_ref, decay_ref, skip_ref,
                   gmall_ref, sel_ref, x_ref, gated_ref, gact_ref, tail_ref, dt_ref, slope_ref, start_ref,
                   gate_v, part_v, recv_v, x_v, gated_v, gact_v, tail_v, dt_v, slope_v, start_v,
                   ext_s, u_s, y_s, coef_s, bt_s, hist_a, hist_b, state_s, rate_s,
                   load_sem, own_sem, out_sem, grecv, gside, gup, gdown, glend, send1, recv1, send2, recv2, *, chunks, copies, n):
    zs, ys = grid_of(chunks, copies)
    me = lax.axis_index("seq")
    z, y = me // ys, me % ys
    tokens, model = gm_ref.shape
    rows, length, width = ci_ref.shape[1:]
    rank = stepw_ref.shape[0]
    half = tokens // 2
    even = ys == 2 and zs % 2 == 0
    load = pltpu.make_async_copy(gate_ref, gate_v, load_sem)
    load.start()
    own = pltpu.make_async_copy(gm_ref, gmall_ref.at[me], own_sem)
    own.start()
    meet(chunks, 1)

    def block(o, yy, h):
        return gmall_ref.at[o * ys + yy, pl.ds(h * half, half)]

    def source(o, h, k):
        return gm_ref.at[pl.ds(h * half, half)] if k is None else block(o, y, h)

    def up(o, h, k=0):
        return remote(source(o, h, k), block(o, y, h), gup.at[o, h], grecv.at[o * ys + y, h], {"seq": (z + 1) * ys + y})

    def down(o, h, k=0):
        return remote(source(o, h, k), block(o, y, h), gdown.at[o, h], grecv.at[o * ys + y, h], {"seq": (z - 1) * ys + y})

    def side(o, j, h, k=0):
        return remote(source(o, h, k), block(o, y, h), gside.at[o, j - 1, h], grecv.at[o * ys + y, h], {"seq": z * ys + lax.rem(y + j, ys)})

    def landed(o, yy, h):
        return remote(block(o, yy, h), block(o, yy, h), gside.at[o, 0, h], grecv.at[o * ys + yy, h], {"seq": lax.rem(me + 1, chunks)})

    def when(cond, fn):
        pl.when(cond)(fn)

    for h in range(2):
        when(z + 1 < zs, lambda: up(z, h, None).start())
        when(z > 0, lambda: down(z, h, None).start())
        for j in range(1, ys):
            side(z, j, h, None).start()

    partner = z + 1 - 2 * (z % 2)

    def sides(o, h, act):
        if even and h == 1:
            when(o != partner, lambda: act(side(o, 1, h)))
        else:
            for j in range(1, ys):
                act(side(o, j, h))

    def lend():
        return remote(block(z, 1 - y, 1), block(z, 1 - y, 1), glend, grecv.at[z * ys + 1 - y, 1], {"seq": partner * ys + y})

    def lend_on():
        if even:
            landed(z, 1 - y, 1).wait_recv()
            lend().start()

    def relay(k):
        for h in range(2):
            @pl.when(z - k >= 0)
            def _():
                landed(z - k, y, h).wait_recv()
                when(z + 1 < zs, lambda: up(z - k, h).start())
                sides(z - k, h, lambda one: one.start())

            @pl.when(z + k < zs)
            def _():
                landed(z + k, y, h).wait_recv()
                when(z > 0, lambda: down(z + k, h).start())
                sides(z + k, h, lambda one: one.start())

    rate_s[...] = -jnp.exp(decay_ref[...].astype(F32)) * LOG2E

    def conv(i, _):
        r, c = i // chunks, i % chunks
        x, part = conv_step(ci_ref[c, r], c == 0, taps_ref, cbias_ref, selw_ref, ext_s)
        x_v[c, r] = x
        part_v[c, r] = part
        return 0

    lax.fori_loop(0, rows * chunks, conv, 0)
    x_out = pltpu.make_async_copy(x_v, x_ref, out_sem.at[0, 0])
    x_out.start()

    def first(s):
        return remote(part_v.at[s], recv_v.at[me], send1.at[s], recv1.at[me], {"seq": s})

    def landed_first(s):
        return remote(part_v.at[s], recv_v.at[s], send1.at[s], recv1.at[s], {"seq": s})

    def second(s):
        return remote(sel_ref.at[me], sel_ref.at[me], send2.at[s], recv2.at[me], {"seq": s})

    def landed_second(s):
        return remote(sel_ref.at[s], sel_ref.at[s], send2.at[s], recv2.at[s], {"seq": s})

    def every_other(fn):
        def one(k, _):
            fn(lax.rem(me + k, chunks))
            return 0
        lax.fori_loop(1, chunks, one, 0)

    every_other(lambda s: first(s).start())
    recv_v[me] = part_v[me]
    every_other(lambda s: landed_first(s).wait_recv())
    total = recv_v[0].astype(F32)
    for s in range(1, chunks):
        total = total + recv_v[s].astype(F32)
    sel_ref[me] = total.astype(BF16)
    every_other(lambda s: second(s).start())
    if zs > 1:
        relay(1)
    if zs <= 2:
        lend_on()
    every_other(lambda s: landed_second(s).wait_recv())
    load.wait()
    pairs = ((gated_v, gated_ref), (gact_v, gact_ref), (tail_v, tail_ref), (dt_v, dt_ref), (slope_v, slope_ref), (start_v, start_ref))

    def outs(c, r):
        return [pltpu.make_async_copy(src.at[c, r], dst.at[c, r], out_sem.at[1 + k, c * rows + r]) for k, (src, dst) in enumerate(pairs)]

    def scan(i, _):
        r, c = i // chunks, i % chunks
        start_v[c, r] = jnp.where(c == 0, 0.0, state_s[...])
        scan_step(sel_ref[c, r].astype(F32), x_v[c, r].astype(F32), gate_v[c, r], c == 0, stepw_ref, sbias_ref, skip_ref,
                  gated_v.at[c, r], gact_v.at[c, r], tail_v.at[c, r], dt_v.at[c, r], slope_v.at[c, r],
                  u_s, y_s, coef_s, bt_s, hist_a, hist_b, state_s, rate_s, rank, n)
        for one in outs(c, r):
            one.start()
        return 0

    count = rows * chunks
    parts = max(1, zs - 2)
    for k in range(parts):
        lax.fori_loop(count * k // parts, count * (k + 1) // parts, scan, 0)
        if 2 + k < zs:
            relay(2 + k)
        if k == 0 and zs > 2:
            lend_on()

    def others(o, _):
        for j in range(1, ys):
            landed(o, lax.rem(y + j, ys), 0).wait_recv()
            if even:
                when(o != z, lambda: landed(o, 1 - y, 1).wait_recv())
            else:
                landed(o, lax.rem(y + j, ys), 1).wait_recv()
        return 0

    lax.fori_loop(0, zs, others, 0)
    own.wait()
    x_out.wait()

    def settle(i, _):
        for one in outs(i // rows, i % rows):
            one.wait()
        return 0

    lax.fori_loop(0, count, settle, 0)
    every_other(lambda s: first(s).wait_send())
    every_other(lambda s: second(s).wait_send())

    def drain(k, _):
        for h in range(2):
            @pl.when(z - k >= 0)
            def _():
                when(z + 1 < zs, lambda: up(z - k, h).wait_send())
                sides(z - k, h, lambda one: one.wait_send())

            @pl.when((z + k < zs) & (k > 0))
            def _():
                when(z > 0, lambda: down(z + k, h).wait_send())
                sides(z + k, h, lambda one: one.wait_send())
        return 0

    lax.fori_loop(0, zs, drain, 0)
    for h in range(2):
        when(z > 0, lambda: down(z, h).wait_send())
    if even:
        lend().wait_send()


def forward(ci, gate, gm, taps, cbias, selw, stepw, sbias, decay, skip, copies, n):
    chunks, rows, length, width = ci.shape
    tokens, model = gm.shape
    zs, ys = grid_of(chunks, copies)
    wide = BLOCK * n
    sds = jax.ShapeDtypeStruct
    dma = pltpu.SemaphoreType.DMA
    vmem = pl.BlockSpec(memory_space=pltpu.VMEM)
    hbm = pl.BlockSpec(memory_space=pl.ANY)
    coef = (chunks, rows, selw.shape[0], length)
    starts = (chunks, rows, n, width)
    full = ci.shape
    return pl.pallas_call(
        functools.partial(forward_kernel, chunks=chunks, copies=copies, n=n),
        in_specs=[vmem, hbm] + [vmem] * 8,
        out_specs=[hbm, vmem] + [hbm] * 7,
        out_shape=[sds((chunks, tokens, model), BF16), sds(coef, BF16), sds(full, BF16), sds(full, BF16), sds(full, F32), sds(full, BF16),
                   sds(full, F32), sds(full, F32), sds(starts, F32)],
        scratch_shapes=[
            pltpu.VMEM(full, F32), pltpu.VMEM(coef, BF16), pltpu.VMEM(coef, BF16), pltpu.VMEM(full, BF16), pltpu.VMEM(full, BF16),
            pltpu.VMEM(full, F32), pltpu.VMEM(full, BF16), pltpu.VMEM(full, F32), pltpu.VMEM(full, F32), pltpu.VMEM(starts, F32),
            pltpu.VMEM((length + 8, width), F32), pltpu.VMEM((length, width), F32), pltpu.VMEM((length, width), F32),
            pltpu.VMEM((length, wide), BF16), pltpu.VMEM((2 * n, length), F32), pltpu.VMEM((wide, width), BF16), pltpu.VMEM((wide, width), BF16),
            pltpu.VMEM((n, width), F32), pltpu.VMEM((n, width), F32),
            dma(()), dma(()), dma((7, rows * chunks)), dma((chunks, 2)), dma((zs, max(1, ys - 1), 2)), dma((zs, 2)), dma((zs, 2)), dma(()),
            dma((chunks,)), dma((chunks,)), dma((chunks,)), dma((chunks,)),
        ],
        compiler_params=pltpu.CompilerParams(collective_id=1, has_side_effects=True, vmem_limit_bytes=60 * 1024 * 1024),
        name="forward",
    )(ci, gate, gm, taps, cbias, selw, stepw, sbias, decay, skip)


def order_of(zs):
    return [sorted(range(zs), key=lambda t: (-abs(t - z), t)) for z in range(zs)]


def scatter_kernel(*refs, chunks, copies, split):
    if split:
        (gc_ref, gg_ref, w_ref, late_ref, ginc_ref, ging_ref, red_ref, sum_ref, all_ref,
         ysend_v, yrecv_v, own_v, zrecv_v, lend_v, late_v, w_v, g1_v, mine_v, g2_v, t_v, fin_v, load_sem,
         ysend, yrecv, zup, zdown, zrecv, lend_sem, lsend, lrecv,
         g1send, g1recv, g2send, g2recv, g3send, g3recv, g4send, g4recv) = refs
    else:
        (gc_ref, gg_ref, w_ref, late_ref, red_ref, sum_ref,
         ysend_v, yrecv_v, own_v, zrecv_v, lend_v, late_v, w_v, load_sem,
         ysend, yrecv, zup, zdown, zrecv, lend_sem, lsend, lrecv) = refs
    zs, ys = grid_of(chunks, copies)
    xs = copies // 2
    me, mine = lax.axis_index("seq"), lax.axis_index("dp")
    z, y = me // ys, me % ys
    x, c = mine // 2, mine % 2
    tokens, width = gc_ref.shape[1:]
    model = w_ref.shape[0]
    half = tokens // 2
    tile = min(256, model)
    tables = order_of(zs)
    partner = z + 1 - 2 * (z % 2)

    def dest(i):
        got = 0
        for k in range(zs):
            got = got + jnp.where(z == k, tables[k][i], 0)
        return got

    w_in = pltpu.make_async_copy(w_ref, w_v, load_sem.at[0])
    w_in.start()
    if split:
        piece, inner2 = fin_v.shape
        inner = inner2 // 2
        sides = (ginc_ref, ging_ref)
        cols = [pl.ds(part * width, width) for part in range(2)]
        loads = [[pltpu.make_async_copy(sides[part].at[:, q * 2 + c], mine_v.at[q, :, :, cols[part]], load_sem.at[1 + q * 2 + part]) for part in range(2)]
                 for q in range(xs)]
        for q in range(xs):
            for part in range(2):
                loads[q][part].start()
    meet(chunks, copies)

    def late_to(d):
        return remote(late_ref, late_v.at[mine], lsend.at[d], lrecv.at[mine], {"dp": d})

    def late_from(d):
        return remote(late_v.at[d], late_v.at[d], lsend.at[d], lrecv.at[d], {"dp": d})

    def every_copy(fn):
        def one(k, _):
            fn(lax.rem(mine + k, copies))
            return 0
        lax.fori_loop(1, copies, one, 0)

    if split:
        def g1(q, part):
            return remote(sides[part].at[:, q * 2 + 1 - c], g1_v.at[q, :, :, cols[part]], g1send.at[q, part], g1recv.at[q, part], {"dp": x * 2 + 1 - c})

        for q in range(xs):
            for part in range(2):
                g1(q, part).start()
    w_in.wait()

    def partial(s, out, at):
        def one(i, _):
            sl = pl.ds(pl.multiple_of(i * tile, tile), tile)
            got = nt_dot(gc_ref[s], w_v[sl, :width]) + nt_dot(gg_ref[s], w_v[sl, width:])
            out[at, :, sl] = got.astype(BF16)
            return 0
        lax.fori_loop(0, model // tile, one, 0)

    def to_side(i, j, h):
        rows = pl.ds(h * half, half)
        k = i * (ys - 1) + j - 1
        return remote(ysend_v.at[k % ysend_v.shape[0], rows], yrecv_v.at[k, rows], ysend.at[k, h], yrecv.at[k, h], {"seq": z * ys + lax.rem(y + j, ys)})

    slots = ysend_v.shape[0]
    even = ys == 2 and zs % 2 == 0 and slots == zs

    def lend(i):
        return remote(ysend_v.at[i, pl.ds(half, half)], lend_v, lend_sem.at[0], lend_sem.at[1], {"seq": partner * ys + y})

    def send_side(i, j, h):
        if not even or h == 0:
            to_side(i, j, h).start()
            return

        @pl.when(dest(i) != partner)
        def _():
            if i == zs - 1:
                lend(i).wait_recv()

                def one(r, _):
                    sl = pl.ds(pl.multiple_of(half + r * 32, 32), 32)
                    ysend_v[i, sl, :] = (ysend_v[i, sl, :].astype(F32) + lend_v[pl.ds(pl.multiple_of(r * 32, 32), 32), :].astype(F32)).astype(BF16)
                    return 0
                lax.fori_loop(0, half // 32, one, 0)
            to_side(i, j, h).start()

    def if_sent(i, h, fn):
        if even and h == 1:
            pl.when(dest(i) != partner)(fn)
        else:
            fn()

    ahead = 2 if slots == zs * (ys - 1) else zs
    def outgoing(i):
        for j in range(1, ys):
            k = i * (ys - 1) + j - 1
            if k >= slots:
                for h in range(2):
                    to_side((k - slots) // (ys - 1), (k - slots) % (ys - 1) + 1, h).wait_send()
            partial(dest(i) * ys + lax.rem(y + j, ys), ysend_v, k % slots)
            if i < ahead:
                for h in range(2):
                    send_side(i, j, h)
            if even:
                pl.when(dest(i) == partner)(lambda: lend(i).start())

    if split:
        def g2(q, part):
            return remote(mine_v.at[q, :, :, cols[part]], g2_v.at[x, :, :, cols[part]], g2send.at[q, part], g2recv.at[x, part], {"dp": q * 2 + c})

        def g2_from(q, part):
            return remote(g2_v.at[q, :, :, cols[part]], g2_v.at[q, :, :, cols[part]], g2send.at[q, part], g2recv.at[q, part], {"dp": q * 2 + c})

        for i in range(min(2, zs)):
            outgoing(i)
        for part in range(2):
            for q in range(xs):
                loads[q][part].wait()
                g1(q, part).wait_recv()

                def fold(s, _):
                    mine_v[q, s, :, cols[part]] = (mine_v[q, s, :, cols[part]].astype(F32) + g1_v[q, s, :, cols[part]].astype(F32)).astype(BF16)
                    return 0
                lax.fori_loop(0, chunks, fold, 0)

                @pl.when(q != x)
                def _():
                    g2(q, part).start()

        def columns(part, s):
            return pl.ds(pl.multiple_of(part * inner + s * width, width), width)

        def g3(s, part):
            return remote(t_v.at[s, :, cols[part]], fin_v.at[:, columns(part, me)], g3send.at[s, part], g3recv.at[me, part], {"seq": s})

        def g3_from(s, part):
            return remote(fin_v.at[:, columns(part, s)], fin_v.at[:, columns(part, s)], g3send.at[s, part], g3recv.at[s, part], {"seq": s})

        def every_other(fn):
            def one(k, _):
                fn(lax.rem(me + k, chunks))
                return 0
            lax.fori_loop(1, chunks, one, 0)

        def third(part):
            for q in range(xs):
                @pl.when(q != x)
                def _():
                    g2_from(q, part).wait_recv()

            def fold(s, _):
                total = mine_v[x, s, :, cols[part]].astype(F32)
                for q in range(1, xs):
                    total = total + g2_v[lax.rem(x + q, xs), s, :, cols[part]].astype(F32)
                t_v[s, :, cols[part]] = total.astype(BF16)
                return 0
            lax.fori_loop(0, chunks, fold, 0)
            every_other(lambda s: g3(s, part).start())
            fin_v[:, columns(part, me)] = t_v[me, :, cols[part]]

        def rows_of(d):
            return pl.ds(pl.multiple_of(d * piece, piece), piece)

        sides_of = [pl.ds(part * inner, inner) for part in range(2)]

        def g4(d_src, k, d, part):
            src = fin_v.at[:, sides_of[part]] if d_src is None else all_ref.at[rows_of(d_src), sides_of[part]]
            row = mine if d_src is None else d_src
            return remote(src, all_ref.at[rows_of(row), sides_of[part]], g4send.at[k, part], g4recv.at[row, part], {"dp": d})

        def g4_from(d, part):
            to = all_ref.at[rows_of(d), sides_of[part]]
            return remote(to, to, g4send.at[0, part], g4recv.at[d, part], {"dp": d})

        keep = [pltpu.make_async_copy(fin_v.at[:, sides_of[part]], all_ref.at[rows_of(mine), sides_of[part]], load_sem.at[part]) for part in range(2)]

        def fourth(part):
            every_other(lambda s: g3_from(s, part).wait_recv())
            for j in range(1, xs):
                g4(None, j, lax.rem(x + j, xs) * 2 + c, part).start()
            g4(None, 0, x * 2 + 1 - c, part).start()
            keep[part].start()

    for i in range(min(2, zs) if split else 0, zs):
        outgoing(i)
    every_copy(lambda d: late_to(d).start())

    def arrived(i, j, h):
        rows = pl.ds(h * half, half)
        k = i * (ys - 1) + j - 1
        return remote(yrecv_v.at[k, rows], yrecv_v.at[k, rows], ysend.at[k, h], yrecv.at[k, h], {"seq": z * ys + lax.rem(y + j, ys)})

    def climb(t, h):
        rows = pl.ds(h * half, half)
        return remote(own_v.at[t, rows], zrecv_v.at[t, rows], zup.at[t, h], zrecv.at[t, h], {"seq": (z + 1) * ys + y})

    def sink(t, h):
        rows = pl.ds(h * half, half)
        slot = jnp.where(t == z - 1, zs, t)
        return remote(own_v.at[t, rows], zrecv_v.at[slot, rows], zdown.at[t, h], zrecv.at[slot, h], {"seq": (z - 1) * ys + y})

    def from_z(slot, h):
        rows = pl.ds(h * half, half)
        return remote(zrecv_v.at[slot, rows], zrecv_v.at[slot, rows], zup.at[0, h], zrecv.at[slot, h], {"seq": lax.rem(me + 1, chunks)})

    def accumulate(t, h, read):
        def one(r, _):
            sl = pl.ds(pl.multiple_of(h * half + r * 32, 32), 32)
            own_v[t, sl, :] = (own_v[t, sl, :].astype(F32) + read(sl)).astype(BF16)
            return 0
        lax.fori_loop(0, half // 32, one, 0)

    for i in range(zs):
        t = dest(i)
        partial(t * ys + y, own_v, t)
        for h in range(2):
            for j in range(1, ys):
                if_sent(i, h, lambda: arrived(i, ys - j, h).wait_recv())

            def side_sum(sl):
                total = yrecv_v[i * (ys - 1), sl, :].astype(F32)
                for j in range(2, ys):
                    total = total + yrecv_v[i * (ys - 1) + j - 1, sl, :].astype(F32)
                return total

            if ys > 1:
                if_sent(i, h, lambda: accumulate(t, h, side_sum))

            @pl.when(((t > z) & (z > 0)) | ((t == z) & (z > 0)))
            def _():
                from_z(t, h).wait_recv()
                accumulate(t, h, lambda sl: zrecv_v[t, sl, :].astype(F32))

            @pl.when((t < z) & (z + 1 < zs))
            def _():
                from_z(t, h).wait_recv()
                accumulate(t, h, lambda sl: zrecv_v[t, sl, :].astype(F32))

            @pl.when((t == z) & (z + 1 < zs))
            def _():
                from_z(zs, h).wait_recv()
                accumulate(t, h, lambda sl: zrecv_v[zs, sl, :].astype(F32))

            @pl.when(t > z)
            def _():
                climb(t, h).start()

            @pl.when(t < z)
            def _():
                sink(t, h).start()
        if split and i == 0:
            third(0)
            third(1)
        if split and i == min(1, zs - 1):
            fourth(0)
            fourth(1)
        if i + ahead < zs:
            for j in range(1, ys):
                for h in range(2):
                    send_side(i + ahead, j, h)

    red_ref[...] = own_v[z]
    every_copy(lambda d: late_from(d).wait_recv())
    total = late_ref[...].astype(F32)
    for k in range(1, copies):
        total = total + late_v[lax.rem(mine + k, copies)].astype(F32)
    sum_ref[...] = total
    if split:
        for part in range(2):
            for j in range(1, xs):
                d = lax.rem(x + j, xs) * 2 + c
                g4_from(d, part).wait_recv()
                g4(d, xs - 1 + j, x * 2 + 1 - c, part).start()
        for part in range(2):
            keep[part].wait()
            for j in range(xs):
                g4_from(lax.rem(x + j, xs) * 2 + 1 - c, part).wait_recv()

    every_copy(lambda d: late_to(d).wait_send())
    count = zs * (ys - 1)
    for k in range(max(0, count - slots), count):
        for h in range(2):
            if_sent(k // (ys - 1), h, lambda: to_side(k // (ys - 1), k % (ys - 1) + 1, h).wait_send())
    if even:
        lend(0).wait_send()
    for i in range(zs):
        t = dest(i)
        for h in range(2):
            @pl.when(t > z)
            def _():
                climb(t, h).wait_send()

            @pl.when(t < z)
            def _():
                sink(t, h).wait_send()
    if split:
        for part in range(2):
            for q in range(xs):
                g1(q, part).wait_send()

                @pl.when(q != x)
                def _():
                    g2(q, part).wait_send()
            every_other(lambda s: g3(s, part).wait_send())
            for j in range(xs):
                g4(None, j, mine, part).wait_send()
            for j in range(1, xs):
                g4(lax.rem(x + j, xs) * 2 + c, xs - 1 + j, mine, part).wait_send()


def scatter_sums(gc, gg, w_all, late, ginc, ging, chunks, copies, split):
    tokens, width = gc.shape[1:]
    model = w_all.shape[0]
    zs, ys = grid_of(chunks, copies)
    xs = max(1, copies // 2)
    others = max(1, zs * (ys - 1))
    slots = min(others, 4)
    any_spec = pl.BlockSpec(memory_space=pl.ANY)
    vmem = pl.BlockSpec(memory_space=pltpu.VMEM)
    sds = jax.ShapeDtypeStruct
    dma = pltpu.SemaphoreType.DMA
    args = [gc, gg, w_all, late]
    in_specs = [vmem, vmem, any_spec, vmem]
    out_specs = [vmem, vmem]
    out_shape = [sds((tokens, model), BF16), sds(late.shape, F32)]
    scratch = [pltpu.VMEM((slots, tokens, model), BF16), pltpu.VMEM((others, tokens, model), BF16),
               pltpu.VMEM((zs, tokens, model), BF16), pltpu.VMEM((zs + 1, tokens, model), BF16), pltpu.VMEM((tokens // 2, model), BF16),
               pltpu.VMEM((copies,) + late.shape, BF16), pltpu.VMEM(w_all.shape, BF16)]
    sems = [dma((1 + 2 * xs,)), dma((others, 2)), dma((others, 2)), dma((zs, 2)), dma((zs, 2)), dma((zs + 1, 2)), dma((2,)), dma((copies,)), dma((copies,))]
    if split:
        piece = ginc.shape[2]
        slab = (xs, chunks, piece, 2 * width)
        args += [ginc, ging]
        in_specs += [any_spec] * 2
        out_specs.append(any_spec)
        out_shape.append(sds((copies * piece, 2 * chunks * width), BF16))
        scratch += [pltpu.VMEM(slab, BF16), pltpu.VMEM(slab, BF16), pltpu.VMEM(slab, BF16), pltpu.VMEM(slab[1:], BF16),
                    pltpu.VMEM((piece, 2 * chunks * width), BF16)]
        sems += [dma((xs, 2)), dma((xs, 2)), dma((xs, 2)), dma((xs, 2)), dma((chunks, 2)), dma((chunks, 2)), dma((2 * xs, 2)), dma((copies, 2))]
    return pl.pallas_call(
        functools.partial(scatter_kernel, chunks=chunks, copies=copies, split=split),
        in_specs=in_specs,
        out_specs=out_specs,
        out_shape=out_shape,
        scratch_shapes=scratch + sems,
        compiler_params=pltpu.CompilerParams(collective_id=3, has_side_effects=True, vmem_limit_bytes=62 * 1024 * 1024),
        name="scatter_sums",
    )(*args)
def backward_kernel(*refs, chunks, copies, n, inside, extra):
    ins = 15 + (1 if inside else 0) + (1 if extra else 0)
    (gg_ref, gact_ref, tail_ref, x_ref, dt_ref, slope_ref, start_ref, sel_ref, ci_ref, stepw_ref, decay_ref, skip_ref,
     taps_ref, cbias_ref, selw_ref) = refs[:15]
    mixed_ref = refs[15] if inside else None
    gout_ref = refs[ins - 1] if extra else None
    outs = 9 + (1 if inside else 0) + (1 if extra else 0)
    (ggate_ref, gci_ref, gstepw_ref, gsbias_ref, gdecay_ref, gskip_ref, gtaps_ref, gcbias_ref, gselw_ref) = refs[ins:ins + 9]
    red_ref = refs[ins + 9] if inside else None
    gsum_ref = refs[ins + outs - 1] if extra else None
    refs = refs[ins + outs:]
    (gg_v, gact_v, tail_v, x_v, dt_v, slope_v, start_v, ggate_v, gci_v, gvals_v, part_v, recv_v, sel2_v,
     u_s, gy_s, gu_s, ah_s, bcoef_s, bt_s, hist_s, adj_a, harm_a, adj_b, harm_b, db_s, dc_s, carry_s, gd_s, rate_s, factor_s, kept_s,
     ext_s, gext_s, in_sem, ggate_sem, gci_sem, send1, recv1, send2, recv2) = refs[:40]
    refs = refs[40:]
    if inside:
        own_v, yrecv_v, zrecv_v, own_sem, ysend, yrecv, zup, zdown, zrecv = refs[:9]
        refs = refs[9:]
    if extra:
        core_v, half_v, far_v, esend, erecv, asend, arecv, bsend, brecv = refs
    zs, ys = grid_of(chunks, copies)
    xs = copies // 2
    me, mine = lax.axis_index("seq"), lax.axis_index("dp")
    z, y = me // ys, me % ys
    xd, cd = mine // 2, mine % 2
    rows = sel_ref.shape[1]
    rank = stepw_ref.shape[0]
    count = rows * chunks

    def where_of(i):
        return chunks - 1 - i % chunks, i // chunks

    streams = ((gg_ref, gg_v), (gact_ref, gact_v), (tail_ref, tail_v), (x_ref, x_v), (dt_ref, dt_v), (slope_ref, slope_v), (start_ref, start_v))

    def fetch(i):
        c, r = where_of(i)
        return [pltpu.make_async_copy(src.at[c, r], dst.at[i % 2], in_sem.at[k, i % 2]) for k, (src, dst) in enumerate(streams)]

    for one in fetch(0):
        one.start()
    if inside:
        tokens, model = red_ref.shape
        half = tokens // 2
        own_loads = [pltpu.make_async_copy(mixed_ref.at[t * ys + y], own_v.at[t], own_sem.at[t]) for t in range(zs)]
        for one in own_loads:
            one.start()
    meet(chunks, copies if extra else 1)

    if inside:
        tables = order_of(zs)

        def dest(i):
            got = 0
            for k in range(zs):
                for q in range(zs):
                    got = got + jnp.where((z == k) & (i == q), tables[k][q], 0)
            return got

        def part_rows(h):
            return pl.ds(h * half, half)

        def to_side(i, h):
            return remote(mixed_ref.at[dest(i) * ys + 1 - y, part_rows(h)], yrecv_v.at[i, part_rows(h)], ysend.at[i, h], yrecv.at[i, h], {"seq": z * ys + 1 - y})

        def arrived(i, h):
            return remote(yrecv_v.at[i, part_rows(h)], yrecv_v.at[i, part_rows(h)], ysend.at[i, h], yrecv.at[i, h], {"seq": z * ys + 1 - y})

        def climb(t, h):
            return remote(own_v.at[t, part_rows(h)], zrecv_v.at[t, part_rows(h)], zup.at[t, h], zrecv.at[t, h], {"seq": (z + 1) * ys + y})

        def sink(t, h):
            slot = jnp.where(t == z - 1, zs, t)
            return remote(own_v.at[t, part_rows(h)], zrecv_v.at[slot, part_rows(h)], zdown.at[t, h], zrecv.at[slot, h], {"seq": (z - 1) * ys + y})

        def from_z(slot, h):
            return remote(zrecv_v.at[slot, part_rows(h)], zrecv_v.at[slot, part_rows(h)], zup.at[0, h], zrecv.at[slot, h], {"seq": lax.rem(me + 1, chunks)})

        def accumulate(t, h, buf, slot):
            def one(r, _):
                sl = pl.ds(pl.multiple_of(h * half + r * 32, 32), 32)
                own_v[t, sl, :] = own_v[t, sl, :] + buf[slot, sl, :]
                return 0
            lax.fori_loop(0, half // 32, one, 0)

        def settle(i):
            t = dest(i)
            for h in range(2):
                arrived(i, h).wait_recv()
                accumulate(t, h, yrecv_v, i)

                @pl.when((t >= z) & (z > 0))
                def _():
                    from_z(t, h).wait_recv()
                    accumulate(t, h, zrecv_v, t)

                @pl.when((t < z) & (z + 1 < zs))
                def _():
                    from_z(t, h).wait_recv()
                    accumulate(t, h, zrecv_v, t)

                @pl.when((t == z) & (z + 1 < zs))
                def _():
                    from_z(zs, h).wait_recv()
                    accumulate(t, h, zrecv_v, zs)

                @pl.when(t > z)
                def _():
                    climb(t, h).start()

                @pl.when(t < z)
                def _():
                    sink(t, h).start()

            @pl.when(i + 2 < zs)
            def _():
                for h in range(2):
                    to_side(i + 2, h).start()

        for i in range(2):
            for h in range(2):
                to_side(i, h).start()
        edge = (z == 0) | (z == zs - 1)

    if extra:
        grows = gout_ref.shape[0] // 2

        def part_of(core):
            return pl.ds(pl.multiple_of(core * grows, grows), grows)

        to_core = remote(gout_ref.at[part_of(1 - cd)], core_v, esend, erecv, {"dp": xd * 2 + 1 - cd})

        def across(j):
            return remote(half_v, far_v.at[xd], asend.at[j], arecv.at[xd], {"dp": lax.rem(xd + j, xs) * 2 + cd})

        def from_across(j):
            q = lax.rem(xd + j, xs)
            return remote(far_v.at[q], far_v.at[q], asend.at[j], arecv.at[q], {"dp": q * 2 + cd})

        back_out = remote(gsum_ref.at[part_of(cd)], gsum_ref.at[part_of(cd)], bsend, brecv, {"dp": xd * 2 + 1 - cd})
        back_in = remote(gsum_ref.at[part_of(1 - cd)], gsum_ref.at[part_of(1 - cd)], bsend, brecv, {"dp": xd * 2 + 1 - cd})
        to_core.start()

        def by_rows(fn):
            def one(i, _):
                fn(pl.ds(pl.multiple_of(i * 16, 16), 16), pl.ds(pl.multiple_of(cd * grows + i * 16, 16), 16))
                return 0
            lax.fori_loop(0, grows // 16, one, 0)

        def chip_sum():
            to_core.wait_recv()

            def fold(at, full):
                half_v[at, :] = (gout_ref[full, :].astype(F32) + core_v[at, :].astype(F32)).astype(BF16)
            by_rows(fold)
            for j in range(1, xs):
                across(j).start()

        def whole_sum():
            for j in range(1, xs):
                from_across(j).wait_recv()

            def fold(at, full):
                total = half_v[at, :].astype(F32)
                for j in range(1, xs):
                    total = total + far_v[lax.rem(xd + j, xs), at, :].astype(F32)
                gsum_ref[full, :] = total.astype(BF16)
            by_rows(fold)
            back_out.start()

    def first(s, r):
        return remote(part_v.at[s, r], recv_v.at[me, r], send1.at[s, r], recv1.at[me, r], {"seq": s})

    def landed_first(s, r):
        return remote(part_v.at[s, r], recv_v.at[s, r], send1.at[s, r], recv1.at[s, r], {"seq": s})

    def second(s, r):
        return remote(sel2_v.at[me, r], sel2_v.at[me, r], send2.at[s, r], recv2.at[me, r], {"seq": s})

    def landed_second(s, r):
        return remote(sel2_v.at[s, r], sel2_v.at[s, r], send2.at[s, r], recv2.at[s, r], {"seq": s})

    def every_other(fn):
        def one(k, _):
            fn(lax.rem(me + k, chunks))
            return 0
        lax.fori_loop(1, chunks, one, 0)

    def send_row(r):
        every_other(lambda s: first(s, r).start())
        recv_v[me, r] = part_v[me, r]

    def sum_row(r):
        every_other(lambda s: landed_first(s, r).wait_recv())
        total = recv_v[0, r].astype(F32)
        for s in range(1, chunks):
            total = total + recv_v[s, r].astype(F32)
        sel2_v[me, r] = total.astype(BF16)
        every_other(lambda s: second(s, r).start())

    for ref in (gstepw_ref, gsbias_ref, gskip_ref, gd_s, gtaps_ref, gcbias_ref, gselw_ref):
        ref[...] = jnp.zeros_like(ref)
    rate_s[...] = -jnp.exp(decay_ref[...].astype(F32)) * LOG2E

    def ggate_out(i):
        c, r = where_of(i)
        return pltpu.make_async_copy(ggate_v.at[i % 2], ggate_ref.at[c, r], ggate_sem.at[i % 2])

    def gci_out(i):
        c, r = where_of(i)
        return pltpu.make_async_copy(gci_v.at[i % 2], gci_ref.at[c, r], gci_sem.at[i % 2])

    def scan(i, _):
        c, r = where_of(i)
        slot = i % 2

        @pl.when(i + 1 < count)
        def _():
            for one in fetch(i + 1):
                one.start()

        @pl.when(i >= 2)
        def _():
            ggate_out(i - 2).wait()

        for one in fetch(i):
            one.wait()
        back_step(sel_ref[c, r].astype(F32), x_v[slot].astype(F32), i % chunks == 0, gact_v.at[slot], gg_v.at[slot], tail_v.at[slot],
                  start_v.at[slot], dt_v.at[slot], slope_v.at[slot], stepw_ref, skip_ref,
                  ggate_v.at[slot], gvals_v.at[c, r], part_v.at[c, r], gstepw_ref, gsbias_ref, gskip_ref,
                  u_s, gy_s, gu_s, ah_s, bcoef_s, bt_s, hist_s, adj_a, harm_a, adj_b, harm_b, db_s, dc_s, carry_s, gd_s, rate_s, factor_s, kept_s, rank, n)
        ggate_out(i).start()
        late = min(3, chunks - 1)

        @pl.when((i % chunks == chunks - 1) & (r + 1 < rows))
        def _():
            send_row(r)

        @pl.when((i % chunks == late) & (r > 0))
        def _():
            sum_row(r - 1)

        if extra:
            pl.when(i == 2)(chip_sum)
            pl.when(i == 8)(whole_sum)
        if inside:
            lo = jnp.where(edge, jnp.where(i == 4, 0, jnp.where(i == 9, 1, 2)), jnp.where(i == 9, 0, 1))
            hi = jnp.where(edge, lo + 1, jnp.where(i == 9, 1, jnp.where(i == 13, 3, 0)))

            @pl.when((i == 4) | (i == 9) | (i == 13))
            def _():
                for k in range(own_v.shape[0]):
                    pl.when(i == 4)(own_loads[k].wait)

                def one(k, _):
                    settle(k)
                    return 0
                lax.fori_loop(lo, hi, one, 0)
        return 0

    lax.fori_loop(0, count, scan, 0)
    send_row(rows - 1)
    gdecay_ref[...] = gd_s[...] * rate_s[...] * (1.0 / LOG2E)
    for i in range(max(0, count - 2), count):
        ggate_out(i).wait()

    def conv(i, _):
        c, r = where_of(i)

        @pl.when(i >= 2)
        def _():
            gci_out(i - 2).wait()

        conv_back_step(ci_ref.at[c, r], ci_ref.at[jnp.maximum(c - 1, 0), r], c == 0, i % chunks == 0, gvals_v.at[c, r], sel2_v.at[c, r],
                       taps_ref, cbias_ref, selw_ref, gci_v.at[i % 2], gtaps_ref, gcbias_ref, gselw_ref, ext_s, gext_s)
        gci_out(i).start()
        return 0

    for r in range(rows - 1):
        every_other(lambda s: landed_second(s, r).wait_recv())
    lax.fori_loop(0, count - chunks, conv, 0)
    sum_row(rows - 1)
    if inside:
        settle(zs - 1)
        red_ref[...] = own_v[z]
    every_other(lambda s: landed_second(s, rows - 1).wait_recv())
    lax.fori_loop(count - chunks, count, conv, 0)
    for i in range(max(0, count - 2), count):
        gci_out(i).wait()
    for r in range(rows):
        every_other(lambda s: first(s, r).wait_send())
        every_other(lambda s: second(s, r).wait_send())
    if extra:
        to_core.wait_send()
        for j in range(1, xs):
            across(j).wait_send()
        back_in.wait_recv()
        back_out.wait_send()
    if inside:
        for i in range(zs):
            t = dest(i)
            for h in range(2):
                to_side(i, h).wait_send()

                @pl.when(t > z)
                def _():
                    climb(t, h).wait_send()

                @pl.when(t < z)
                def _():
                    sink(t, h).wait_send()


def backward(gg, gact, tail, x, dt, slope, starts, sel, ci, stepw, decay, skip, taps, cbias, selw, mixed, gout, copies, n):
    chunks, rows, length, width = ci.shape
    rank = stepw.shape[0]
    zs, ys = grid_of(chunks, copies)
    xs = max(1, copies // 2)
    wide = BLOCK * n
    inside = mixed is not None
    extra = copies % 2 == 0
    sds = jax.ShapeDtypeStruct
    dma = pltpu.SemaphoreType.DMA
    vmem = pl.BlockSpec(memory_space=pltpu.VMEM)
    hbm = pl.BlockSpec(memory_space=pl.ANY)
    args = [gg, gact, tail, x, dt, slope, starts, sel, ci, stepw, decay, skip, taps, cbias, selw]
    in_specs = [hbm] * 7 + [vmem] * 8
    out_specs = [hbm] * 2 + [vmem] * 7
    out_shape = [sds(ci.shape, BF16), sds(ci.shape, BF16), sds((rank, width), F32), sds((1, width), F32), sds((n, width), F32), sds((1, width), F32),
                 sds(taps.shape, F32), sds((1, width), F32), sds(selw.shape, F32)]
    tile, coef = (length, width), sel.shape
    scratch = [pltpu.VMEM((2,) + tile, F32), pltpu.VMEM((2,) + tile, F32), pltpu.VMEM((2,) + tile, BF16), pltpu.VMEM((2,) + tile, BF16),
               pltpu.VMEM((2,) + tile, F32), pltpu.VMEM((2,) + tile, F32), pltpu.VMEM((2, n, width), F32),
               pltpu.VMEM((2,) + tile, BF16), pltpu.VMEM((2,) + tile, BF16), pltpu.VMEM(ci.shape, F32),
               pltpu.VMEM(coef, BF16), pltpu.VMEM(coef, BF16), pltpu.VMEM(coef, BF16),
               pltpu.VMEM(tile, F32), pltpu.VMEM(tile, F32), pltpu.VMEM(tile, F32), pltpu.VMEM(tile, F32),
               pltpu.VMEM((length, wide), BF16), pltpu.VMEM((2 * n, length), F32), pltpu.VMEM((length * n, width), BF16),
               pltpu.VMEM((wide, width), BF16), pltpu.VMEM((wide, width), BF16), pltpu.VMEM((wide, width), BF16), pltpu.VMEM((wide, width), BF16),
               pltpu.VMEM((length, wide), F32), pltpu.VMEM((length, wide), F32),
               pltpu.VMEM((n, width), F32), pltpu.VMEM((n, width), F32), pltpu.VMEM((n, width), F32),
               pltpu.VMEM((length * n, width), F32), pltpu.VMEM((length * n, width), F32),
               pltpu.VMEM((length + 8, width), F32), pltpu.VMEM((length + 8, width), F32),
               dma((7, 2)), dma((2,)), dma((2,)), dma((chunks, rows)), dma((chunks, rows)), dma((chunks, rows)), dma((chunks, rows))]
    if inside:
        tokens, model = mixed.shape[1:]
        args.append(mixed)
        in_specs.append(hbm)
        out_specs.append(vmem)
        out_shape.append(sds((tokens, model), BF16))
        scratch += [pltpu.VMEM((zs, tokens, model), BF16), pltpu.VMEM((zs, tokens, model), BF16), pltpu.VMEM((zs + 1, tokens, model), BF16),
                    dma((zs,)), dma((zs, 2)), dma((zs, 2)), dma((zs, 2)), dma((zs, 2)), dma((zs + 1, 2))]
    if extra:
        args.append(gout)
        in_specs.append(vmem)
        out_specs.append(vmem)
        out_shape.append(sds(gout.shape, BF16))
        part = (gout.shape[0] // 2, gout.shape[1])
        scratch += [pltpu.VMEM(part, BF16), pltpu.VMEM(part, BF16), pltpu.VMEM((xs,) + part, BF16),
                    dma(()), dma(()), dma((xs,)), dma((xs,)), dma(()), dma(())]
    return pl.pallas_call(
        functools.partial(backward_kernel, chunks=chunks, copies=copies, n=n, inside=inside, extra=extra),
        in_specs=in_specs,
        out_specs=out_specs,
        out_shape=out_shape,
        scratch_shapes=scratch,
        compiler_params=pltpu.CompilerParams(collective_id=2, has_side_effects=True, vmem_limit_bytes=63 * 1024 * 1024),
        name="backward",
    )(*args)


from jax.sharding import PartitionSpec as P


def local(hidden, grad_out, lengths, norm_gain, input_weight, conv_weight, conv_bias, select_weight,
          step_weight, step_bias, decay_log, skip_weight, output_weight):
    rows, length, model = hidden.shape
    chunks = lax.axis_size("seq")
    copies = lax.axis_size("dp")
    width = output_weight.shape[0]
    share = input_weight.shape[0]
    rank = step_weight.shape[0]
    n = decay_log.shape[0]
    tokens = chunks * rows * length
    here = lax.axis_index("seq")

    split = (share // copies) % 16 == 0 and copies % 2 == 0
    normed, ci, gate, w_all, gain_row = gather_project(
        hidden.reshape(rows * length, model), input_weight, norm_gain.astype(F32).reshape(1, share), chunks, copies, share, split)
    normed = normed.reshape(tokens, model)
    slots = here * length + lax.broadcasted_iota(jnp.int32, (rows, length), 1)
    valid = (slots < lengths[:, None]).astype(F32)[..., None]
    cotangent = grad_out.astype(F32) * valid
    shaped = lambda a: a.reshape(chunks, rows, length, a.shape[-1])
    ci, gate = shaped(ci), shaped(gate)
    bias_row = conv_bias.reshape(1, width)
    step_row = step_bias.reshape(1, width)
    skip_row = skip_weight.reshape(1, width)
    gm, sel, x, gated, gact, tail, dt, slope, starts = forward(
        ci, gate, cotangent.astype(BF16).reshape(rows * length, model), conv_weight, bias_row, select_weight,
        step_weight, step_row, decay_log, skip_row, copies, n)
    gm = gm.reshape(tokens, model)
    gated2 = gated.reshape(tokens, width)
    mixed = shaped(jnp.dot(gated2, output_weight, preferred_element_type=F32).astype(BF16))
    zs, ys = grid_of(chunks, copies)
    inside = ys == 2 and zs == 4
    source = hidden.astype(F32)
    gg = shaped(lax.dot_general(gm, output_weight, (((1,), (1,)), ((), ())), preferred_element_type=F32))
    tn = lambda a, b: lax.dot_general(a, b, (((0,), (0,)), ((), ())), preferred_element_type=F32)
    gout = tn(gated2, gm).astype(BF16)
    flat = lambda a: a.reshape(chunks, rows * length, a.shape[-1])
    got = backward(gg, gact, tail, x, dt, slope, starts, sel, ci, step_weight, decay_log, skip_row, conv_weight, bias_row, select_weight,
                   flat(mixed) if inside else None, gout, copies, n)
    ggate, gci, gstepw, gstepb, gdecay, gskip, gtaps, gconvb, gselw = got[:9]
    mixed = got[9].reshape(rows, length, model) if inside else lax.psum_scatter(mixed, "seq", scatter_dimension=0, tiled=False)
    gout = got[-1].astype(F32)
    output = ((source + mixed.astype(F32)) * valid).astype(BF16)
    tap_count = gtaps.shape[0]
    gci2 = gci.reshape(tokens, width)
    ggate2 = ggate.reshape(tokens, width)
    ginc, ging = (tn(normed, g).astype(BF16).reshape(chunks, copies, share // copies, width) for g in (gci2, ggate2))
    late = jnp.concatenate([gselw, gstepw, gdecay, gtaps, gstepb, gskip, gconvb], axis=0).astype(BF16)
    late = jnp.pad(late, ((0, -late.shape[0] % 16), (0, 0)))
    got = scatter_sums(flat(gci), flat(ggate), w_all, late, ginc, ging, chunks, copies, split)
    scaled, late = got[:2]
    if split:
        gin = got[2].astype(F32)
    else:
        gin = jnp.stack([ginc, ging], axis=3)
        gin = lax.psum_scatter(gin, "dp", scatter_dimension=1, tiled=False)
        gin = lax.all_to_all(gin, "seq", split_axis=0, concat_axis=2, tiled=False)
        gin = lax.all_gather(gin.reshape(share // copies, 2 * chunks * width), "dp", axis=0, tiled=True).astype(F32)
    ggain = jnp.sum(gin * input_weight.astype(F32), axis=1) / norm_gain.astype(F32)
    scaled = scaled.reshape(rows, length, model).astype(F32) * gain_row
    inverse = lax.rsqrt(jnp.mean(source * source, axis=-1, keepdims=True) + EPSILON)
    ghidden = inverse * scaled - source * inverse ** 3 * jnp.mean(scaled * source, axis=-1, keepdims=True) + cotangent
    sizes = (gselw.shape[0], rank, n, tap_count)
    ends = [sum(sizes[:k + 1]) for k in range(len(sizes))]
    gselw, gstepw, gdecay, gtaps = (late[e - k:e] for e, k in zip(ends, sizes))
    gstepb, gskip, gconvb = (late[ends[-1] + k] for k in range(3))
    return (output, ghidden, ggain, gin, gtaps, gconvb, gselw, gstepw, gstepb,
            gdecay, gskip, gout)


def solution(mesh):
    tok, vec, col, row = P("dp", "seq", None), P("seq"), P(None, "seq"), P("seq", None)
    return jax.shard_map(
        local,
        mesh=mesh,
        in_specs=(tok, tok, P("dp"), vec, row, col, vec, col, col, vec, col, vec, row),
        out_specs=(tok, tok, vec, row, col, vec, col, col, vec, col, vec, row),
        check_vma=False,
    )
```

```python
import functools
import jax
import jax.numpy as jnp
from jax import lax
from jax.experimental import pallas as pl
from jax.experimental.pallas import tpu as pltpu

BLOCK = 16
EPSILON = 1e-05
LOG2E = 1.4426950408889634
F32 = jnp.float32
BF16 = jnp.bfloat16


def inverse_of(whole):
    guess = pl.reciprocal(whole, approx=True)
    return guess * (2.0 - whole * guess)


def gates_of(pre):
    small = jnp.exp2(jnp.abs(pre) * -LOG2E)
    whole = 1.0 + small
    log_part = jnp.where(small < 1e-3, small * (1.0 - small * (0.5 - small * (1.0 / 3.0))), jnp.log(whole))
    return jnp.maximum(pre, 0.0) + log_part, jnp.where(pre >= 0.0, 1.0, small) * inverse_of(whole)


def sigmoid(v):
    return 0.5 + 0.5 * jnp.tanh(0.5 * v)


def nt_dot(a, b):
    return lax.dot_general(a, b, (((1,), (1,)), ((), ())), preferred_element_type=F32)


def lane_tiles(width):
    step = min(width, 512)
    return [slice(k, k + step) for k in range(0, width, step)]


def tile_matrix(n, wide):
    col = lax.broadcasted_iota(jnp.int32, (n, wide), 1)
    row = lax.broadcasted_iota(jnp.int32, (n, wide), 0)
    return (col % n == row).astype(F32)


def diagonal_mask(rows, n, wide):
    col = lax.broadcasted_iota(jnp.int32, (rows, wide), 1)
    row = lax.broadcasted_iota(jnp.int32, (rows, wide), 0)
    return col // n == row % BLOCK


def scan_step(selected, x, gate, fresh, stepw_ref, bias_ref, skip_ref, gated_ref, gact_ref, tail_ref, dt_ref, slope_ref,
              u_s, y_s, coef_s, bt_s, hist_a, hist_b, state_s, rate_s, rank, n):
    length = x.shape[0]
    wide = BLOCK * n
    state_s[...] = jnp.where(fresh, 0.0, state_s[...])
    low = selected[:rank].T.astype(BF16)
    pre = jnp.dot(low, stepw_ref[...], preferred_element_type=F32) + bias_ref[...]
    dt, slope = gates_of(pre)
    dt_ref[...] = dt
    slope_ref[...] = slope
    u_s[...] = dt * x
    bt_s[...] = selected[rank:]
    spread = jnp.dot(selected[rank:].T[:, n:], tile_matrix(n, wide), preferred_element_type=F32)
    coef_s[...] = jnp.where(diagonal_mask(length, n, wide), spread, 0.0).astype(BF16)
    blocks = length // BLOCK

    def finish(k, hist):
        rows = pl.ds(pl.multiple_of(k * BLOCK, BLOCK), BLOCK)
        y_s[rows, :] = jnp.dot(coef_s[rows, :], hist[...], preferred_element_type=F32)

    def block(k, state, hist):
        at = pl.multiple_of(k * BLOCK, BLOCK)
        bs = pltpu.roll(bt_s[0:n, :], length - at, 1)
        dts = dt_ref[pl.ds(at, BLOCK), :]
        us = u_s[pl.ds(at, BLOCK), :]
        rate = rate_s[...]
        for i in range(BLOCK):
            factor = jnp.exp2(dts[i:i + 1, :] * rate)
            state = factor * state + us[i:i + 1, :] * bs[:, i:i + 1]
            hist[i * n:(i + 1) * n, :] = state.astype(BF16)
        return state

    def pair(j, state):
        finish(jnp.maximum(2 * j - 1, 0), hist_b)
        state = block(2 * j, state, hist_a)
        finish(2 * j, hist_a)
        return block(2 * j + 1, state, hist_b)

    state_s[...] = lax.fori_loop(0, blocks // 2, pair, state_s[...])
    finish(blocks - 1, hist_b)
    ssm = y_s[...] + skip_ref[...] * x
    sg = sigmoid(gate)
    gact = gate * sg
    gact_ref[...] = gact
    tail_ref[...] = (ssm * sg * (1.0 + gate * (1.0 - sg))).astype(BF16)
    gated_ref[...] = (ssm * gact).astype(BF16)


def back_step(selected, x, fresh, gact_ref, gg_ref, start_ref, dt_ref, slope_ref, stepw_ref, skip_ref,
              gvals_ref, gsel_ref, gstepw_ref, gbias_ref, gskip_ref,
              u_s, gy_s, gu_s, ah_s, bcoef_s, bt_s, hist_s, adj_a, harm_a, adj_b, harm_b, db_s, dc_s, carry_s, gd_s, rate_s, factor_s, kept_s, rank, n):
    length = x.shape[0]
    wide = BLOCK * n
    blocks = length // BLOCK
    carry_s[...] = jnp.where(fresh, 0.0, carry_s[...])
    gg = gg_ref[...]
    gy = gg * gact_ref[...]
    gskip_ref[...] += jnp.sum(gy * x, axis=0, keepdims=True)
    gy_s[...] = gy
    dt = dt_ref[...]
    u_s[...] = dt * x
    bt_s[...] = selected[rank:]
    tiles = tile_matrix(n, wide)
    spread = jnp.dot(selected[rank:].T[:, :n], tiles, preferred_element_type=F32)
    bcoef_s[...] = jnp.where(diagonal_mask(length, n, wide), spread, 0.0).astype(BF16)
    keep = diagonal_mask(BLOCK, n, wide)
    ones = keep.astype(BF16)
    lanes = lane_tiles(x.shape[1])
    state_s = start_ref

    def steps(lane):
        def again(k, state):
            at = pl.multiple_of(k * BLOCK, BLOCK)
            bs = pltpu.roll(bt_s[0:n, :], length - at, 1)
            dts = dt_ref[pl.ds(at, BLOCK), lane]
            us = u_s[pl.ds(at, BLOCK), lane]
            rate = rate_s[:, lane]
            for i in range(BLOCK):
                here = pl.ds(pl.multiple_of((at + i) * n, n), n)
                factor = jnp.exp2(dts[i:i + 1, :] * rate)
                factor_s[here, lane] = factor
                old = factor * state
                kept_s[here, lane] = old
                state = old + us[i:i + 1, :] * bs[:, i:i + 1]
                hist_s[here, lane] = state.astype(BF16)
            return state

        lax.fori_loop(0, blocks, again, state_s[:, lane])

        def products(k, adj_s, harm_s):
            at = pl.multiple_of(k * BLOCK, BLOCK)
            rows = pl.ds(at, BLOCK)
            adj = adj_s[:, lane]
            gu_s[rows, lane] = jnp.dot(bcoef_s[rows, :], adj, preferred_element_type=F32)
            ah_s[rows, lane] = jnp.dot(ones, harm_s[:, lane], preferred_element_type=F32)
            db = jnp.where(keep, nt_dot(u_s[rows, lane].astype(BF16), adj), 0.0)
            states = hist_s[pl.ds(pl.multiple_of(at * n, n), wide), lane]
            dc = jnp.where(keep, nt_dot(gy_s[rows, lane].astype(BF16), states), 0.0)
            if lane.start == 0:
                db_s[rows, :] = db
                dc_s[rows, :] = dc
            else:
                db_s[rows, :] += db
                dc_s[rows, :] += dc

        def block(k, carry, adj_s, harm_s):
            at = pl.multiple_of(k * BLOCK, BLOCK)
            cs = pltpu.roll(bt_s[n:2 * n, :], length - at, 1)
            dts = dt_ref[pl.ds(at, BLOCK), lane]
            gys = gy_s[pl.ds(at, BLOCK), lane]
            rate = rate_s[:, lane]
            gd = gd_s[:, lane]
            for i in range(BLOCK - 1, -1, -1):
                here = pl.ds(pl.multiple_of((at + i) * n, n), n)
                g = cs[:, i:i + 1] * gys[i:i + 1, :] + carry
                adj_s[i * n:(i + 1) * n, lane] = g.astype(BF16)
                carry = factor_s[here, lane] * g
                h = g * kept_s[here, lane]
                harm_s[i * n:(i + 1) * n, lane] = (h * rate).astype(BF16)
                gd = gd + dts[i:i + 1, :] * h
            gd_s[:, lane] = gd
            return carry

        def pair(j, carry):
            k = blocks - 1 - 2 * j
            if lane.start == 0:
                products(jnp.minimum(k + 1, blocks - 1), adj_b, harm_b)
            else:
                @pl.when(j > 0)
                def _():
                    products(k + 1, adj_b, harm_b)
            carry = block(k, carry, adj_a, harm_a)
            products(k, adj_a, harm_a)
            return block(k - 1, carry, adj_b, harm_b)

        carry_s[:, lane] = lax.fori_loop(0, blocks // 2, pair, carry_s[:, lane])
        products(0, adj_b, harm_b)

    for lane in lanes:
        steps(lane)
    gu = gu_s[...]
    gpre = ((x * gu + ah_s[...] * (1.0 / LOG2E)) * slope_ref[...]).astype(BF16)
    gvals_ref[...] = (gy * skip_ref[...] + dt * gu).astype(gvals_ref.dtype)
    gbias_ref[...] += jnp.sum(gpre.astype(F32), axis=0, keepdims=True)
    gstepw_ref[...] += jnp.dot(selected[:rank].astype(BF16), gpre, preferred_element_type=F32)
    fold = lambda ref: nt_dot(tiles.astype(BF16), ref[...].astype(BF16))
    gsel_ref[0:rank, :] = nt_dot(stepw_ref[...], gpre).astype(BF16)
    gsel_ref[rank:rank + n, :] = fold(db_s).astype(BF16)
    gsel_ref[rank + n:rank + 2 * n, :] = fold(dc_s).astype(BF16)


def conv_step(ci, fresh, taps_ref, bias_ref, selw_ref, ext_s):
    length = ci.shape[0]
    tap_count = taps_ref.shape[0]
    ext_s[0:8, :] = jnp.where(fresh, 0.0, ext_s[length:length + 8, :])
    ext_s[8:, :] = ci.astype(F32)
    total = bias_ref[...].astype(F32)
    for k in range(tap_count):
        total = total + taps_ref[k:k + 1, :].astype(F32) * ext_s[pl.ds(8 - tap_count + 1 + k, length), :]
    x = (total * sigmoid(total)).astype(BF16)
    return x, nt_dot(selw_ref[...], x).astype(BF16)


def conv_back_step(ci_ref, prev_ref, first, fresh, gvals_ref, gsel_ref, taps_ref, bias_ref, selw_ref,
                   gci_ref, gtaps_ref, gbias_ref, gselw_ref, ext_s, gext_s):
    length = ci_ref.shape[0]
    tap_count = taps_ref.shape[0]
    gext_s[length:, :] = jnp.where(fresh, 0.0, gext_s[length:, :])
    ext_s[8:, :] = ci_ref[...].astype(F32)
    before = prev_ref[...][length - 16:, :].astype(F32)[8:, :]
    ext_s[0:8, :] = jnp.where(first, 0.0, before)
    total = bias_ref[...].astype(F32)
    for k in range(tap_count):
        total = total + taps_ref[k:k + 1, :].astype(F32) * ext_s[pl.ds(8 - tap_count + 1 + k, length), :]
    sg = sigmoid(total)
    x = (total * sg).astype(BF16)
    gsel = gsel_ref[...]
    gvals = gvals_ref[...] + jnp.dot(gsel.astype(F32).T.astype(BF16), selw_ref[...], preferred_element_type=F32)
    gconv = gvals * sg * (1.0 + total * (1.0 - sg))
    gbias_ref[...] += jnp.sum(gconv, axis=0, keepdims=True)
    for k in range(tap_count):
        gtaps_ref[k:k + 1, :] += jnp.sum(gconv * ext_s[pl.ds(8 - tap_count + 1 + k, length), :], axis=0, keepdims=True)
    gselw_ref[...] += jnp.dot(gsel, x, preferred_element_type=F32)
    gext_s[0:length, :] = gconv
    gci = jnp.zeros_like(gconv)
    for k in range(tap_count):
        gci = gci + taps_ref[k:k + 1, :].astype(F32) * gext_s[pl.ds(tap_count - 1 - k, length), :]
    gci_ref[...] = gci.astype(BF16)
    gext_s[length:, :] = gconv[0:8, :]


MESH = pl.DeviceIdType.MESH


def remote(src, dst, send, recv, device):
    return pltpu.make_async_remote_copy(src_ref=src, dst_ref=dst, send_sem=send, recv_sem=recv, device_id=device, device_id_type=MESH)


def grid_of(chunks, copies):
    deep = max(1, copies // 2)
    return (chunks // deep, deep) if chunks % deep == 0 else (chunks, 1)


def meet(chunks, copies):
    me, mine = lax.axis_index("seq"), lax.axis_index("dp")
    barrier = pltpu.get_barrier_semaphore()

    def greet(k, _):
        pl.semaphore_signal(barrier, inc=1, device_id={"seq": lax.rem(me + k, chunks)}, device_id_type=MESH)
        return 0

    def greet_copy(k, _):
        pl.semaphore_signal(barrier, inc=1, device_id={"dp": lax.rem(mine + k, copies)}, device_id_type=MESH)
        return 0

    lax.fori_loop(1, chunks, greet, 0)
    if copies > 1:
        lax.fori_loop(1, copies, greet_copy, 0)
    pl.semaphore_wait(barrier, chunks - 1 + max(copies - 1, 0))


def gather_project_kernel(hid_ref, wq_ref, gain_ref, n_ref, ci_ref, gate_ref, w_ref, row_ref,
                          hid_v, gain_v, w_v, n_v, ci_v, gate_v,
                          load_sem, out_sem, hrecv, hside, hup, hdown, hlend,
                          w1send, w1recv, w2recv, w2send, w3send, gsend, grecv, *, chunks, copies, share, split):
    zs, ys = grid_of(chunks, copies)
    xs = copies // 2
    me, mine = lax.axis_index("seq"), lax.axis_index("dp")
    z, y = me // ys, me % ys
    x, c = mine // 2, mine % 2
    tokens, model = hid_v.shape[1:]
    width = ci_v.shape[1]
    inner = chunks * width
    half = tokens // 2
    even = ys == 2 and zs % 2 == 0
    piece = share // (copies if split else 1)
    spot = mine if split else 0
    load = pltpu.make_async_copy(hid_ref, hid_v.at[me], load_sem)
    load.start()
    meet(chunks, copies)
    load.wait()

    def w_rows(s, d):
        return pl.ds(pl.multiple_of(s * share + d * piece, piece), piece)

    def w_first(s, part):
        src = wq_ref.at[pl.ds(pl.multiple_of(spot * piece, piece), piece), pl.ds(pl.multiple_of(part * inner + s * width, width), width)]
        return remote(src, w_v.at[w_rows(me, spot), pl.ds(part * width, width)], w1send.at[s, part], w1recv.at[me, part], {"seq": s})

    def w_landed(s, part):
        dst = w_v.at[w_rows(s, spot), pl.ds(part * width, width)]
        return remote(dst, dst, w1send.at[s, part], w1recv.at[s, part], {"seq": s})

    def w_own(part):
        src = wq_ref.at[pl.ds(pl.multiple_of(spot * piece, piece), piece), pl.ds(pl.multiple_of(part * inner + me * width, width), width)]
        return pltpu.make_async_copy(src, w_v.at[w_rows(me, spot), pl.ds(part * width, width)], out_sem.at[part])

    def every_other(fn):
        def one(k, _):
            fn(lax.rem(me + k, chunks))
            return 0
        lax.fori_loop(1, chunks, one, 0)

    def gain_to(s):
        return remote(gain_ref, gain_v.at[me], gsend.at[s], grecv.at[me], {"seq": s})

    def gain_from(s):
        return remote(gain_v.at[s], gain_v.at[s], gsend.at[s], grecv.at[s], {"seq": s})

    def send_first(s):
        gain_to(s).start()
        w_first(s, 0).start()
        w_first(s, 1).start()

    def block(o, yy, h):
        return hid_v.at[o * ys + yy, pl.ds(h * half, half)]

    def up(o, h):
        return remote(block(o, y, h), block(o, y, h), hup.at[o, h], hrecv.at[o * ys + y, h], {"seq": (z + 1) * ys + y})

    def down(o, h):
        return remote(block(o, y, h), block(o, y, h), hdown.at[o, h], hrecv.at[o * ys + y, h], {"seq": (z - 1) * ys + y})

    def side(o, j, h):
        other = lax.rem(y + j, ys)
        return remote(block(o, y, h), block(o, y, h), hside.at[o, j - 1, h], hrecv.at[o * ys + y, h], {"seq": z * ys + other})

    def landed(o, yy, h):
        return remote(block(o, yy, h), block(o, yy, h), hside.at[o, 0, h], hrecv.at[o * ys + yy, h], {"seq": lax.rem(me + 1, chunks)})

    def when(cond, fn):
        pl.when(cond)(fn)

    gain_own = pltpu.make_async_copy(gain_ref, gain_v.at[me], out_sem.at[2])
    gain_own.start()
    for part in range(2):
        w_own(part).start()
    for h in range(2):
        when(z + 1 < zs, lambda: up(z, h).start())
        when(z > 0, lambda: down(z, h).start())
        for j in range(1, ys):
            side(z, j, h).start()
    every_other(send_first)

    partner = z + 1 - 2 * (z % 2)

    def sides(o, h, act):
        if even and h == 1:
            when(o != partner, lambda: act(side(o, 1, h)))
        else:
            for j in range(1, ys):
                act(side(o, j, h))

    def lend():
        return remote(block(z, 1 - y, 1), block(z, 1 - y, 1), hlend, hrecv.at[z * ys + 1 - y, 1], {"seq": partner * ys + y})

    def lend_on():
        if even:
            landed(z, 1 - y, 1).wait_recv()
            lend().start()

    def relay(k):
        for h in range(2):
            @pl.when(z - k >= 0)
            def _():
                landed(z - k, y, h).wait_recv()
                when(z + 1 < zs, lambda: up(z - k, h).start())
                sides(z - k, h, lambda one: one.start())

            @pl.when(z + k < zs)
            def _():
                landed(z + k, y, h).wait_recv()
                when(z > 0, lambda: down(z + k, h).start())
                sides(z + k, h, lambda one: one.start())

    def shared(s, d, sems, k, device):
        return remote(w_v.at[w_rows(s, d)], w_v.at[w_rows(s, d)], sems.at[s, k], w2recv.at[s, d], device)

    def spread(s):
        for j in range(1, xs):
            shared(s, mine, w2send, j - 1, {"dp": lax.rem(x + j, xs) * 2 + c}).start()
        shared(s, mine, w3send, 0, {"dp": x * 2 + 1 - c}).start()

    gain_own.wait()
    for part in range(2):
        w_own(part).wait()
    if split:
        spread(me)

    def take_first(s):
        gain_from(s).wait_recv()
        for part in range(2):
            w_landed(s, part).wait_recv()
        if split:
            spread(s)

    if zs > 1:
        relay(1)
    every_other(take_first)

    def take_second(s, _):
        for j in range(1, xs):
            d = lax.rem(x + j, xs) * 2 + c
            shared(s, d, w2send, j - 1, {"dp": d}).wait_recv()
            shared(s, d, w3send, j, {"dp": x * 2 + 1 - c}).start()
        return 0

    def take_third(s, _):
        for j in range(xs):
            d = lax.rem(x + j, xs) * 2 + 1 - c
            shared(s, d, w2send, 0, {"dp": d}).wait_recv()
        return 0

    if zs > 2:
        relay(2)
    lend_on()
    if split:
        lax.fori_loop(0, chunks, take_second, 0)
    if split:
        lax.fori_loop(0, chunks, take_third, 0)

    row_ref[...] = jnp.concatenate([gain_v[s] for s in range(chunks)], axis=-1)
    w_out = pltpu.make_async_copy(w_v, w_ref, load_sem)
    w_out.start()
    steps = 4 if width >= 512 else 1
    tile = 2 * width // steps

    def project(at):
        def rows(i, _):
            sl = pl.ds(pl.multiple_of(i * 32, 32), 32)
            h = hid_v[at, sl, :].astype(F32)
            inverse = lax.rsqrt(jnp.mean(h * h, axis=-1, keepdims=True) + EPSILON)
            n_v[sl, :] = (h * inverse * row_ref[...]).astype(BF16)
            return 0
        lax.fori_loop(0, tokens // 32, rows, 0)
        n_out = pltpu.make_async_copy(n_v, n_ref.at[at], out_sem.at[0])
        n_out.start()

        def columns(i, _):
            sl = pl.ds(pl.multiple_of(i * tile, tile), tile)
            got = jnp.dot(n_v[...], w_v[:, sl], preferred_element_type=F32)
            if steps == 1:
                ci_v[...] = got[:, :width].astype(BF16)
                gate_v[...] = got[:, width:]
            else:
                @pl.when(i < steps // 2)
                def _():
                    ci_v[:, sl] = got.astype(BF16)

                @pl.when(i >= steps // 2)
                def _():
                    gate_v[:, pl.ds(pl.multiple_of(i * tile - width, tile), tile)] = got
            return 0
        lax.fori_loop(0, steps, columns, 0)
        ci_out = pltpu.make_async_copy(ci_v, ci_ref.at[at], out_sem.at[1])
        gate_out = pltpu.make_async_copy(gate_v, gate_ref.at[at], out_sem.at[2])
        ci_out.start()
        gate_out.start()
        n_out.wait()
        ci_out.wait()
        gate_out.wait()

    def work(first, last):
        def one(i, _):
            k0, j = i // (2 * ys), i % (2 * ys)
            lower, yy = j // ys, j % ys
            own = yy == y
            k = k0 - jnp.where(own, 0, 1)
            o = z + k * (2 * lower - 1)
            ok = (k >= 0) & (k < zs) & (o >= 0) & (o < zs) & ((lower == 0) | (k > 0))
            if even:
                ok = ok & (own | (o != partner))

            @pl.when(ok & jnp.logical_not(own))
            def _():
                landed(o, yy, 0).wait_recv()
                if even:
                    when(o != z, lambda: landed(o, yy, 1).wait_recv())
                else:
                    landed(o, yy, 1).wait_recv()

            @pl.when(ok)
            def _():
                project(o * ys + yy)
            return 0
        lax.fori_loop(first * 2 * ys, last * 2 * ys, one, 0)

    work(0, min(2, zs))

    def later(k, _):
        relay(k)
        work(k - 1, k)
        return 0

    lax.fori_loop(3, zs, later, 0)
    work(max(2, zs - 1), zs)
    work(zs, zs + 1)
    if even:
        for h in range(2):
            landed(partner, 1 - y, h).wait_recv()
        project(partner * ys + 1 - y)
    w_out.wait()

    def drain_first(s):
        gain_to(s).wait_send()
        for part in range(2):
            w_first(s, part).wait_send()

    every_other(drain_first)

    def drain_second(s, _):
        for j in range(1, xs):
            shared(s, mine, w2send, j - 1, {"dp": mine}).wait_send()
        for j in range(xs):
            shared(s, mine, w3send, j, {"dp": mine}).wait_send()
        return 0

    if split:
        lax.fori_loop(0, chunks, drain_second, 0)

    def drain(k, _):
        for h in range(2):
            @pl.when(z - k >= 0)
            def _():
                when(z + 1 < zs, lambda: up(z - k, h).wait_send())
                sides(z - k, h, lambda one: one.wait_send())

            @pl.when((z + k < zs) & (k > 0))
            def _():
                when(z > 0, lambda: down(z + k, h).wait_send())
                sides(z + k, h, lambda one: one.wait_send())
        return 0

    lax.fori_loop(0, zs, drain, 0)
    for h in range(2):
        when(z > 0, lambda: down(z, h).wait_send())
    if even:
        lend().wait_send()


def gather_project(hidden, wq, gain, chunks, copies, share, split):
    tokens, model = hidden.shape
    width = wq.shape[1] // 2 // chunks
    zs, ys = grid_of(chunks, copies)
    any_spec = pl.BlockSpec(memory_space=pl.ANY)
    sds = jax.ShapeDtypeStruct
    dma = pltpu.SemaphoreType.DMA
    return pl.pallas_call(
        functools.partial(gather_project_kernel, chunks=chunks, copies=copies, share=share, split=split),
        in_specs=[any_spec] * 3,
        out_specs=[any_spec] * 4 + [pl.BlockSpec(memory_space=pltpu.VMEM)],
        out_shape=[sds((chunks, tokens, model), BF16), sds((chunks, tokens, width), BF16),
                   sds((chunks, tokens, width), F32), sds((model, 2 * width), BF16), sds((1, model), F32)],
        scratch_shapes=[
            pltpu.VMEM((chunks, tokens, model), BF16), pltpu.VMEM((chunks, 1, share), F32), pltpu.VMEM((model, 2 * width), BF16),
            pltpu.VMEM((tokens, model), BF16), pltpu.VMEM((tokens, width), BF16), pltpu.VMEM((tokens, width), F32),
            dma(()), dma((3,)), dma((chunks, 2)), dma((zs, max(1, ys - 1), 2)), dma((zs, 2)), dma((zs, 2)), dma(()),
            dma((chunks, 2)), dma((chunks, 2)), dma((chunks, copies)), dma((chunks, max(1, copies // 2))), dma((chunks, max(1, copies // 2))),
            dma((chunks,)), dma((chunks,)),
        ],
        compiler_params=pltpu.CompilerParams(collective_id=0, has_side_effects=True, vmem_limit_bytes=60 * 1024 * 1024),
        name="gather_project",
    )(hidden, wq, gain)


SPLIT = 9


def forward_kernel(ci_ref, gate_ref, gm_ref, taps_ref, cbias_ref, selw_ref, stepw_ref, sbias_ref, decay_ref, skip_ref, wout_ref,
                   gmall_ref, sel_ref, x_ref, gated_ref, gact_ref, dt_ref, slope_ref, start_ref, mixed_ref, gg_ref, ggate_ref,
                   gate_v, part_v, recv_v, x_v, gated_v, gact_v, tail_v, dt_v, slope_v, start_v,
                   gm_v, mixed_v, gg_v, ggate_v,
                   ext_s, u_s, y_s, coef_s, bt_s, hist_a, hist_b, state_s, rate_s,
                   load_sem, own_sem, out_sem, gm_sem, mixed_sem, gg_sem, grecv, gside, gup, gdown, glend, send1, recv1, send2, recv2, *, chunks, copies, n):
    zs, ys = grid_of(chunks, copies)
    me = lax.axis_index("seq")
    z, y = me // ys, me % ys
    tokens, model = gm_ref.shape
    rows, length, width = ci_ref.shape[1:]
    rank = stepw_ref.shape[0]
    half = tokens // 2
    even = ys == 2 and zs % 2 == 0
    load = pltpu.make_async_copy(gate_ref, gate_v, load_sem)
    load.start()
    own = pltpu.make_async_copy(gm_ref, gmall_ref.at[me], own_sem)
    own.start()
    meet(chunks, 1)

    def block(o, yy, h):
        return gmall_ref.at[o * ys + yy, pl.ds(h * half, half)]

    def source(o, h, k):
        return gm_ref.at[pl.ds(h * half, half)] if k is None else block(o, y, h)

    def up(o, h, k=0):
        return remote(source(o, h, k), block(o, y, h), gup.at[o, h], grecv.at[o * ys + y, h], {"seq": (z + 1) * ys + y})

    def down(o, h, k=0):
        return remote(source(o, h, k), block(o, y, h), gdown.at[o, h], grecv.at[o * ys + y, h], {"seq": (z - 1) * ys + y})

    def side(o, j, h, k=0):
        return remote(source(o, h, k), block(o, y, h), gside.at[o, j - 1, h], grecv.at[o * ys + y, h], {"seq": z * ys + lax.rem(y + j, ys)})

    def landed(o, yy, h):
        return remote(block(o, yy, h), block(o, yy, h), gside.at[o, 0, h], grecv.at[o * ys + yy, h], {"seq": lax.rem(me + 1, chunks)})

    def when(cond, fn):
        pl.when(cond)(fn)

    def first_sends(h):
        when(z + 1 < zs, lambda: up(z, h, None).start())
        when(z > 0, lambda: down(z, h, None).start())
        for j in range(1, ys):
            side(z, j, h, None).start()

    first_sends(0)

    partner = z + 1 - 2 * (z % 2)

    def sides(o, h, act):
        if even and h == 1:
            when(o != partner, lambda: act(side(o, 1, h)))
        else:
            for j in range(1, ys):
                act(side(o, j, h))

    def lend():
        return remote(block(z, 1 - y, 1), block(z, 1 - y, 1), glend, grecv.at[z * ys + 1 - y, 1], {"seq": partner * ys + y})

    def lend_on():
        if even:
            landed(z, 1 - y, 1).wait_recv()
            lend().start()

    def relay(k):
        for h in range(2):
            @pl.when(z - k >= 0)
            def _():
                landed(z - k, y, h).wait_recv()
                when(z + 1 < zs, lambda: up(z - k, h).start())
                sides(z - k, h, lambda one: one.start())

            @pl.when(z + k < zs)
            def _():
                landed(z + k, y, h).wait_recv()
                when(z > 0, lambda: down(z + k, h).start())
                sides(z + k, h, lambda one: one.start())

    rate_s[...] = -jnp.exp(decay_ref[...].astype(F32)) * LOG2E

    def conv(i, _):
        r, c = i // chunks, i % chunks
        x, part = conv_step(ci_ref[c, r], c == 0, taps_ref, cbias_ref, selw_ref, ext_s)
        x_v[c, r] = x
        part_v[c, r] = part
        return 0

    lax.fori_loop(0, rows * chunks, conv, 0)
    x_out = pltpu.make_async_copy(x_v, x_ref, out_sem.at[0, 0])
    x_out.start()

    def first(s):
        return remote(part_v.at[s], recv_v.at[me], send1.at[s], recv1.at[me], {"seq": s})

    def landed_first(s):
        return remote(part_v.at[s], recv_v.at[s], send1.at[s], recv1.at[s], {"seq": s})

    def second(s):
        return remote(sel_ref.at[me], sel_ref.at[me], send2.at[s], recv2.at[me], {"seq": s})

    def landed_second(s):
        return remote(sel_ref.at[s], sel_ref.at[s], send2.at[s], recv2.at[s], {"seq": s})

    def every_other(fn):
        def one(k, _):
            fn(lax.rem(me + k, chunks))
            return 0
        lax.fori_loop(1, chunks, one, 0)

    every_other(lambda s: first(s).start())
    first_sends(1)
    recv_v[me] = part_v[me]
    every_other(lambda s: landed_first(s).wait_recv())
    total = recv_v[0].astype(F32)
    for s in range(1, chunks):
        total = total + recv_v[s].astype(F32)
    sel_ref[me] = total.astype(BF16)
    every_other(lambda s: second(s).start())
    if zs > 1:
        relay(1)
    if zs <= 2:
        lend_on()
    every_other(lambda s: landed_second(s).wait_recv())
    load.wait()
    pairs = ((gated_v, gated_ref), (gact_v, gact_ref), (dt_v, dt_ref), (slope_v, slope_ref), (start_v, start_ref))

    def outs(c, r):
        return [pltpu.make_async_copy(src.at[c, r], dst.at[c, r], out_sem.at[1 + k, c * rows + r]) for k, (src, dst) in enumerate(pairs)]

    def scan(i, _):
        r, c = i // chunks, i % chunks
        start_v[c, r] = jnp.where(c == 0, 0.0, state_s[...])
        scan_step(sel_ref[c, r].astype(F32), x_v[c, r].astype(F32), gate_v[c, r], c == 0, stepw_ref, sbias_ref, skip_ref,
                  gated_v.at[c, r], gact_v.at[c, r], tail_v.at[c, r], dt_v.at[c, r], slope_v.at[c, r],
                  u_s, y_s, coef_s, bt_s, hist_a, hist_b, state_s, rate_s, rank, n)
        for one in outs(c, r):
            one.start()
        return 0

    count = rows * chunks
    if zs > 2:
        relay(2)
        lend_on()
    cuts = [count * SPLIT // 16 + (count - count * SPLIT // 16) * k // max(1, zs - 3) for k in range(zs - 2)] if zs > 3 else []
    at = 0
    for k, cut in enumerate(cuts[:-1]):
        lax.fori_loop(at, cut, scan, 0)
        relay(3 + k)
        at = cut
    lax.fori_loop(at, count, scan, 0)

    tile = min(512, model)

    def mixed_out(s):
        return pltpu.make_async_copy(mixed_v.at[s % 2], mixed_ref.at[s], mixed_sem.at[s % 2])

    def mix(s, _):
        @pl.when(s >= 2)
        def _():
            mixed_out(s - 2).wait()

        lhs = gated_v[s].reshape(tokens, width)

        def one(i, _):
            sl = pl.ds(pl.multiple_of(i * tile, tile), tile)
            mixed_v[s % 2, :, sl] = jnp.dot(lhs, wout_ref[:, sl], preferred_element_type=F32).astype(BF16)
            return 0
        lax.fori_loop(0, model // tile, one, 0)
        mixed_out(s).start()
        return 0

    lax.fori_loop(0, chunks, mix, 0)
    for s in range(chunks - 2, chunks):
        mixed_out(s).wait()

    own.wait()

    def bring(s):
        return pltpu.make_async_copy(gmall_ref.at[s], gm_v, gm_sem)

    def back(s):
        bring(s).start()
        bring(s).wait()
        got = nt_dot(gm_v[...], wout_ref[...])
        gg_v[...] = got.reshape(gg_v.shape)
        ggate_v[...] = (got * tail_v[s].reshape(tokens, width).astype(F32)).astype(BF16).reshape(ggate_v.shape)
        one, two = pltpu.make_async_copy(gg_v, gg_ref.at[s], gg_sem.at[0]), pltpu.make_async_copy(ggate_v, ggate_ref.at[s], gg_sem.at[1])
        one.start()
        two.start()
        one.wait()
        two.wait()

    last = [[k] + [q for q in range(zs) if q not in (k, k + 1 - 2 * (k % 2))] + [k + 1 - 2 * (k % 2)] for k in range(zs)] if even else [list(range(zs))] * zs

    def others(i, _):
        lower, k = i // zs, i % zs
        o = 0
        for p in range(zs):
            for q in range(zs):
                o = o + jnp.where((z == p) & (k == q), last[p][q], 0)

        @pl.when(lower > 0)
        def _():
            landed(o, lax.rem(y + lower, ys), 0).wait_recv()
            if even:
                when(o != z, lambda: landed(o, 1 - y, 1).wait_recv())
            else:
                landed(o, lax.rem(y + lower, ys), 1).wait_recv()

        back(o * ys + lax.rem(y + lower, ys))
        return 0

    lax.fori_loop(0, ys * zs, others, 0)
    x_out.wait()

    def settle(i, _):
        for one in outs(i // rows, i % rows):
            one.wait()
        return 0

    lax.fori_loop(0, count, settle, 0)
    every_other(lambda s: first(s).wait_send())
    every_other(lambda s: second(s).wait_send())

    def drain(k, _):
        for h in range(2):
            @pl.when(z - k >= 0)
            def _():
                when(z + 1 < zs, lambda: up(z - k, h).wait_send())
                sides(z - k, h, lambda one: one.wait_send())

            @pl.when((z + k < zs) & (k > 0))
            def _():
                when(z > 0, lambda: down(z + k, h).wait_send())
                sides(z + k, h, lambda one: one.wait_send())
        return 0

    lax.fori_loop(0, zs, drain, 0)
    for h in range(2):
        when(z > 0, lambda: down(z, h).wait_send())
    if even:
        lend().wait_send()


def forward(ci, gate, gm, taps, cbias, selw, stepw, sbias, decay, skip, wout, copies, n):
    chunks, rows, length, width = ci.shape
    tokens, model = gm.shape
    zs, ys = grid_of(chunks, copies)
    wide = BLOCK * n
    sds = jax.ShapeDtypeStruct
    dma = pltpu.SemaphoreType.DMA
    vmem = pl.BlockSpec(memory_space=pltpu.VMEM)
    hbm = pl.BlockSpec(memory_space=pl.ANY)
    coef = (chunks, rows, selw.shape[0], length)
    starts = (chunks, rows, n, width)
    full = ci.shape
    return pl.pallas_call(
        functools.partial(forward_kernel, chunks=chunks, copies=copies, n=n),
        in_specs=[vmem, hbm] + [vmem] * 9,
        out_specs=[hbm, vmem] + [hbm] * 9,
        out_shape=[sds((chunks, tokens, model), BF16), sds(coef, BF16), sds(full, BF16), sds(full, BF16), sds(full, F32),
                   sds(full, F32), sds(full, F32), sds(starts, F32), sds((chunks, tokens, model), BF16), sds(full, F32), sds(full, BF16)],
        scratch_shapes=[
            pltpu.VMEM(full, F32), pltpu.VMEM(coef, BF16), pltpu.VMEM(coef, BF16), pltpu.VMEM(full, BF16), pltpu.VMEM(full, BF16),
            pltpu.VMEM(full, F32), pltpu.VMEM(full, BF16), pltpu.VMEM(full, F32), pltpu.VMEM(full, F32), pltpu.VMEM(starts, F32),
            pltpu.VMEM((tokens, model), BF16), pltpu.VMEM((2, tokens, model), BF16), pltpu.VMEM(full[1:], F32), pltpu.VMEM(full[1:], BF16),
            pltpu.VMEM((length + 8, width), F32), pltpu.VMEM((length, width), F32), pltpu.VMEM((length, width), F32),
            pltpu.VMEM((length, wide), BF16), pltpu.VMEM((2 * n, length), F32), pltpu.VMEM((wide, width), BF16), pltpu.VMEM((wide, width), BF16),
            pltpu.VMEM((n, width), F32), pltpu.VMEM((n, width), F32),
            dma(()), dma(()), dma((7, rows * chunks)), dma(()), dma((2,)), dma((2,)), dma((chunks, 2)), dma((zs, max(1, ys - 1), 2)), dma((zs, 2)), dma((zs, 2)), dma(()),
            dma((chunks,)), dma((chunks,)), dma((chunks,)), dma((chunks,)),
        ],
        compiler_params=pltpu.CompilerParams(collective_id=1, has_side_effects=True, vmem_limit_bytes=60 * 1024 * 1024),
        name="forward",
    )(ci, gate, gm, taps, cbias, selw, stepw, sbias, decay, skip, wout)


class Exchange:
    def __init__(self, gin, out, bufs, sems, chunks, copies):
        self.gin, self.out = gin, out
        self.g1, self.mine_v, self.g2, self.t_v, self.fin = bufs
        self.load, self.s1, self.r1, self.s2, self.r2, self.s3, self.r3, self.s4, self.r4 = sems
        self.chunks, self.xs = chunks, copies // 2
        self.me, self.mine = lax.axis_index("seq"), lax.axis_index("dp")
        self.x, self.c = self.mine // 2, self.mine % 2
        self.piece, self.width = self.t_v.shape[1:]

    def own(self, q):
        return pltpu.make_async_copy(self.gin.at[:, q * 2 + self.c], self.mine_v.at[q], self.load.at[q])

    def to_core(self, q):
        return remote(self.gin.at[:, q * 2 + 1 - self.c], self.g1.at[q], self.s1.at[q], self.r1.at[q], {"dp": self.x * 2 + 1 - self.c})

    def across(self, q):
        return remote(self.mine_v.at[q], self.g2.at[self.x], self.s2.at[q], self.r2.at[self.x], {"dp": q * 2 + self.c})

    def from_across(self, q):
        return remote(self.g2.at[q], self.g2.at[q], self.s2.at[q], self.r2.at[q], {"dp": q * 2 + self.c})

    def columns(self, s):
        return self.fin.at[:, pl.ds(pl.multiple_of(s * self.width, self.width), self.width)]

    def turn(self, s):
        return remote(self.t_v.at[s], self.columns(self.me), self.s3.at[s], self.r3.at[self.me], {"seq": s})

    def turned(self, s):
        return remote(self.columns(s), self.columns(s), self.s3.at[s], self.r3.at[s], {"seq": s})

    def rows_of(self, d):
        return self.out.at[pl.ds(pl.multiple_of(d * self.piece, self.piece), self.piece)]

    def share_to(self, k, d):
        return remote(self.fin, self.rows_of(self.mine), self.s4.at[k], self.r4.at[self.mine], {"dp": d})

    def hand_on(self, row, k):
        return remote(self.rows_of(row), self.rows_of(row), self.s4.at[k], self.r4.at[row], {"dp": self.x * 2 + 1 - self.c})

    def shared(self, d):
        return remote(self.rows_of(d), self.rows_of(d), self.s4.at[0], self.r4.at[d], {"dp": d})

    def keep(self):
        return pltpu.make_async_copy(self.fin, self.rows_of(self.mine), self.load.at[self.xs])

    def others(self, fn):
        def one(k, _):
            fn(lax.rem(self.me + k, self.chunks))
            return 0
        lax.fori_loop(1, self.chunks, one, 0)

    def column_peers(self):
        return [lax.rem(self.x + j, self.xs) * 2 + self.c for j in range(1, self.xs)]

    def begin(self):
        for q in range(self.xs):
            self.own(q).start()
            self.to_core(q).start()

    def chip(self):
        for q in range(self.xs):
            self.own(q).wait()
            self.to_core(q).wait_recv()

            def fold(s, _):
                self.mine_v[q, s] = (self.mine_v[q, s].astype(F32) + self.g1[q, s].astype(F32)).astype(BF16)
                return 0
            lax.fori_loop(0, self.chunks, fold, 0)
            pl.when(q != self.x)(lambda: self.across(q).start())

    def spread(self):
        for q in range(self.xs):
            pl.when(q != self.x)(lambda: self.from_across(q).wait_recv())

        def fold(s, _):
            total = self.mine_v[self.x, s].astype(F32)
            for j in range(1, self.xs):
                total = total + self.g2[lax.rem(self.x + j, self.xs), s].astype(F32)
            self.t_v[s] = total.astype(BF16)
            return 0
        lax.fori_loop(0, self.chunks, fold, 0)
        self.others(lambda s: self.turn(s).start())
        self.columns(self.me)[...] = self.t_v[self.me]

    def share(self):
        self.others(lambda s: self.turned(s).wait_recv())
        for j, d in enumerate(self.column_peers()):
            self.share_to(1 + j, d).start()
        self.share_to(0, self.x * 2 + 1 - self.c).start()
        self.keep().start()

    def pass_on(self):
        for j, d in enumerate(self.column_peers()):
            self.shared(d).wait_recv()
            self.hand_on(d, self.xs + j).start()

    def finish(self):
        self.keep().wait()
        for j in range(self.xs):
            self.shared(lax.rem(self.x + j, self.xs) * 2 + 1 - self.c).wait_recv()
        for q in range(self.xs):
            self.to_core(q).wait_send()
            pl.when(q != self.x)(lambda: self.across(q).wait_send())
        self.others(lambda s: self.turn(s).wait_send())
        for j in range(self.xs):
            self.share_to(j, self.mine).wait_send()
        for j, d in enumerate(self.column_peers()):
            self.hand_on(d, self.xs + j).wait_send()


def exchange_scratch(chunks, copies, piece, width):
    xs = copies // 2
    dma = pltpu.SemaphoreType.DMA
    slab = (chunks, piece, width)
    bufs = [pltpu.VMEM((xs,) + slab, BF16), pltpu.VMEM((xs,) + slab, BF16), pltpu.VMEM((xs,) + slab, BF16), pltpu.VMEM(slab, BF16),
            pltpu.VMEM((piece, chunks * width), BF16)]
    return bufs + [dma((xs + 1,)), dma((xs,)), dma((xs,)), dma((xs,)), dma((xs,)), dma((chunks,)), dma((chunks,)), dma((2 * xs,)), dma((copies,))]


def order_of(zs):
    return [sorted(range(zs), key=lambda t: (-abs(t - z), t)) for z in range(zs)]


def scatter_kernel(*refs, chunks, copies, split):
    gc_ref, gg_ref, w_ref, late_ref = refs[:4]
    norm_ref = refs[4] if split else None
    refs = refs[4 + split:]
    red_ref, sum_ref = refs[:2]
    all_ref = refs[2] if split else None
    refs = refs[2 + split:]
    (ysend_v, yrecv_v, own_v, zrecv_v, lend_v, late_v, w_v, load_sem,
     ysend, yrecv, zup, zdown, zrecv, lend_sem, lsend, lrecv) = refs[:16]
    if split:
        gin_v, norm_v, norm_sem = refs[16:19]
        trade = Exchange(gin_v, all_ref, refs[19:24], refs[24:33], chunks, copies)
    zs, ys = grid_of(chunks, copies)
    xs = copies // 2
    me, mine = lax.axis_index("seq"), lax.axis_index("dp")
    z, y = me // ys, me % ys
    x, c = mine // 2, mine % 2
    tokens, width = gc_ref.shape[1:]
    model = w_ref.shape[0]
    half = tokens // 2
    tile = min(256, model)
    tables = order_of(zs)
    partner = z + 1 - 2 * (z % 2)

    def dest(i):
        got = 0
        for k in range(zs):
            got = got + jnp.where(z == k, tables[k][i], 0)
        return got

    w_in = pltpu.make_async_copy(w_ref, w_v, load_sem.at[0])
    w_in.start()

    def norm_in(s):
        cols = pl.ds(pl.multiple_of(s * norm_v.shape[-1], norm_v.shape[-1]), norm_v.shape[-1])
        return pltpu.make_async_copy(norm_ref.at[:, :, cols], norm_v.at[s % 2], norm_sem.at[s % 2])

    if split:
        norm_in(0).start()
    meet(chunks, copies)

    def late_to(d):
        return remote(late_ref, late_v.at[mine], lsend.at[d], lrecv.at[mine], {"dp": d})

    def late_from(d):
        return remote(late_v.at[d], late_v.at[d], lsend.at[d], lrecv.at[d], {"dp": d})

    def every_copy(fn):
        def one(k, _):
            fn(lax.rem(mine + k, copies))
            return 0
        lax.fori_loop(1, copies, one, 0)

    w_in.wait()

    def partial(s, out, at):
        def one(i, _):
            sl = pl.ds(pl.multiple_of(i * tile, tile), tile)
            got = nt_dot(gc_ref[s], w_v[sl, :width]) + nt_dot(gg_ref[s], w_v[sl, width:])
            out[at, :, sl] = got.astype(BF16)
            return 0
        lax.fori_loop(0, model // tile, one, 0)

    def to_side(i, j, h):
        rows = pl.ds(h * half, half)
        k = i * (ys - 1) + j - 1
        return remote(ysend_v.at[k % ysend_v.shape[0], rows], yrecv_v.at[k, rows], ysend.at[k, h], yrecv.at[k, h], {"seq": z * ys + lax.rem(y + j, ys)})

    slots = ysend_v.shape[0]
    even = ys == 2 and zs % 2 == 0 and slots == zs

    def lend(i):
        return remote(ysend_v.at[i, pl.ds(half, half)], lend_v, lend_sem.at[0], lend_sem.at[1], {"seq": partner * ys + y})

    def send_side(i, j, h):
        if not even or h == 0:
            to_side(i, j, h).start()
            return

        @pl.when(dest(i) != partner)
        def _():
            if i == zs - 1:
                lend(i).wait_recv()

                def one(r, _):
                    sl = pl.ds(pl.multiple_of(half + r * 32, 32), 32)
                    ysend_v[i, sl, :] = (ysend_v[i, sl, :].astype(F32) + lend_v[pl.ds(pl.multiple_of(r * 32, 32), 32), :].astype(F32)).astype(BF16)
                    return 0
                lax.fori_loop(0, half // 32, one, 0)
            to_side(i, j, h).start()

    def if_sent(i, h, fn):
        if even and h == 1:
            pl.when(dest(i) != partner)(fn)
        else:
            fn()

    ahead = 2 if slots == zs * (ys - 1) else zs
    def outgoing(i):
        for j in range(1, ys):
            k = i * (ys - 1) + j - 1
            if k >= slots:
                for h in range(2):
                    to_side((k - slots) // (ys - 1), (k - slots) % (ys - 1) + 1, h).wait_send()
            partial(dest(i) * ys + lax.rem(y + j, ys), ysend_v, k % slots)
            if i < ahead:
                for h in range(2):
                    send_side(i, j, h)
            if even:
                pl.when(dest(i) == partner)(lambda: lend(i).start())

    if split:
        for i in range(min(2, zs)):
            outgoing(i)

        def weights(s, _):
            @pl.when(s + 1 < chunks)
            def _():
                norm_in(s + 1).start()

            norm_in(s).wait()
            n_all = norm_v[s % 2].reshape(chunks * tokens, norm_v.shape[-1])
            got = lax.dot_general(n_all, gc_ref[...].reshape(chunks * tokens, width), (((0,), (0,)), ((), ())), preferred_element_type=F32)
            gin_v[s] = got.astype(BF16).reshape(gin_v.shape[1:])
            return 0

        lax.fori_loop(0, chunks, weights, 0)
        trade.begin()

    for i in range(min(2, zs) if split else 0, zs):
        outgoing(i)
    if split:
        trade.chip()
    every_copy(lambda d: late_to(d).start())

    def arrived(i, j, h):
        rows = pl.ds(h * half, half)
        k = i * (ys - 1) + j - 1
        return remote(yrecv_v.at[k, rows], yrecv_v.at[k, rows], ysend.at[k, h], yrecv.at[k, h], {"seq": z * ys + lax.rem(y + j, ys)})

    def climb(t, h):
        rows = pl.ds(h * half, half)
        return remote(own_v.at[t, rows], zrecv_v.at[t, rows], zup.at[t, h], zrecv.at[t, h], {"seq": (z + 1) * ys + y})

    def sink(t, h):
        rows = pl.ds(h * half, half)
        slot = jnp.where(t == z - 1, zs, t)
        return remote(own_v.at[t, rows], zrecv_v.at[slot, rows], zdown.at[t, h], zrecv.at[slot, h], {"seq": (z - 1) * ys + y})

    def from_z(slot, h):
        rows = pl.ds(h * half, half)
        return remote(zrecv_v.at[slot, rows], zrecv_v.at[slot, rows], zup.at[0, h], zrecv.at[slot, h], {"seq": lax.rem(me + 1, chunks)})

    def accumulate(t, h, read):
        def one(r, _):
            sl = pl.ds(pl.multiple_of(h * half + r * 32, 32), 32)
            own_v[t, sl, :] = (own_v[t, sl, :].astype(F32) + read(sl)).astype(BF16)
            return 0
        lax.fori_loop(0, half // 32, one, 0)

    for i in range(zs):
        t = dest(i)
        partial(t * ys + y, own_v, t)
        for h in range(2):
            for j in range(1, ys):
                if_sent(i, h, lambda: arrived(i, ys - j, h).wait_recv())

            def side_sum(sl):
                total = yrecv_v[i * (ys - 1), sl, :].astype(F32)
                for j in range(2, ys):
                    total = total + yrecv_v[i * (ys - 1) + j - 1, sl, :].astype(F32)
                return total

            if ys > 1:
                if_sent(i, h, lambda: accumulate(t, h, side_sum))

            @pl.when(((t > z) & (z > 0)) | ((t == z) & (z > 0)))
            def _():
                from_z(t, h).wait_recv()
                accumulate(t, h, lambda sl: zrecv_v[t, sl, :].astype(F32))

            @pl.when((t < z) & (z + 1 < zs))
            def _():
                from_z(t, h).wait_recv()
                accumulate(t, h, lambda sl: zrecv_v[t, sl, :].astype(F32))

            @pl.when((t == z) & (z + 1 < zs))
            def _():
                from_z(zs, h).wait_recv()
                accumulate(t, h, lambda sl: zrecv_v[zs, sl, :].astype(F32))

            @pl.when(t > z)
            def _():
                climb(t, h).start()

            @pl.when(t < z)
            def _():
                sink(t, h).start()
        if split and i == 0:
            trade.spread()
        if split and i == min(1, zs - 1):
            trade.share()
        if i + ahead < zs:
            for j in range(1, ys):
                for h in range(2):
                    send_side(i + ahead, j, h)

    red_ref[...] = own_v[z]
    every_copy(lambda d: late_from(d).wait_recv())
    total = late_ref[...].astype(F32)
    for k in range(1, copies):
        total = total + late_v[lax.rem(mine + k, copies)].astype(F32)
    sum_ref[...] = total
    if split:
        trade.pass_on()
        trade.finish()

    every_copy(lambda d: late_to(d).wait_send())
    count = zs * (ys - 1)
    for k in range(max(0, count - slots), count):
        for h in range(2):
            if_sent(k // (ys - 1), h, lambda: to_side(k // (ys - 1), k % (ys - 1) + 1, h).wait_send())
    if even:
        lend(0).wait_send()
    for i in range(zs):
        t = dest(i)
        for h in range(2):
            @pl.when(t > z)
            def _():
                climb(t, h).wait_send()

            @pl.when(t < z)
            def _():
                sink(t, h).wait_send()


def scatter_sums(gc, gg, w_all, late, normed, chunks, copies, split):
    tokens, width = gc.shape[1:]
    model = w_all.shape[0]
    zs, ys = grid_of(chunks, copies)
    xs = max(1, copies // 2)
    others = max(1, zs * (ys - 1))
    slots = min(others, 4)
    any_spec = pl.BlockSpec(memory_space=pl.ANY)
    vmem = pl.BlockSpec(memory_space=pltpu.VMEM)
    sds = jax.ShapeDtypeStruct
    dma = pltpu.SemaphoreType.DMA
    args = [gc, gg, w_all, late]
    in_specs = [vmem, vmem, any_spec, vmem]
    out_specs = [vmem, vmem]
    out_shape = [sds((tokens, model), BF16), sds(late.shape, F32)]
    scratch = [pltpu.VMEM((slots, tokens, model), BF16), pltpu.VMEM((others, tokens, model), BF16),
               pltpu.VMEM((zs, tokens, model), BF16), pltpu.VMEM((zs + 1, tokens, model), BF16), pltpu.VMEM((tokens // 2, model), BF16),
               pltpu.VMEM((copies,) + late.shape, BF16), pltpu.VMEM(w_all.shape, BF16)]
    sems = [dma((1,)), dma((others, 2)), dma((others, 2)), dma((zs, 2)), dma((zs, 2)), dma((zs + 1, 2)), dma((2,)), dma((copies,)), dma((copies,))]
    if split:
        share = model // chunks
        piece = share // copies
        args.append(normed)
        in_specs.append(any_spec)
        out_specs.append(any_spec)
        out_shape.append(sds((share, chunks * width), BF16))
        sems += [pltpu.VMEM((chunks, copies, piece, width), BF16), pltpu.VMEM((2, chunks, tokens, share), BF16), dma((2,))]
        sems += exchange_scratch(chunks, copies, piece, width)
    return pl.pallas_call(
        functools.partial(scatter_kernel, chunks=chunks, copies=copies, split=split),
        in_specs=in_specs,
        out_specs=out_specs,
        out_shape=out_shape,
        scratch_shapes=scratch + sems,
        compiler_params=pltpu.CompilerParams(collective_id=3, has_side_effects=True, vmem_limit_bytes=62 * 1024 * 1024),
        name="scatter_sums",
    )(*args)
def backward_kernel(*refs, chunks, copies, n, inside, extra, split):
    ins = 14 + (1 if inside else 0) + (1 if split else 0) + (1 if extra else 0)
    (gg_ref, gact_ref, x_ref, dt_ref, slope_ref, start_ref, sel_ref, ci_ref, stepw_ref, decay_ref, skip_ref,
     taps_ref, cbias_ref, selw_ref) = refs[:14]
    mixed_ref = refs[14] if inside else None
    gin_ref = refs[ins - 1 - extra] if split else None
    gout_ref = refs[ins - 1] if extra else None
    outs = 2 + (1 if inside else 0) + (1 if split else 0) + (1 if extra else 0)
    gci_ref, late_ref = refs[ins:ins + 2]
    red_ref = refs[ins + 2] if inside else None
    all_ref = refs[ins + outs - 1 - extra] if split else None
    gsum_ref = refs[ins + outs - 1] if extra else None
    refs = refs[ins + outs:]
    (gg_v, gact_v, x_v, dt_v, slope_v, start_v, gci_v, gvals_v, part_v, recv_v, sel2_v,
     u_s, gy_s, gu_s, ah_s, bcoef_s, bt_s, hist_s, adj_a, harm_a, adj_b, harm_b, db_s, dc_s, carry_s, gd_s, rate_s, factor_s, kept_s,
     gstepw_ref, gsbias_ref, gskip_ref, gtaps_ref, gcbias_ref, gselw_ref,
     ext_s, gext_s, in_sem, gci_sem, send1, recv1, send2, recv2) = refs[:43]
    refs = refs[43:]
    if inside:
        own_v, yrecv_v, zrecv_v, own_sem, ysend, yrecv, zup, zdown, zrecv = refs[:9]
        refs = refs[9:]
    if extra:
        core_v, half_v, far_v, esend, erecv, asend, arecv, bsend, brecv = refs[:9]
        refs = refs[9:]
    if split:
        trade = Exchange(gin_ref, all_ref, refs[:5], refs[5:14], chunks, copies)
    zs, ys = grid_of(chunks, copies)
    xs = copies // 2
    me, mine = lax.axis_index("seq"), lax.axis_index("dp")
    z, y = me // ys, me % ys
    xd, cd = mine // 2, mine % 2
    rows = sel_ref.shape[1]
    rank = stepw_ref.shape[0]
    count = rows * chunks

    def where_of(i):
        return chunks - 1 - i % chunks, i // chunks

    streams = ((gg_ref, gg_v), (gact_ref, gact_v), (x_ref, x_v), (dt_ref, dt_v), (slope_ref, slope_v), (start_ref, start_v))

    def fetch(i):
        c, r = where_of(i)
        return [pltpu.make_async_copy(src.at[c, r], dst.at[i % 2], in_sem.at[k, i % 2]) for k, (src, dst) in enumerate(streams)]

    for one in fetch(0):
        one.start()
    if inside:
        tokens, model = red_ref.shape
        half = tokens // 2
        own_loads = [pltpu.make_async_copy(mixed_ref.at[t * ys + y], own_v.at[t], own_sem.at[t]) for t in range(zs)]
        for one in own_loads:
            one.start()
    meet(chunks, copies if extra else 1)

    if split:
        trade.begin()

    if inside:
        tables = order_of(zs)

        def dest(i):
            got = 0
            for k in range(zs):
                for q in range(zs):
                    got = got + jnp.where((z == k) & (i == q), tables[k][q], 0)
            return got

        def part_rows(h):
            return pl.ds(h * half, half)

        def to_side(i, h):
            return remote(mixed_ref.at[dest(i) * ys + 1 - y, part_rows(h)], yrecv_v.at[i, part_rows(h)], ysend.at[i, h], yrecv.at[i, h], {"seq": z * ys + 1 - y})

        def arrived(i, h):
            return remote(yrecv_v.at[i, part_rows(h)], yrecv_v.at[i, part_rows(h)], ysend.at[i, h], yrecv.at[i, h], {"seq": z * ys + 1 - y})

        def climb(t, h):
            return remote(own_v.at[t, part_rows(h)], zrecv_v.at[t, part_rows(h)], zup.at[t, h], zrecv.at[t, h], {"seq": (z + 1) * ys + y})

        def sink(t, h):
            slot = jnp.where(t == z - 1, zs, t)
            return remote(own_v.at[t, part_rows(h)], zrecv_v.at[slot, part_rows(h)], zdown.at[t, h], zrecv.at[slot, h], {"seq": (z - 1) * ys + y})

        def from_z(slot, h):
            return remote(zrecv_v.at[slot, part_rows(h)], zrecv_v.at[slot, part_rows(h)], zup.at[0, h], zrecv.at[slot, h], {"seq": lax.rem(me + 1, chunks)})

        def accumulate(t, h, buf, slot):
            def one(r, _):
                sl = pl.ds(pl.multiple_of(h * half + r * 32, 32), 32)
                own_v[t, sl, :] = own_v[t, sl, :] + buf[slot, sl, :]
                return 0
            lax.fori_loop(0, half // 32, one, 0)

        def settle(i):
            t = dest(i)
            for h in range(2):
                arrived(i, h).wait_recv()
                accumulate(t, h, yrecv_v, i)

                @pl.when((t >= z) & (z > 0))
                def _():
                    from_z(t, h).wait_recv()
                    accumulate(t, h, zrecv_v, t)

                @pl.when((t < z) & (z + 1 < zs))
                def _():
                    from_z(t, h).wait_recv()
                    accumulate(t, h, zrecv_v, t)

                @pl.when((t == z) & (z + 1 < zs))
                def _():
                    from_z(zs, h).wait_recv()
                    accumulate(t, h, zrecv_v, zs)

                @pl.when(t > z)
                def _():
                    climb(t, h).start()

                @pl.when(t < z)
                def _():
                    sink(t, h).start()

            @pl.when(i + 2 < zs)
            def _():
                for h in range(2):
                    to_side(i + 2, h).start()

        for i in range(2):
            for h in range(2):
                to_side(i, h).start()
        edge = (z == 0) | (z == zs - 1)

    if extra:
        grows = gout_ref.shape[0] // 2

        def part_of(core):
            return pl.ds(pl.multiple_of(core * grows, grows), grows)

        to_core = remote(gout_ref.at[part_of(1 - cd)], core_v, esend, erecv, {"dp": xd * 2 + 1 - cd})

        def across(j):
            return remote(half_v, far_v.at[xd], asend.at[j], arecv.at[xd], {"dp": lax.rem(xd + j, xs) * 2 + cd})

        def from_across(j):
            q = lax.rem(xd + j, xs)
            return remote(far_v.at[q], far_v.at[q], asend.at[j], arecv.at[q], {"dp": q * 2 + cd})

        back_out = remote(gsum_ref.at[part_of(cd)], gsum_ref.at[part_of(cd)], bsend, brecv, {"dp": xd * 2 + 1 - cd})
        back_in = remote(gsum_ref.at[part_of(1 - cd)], gsum_ref.at[part_of(1 - cd)], bsend, brecv, {"dp": xd * 2 + 1 - cd})
        to_core.start()

        def by_rows(fn):
            def one(i, _):
                fn(pl.ds(pl.multiple_of(i * 16, 16), 16), pl.ds(pl.multiple_of(cd * grows + i * 16, 16), 16))
                return 0
            lax.fori_loop(0, grows // 16, one, 0)

        def chip_sum():
            to_core.wait_recv()

            def fold(at, full):
                half_v[at, :] = (gout_ref[full, :].astype(F32) + core_v[at, :].astype(F32)).astype(BF16)
            by_rows(fold)
            for j in range(1, xs):
                across(j).start()

        def whole_sum():
            for j in range(1, xs):
                from_across(j).wait_recv()

            def fold(at, full):
                total = half_v[at, :].astype(F32)
                for j in range(1, xs):
                    total = total + far_v[lax.rem(xd + j, xs), at, :].astype(F32)
                gsum_ref[full, :] = total.astype(BF16)
            by_rows(fold)
            back_out.start()

    def first(s, r):
        return remote(part_v.at[s, r], recv_v.at[me, r], send1.at[s, r], recv1.at[me, r], {"seq": s})

    def landed_first(s, r):
        return remote(part_v.at[s, r], recv_v.at[s, r], send1.at[s, r], recv1.at[s, r], {"seq": s})

    def second(s, r):
        return remote(sel2_v.at[me, r], sel2_v.at[me, r], send2.at[s, r], recv2.at[me, r], {"seq": s})

    def landed_second(s, r):
        return remote(sel2_v.at[s, r], sel2_v.at[s, r], send2.at[s, r], recv2.at[s, r], {"seq": s})

    def every_other(fn):
        def one(k, _):
            fn(lax.rem(me + k, chunks))
            return 0
        lax.fori_loop(1, chunks, one, 0)

    def send_row(r):
        every_other(lambda s: first(s, r).start())
        recv_v[me, r] = part_v[me, r]

    def sum_row(r):
        every_other(lambda s: landed_first(s, r).wait_recv())
        total = recv_v[0, r].astype(F32)
        for s in range(1, chunks):
            total = total + recv_v[s, r].astype(F32)
        sel2_v[me, r] = total.astype(BF16)
        every_other(lambda s: second(s, r).start())

    for ref in (gstepw_ref, gsbias_ref, gskip_ref, gd_s, gtaps_ref, gcbias_ref, gselw_ref):
        ref[...] = jnp.zeros_like(ref)
    rate_s[...] = -jnp.exp(decay_ref[...].astype(F32)) * LOG2E

    def gci_out(i):
        c, r = where_of(i)
        return pltpu.make_async_copy(gci_v.at[i % 2], gci_ref.at[c, r], gci_sem.at[i % 2])

    def scan(i, _):
        c, r = where_of(i)
        slot = i % 2

        @pl.when(i + 1 < count)
        def _():
            for one in fetch(i + 1):
                one.start()

        for one in fetch(i):
            one.wait()
        back_step(sel_ref[c, r].astype(F32), x_v[slot].astype(F32), i % chunks == 0, gact_v.at[slot], gg_v.at[slot],
                  start_v.at[slot], dt_v.at[slot], slope_v.at[slot], stepw_ref, skip_ref,
                  gvals_v.at[c, r], part_v.at[c, r], gstepw_ref, gsbias_ref, gskip_ref,
                  u_s, gy_s, gu_s, ah_s, bcoef_s, bt_s, hist_s, adj_a, harm_a, adj_b, harm_b, db_s, dc_s, carry_s, gd_s, rate_s, factor_s, kept_s, rank, n)
        late = min(3, chunks - 1)

        @pl.when((i % chunks == chunks - 1) & (r + 1 < rows))
        def _():
            send_row(r)

        @pl.when((i % chunks == late) & (r > 0))
        def _():
            sum_row(r - 1)

        if split:
            pl.when(i == 1)(trade.chip)
            pl.when(i == 5)(trade.spread)
            pl.when(i == 14)(trade.share)
        if extra:
            pl.when(i == 2)(chip_sum)
            pl.when(i == 8)(whole_sum)
        if inside:
            lo = jnp.where(edge, jnp.where(i == 4, 0, jnp.where(i == 9, 1, 2)), jnp.where(i == 9, 0, 1))
            hi = jnp.where(edge, lo + 1, jnp.where(i == 9, 1, jnp.where(i == 13, 3, 0)))

            @pl.when((i == 4) | (i == 9) | (i == 13))
            def _():
                for k in range(own_v.shape[0]):
                    pl.when(i == 4)(own_loads[k].wait)

                def one(k, _):
                    settle(k)
                    return 0
                lax.fori_loop(lo, hi, one, 0)
        return 0

    lax.fori_loop(0, count, scan, 0)
    send_row(rows - 1)

    def conv(i, _):
        c, r = where_of(i)

        @pl.when(i >= 2)
        def _():
            gci_out(i - 2).wait()

        conv_back_step(ci_ref.at[c, r], ci_ref.at[jnp.maximum(c - 1, 0), r], c == 0, i % chunks == 0, gvals_v.at[c, r], sel2_v.at[c, r],
                       taps_ref, cbias_ref, selw_ref, gci_v.at[i % 2], gtaps_ref, gcbias_ref, gselw_ref, ext_s, gext_s)
        gci_out(i).start()
        return 0

    for r in range(rows - 1):
        every_other(lambda s: landed_second(s, r).wait_recv())
    lax.fori_loop(0, count - chunks, conv, 0)
    sum_row(rows - 1)
    if inside:
        settle(zs - 1)
        red_ref[...] = own_v[z]
    if split:
        trade.pass_on()
    every_other(lambda s: landed_second(s, rows - 1).wait_recv())
    lax.fori_loop(count - chunks, count, conv, 0)
    picked, taps = gselw_ref.shape[0], gtaps_ref.shape[0]
    late_ref[0:picked, :] = gselw_ref[...].astype(BF16)
    late_ref[picked:picked + rank, :] = gstepw_ref[...].astype(BF16)
    late_ref[picked + rank:picked + rank + n, :] = (gd_s[...] * rate_s[...] * (1.0 / LOG2E)).astype(BF16)
    filler = jnp.zeros((13 - taps, gtaps_ref.shape[1]), F32)
    late_ref[picked + rank + n:, :] = jnp.concatenate([gtaps_ref[...], gsbias_ref[...], gskip_ref[...], gcbias_ref[...], filler], axis=0).astype(BF16)
    for i in range(max(0, count - 2), count):
        gci_out(i).wait()
    if split:
        trade.finish()
    for r in range(rows):
        every_other(lambda s: first(s, r).wait_send())
        every_other(lambda s: second(s, r).wait_send())
    if extra:
        to_core.wait_send()
        for j in range(1, xs):
            across(j).wait_send()
        back_in.wait_recv()
        back_out.wait_send()
    if inside:
        for i in range(zs):
            t = dest(i)
            for h in range(2):
                to_side(i, h).wait_send()

                @pl.when(t > z)
                def _():
                    climb(t, h).wait_send()

                @pl.when(t < z)
                def _():
                    sink(t, h).wait_send()


def backward(gg, gact, x, dt, slope, starts, sel, ci, stepw, decay, skip, taps, cbias, selw, mixed, ging, gout, copies, n):
    chunks, rows, length, width = ci.shape
    rank = stepw.shape[0]
    zs, ys = grid_of(chunks, copies)
    xs = max(1, copies // 2)
    wide = BLOCK * n
    inside = mixed is not None
    extra = copies % 2 == 0
    split = ging is not None
    sds = jax.ShapeDtypeStruct
    dma = pltpu.SemaphoreType.DMA
    vmem = pl.BlockSpec(memory_space=pltpu.VMEM)
    hbm = pl.BlockSpec(memory_space=pl.ANY)
    args = [gg, gact, x, dt, slope, starts, sel, ci, stepw, decay, skip, taps, cbias, selw]
    in_specs = [hbm] * 6 + [vmem] * 8
    out_specs = [hbm, vmem]
    out_shape = [sds(ci.shape, BF16), sds((selw.shape[0] + rank + n + 16, width), BF16)]
    tile, coef = (length, width), sel.shape
    scratch = [pltpu.VMEM((2,) + tile, F32), pltpu.VMEM((2,) + tile, F32), pltpu.VMEM((2,) + tile, BF16),
               pltpu.VMEM((2,) + tile, F32), pltpu.VMEM((2,) + tile, F32), pltpu.VMEM((2, n, width), F32),
               pltpu.VMEM((2,) + tile, BF16), pltpu.VMEM(ci.shape, F32),
               pltpu.VMEM(coef, BF16), pltpu.VMEM(coef, BF16), pltpu.VMEM(coef, BF16),
               pltpu.VMEM(tile, F32), pltpu.VMEM(tile, F32), pltpu.VMEM(tile, F32), pltpu.VMEM(tile, F32),
               pltpu.VMEM((length, wide), BF16), pltpu.VMEM((2 * n, length), F32), pltpu.VMEM((length * n, width), BF16),
               pltpu.VMEM((wide, width), BF16), pltpu.VMEM((wide, width), BF16), pltpu.VMEM((wide, width), BF16), pltpu.VMEM((wide, width), BF16),
               pltpu.VMEM((length, wide), F32), pltpu.VMEM((length, wide), F32),
               pltpu.VMEM((n, width), F32), pltpu.VMEM((n, width), F32), pltpu.VMEM((n, width), F32),
               pltpu.VMEM((length * n, width), F32), pltpu.VMEM((length * n, width), F32),
               pltpu.VMEM((rank, width), F32), pltpu.VMEM((1, width), F32), pltpu.VMEM((1, width), F32),
               pltpu.VMEM(taps.shape, F32), pltpu.VMEM((1, width), F32), pltpu.VMEM(selw.shape, F32),
               pltpu.VMEM((length + 8, width), F32), pltpu.VMEM((length + 8, width), F32),
               dma((6, 2)), dma((2,)), dma((chunks, rows)), dma((chunks, rows)), dma((chunks, rows)), dma((chunks, rows))]
    if inside:
        tokens, model = mixed.shape[1:]
        args.append(mixed)
        in_specs.append(hbm)
        out_specs.append(vmem)
        out_shape.append(sds((tokens, model), BF16))
        scratch += [pltpu.VMEM((zs, tokens, model), BF16), pltpu.VMEM((zs, tokens, model), BF16), pltpu.VMEM((zs + 1, tokens, model), BF16),
                    dma((zs,)), dma((zs, 2)), dma((zs, 2)), dma((zs, 2)), dma((zs, 2)), dma((zs + 1, 2))]
    if split:
        args.append(ging)
        in_specs.append(hbm)
        out_specs.append(hbm)
        out_shape.append(sds((copies * ging.shape[2], chunks * width), BF16))
    if extra:
        args.append(gout)
        in_specs.append(vmem)
        out_specs.append(vmem)
        out_shape.append(sds(gout.shape, BF16))
        part = (gout.shape[0] // 2, gout.shape[1])
        scratch += [pltpu.VMEM(part, BF16), pltpu.VMEM(part, BF16), pltpu.VMEM((xs,) + part, BF16),
                    dma(()), dma(()), dma((xs,)), dma((xs,)), dma(()), dma(())]
    if split:
        scratch += exchange_scratch(chunks, copies, ging.shape[2], width)
    return pl.pallas_call(
        functools.partial(backward_kernel, chunks=chunks, copies=copies, n=n, inside=inside, extra=extra, split=split),
        in_specs=in_specs,
        out_specs=out_specs,
        out_shape=out_shape,
        scratch_shapes=scratch,
        compiler_params=pltpu.CompilerParams(collective_id=2, has_side_effects=True, vmem_limit_bytes=63 * 1024 * 1024),
        name="backward",
    )(*args)


from jax.sharding import PartitionSpec as P


def local(hidden, grad_out, lengths, norm_gain, input_weight, conv_weight, conv_bias, select_weight,
          step_weight, step_bias, decay_log, skip_weight, output_weight):
    rows, length, model = hidden.shape
    chunks = lax.axis_size("seq")
    copies = lax.axis_size("dp")
    width = output_weight.shape[0]
    share = input_weight.shape[0]
    rank = step_weight.shape[0]
    n = decay_log.shape[0]
    tokens = chunks * rows * length
    here = lax.axis_index("seq")

    split = (share // copies) % 16 == 0 and copies % 2 == 0
    normed, ci, gate, w_all, gain_row = gather_project(
        hidden.reshape(rows * length, model), input_weight, norm_gain.astype(F32).reshape(1, share), chunks, copies, share, split)
    normed = normed.reshape(tokens, model)
    slots = here * length + lax.broadcasted_iota(jnp.int32, (rows, length), 1)
    valid = (slots < lengths[:, None]).astype(F32)[..., None]
    cotangent = grad_out.astype(F32) * valid
    shaped = lambda a: a.reshape(chunks, rows, length, a.shape[-1])
    ci, gate = shaped(ci), shaped(gate)
    bias_row = conv_bias.reshape(1, width)
    step_row = step_bias.reshape(1, width)
    skip_row = skip_weight.reshape(1, width)
    gm, sel, x, gated, gact, dt, slope, starts, mixed, gg, ggate = forward(
        ci, gate, cotangent.astype(BF16).reshape(rows * length, model), conv_weight, bias_row, select_weight,
        step_weight, step_row, decay_log, skip_row, output_weight, copies, n)
    gm = gm.reshape(tokens, model)
    gated2 = gated.reshape(tokens, width)
    ggate = ggate.reshape(tokens, width)
    zs, ys = grid_of(chunks, copies)
    inside = ys == 2 and zs == 4
    source = hidden.astype(F32)
    tn = lambda a, b: lax.dot_general(a, b, (((0,), (0,)), ((), ())), preferred_element_type=F32)
    blocks = lambda g: tn(normed, g).astype(BF16).reshape(chunks, copies, share // copies, width)
    ging = blocks(ggate)
    gout = tn(gated2, gm).astype(BF16)
    flat = lambda a: a.reshape(chunks, rows * length, a.shape[-1])
    got = backward(gg, gact, x, dt, slope, starts, sel, ci, step_weight, decay_log, skip_row, conv_weight, bias_row, select_weight,
                   mixed if inside else None, ging if split else None, gout, copies, n)
    gci, late = got[:2]
    mixed = got[2].reshape(rows, length, model) if inside else lax.psum_scatter(shaped(mixed), "seq", scatter_dimension=0, tiled=False)
    gout = got[-1].astype(F32)
    output = ((source + mixed.astype(F32)) * valid).astype(BF16)
    tap_count = conv_weight.shape[0]
    done = scatter_sums(flat(gci), ggate.reshape(chunks, rows * length, width), w_all, late, flat(shaped(normed)), chunks, copies, split)
    scaled, late = done[:2]
    if split:
        gin = jnp.concatenate([done[2], got[-2]], axis=1).astype(F32)
    else:
        gin = jnp.stack([blocks(gci.reshape(tokens, width)), ging], axis=3)
        gin = lax.psum_scatter(gin, "dp", scatter_dimension=1, tiled=False)
        gin = lax.all_to_all(gin, "seq", split_axis=0, concat_axis=2, tiled=False)
        gin = lax.all_gather(gin.reshape(share // copies, 2 * chunks * width), "dp", axis=0, tiled=True).astype(F32)
    ggain = jnp.sum(gin * input_weight.astype(F32), axis=1) / norm_gain.astype(F32)
    scaled = scaled.reshape(rows, length, model).astype(F32) * gain_row
    inverse = lax.rsqrt(jnp.mean(source * source, axis=-1, keepdims=True) + EPSILON)
    ghidden = inverse * scaled - source * inverse ** 3 * jnp.mean(scaled * source, axis=-1, keepdims=True) + cotangent
    sizes = (select_weight.shape[0], rank, n, tap_count)
    ends = [sum(sizes[:k + 1]) for k in range(len(sizes))]
    gselw, gstepw, gdecay, gtaps = (late[e - k:e] for e, k in zip(ends, sizes))
    gstepb, gskip, gconvb = (late[ends[-1] + k] for k in range(3))
    return (output, ghidden, ggain, gin, gtaps, gconvb, gselw, gstepw, gstepb,
            gdecay, gskip, gout)


def solution(mesh):
    tok, vec, col, row = P("dp", "seq", None), P("seq"), P(None, "seq"), P("seq", None)
    return jax.shard_map(
        local,
        mesh=mesh,
        in_specs=(tok, tok, P("dp"), vec, row, col, vec, col, col, vec, col, vec, row),
        out_specs=(tok, tok, vec, row, col, vec, col, col, vec, col, vec, row),
        check_vma=False,
    )
```

```python
import functools
import jax
import jax.numpy as jnp
from jax import lax
from jax.experimental import pallas as pl
from jax.experimental.pallas import tpu as pltpu

BLOCK = 16
EPSILON = 1e-05
LOG2E = 1.4426950408889634
F32 = jnp.float32
BF16 = jnp.bfloat16


def inverse_of(whole):
    guess = pl.reciprocal(whole, approx=True)
    return guess * (2.0 - whole * guess)


def gates_of(pre):
    small = jnp.exp2(jnp.abs(pre) * -LOG2E)
    whole = 1.0 + small
    log_part = jnp.where(small < 1e-3, small * (1.0 - small * (0.5 - small * (1.0 / 3.0))), jnp.log(whole))
    return jnp.maximum(pre, 0.0) + log_part, jnp.where(pre >= 0.0, 1.0, small) * inverse_of(whole)


def sigmoid(v):
    return 0.5 + 0.5 * jnp.tanh(0.5 * v)


def nt_dot(a, b):
    return lax.dot_general(a, b, (((1,), (1,)), ((), ())), preferred_element_type=F32)


def lane_tiles(width):
    step = min(width, 512)
    return [slice(k, k + step) for k in range(0, width, step)]


def tile_matrix(n, wide):
    col = lax.broadcasted_iota(jnp.int32, (n, wide), 1)
    row = lax.broadcasted_iota(jnp.int32, (n, wide), 0)
    return (col % n == row).astype(F32)


def diagonal_mask(rows, n, wide):
    col = lax.broadcasted_iota(jnp.int32, (rows, wide), 1)
    row = lax.broadcasted_iota(jnp.int32, (rows, wide), 0)
    return col // n == row % BLOCK


def scan_step(selected, x, gate, fresh, stepw_ref, bias_ref, skip_ref, gated_ref, gact_ref, tail_ref, dt_ref, slope_ref,
              u_s, y_s, coef_s, bt_s, hist_a, hist_b, state_s, rate_s, rank, n):
    length = x.shape[0]
    wide = BLOCK * n
    state_s[...] = jnp.where(fresh, 0.0, state_s[...])
    low = selected[:rank].T.astype(BF16)
    pre = jnp.dot(low, stepw_ref[...], preferred_element_type=F32) + bias_ref[...]
    dt, slope = gates_of(pre)
    dt_ref[...] = dt
    slope_ref[...] = slope
    u_s[...] = dt * x
    bt_s[...] = selected[rank:]
    spread = jnp.dot(selected[rank:].T[:, n:], tile_matrix(n, wide), preferred_element_type=F32)
    coef_s[...] = jnp.where(diagonal_mask(length, n, wide), spread, 0.0).astype(BF16)
    blocks = length // BLOCK

    def finish(k, hist):
        rows = pl.ds(pl.multiple_of(k * BLOCK, BLOCK), BLOCK)
        y_s[rows, :] = jnp.dot(coef_s[rows, :], hist[...], preferred_element_type=F32)

    def block(k, state, hist):
        at = pl.multiple_of(k * BLOCK, BLOCK)
        bs = pltpu.roll(bt_s[0:n, :], length - at, 1)
        dts = dt_ref[pl.ds(at, BLOCK), :]
        us = u_s[pl.ds(at, BLOCK), :]
        rate = rate_s[...]
        for i in range(BLOCK):
            factor = jnp.exp2(dts[i:i + 1, :] * rate)
            state = factor * state + us[i:i + 1, :] * bs[:, i:i + 1]
            hist[i * n:(i + 1) * n, :] = state.astype(BF16)
        return state

    def pair(j, state):
        finish(jnp.maximum(2 * j - 1, 0), hist_b)
        state = block(2 * j, state, hist_a)
        finish(2 * j, hist_a)
        return block(2 * j + 1, state, hist_b)

    state_s[...] = lax.fori_loop(0, blocks // 2, pair, state_s[...])
    finish(blocks - 1, hist_b)
    ssm = y_s[...] + skip_ref[...] * x
    sg = sigmoid(gate)
    gact = gate * sg
    gact_ref[...] = gact
    tail_ref[...] = (ssm * sg * (1.0 + gate * (1.0 - sg))).astype(BF16)
    gated_ref[...] = (ssm * gact).astype(BF16)


def back_step(selected, x, fresh, gact_ref, gg_ref, start_ref, dt_ref, slope_ref, stepw_ref, skip_ref,
              gvals_ref, gsel_ref, gstepw_ref, gbias_ref, gskip_ref,
              u_s, gy_s, gu_s, ah_s, bcoef_s, bt_s, hist_s, adj_a, harm_a, adj_b, harm_b, db_s, dc_s, carry_s, gd_s, rate_s, factor_s, kept_s, rank, n):
    length = x.shape[0]
    wide = BLOCK * n
    blocks = length // BLOCK
    carry_s[...] = jnp.where(fresh, 0.0, carry_s[...])
    gg = gg_ref[...]
    gy = gg * gact_ref[...]
    gskip_ref[...] += jnp.sum(gy * x, axis=0, keepdims=True)
    gy_s[...] = gy
    dt = dt_ref[...]
    u_s[...] = dt * x
    bt_s[...] = selected[rank:]
    tiles = tile_matrix(n, wide)
    spread = jnp.dot(selected[rank:].T[:, :n], tiles, preferred_element_type=F32)
    bcoef_s[...] = jnp.where(diagonal_mask(length, n, wide), spread, 0.0).astype(BF16)
    keep = diagonal_mask(BLOCK, n, wide)
    ones = keep.astype(BF16)
    lanes = lane_tiles(x.shape[1])
    state_s = start_ref

    def steps(lane):
        def again(k, state):
            at = pl.multiple_of(k * BLOCK, BLOCK)
            bs = pltpu.roll(bt_s[0:n, :], length - at, 1)
            dts = dt_ref[pl.ds(at, BLOCK), lane]
            us = u_s[pl.ds(at, BLOCK), lane]
            rate = rate_s[:, lane]
            for i in range(BLOCK):
                here = pl.ds(pl.multiple_of((at + i) * n, n), n)
                factor = jnp.exp2(dts[i:i + 1, :] * rate)
                factor_s[here, lane] = factor
                old = factor * state
                kept_s[here, lane] = old
                state = old + us[i:i + 1, :] * bs[:, i:i + 1]
                hist_s[here, lane] = state.astype(BF16)
            return state

        lax.fori_loop(0, blocks, again, state_s[:, lane])

        def products(k, adj_s, harm_s):
            at = pl.multiple_of(k * BLOCK, BLOCK)
            rows = pl.ds(at, BLOCK)
            adj = adj_s[:, lane]
            gu_s[rows, lane] = jnp.dot(bcoef_s[rows, :], adj, preferred_element_type=F32)
            ah_s[rows, lane] = jnp.dot(ones, harm_s[:, lane], preferred_element_type=F32)
            db = jnp.where(keep, nt_dot(u_s[rows, lane].astype(BF16), adj), 0.0)
            states = hist_s[pl.ds(pl.multiple_of(at * n, n), wide), lane]
            dc = jnp.where(keep, nt_dot(gy_s[rows, lane].astype(BF16), states), 0.0)
            if lane.start == 0:
                db_s[rows, :] = db
                dc_s[rows, :] = dc
            else:
                db_s[rows, :] += db
                dc_s[rows, :] += dc

        def block(k, carry, adj_s, harm_s):
            at = pl.multiple_of(k * BLOCK, BLOCK)
            cs = pltpu.roll(bt_s[n:2 * n, :], length - at, 1)
            dts = dt_ref[pl.ds(at, BLOCK), lane]
            gys = gy_s[pl.ds(at, BLOCK), lane]
            rate = rate_s[:, lane]
            gd = gd_s[:, lane]
            for i in range(BLOCK - 1, -1, -1):
                here = pl.ds(pl.multiple_of((at + i) * n, n), n)
                g = cs[:, i:i + 1] * gys[i:i + 1, :] + carry
                adj_s[i * n:(i + 1) * n, lane] = g.astype(BF16)
                carry = factor_s[here, lane] * g
                h = g * kept_s[here, lane]
                harm_s[i * n:(i + 1) * n, lane] = (h * rate).astype(BF16)
                gd = gd + dts[i:i + 1, :] * h
            gd_s[:, lane] = gd
            return carry

        def pair(j, carry):
            k = blocks - 1 - 2 * j
            if lane.start == 0:
                products(jnp.minimum(k + 1, blocks - 1), adj_b, harm_b)
            else:
                @pl.when(j > 0)
                def _():
                    products(k + 1, adj_b, harm_b)
            carry = block(k, carry, adj_a, harm_a)
            products(k, adj_a, harm_a)
            return block(k - 1, carry, adj_b, harm_b)

        carry_s[:, lane] = lax.fori_loop(0, blocks // 2, pair, carry_s[:, lane])
        products(0, adj_b, harm_b)

    for lane in lanes:
        steps(lane)
    gu = gu_s[...]
    gpre = ((x * gu + ah_s[...] * (1.0 / LOG2E)) * slope_ref[...]).astype(BF16)
    gvals_ref[...] = (gy * skip_ref[...] + dt * gu).astype(gvals_ref.dtype)
    gbias_ref[...] += jnp.sum(gpre.astype(F32), axis=0, keepdims=True)
    gstepw_ref[...] += jnp.dot(selected[:rank].astype(BF16), gpre, preferred_element_type=F32)
    fold = lambda ref: nt_dot(tiles.astype(BF16), ref[...].astype(BF16))
    gsel_ref[0:rank, :] = nt_dot(stepw_ref[...], gpre).astype(BF16)
    gsel_ref[rank:rank + n, :] = fold(db_s).astype(BF16)
    gsel_ref[rank + n:rank + 2 * n, :] = fold(dc_s).astype(BF16)


def conv_step(ci, fresh, taps_ref, bias_ref, selw_ref, ext_s):
    length = ci.shape[0]
    tap_count = taps_ref.shape[0]
    ext_s[0:8, :] = jnp.where(fresh, 0.0, ext_s[length:length + 8, :])
    ext_s[8:, :] = ci.astype(F32)
    total = bias_ref[...].astype(F32)
    for k in range(tap_count):
        total = total + taps_ref[k:k + 1, :].astype(F32) * ext_s[pl.ds(8 - tap_count + 1 + k, length), :]
    x = (total * sigmoid(total)).astype(BF16)
    return x, nt_dot(selw_ref[...], x).astype(BF16)


def conv_back_step(ci_ref, prev_ref, first, fresh, gvals_ref, gsel_ref, taps_ref, bias_ref, selw_ref,
                   gci_ref, gtaps_ref, gbias_ref, gselw_ref, ext_s, gext_s):
    length = ci_ref.shape[0]
    tap_count = taps_ref.shape[0]
    gext_s[length:, :] = jnp.where(fresh, 0.0, gext_s[length:, :])
    ext_s[8:, :] = ci_ref[...].astype(F32)
    before = prev_ref[...][length - 16:, :].astype(F32)[8:, :]
    ext_s[0:8, :] = jnp.where(first, 0.0, before)
    total = bias_ref[...].astype(F32)
    for k in range(tap_count):
        total = total + taps_ref[k:k + 1, :].astype(F32) * ext_s[pl.ds(8 - tap_count + 1 + k, length), :]
    sg = sigmoid(total)
    x = (total * sg).astype(BF16)
    gsel = gsel_ref[...]
    gvals = gvals_ref[...] + jnp.dot(gsel.astype(F32).T.astype(BF16), selw_ref[...], preferred_element_type=F32)
    gconv = gvals * sg * (1.0 + total * (1.0 - sg))
    gbias_ref[...] += jnp.sum(gconv, axis=0, keepdims=True)
    for k in range(tap_count):
        gtaps_ref[k:k + 1, :] += jnp.sum(gconv * ext_s[pl.ds(8 - tap_count + 1 + k, length), :], axis=0, keepdims=True)
    gselw_ref[...] += jnp.dot(gsel, x, preferred_element_type=F32)
    gext_s[0:length, :] = gconv
    gci = jnp.zeros_like(gconv)
    for k in range(tap_count):
        gci = gci + taps_ref[k:k + 1, :].astype(F32) * gext_s[pl.ds(tap_count - 1 - k, length), :]
    gci_ref[...] = gci.astype(BF16)
    gext_s[length:, :] = gconv[0:8, :]


MESH = pl.DeviceIdType.MESH


def remote(src, dst, send, recv, device):
    return pltpu.make_async_remote_copy(src_ref=src, dst_ref=dst, send_sem=send, recv_sem=recv, device_id=device, device_id_type=MESH)


def grid_of(chunks, copies):
    deep = max(1, copies // 2)
    return (chunks // deep, deep) if chunks % deep == 0 else (chunks, 1)


def meet(chunks, copies):
    me, mine = lax.axis_index("seq"), lax.axis_index("dp")
    barrier = pltpu.get_barrier_semaphore()

    def greet(k, _):
        pl.semaphore_signal(barrier, inc=1, device_id={"seq": lax.rem(me + k, chunks)}, device_id_type=MESH)
        return 0

    def greet_copy(k, _):
        pl.semaphore_signal(barrier, inc=1, device_id={"dp": lax.rem(mine + k, copies)}, device_id_type=MESH)
        return 0

    lax.fori_loop(1, chunks, greet, 0)
    if copies > 1:
        lax.fori_loop(1, copies, greet_copy, 0)
    pl.semaphore_wait(barrier, chunks - 1 + max(copies - 1, 0))


def gather_project_kernel(hid_ref, wq_ref, gain_ref, n_ref, ci_ref, gate_ref, w_ref, row_ref,
                          hid_v, gain_v, w_v, n_v, ci_v, gate_v,
                          load_sem, out_sem, hrecv, hside, hup, hdown, hlend,
                          w1send, w1recv, w2recv, w2send, w3send, gsend, grecv, *, chunks, copies, share, split):
    zs, ys = grid_of(chunks, copies)
    xs = copies // 2
    me, mine = lax.axis_index("seq"), lax.axis_index("dp")
    z, y = me // ys, me % ys
    x, c = mine // 2, mine % 2
    tokens, model = hid_v.shape[1:]
    width = ci_v.shape[1]
    inner = chunks * width
    half = tokens // 2
    even = ys == 2 and zs % 2 == 0
    piece = share // (copies if split else 1)
    spot = mine if split else 0
    load = pltpu.make_async_copy(hid_ref, hid_v.at[me], load_sem)
    load.start()
    meet(chunks, copies)
    load.wait()

    def w_rows(s, d):
        return pl.ds(pl.multiple_of(s * share + d * piece, piece), piece)

    def w_first(s, part):
        src = wq_ref.at[pl.ds(pl.multiple_of(spot * piece, piece), piece), pl.ds(pl.multiple_of(part * inner + s * width, width), width)]
        return remote(src, w_v.at[w_rows(me, spot), pl.ds(part * width, width)], w1send.at[s, part], w1recv.at[me, part], {"seq": s})

    def w_landed(s, part):
        dst = w_v.at[w_rows(s, spot), pl.ds(part * width, width)]
        return remote(dst, dst, w1send.at[s, part], w1recv.at[s, part], {"seq": s})

    def w_own(part):
        src = wq_ref.at[pl.ds(pl.multiple_of(spot * piece, piece), piece), pl.ds(pl.multiple_of(part * inner + me * width, width), width)]
        return pltpu.make_async_copy(src, w_v.at[w_rows(me, spot), pl.ds(part * width, width)], out_sem.at[part])

    def every_other(fn):
        def one(k, _):
            fn(lax.rem(me + k, chunks))
            return 0
        lax.fori_loop(1, chunks, one, 0)

    def gain_to(s):
        return remote(gain_ref, gain_v.at[me], gsend.at[s], grecv.at[me], {"seq": s})

    def gain_from(s):
        return remote(gain_v.at[s], gain_v.at[s], gsend.at[s], grecv.at[s], {"seq": s})

    def send_first(s):
        gain_to(s).start()
        w_first(s, 0).start()
        w_first(s, 1).start()

    def block(o, yy, h):
        return hid_v.at[o * ys + yy, pl.ds(h * half, half)]

    def up(o, h):
        return remote(block(o, y, h), block(o, y, h), hup.at[o, h], hrecv.at[o * ys + y, h], {"seq": (z + 1) * ys + y})

    def down(o, h):
        return remote(block(o, y, h), block(o, y, h), hdown.at[o, h], hrecv.at[o * ys + y, h], {"seq": (z - 1) * ys + y})

    def side(o, j, h):
        other = lax.rem(y + j, ys)
        return remote(block(o, y, h), block(o, y, h), hside.at[o, j - 1, h], hrecv.at[o * ys + y, h], {"seq": z * ys + other})

    def landed(o, yy, h):
        return remote(block(o, yy, h), block(o, yy, h), hside.at[o, 0, h], hrecv.at[o * ys + yy, h], {"seq": lax.rem(me + 1, chunks)})

    def when(cond, fn):
        pl.when(cond)(fn)

    gain_own = pltpu.make_async_copy(gain_ref, gain_v.at[me], out_sem.at[2])
    gain_own.start()
    for part in range(2):
        w_own(part).start()
    for h in range(2):
        when(z + 1 < zs, lambda: up(z, h).start())
        when(z > 0, lambda: down(z, h).start())
        for j in range(1, ys):
            side(z, j, h).start()
    every_other(send_first)

    partner = z + 1 - 2 * (z % 2)

    def sides(o, h, act):
        if even and h == 1:
            when(o != partner, lambda: act(side(o, 1, h)))
        else:
            for j in range(1, ys):
                act(side(o, j, h))

    def lend():
        return remote(block(z, 1 - y, 1), block(z, 1 - y, 1), hlend, hrecv.at[z * ys + 1 - y, 1], {"seq": partner * ys + y})

    def lend_on():
        if even:
            landed(z, 1 - y, 1).wait_recv()
            lend().start()

    def relay(k):
        for h in range(2):
            @pl.when(z - k >= 0)
            def _():
                landed(z - k, y, h).wait_recv()
                when(z + 1 < zs, lambda: up(z - k, h).start())
                sides(z - k, h, lambda one: one.start())

            @pl.when(z + k < zs)
            def _():
                landed(z + k, y, h).wait_recv()
                when(z > 0, lambda: down(z + k, h).start())
                sides(z + k, h, lambda one: one.start())

    def shared(s, d, sems, k, device):
        return remote(w_v.at[w_rows(s, d)], w_v.at[w_rows(s, d)], sems.at[s, k], w2recv.at[s, d], device)

    def spread(s):
        for j in range(1, xs):
            shared(s, mine, w2send, j - 1, {"dp": lax.rem(x + j, xs) * 2 + c}).start()
        shared(s, mine, w3send, 0, {"dp": x * 2 + 1 - c}).start()

    gain_own.wait()
    for part in range(2):
        w_own(part).wait()
    if split:
        spread(me)

    def take_first(s):
        gain_from(s).wait_recv()
        for part in range(2):
            w_landed(s, part).wait_recv()
        if split:
            spread(s)

    if zs > 1:
        relay(1)
    every_other(take_first)

    def take_second(s, _):
        for j in range(1, xs):
            d = lax.rem(x + j, xs) * 2 + c
            shared(s, d, w2send, j - 1, {"dp": d}).wait_recv()
            shared(s, d, w3send, j, {"dp": x * 2 + 1 - c}).start()
        return 0

    def take_third(s, _):
        for j in range(xs):
            d = lax.rem(x + j, xs) * 2 + 1 - c
            shared(s, d, w2send, 0, {"dp": d}).wait_recv()
        return 0

    if zs > 2:
        relay(2)
    lend_on()
    if split:
        lax.fori_loop(0, chunks, take_second, 0)
    if split:
        lax.fori_loop(0, chunks, take_third, 0)

    row_ref[...] = jnp.concatenate([gain_v[s] for s in range(chunks)], axis=-1)
    w_out = pltpu.make_async_copy(w_v, w_ref, load_sem)
    w_out.start()
    steps = 4 if width >= 512 else 1
    tile = 2 * width // steps

    def project(at):
        def rows(i, _):
            sl = pl.ds(pl.multiple_of(i * 32, 32), 32)
            h = hid_v[at, sl, :].astype(F32)
            inverse = lax.rsqrt(jnp.mean(h * h, axis=-1, keepdims=True) + EPSILON)
            n_v[sl, :] = (h * inverse * row_ref[...]).astype(BF16)
            return 0
        lax.fori_loop(0, tokens // 32, rows, 0)
        n_out = pltpu.make_async_copy(n_v, n_ref.at[at], out_sem.at[0])
        n_out.start()

        def columns(i, _):
            sl = pl.ds(pl.multiple_of(i * tile, tile), tile)
            got = jnp.dot(n_v[...], w_v[:, sl], preferred_element_type=F32)
            if steps == 1:
                ci_v[...] = got[:, :width].astype(BF16)
                gate_v[...] = got[:, width:]
            else:
                @pl.when(i < steps // 2)
                def _():
                    ci_v[:, sl] = got.astype(BF16)

                @pl.when(i >= steps // 2)
                def _():
                    gate_v[:, pl.ds(pl.multiple_of(i * tile - width, tile), tile)] = got
            return 0
        lax.fori_loop(0, steps, columns, 0)
        ci_out = pltpu.make_async_copy(ci_v, ci_ref.at[at], out_sem.at[1])
        gate_out = pltpu.make_async_copy(gate_v, gate_ref.at[at], out_sem.at[2])
        ci_out.start()
        gate_out.start()
        n_out.wait()
        ci_out.wait()
        gate_out.wait()

    def work(first, last):
        def one(i, _):
            k0, j = i // (2 * ys), i % (2 * ys)
            lower, yy = j // ys, j % ys
            own = yy == y
            k = k0 - jnp.where(own, 0, 1)
            o = z + k * (2 * lower - 1)
            ok = (k >= 0) & (k < zs) & (o >= 0) & (o < zs) & ((lower == 0) | (k > 0))
            if even:
                ok = ok & (own | (o != partner))

            @pl.when(ok & jnp.logical_not(own))
            def _():
                landed(o, yy, 0).wait_recv()
                if even:
                    when(o != z, lambda: landed(o, yy, 1).wait_recv())
                else:
                    landed(o, yy, 1).wait_recv()

            @pl.when(ok)
            def _():
                project(o * ys + yy)
            return 0
        lax.fori_loop(first * 2 * ys, last * 2 * ys, one, 0)

    work(0, min(2, zs))

    def later(k, _):
        relay(k)
        work(k - 1, k)
        return 0

    lax.fori_loop(3, zs, later, 0)
    work(max(2, zs - 1), zs)
    work(zs, zs + 1)
    if even:
        for h in range(2):
            landed(partner, 1 - y, h).wait_recv()
        project(partner * ys + 1 - y)
    w_out.wait()

    def drain_first(s):
        gain_to(s).wait_send()
        for part in range(2):
            w_first(s, part).wait_send()

    every_other(drain_first)

    def drain_second(s, _):
        for j in range(1, xs):
            shared(s, mine, w2send, j - 1, {"dp": mine}).wait_send()
        for j in range(xs):
            shared(s, mine, w3send, j, {"dp": mine}).wait_send()
        return 0

    if split:
        lax.fori_loop(0, chunks, drain_second, 0)

    def drain(k, _):
        for h in range(2):
            @pl.when(z - k >= 0)
            def _():
                when(z + 1 < zs, lambda: up(z - k, h).wait_send())
                sides(z - k, h, lambda one: one.wait_send())

            @pl.when((z + k < zs) & (k > 0))
            def _():
                when(z > 0, lambda: down(z + k, h).wait_send())
                sides(z + k, h, lambda one: one.wait_send())
        return 0

    lax.fori_loop(0, zs, drain, 0)
    for h in range(2):
        when(z > 0, lambda: down(z, h).wait_send())
    if even:
        lend().wait_send()


def gather_project(hidden, wq, gain, chunks, copies, share, split):
    tokens, model = hidden.shape
    width = wq.shape[1] // 2 // chunks
    zs, ys = grid_of(chunks, copies)
    any_spec = pl.BlockSpec(memory_space=pl.ANY)
    sds = jax.ShapeDtypeStruct
    dma = pltpu.SemaphoreType.DMA
    return pl.pallas_call(
        functools.partial(gather_project_kernel, chunks=chunks, copies=copies, share=share, split=split),
        in_specs=[any_spec] * 3,
        out_specs=[any_spec] * 4 + [pl.BlockSpec(memory_space=pltpu.VMEM)],
        out_shape=[sds((chunks, tokens, model), BF16), sds((chunks, tokens, width), BF16),
                   sds((chunks, tokens, width), F32), sds((model, 2 * width), BF16), sds((1, model), F32)],
        scratch_shapes=[
            pltpu.VMEM((chunks, tokens, model), BF16), pltpu.VMEM((chunks, 1, share), F32), pltpu.VMEM((model, 2 * width), BF16),
            pltpu.VMEM((tokens, model), BF16), pltpu.VMEM((tokens, width), BF16), pltpu.VMEM((tokens, width), F32),
            dma(()), dma((3,)), dma((chunks, 2)), dma((zs, max(1, ys - 1), 2)), dma((zs, 2)), dma((zs, 2)), dma(()),
            dma((chunks, 2)), dma((chunks, 2)), dma((chunks, copies)), dma((chunks, max(1, copies // 2))), dma((chunks, max(1, copies // 2))),
            dma((chunks,)), dma((chunks,)),
        ],
        compiler_params=pltpu.CompilerParams(collective_id=0, has_side_effects=True, vmem_limit_bytes=60 * 1024 * 1024),
        name="gather_project",
    )(hidden, wq, gain)


SPLITS = (8, 14)


def forward_kernel(ci_ref, gate_ref, gm_ref, taps_ref, cbias_ref, selw_ref, stepw_ref, sbias_ref, decay_ref, skip_ref, wout_ref,
                   gmall_ref, sel_ref, x_ref, gated_ref, gact_ref, tail_ref, dt_ref, slope_ref, start_ref, mixed_ref,
                   gate_v, part_v, recv_v, x_v, gated_v, gact_v, tail_v, dt_v, slope_v, start_v,
                   mixed_v,
                   ext_s, u_s, y_s, coef_s, bt_s, hist_a, hist_b, state_s, rate_s,
                   load_sem, own_sem, out_sem, mixed_sem, grecv, gside, gup, gdown, glend, send1, recv1, send2, recv2, *, chunks, copies, n):
    zs, ys = grid_of(chunks, copies)
    me = lax.axis_index("seq")
    z, y = me // ys, me % ys
    tokens, model = gm_ref.shape
    rows, length, width = ci_ref.shape[1:]
    rank = stepw_ref.shape[0]
    half = tokens // 2
    even = ys == 2 and zs % 2 == 0
    load = pltpu.make_async_copy(gate_ref, gate_v, load_sem)
    load.start()
    own = pltpu.make_async_copy(gm_ref, gmall_ref.at[me], own_sem)
    own.start()
    meet(chunks, 1)

    def block(o, yy, h):
        return gmall_ref.at[o * ys + yy, pl.ds(h * half, half)]

    def source(o, h, k):
        return gm_ref.at[pl.ds(h * half, half)] if k is None else block(o, y, h)

    def up(o, h, k=0):
        return remote(source(o, h, k), block(o, y, h), gup.at[o, h], grecv.at[o * ys + y, h], {"seq": (z + 1) * ys + y})

    def down(o, h, k=0):
        return remote(source(o, h, k), block(o, y, h), gdown.at[o, h], grecv.at[o * ys + y, h], {"seq": (z - 1) * ys + y})

    def side(o, j, h, k=0):
        return remote(source(o, h, k), block(o, y, h), gside.at[o, j - 1, h], grecv.at[o * ys + y, h], {"seq": z * ys + lax.rem(y + j, ys)})

    def landed(o, yy, h):
        return remote(block(o, yy, h), block(o, yy, h), gside.at[o, 0, h], grecv.at[o * ys + yy, h], {"seq": lax.rem(me + 1, chunks)})

    def when(cond, fn):
        pl.when(cond)(fn)

    def first_sends(h):
        when(z + 1 < zs, lambda: up(z, h, None).start())
        when(z > 0, lambda: down(z, h, None).start())
        for j in range(1, ys):
            side(z, j, h, None).start()

    first_sends(0)

    partner = z + 1 - 2 * (z % 2)

    def sides(o, h, act):
        if even and h == 1:
            when(o != partner, lambda: act(side(o, 1, h)))
        else:
            for j in range(1, ys):
                act(side(o, j, h))

    def lend():
        return remote(block(z, 1 - y, 1), block(z, 1 - y, 1), glend, grecv.at[z * ys + 1 - y, 1], {"seq": partner * ys + y})

    def lend_on():
        if even:
            landed(z, 1 - y, 1).wait_recv()
            lend().start()

    def relay(k):
        for h in range(2):
            @pl.when(z - k >= 0)
            def _():
                landed(z - k, y, h).wait_recv()
                when(z + 1 < zs, lambda: up(z - k, h).start())
                sides(z - k, h, lambda one: one.start())

            @pl.when(z + k < zs)
            def _():
                landed(z + k, y, h).wait_recv()
                when(z > 0, lambda: down(z + k, h).start())
                sides(z + k, h, lambda one: one.start())

    rate_s[...] = -jnp.exp(decay_ref[...].astype(F32)) * LOG2E

    def conv(i, _):
        r, c = i // chunks, i % chunks
        x, part = conv_step(ci_ref[c, r], c == 0, taps_ref, cbias_ref, selw_ref, ext_s)
        x_v[c, r] = x
        part_v[c, r] = part
        return 0

    def first(s, r):
        return remote(part_v.at[s, r], recv_v.at[me, r], send1.at[s, r], recv1.at[me, r], {"seq": s})

    def landed_first(s, r):
        return remote(part_v.at[s, r], recv_v.at[s, r], send1.at[s, r], recv1.at[s, r], {"seq": s})

    def second(s, r):
        return remote(sel_ref.at[me, r], sel_ref.at[me, r], send2.at[s, r], recv2.at[me, r], {"seq": s})

    def landed_second(s, r):
        return remote(sel_ref.at[s, r], sel_ref.at[s, r], send2.at[s, r], recv2.at[s, r], {"seq": s})

    def every_other(fn):
        def one(k, _):
            fn(lax.rem(me + k, chunks))
            return 0
        lax.fori_loop(1, chunks, one, 0)

    for r in range(rows):
        lax.fori_loop(r * chunks, (r + 1) * chunks, conv, 0)
        every_other(lambda s: first(s, r).start())
        recv_v[me, r] = part_v[me, r]
        if r == 0:
            first_sends(1)
    x_out = pltpu.make_async_copy(x_v, x_ref, out_sem.at[0, 0])
    x_out.start()
    for r in range(rows):
        every_other(lambda s: landed_first(s, r).wait_recv())
        total = recv_v[0, r].astype(F32)
        for s in range(1, chunks):
            total = total + recv_v[s, r].astype(F32)
        sel_ref[me, r] = total.astype(BF16)
        every_other(lambda s: second(s, r).start())
    if zs > 1:
        relay(1)
    if zs <= 2:
        lend_on()
    load.wait()
    pairs = ((gated_v, gated_ref), (gact_v, gact_ref), (tail_v, tail_ref), (dt_v, dt_ref), (slope_v, slope_ref), (start_v, start_ref))

    def outs(c, r):
        return [pltpu.make_async_copy(src.at[c, r], dst.at[c, r], out_sem.at[1 + k, c * rows + r]) for k, (src, dst) in enumerate(pairs)]

    def scan(i, _):
        r, c = i // chunks, i % chunks

        @pl.when(c == 0)
        def _():
            every_other(lambda s: landed_second(s, r).wait_recv())

        start_v[c, r] = jnp.where(c == 0, 0.0, state_s[...])
        scan_step(sel_ref[c, r].astype(F32), x_v[c, r].astype(F32), gate_v[c, r], c == 0, stepw_ref, sbias_ref, skip_ref,
                  gated_v.at[c, r], gact_v.at[c, r], tail_v.at[c, r], dt_v.at[c, r], slope_v.at[c, r],
                  u_s, y_s, coef_s, bt_s, hist_a, hist_b, state_s, rate_s, rank, n)
        for one in outs(c, r):
            one.start()
        return 0

    count = rows * chunks
    at = 0
    for k in range(2, zs):
        cut = min(count, count * (SPLITS[k - 2] if zs == 4 else 16 * (k - 1) // zs) // 16)
        lax.fori_loop(at, cut, scan, 0)
        relay(k)
        if k == 2:
            lend_on()
        at = cut
    lax.fori_loop(at, count, scan, 0)

    tile = min(512, model)

    def mixed_out(s):
        return pltpu.make_async_copy(mixed_v.at[s % 2], mixed_ref.at[s], mixed_sem.at[s % 2])

    def mix(s, _):
        @pl.when(s >= 2)
        def _():
            mixed_out(s - 2).wait()

        lhs = gated_v[s].reshape(tokens, width)

        def one(i, _):
            sl = pl.ds(pl.multiple_of(i * tile, tile), tile)
            mixed_v[s % 2, :, sl] = jnp.dot(lhs, wout_ref[:, sl], preferred_element_type=F32).astype(BF16)
            return 0
        lax.fori_loop(0, model // tile, one, 0)
        mixed_out(s).start()
        return 0

    lax.fori_loop(0, chunks, mix, 0)
    for s in range(chunks - 2, chunks):
        mixed_out(s).wait()

    def others(o, _):
        for j in range(1, ys):
            landed(o, lax.rem(y + j, ys), 0).wait_recv()
            if even:
                when(o != z, lambda: landed(o, 1 - y, 1).wait_recv())
            else:
                landed(o, lax.rem(y + j, ys), 1).wait_recv()
        return 0

    lax.fori_loop(0, zs, others, 0)
    own.wait()
    x_out.wait()

    def settle(i, _):
        for one in outs(i // rows, i % rows):
            one.wait()
        return 0

    lax.fori_loop(0, count, settle, 0)
    for r in range(rows):
        every_other(lambda s: first(s, r).wait_send())
        every_other(lambda s: second(s, r).wait_send())

    def drain(k, _):
        for h in range(2):
            @pl.when(z - k >= 0)
            def _():
                when(z + 1 < zs, lambda: up(z - k, h).wait_send())
                sides(z - k, h, lambda one: one.wait_send())

            @pl.when((z + k < zs) & (k > 0))
            def _():
                when(z > 0, lambda: down(z + k, h).wait_send())
                sides(z + k, h, lambda one: one.wait_send())
        return 0

    lax.fori_loop(0, zs, drain, 0)
    for h in range(2):
        when(z > 0, lambda: down(z, h).wait_send())
    if even:
        lend().wait_send()


def forward(ci, gate, gm, taps, cbias, selw, stepw, sbias, decay, skip, wout, copies, n):
    chunks, rows, length, width = ci.shape
    tokens, model = gm.shape
    zs, ys = grid_of(chunks, copies)
    wide = BLOCK * n
    sds = jax.ShapeDtypeStruct
    dma = pltpu.SemaphoreType.DMA
    vmem = pl.BlockSpec(memory_space=pltpu.VMEM)
    hbm = pl.BlockSpec(memory_space=pl.ANY)
    coef = (chunks, rows, selw.shape[0], length)
    starts = (chunks, rows, n, width)
    full = ci.shape
    return pl.pallas_call(
        functools.partial(forward_kernel, chunks=chunks, copies=copies, n=n),
        in_specs=[vmem, hbm] + [vmem] * 9,
        out_specs=[hbm, vmem] + [hbm] * 8,
        out_shape=[sds((chunks, tokens, model), BF16), sds(coef, BF16), sds(full, BF16), sds(full, BF16), sds(full, F32), sds(full, BF16),
                   sds(full, F32), sds(full, F32), sds(starts, F32), sds((chunks, tokens, model), BF16)],
        scratch_shapes=[
            pltpu.VMEM(full, F32), pltpu.VMEM(coef, BF16), pltpu.VMEM(coef, BF16), pltpu.VMEM(full, BF16), pltpu.VMEM(full, BF16),
            pltpu.VMEM(full, F32), pltpu.VMEM(full, BF16), pltpu.VMEM(full, F32), pltpu.VMEM(full, F32), pltpu.VMEM(starts, F32),
            pltpu.VMEM((2, tokens, model), BF16),
            pltpu.VMEM((length + 8, width), F32), pltpu.VMEM((length, width), F32), pltpu.VMEM((length, width), F32),
            pltpu.VMEM((length, wide), BF16), pltpu.VMEM((2 * n, length), F32), pltpu.VMEM((wide, width), BF16), pltpu.VMEM((wide, width), BF16),
            pltpu.VMEM((n, width), F32), pltpu.VMEM((n, width), F32),
            dma(()), dma(()), dma((7, rows * chunks)), dma((2,)), dma((chunks, 2)), dma((zs, max(1, ys - 1), 2)), dma((zs, 2)), dma((zs, 2)), dma(()),
            dma((chunks, rows)), dma((chunks, rows)), dma((chunks, rows)), dma((chunks, rows)),
        ],
        compiler_params=pltpu.CompilerParams(collective_id=1, has_side_effects=True, vmem_limit_bytes=60 * 1024 * 1024),
        name="forward",
    )(ci, gate, gm, taps, cbias, selw, stepw, sbias, decay, skip, wout)


class Exchange:
    def __init__(self, gin, out, bufs, sems, chunks, copies):
        self.gin, self.out = gin, out
        self.g1, self.mine_v, self.g2, self.t_v, self.fin = bufs
        self.load, self.s1, self.r1, self.s2, self.r2, self.s3, self.r3, self.s4, self.r4 = sems
        self.chunks, self.xs = chunks, copies // 2
        self.me, self.mine = lax.axis_index("seq"), lax.axis_index("dp")
        self.x, self.c = self.mine // 2, self.mine % 2
        self.piece, self.width = self.t_v.shape[1:]

    def own(self, q):
        return pltpu.make_async_copy(self.gin.at[:, q * 2 + self.c], self.mine_v.at[q], self.load.at[q])

    def to_core(self, q):
        return remote(self.gin.at[:, q * 2 + 1 - self.c], self.g1.at[q], self.s1.at[q], self.r1.at[q], {"dp": self.x * 2 + 1 - self.c})

    def across(self, q):
        return remote(self.mine_v.at[q], self.g2.at[self.x], self.s2.at[q], self.r2.at[self.x], {"dp": q * 2 + self.c})

    def from_across(self, q):
        return remote(self.g2.at[q], self.g2.at[q], self.s2.at[q], self.r2.at[q], {"dp": q * 2 + self.c})

    def columns(self, s):
        return self.fin.at[:, pl.ds(pl.multiple_of(s * self.width, self.width), self.width)]

    def turn(self, s):
        return remote(self.t_v.at[s], self.columns(self.me), self.s3.at[s], self.r3.at[self.me], {"seq": s})

    def turned(self, s):
        return remote(self.columns(s), self.columns(s), self.s3.at[s], self.r3.at[s], {"seq": s})

    def rows_of(self, d):
        return self.out.at[pl.ds(pl.multiple_of(d * self.piece, self.piece), self.piece)]

    def share_to(self, k, d):
        return remote(self.fin, self.rows_of(self.mine), self.s4.at[k], self.r4.at[self.mine], {"dp": d})

    def hand_on(self, row, k):
        return remote(self.rows_of(row), self.rows_of(row), self.s4.at[k], self.r4.at[row], {"dp": self.x * 2 + 1 - self.c})

    def shared(self, d):
        return remote(self.rows_of(d), self.rows_of(d), self.s4.at[0], self.r4.at[d], {"dp": d})

    def keep(self):
        return pltpu.make_async_copy(self.fin, self.rows_of(self.mine), self.load.at[self.xs])

    def others(self, fn):
        def one(k, _):
            fn(lax.rem(self.me + k, self.chunks))
            return 0
        lax.fori_loop(1, self.chunks, one, 0)

    def column_peers(self):
        return [lax.rem(self.x + j, self.xs) * 2 + self.c for j in range(1, self.xs)]

    def begin(self):
        for q in range(self.xs):
            self.own(q).start()
            self.to_core(q).start()

    def chip(self):
        for q in range(self.xs):
            self.own(q).wait()
            self.to_core(q).wait_recv()

            def fold(s, _):
                self.mine_v[q, s] = (self.mine_v[q, s].astype(F32) + self.g1[q, s].astype(F32)).astype(BF16)
                return 0
            lax.fori_loop(0, self.chunks, fold, 0)
            pl.when(q != self.x)(lambda: self.across(q).start())

    def spread(self):
        for q in range(self.xs):
            pl.when(q != self.x)(lambda: self.from_across(q).wait_recv())

        def fold(s, _):
            total = self.mine_v[self.x, s].astype(F32)
            for j in range(1, self.xs):
                total = total + self.g2[lax.rem(self.x + j, self.xs), s].astype(F32)
            self.t_v[s] = total.astype(BF16)
            return 0
        lax.fori_loop(0, self.chunks, fold, 0)
        self.others(lambda s: self.turn(s).start())
        self.columns(self.me)[...] = self.t_v[self.me]

    def share(self):
        self.others(lambda s: self.turned(s).wait_recv())
        for j, d in enumerate(self.column_peers()):
            self.share_to(1 + j, d).start()
        self.share_to(0, self.x * 2 + 1 - self.c).start()
        self.keep().start()

    def pass_on(self):
        for j, d in enumerate(self.column_peers()):
            self.shared(d).wait_recv()
            self.hand_on(d, self.xs + j).start()

    def finish(self):
        self.keep().wait()
        for j in range(self.xs):
            self.shared(lax.rem(self.x + j, self.xs) * 2 + 1 - self.c).wait_recv()
        for q in range(self.xs):
            self.to_core(q).wait_send()
            pl.when(q != self.x)(lambda: self.across(q).wait_send())
        self.others(lambda s: self.turn(s).wait_send())
        for j in range(self.xs):
            self.share_to(j, self.mine).wait_send()
        for j, d in enumerate(self.column_peers()):
            self.hand_on(d, self.xs + j).wait_send()


def exchange_scratch(chunks, copies, piece, width):
    xs = copies // 2
    dma = pltpu.SemaphoreType.DMA
    slab = (chunks, piece, width)
    bufs = [pltpu.VMEM((xs,) + slab, BF16), pltpu.VMEM((xs,) + slab, BF16), pltpu.VMEM((xs,) + slab, BF16), pltpu.VMEM(slab, BF16),
            pltpu.VMEM((piece, chunks * width), BF16)]
    return bufs + [dma((xs + 1,)), dma((xs,)), dma((xs,)), dma((xs,)), dma((xs,)), dma((chunks,)), dma((chunks,)), dma((2 * xs,)), dma((copies,))]


def order_of(zs):
    return [sorted(range(zs), key=lambda t: (-abs(t - z), t)) for z in range(zs)]


def scatter_kernel(*refs, chunks, copies, split):
    gc_ref, gg_ref, w_ref, late_ref = refs[:4]
    norm_ref = refs[4] if split else None
    refs = refs[4 + split:]
    red_ref, sum_ref = refs[:2]
    all_ref = refs[2] if split else None
    refs = refs[2 + split:]
    (ysend_v, yrecv_v, own_v, zrecv_v, lend_v, late_v, w_v, load_sem,
     ysend, yrecv, zup, zdown, zrecv, lend_sem, lsend, lrecv) = refs[:16]
    if split:
        gin_v, norm_v, norm_sem = refs[16:19]
        trade = Exchange(gin_v, all_ref, refs[19:24], refs[24:33], chunks, copies)
    zs, ys = grid_of(chunks, copies)
    xs = copies // 2
    me, mine = lax.axis_index("seq"), lax.axis_index("dp")
    z, y = me // ys, me % ys
    x, c = mine // 2, mine % 2
    tokens, width = gc_ref.shape[1:]
    model = w_ref.shape[0]
    half = tokens // 2
    tile = min(256, model)
    tables = order_of(zs)
    partner = z + 1 - 2 * (z % 2)

    def dest(i):
        got = 0
        for k in range(zs):
            got = got + jnp.where(z == k, tables[k][i], 0)
        return got

    w_in = pltpu.make_async_copy(w_ref, w_v, load_sem.at[0])
    w_in.start()

    def norm_in(s):
        cols = pl.ds(pl.multiple_of(s * norm_v.shape[-1], norm_v.shape[-1]), norm_v.shape[-1])
        return pltpu.make_async_copy(norm_ref.at[:, :, cols], norm_v.at[s % 2], norm_sem.at[s % 2])

    if split:
        norm_in(0).start()
    meet(chunks, copies)

    def late_to(d):
        return remote(late_ref, late_v.at[mine], lsend.at[d], lrecv.at[mine], {"dp": d})

    def late_from(d):
        return remote(late_v.at[d], late_v.at[d], lsend.at[d], lrecv.at[d], {"dp": d})

    def every_copy(fn):
        def one(k, _):
            fn(lax.rem(mine + k, copies))
            return 0
        lax.fori_loop(1, copies, one, 0)

    w_in.wait()

    def partial(s, out, at):
        def one(i, _):
            sl = pl.ds(pl.multiple_of(i * tile, tile), tile)
            got = nt_dot(gc_ref[s], w_v[sl, :width]) + nt_dot(gg_ref[s], w_v[sl, width:])
            out[at, :, sl] = got.astype(BF16)
            return 0
        lax.fori_loop(0, model // tile, one, 0)

    def to_side(i, j, h):
        rows = pl.ds(h * half, half)
        k = i * (ys - 1) + j - 1
        return remote(ysend_v.at[k % ysend_v.shape[0], rows], yrecv_v.at[k, rows], ysend.at[k, h], yrecv.at[k, h], {"seq": z * ys + lax.rem(y + j, ys)})

    slots = ysend_v.shape[0]
    even = ys == 2 and zs % 2 == 0 and slots == zs

    def lend(i):
        return remote(ysend_v.at[i, pl.ds(half, half)], lend_v, lend_sem.at[0], lend_sem.at[1], {"seq": partner * ys + y})

    def send_side(i, j, h):
        if not even or h == 0:
            to_side(i, j, h).start()
            return

        @pl.when(dest(i) != partner)
        def _():
            if i == zs - 1:
                lend(i).wait_recv()

                def one(r, _):
                    sl = pl.ds(pl.multiple_of(half + r * 32, 32), 32)
                    ysend_v[i, sl, :] = (ysend_v[i, sl, :].astype(F32) + lend_v[pl.ds(pl.multiple_of(r * 32, 32), 32), :].astype(F32)).astype(BF16)
                    return 0
                lax.fori_loop(0, half // 32, one, 0)
            to_side(i, j, h).start()

    def if_sent(i, h, fn):
        if even and h == 1:
            pl.when(dest(i) != partner)(fn)
        else:
            fn()

    ahead = 2 if slots == zs * (ys - 1) else zs
    def outgoing(i):
        for j in range(1, ys):
            k = i * (ys - 1) + j - 1
            if k >= slots:
                for h in range(2):
                    to_side((k - slots) // (ys - 1), (k - slots) % (ys - 1) + 1, h).wait_send()
            partial(dest(i) * ys + lax.rem(y + j, ys), ysend_v, k % slots)
            if i < ahead:
                for h in range(2):
                    send_side(i, j, h)
            if even:
                pl.when(dest(i) == partner)(lambda: lend(i).start())

    if split:
        for i in range(min(2, zs)):
            outgoing(i)

        def weights(s, _):
            @pl.when(s + 1 < chunks)
            def _():
                norm_in(s + 1).start()

            norm_in(s).wait()
            n_all = norm_v[s % 2].reshape(chunks * tokens, norm_v.shape[-1])
            got = lax.dot_general(n_all, gc_ref[...].reshape(chunks * tokens, width), (((0,), (0,)), ((), ())), preferred_element_type=F32)
            gin_v[s] = got.astype(BF16).reshape(gin_v.shape[1:])
            return 0

        lax.fori_loop(0, chunks, weights, 0)
        trade.begin()

    for i in range(min(2, zs) if split else 0, zs):
        outgoing(i)
    if split:
        trade.chip()
    every_copy(lambda d: late_to(d).start())

    def arrived(i, j, h):
        rows = pl.ds(h * half, half)
        k = i * (ys - 1) + j - 1
        return remote(yrecv_v.at[k, rows], yrecv_v.at[k, rows], ysend.at[k, h], yrecv.at[k, h], {"seq": z * ys + lax.rem(y + j, ys)})

    def climb(t, h):
        rows = pl.ds(h * half, half)
        return remote(own_v.at[t, rows], zrecv_v.at[t, rows], zup.at[t, h], zrecv.at[t, h], {"seq": (z + 1) * ys + y})

    def sink(t, h):
        rows = pl.ds(h * half, half)
        slot = jnp.where(t == z - 1, zs, t)
        return remote(own_v.at[t, rows], zrecv_v.at[slot, rows], zdown.at[t, h], zrecv.at[slot, h], {"seq": (z - 1) * ys + y})

    def from_z(slot, h):
        rows = pl.ds(h * half, half)
        return remote(zrecv_v.at[slot, rows], zrecv_v.at[slot, rows], zup.at[0, h], zrecv.at[slot, h], {"seq": lax.rem(me + 1, chunks)})

    def accumulate(t, h, read):
        def one(r, _):
            sl = pl.ds(pl.multiple_of(h * half + r * 32, 32), 32)
            own_v[t, sl, :] = (own_v[t, sl, :].astype(F32) + read(sl)).astype(BF16)
            return 0
        lax.fori_loop(0, half // 32, one, 0)

    for i in range(zs):
        t = dest(i)
        partial(t * ys + y, own_v, t)
        for h in range(2):
            for j in range(1, ys):
                if_sent(i, h, lambda: arrived(i, ys - j, h).wait_recv())

            def side_sum(sl):
                total = yrecv_v[i * (ys - 1), sl, :].astype(F32)
                for j in range(2, ys):
                    total = total + yrecv_v[i * (ys - 1) + j - 1, sl, :].astype(F32)
                return total

            if ys > 1:
                if_sent(i, h, lambda: accumulate(t, h, side_sum))

            @pl.when(((t > z) & (z > 0)) | ((t == z) & (z > 0)))
            def _():
                from_z(t, h).wait_recv()
                accumulate(t, h, lambda sl: zrecv_v[t, sl, :].astype(F32))

            @pl.when((t < z) & (z + 1 < zs))
            def _():
                from_z(t, h).wait_recv()
                accumulate(t, h, lambda sl: zrecv_v[t, sl, :].astype(F32))

            @pl.when((t == z) & (z + 1 < zs))
            def _():
                from_z(zs, h).wait_recv()
                accumulate(t, h, lambda sl: zrecv_v[zs, sl, :].astype(F32))

            @pl.when(t > z)
            def _():
                climb(t, h).start()

            @pl.when(t < z)
            def _():
                sink(t, h).start()
        if split and i == 0:
            trade.spread()
        if split and i == min(1, zs - 1):
            trade.share()
        if i + ahead < zs:
            for j in range(1, ys):
                for h in range(2):
                    send_side(i + ahead, j, h)

    red_ref[...] = own_v[z]
    every_copy(lambda d: late_from(d).wait_recv())
    total = late_ref[...].astype(F32)
    for k in range(1, copies):
        total = total + late_v[lax.rem(mine + k, copies)].astype(F32)
    sum_ref[...] = total
    if split:
        trade.pass_on()
        trade.finish()

    every_copy(lambda d: late_to(d).wait_send())
    count = zs * (ys - 1)
    for k in range(max(0, count - slots), count):
        for h in range(2):
            if_sent(k // (ys - 1), h, lambda: to_side(k // (ys - 1), k % (ys - 1) + 1, h).wait_send())
    if even:
        lend(0).wait_send()
    for i in range(zs):
        t = dest(i)
        for h in range(2):
            @pl.when(t > z)
            def _():
                climb(t, h).wait_send()

            @pl.when(t < z)
            def _():
                sink(t, h).wait_send()


def scatter_sums(gc, gg, w_all, late, normed, chunks, copies, split):
    tokens, width = gc.shape[1:]
    model = w_all.shape[0]
    zs, ys = grid_of(chunks, copies)
    xs = max(1, copies // 2)
    others = max(1, zs * (ys - 1))
    slots = min(others, 4)
    any_spec = pl.BlockSpec(memory_space=pl.ANY)
    vmem = pl.BlockSpec(memory_space=pltpu.VMEM)
    sds = jax.ShapeDtypeStruct
    dma = pltpu.SemaphoreType.DMA
    args = [gc, gg, w_all, late]
    in_specs = [vmem, vmem, any_spec, vmem]
    out_specs = [vmem, vmem]
    out_shape = [sds((tokens, model), BF16), sds(late.shape, F32)]
    scratch = [pltpu.VMEM((slots, tokens, model), BF16), pltpu.VMEM((others, tokens, model), BF16),
               pltpu.VMEM((zs, tokens, model), BF16), pltpu.VMEM((zs + 1, tokens, model), BF16), pltpu.VMEM((tokens // 2, model), BF16),
               pltpu.VMEM((copies,) + late.shape, BF16), pltpu.VMEM(w_all.shape, BF16)]
    sems = [dma((1,)), dma((others, 2)), dma((others, 2)), dma((zs, 2)), dma((zs, 2)), dma((zs + 1, 2)), dma((2,)), dma((copies,)), dma((copies,))]
    if split:
        share = model // chunks
        piece = share // copies
        args.append(normed)
        in_specs.append(any_spec)
        out_specs.append(any_spec)
        out_shape.append(sds((share, chunks * width), BF16))
        sems += [pltpu.VMEM((chunks, copies, piece, width), BF16), pltpu.VMEM((2, chunks, tokens, share), BF16), dma((2,))]
        sems += exchange_scratch(chunks, copies, piece, width)
    return pl.pallas_call(
        functools.partial(scatter_kernel, chunks=chunks, copies=copies, split=split),
        in_specs=in_specs,
        out_specs=out_specs,
        out_shape=out_shape,
        scratch_shapes=scratch + sems,
        compiler_params=pltpu.CompilerParams(collective_id=3, has_side_effects=True, vmem_limit_bytes=62 * 1024 * 1024),
        name="scatter_sums",
    )(*args)
def backward_kernel(*refs, chunks, copies, n, inside, extra, split):
    ins = 14 + (1 if inside else 0) + (1 if split else 0) + (1 if extra else 0)
    (gg_ref, gact_ref, x_ref, dt_ref, slope_ref, start_ref, sel_ref, ci_ref, stepw_ref, decay_ref, skip_ref,
     taps_ref, cbias_ref, selw_ref) = refs[:14]
    mixed_ref = refs[14] if inside else None
    gin_ref = refs[ins - 1 - extra] if split else None
    gout_ref = refs[ins - 1] if extra else None
    outs = 2 + (1 if inside else 0) + (1 if split else 0) + (1 if extra else 0)
    gci_ref, late_ref = refs[ins:ins + 2]
    red_ref = refs[ins + 2] if inside else None
    all_ref = refs[ins + outs - 1 - extra] if split else None
    gsum_ref = refs[ins + outs - 1] if extra else None
    refs = refs[ins + outs:]
    (gg_v, gact_v, x_v, dt_v, slope_v, start_v, gci_v, gvals_v, part_v, recv_v, sel2_v,
     u_s, gy_s, gu_s, ah_s, bcoef_s, bt_s, hist_s, adj_a, harm_a, adj_b, harm_b, db_s, dc_s, carry_s, gd_s, rate_s, factor_s, kept_s,
     gstepw_ref, gsbias_ref, gskip_ref, gtaps_ref, gcbias_ref, gselw_ref,
     ext_s, gext_s, in_sem, gci_sem, send1, recv1, send2, recv2) = refs[:43]
    refs = refs[43:]
    if inside:
        own_v, yrecv_v, zrecv_v, own_sem, ysend, yrecv, zup, zdown, zrecv = refs[:9]
        refs = refs[9:]
    if extra:
        core_v, half_v, far_v, esend, erecv, asend, arecv, bsend, brecv = refs[:9]
        refs = refs[9:]
    if split:
        trade = Exchange(gin_ref, all_ref, refs[:5], refs[5:14], chunks, copies)
    zs, ys = grid_of(chunks, copies)
    xs = copies // 2
    me, mine = lax.axis_index("seq"), lax.axis_index("dp")
    z, y = me // ys, me % ys
    xd, cd = mine // 2, mine % 2
    rows = sel_ref.shape[1]
    rank = stepw_ref.shape[0]
    count = rows * chunks

    def where_of(i):
        return chunks - 1 - i % chunks, i // chunks

    streams = ((gg_ref, gg_v), (gact_ref, gact_v), (x_ref, x_v), (dt_ref, dt_v), (slope_ref, slope_v), (start_ref, start_v))

    def fetch(i):
        c, r = where_of(i)
        return [pltpu.make_async_copy(src.at[c, r], dst.at[i % 2], in_sem.at[k, i % 2]) for k, (src, dst) in enumerate(streams)]

    for one in fetch(0):
        one.start()
    if inside:
        tokens, model = red_ref.shape
        half = tokens // 2
        own_loads = [pltpu.make_async_copy(mixed_ref.at[t * ys + y], own_v.at[t], own_sem.at[t]) for t in range(zs)]
        for one in own_loads:
            one.start()
    meet(chunks, copies if extra else 1)

    if split:
        trade.begin()

    if inside:
        tables = order_of(zs)

        def dest(i):
            got = 0
            for k in range(zs):
                for q in range(zs):
                    got = got + jnp.where((z == k) & (i == q), tables[k][q], 0)
            return got

        def part_rows(h):
            return pl.ds(h * half, half)

        def to_side(i, h):
            return remote(mixed_ref.at[dest(i) * ys + 1 - y, part_rows(h)], yrecv_v.at[i, part_rows(h)], ysend.at[i, h], yrecv.at[i, h], {"seq": z * ys + 1 - y})

        def arrived(i, h):
            return remote(yrecv_v.at[i, part_rows(h)], yrecv_v.at[i, part_rows(h)], ysend.at[i, h], yrecv.at[i, h], {"seq": z * ys + 1 - y})

        def climb(t, h):
            return remote(own_v.at[t, part_rows(h)], zrecv_v.at[t, part_rows(h)], zup.at[t, h], zrecv.at[t, h], {"seq": (z + 1) * ys + y})

        def sink(t, h):
            slot = jnp.where(t == z - 1, zs, t)
            return remote(own_v.at[t, part_rows(h)], zrecv_v.at[slot, part_rows(h)], zdown.at[t, h], zrecv.at[slot, h], {"seq": (z - 1) * ys + y})

        def from_z(slot, h):
            return remote(zrecv_v.at[slot, part_rows(h)], zrecv_v.at[slot, part_rows(h)], zup.at[0, h], zrecv.at[slot, h], {"seq": lax.rem(me + 1, chunks)})

        def accumulate(t, h, buf, slot):
            def one(r, _):
                sl = pl.ds(pl.multiple_of(h * half + r * 32, 32), 32)
                own_v[t, sl, :] = own_v[t, sl, :] + buf[slot, sl, :]
                return 0
            lax.fori_loop(0, half // 32, one, 0)

        def settle(i):
            t = dest(i)
            for h in range(2):
                arrived(i, h).wait_recv()
                accumulate(t, h, yrecv_v, i)

                @pl.when((t >= z) & (z > 0))
                def _():
                    from_z(t, h).wait_recv()
                    accumulate(t, h, zrecv_v, t)

                @pl.when((t < z) & (z + 1 < zs))
                def _():
                    from_z(t, h).wait_recv()
                    accumulate(t, h, zrecv_v, t)

                @pl.when((t == z) & (z + 1 < zs))
                def _():
                    from_z(zs, h).wait_recv()
                    accumulate(t, h, zrecv_v, zs)

                @pl.when(t > z)
                def _():
                    climb(t, h).start()

                @pl.when(t < z)
                def _():
                    sink(t, h).start()

            @pl.when(i + 2 < zs)
            def _():
                for h in range(2):
                    to_side(i + 2, h).start()

        for i in range(2):
            for h in range(2):
                to_side(i, h).start()
        edge = (z == 0) | (z == zs - 1)

    if extra:
        grows = gout_ref.shape[0] // 2

        def part_of(core):
            return pl.ds(pl.multiple_of(core * grows, grows), grows)

        to_core = remote(gout_ref.at[part_of(1 - cd)], core_v, esend, erecv, {"dp": xd * 2 + 1 - cd})

        def across(j):
            return remote(half_v, far_v.at[xd], asend.at[j], arecv.at[xd], {"dp": lax.rem(xd + j, xs) * 2 + cd})

        def from_across(j):
            q = lax.rem(xd + j, xs)
            return remote(far_v.at[q], far_v.at[q], asend.at[j], arecv.at[q], {"dp": q * 2 + cd})

        back_out = remote(gsum_ref.at[part_of(cd)], gsum_ref.at[part_of(cd)], bsend, brecv, {"dp": xd * 2 + 1 - cd})
        back_in = remote(gsum_ref.at[part_of(1 - cd)], gsum_ref.at[part_of(1 - cd)], bsend, brecv, {"dp": xd * 2 + 1 - cd})
        to_core.start()

        def by_rows(fn):
            def one(i, _):
                fn(pl.ds(pl.multiple_of(i * 16, 16), 16), pl.ds(pl.multiple_of(cd * grows + i * 16, 16), 16))
                return 0
            lax.fori_loop(0, grows // 16, one, 0)

        def chip_sum():
            to_core.wait_recv()

            def fold(at, full):
                half_v[at, :] = (gout_ref[full, :].astype(F32) + core_v[at, :].astype(F32)).astype(BF16)
            by_rows(fold)
            for j in range(1, xs):
                across(j).start()

        def whole_sum():
            for j in range(1, xs):
                from_across(j).wait_recv()

            def fold(at, full):
                total = half_v[at, :].astype(F32)
                for j in range(1, xs):
                    total = total + far_v[lax.rem(xd + j, xs), at, :].astype(F32)
                gsum_ref[full, :] = total.astype(BF16)
            by_rows(fold)
            back_out.start()

    def first(s, r):
        return remote(part_v.at[s, r], recv_v.at[me, r], send1.at[s, r], recv1.at[me, r], {"seq": s})

    def landed_first(s, r):
        return remote(part_v.at[s, r], recv_v.at[s, r], send1.at[s, r], recv1.at[s, r], {"seq": s})

    def second(s, r):
        return remote(sel2_v.at[me, r], sel2_v.at[me, r], send2.at[s, r], recv2.at[me, r], {"seq": s})

    def landed_second(s, r):
        return remote(sel2_v.at[s, r], sel2_v.at[s, r], send2.at[s, r], recv2.at[s, r], {"seq": s})

    def every_other(fn):
        def one(k, _):
            fn(lax.rem(me + k, chunks))
            return 0
        lax.fori_loop(1, chunks, one, 0)

    def send_row(r):
        every_other(lambda s: first(s, r).start())
        recv_v[me, r] = part_v[me, r]

    def sum_row(r):
        every_other(lambda s: landed_first(s, r).wait_recv())
        total = recv_v[0, r].astype(F32)
        for s in range(1, chunks):
            total = total + recv_v[s, r].astype(F32)
        sel2_v[me, r] = total.astype(BF16)
        every_other(lambda s: second(s, r).start())

    for ref in (gstepw_ref, gsbias_ref, gskip_ref, gd_s, gtaps_ref, gcbias_ref, gselw_ref):
        ref[...] = jnp.zeros_like(ref)
    rate_s[...] = -jnp.exp(decay_ref[...].astype(F32)) * LOG2E

    def gci_out(i):
        c, r = where_of(i)
        return pltpu.make_async_copy(gci_v.at[i % 2], gci_ref.at[c, r], gci_sem.at[i % 2])

    def scan(i, _):
        c, r = where_of(i)
        slot = i % 2

        @pl.when(i + 1 < count)
        def _():
            for one in fetch(i + 1):
                one.start()

        for one in fetch(i):
            one.wait()
        back_step(sel_ref[c, r].astype(F32), x_v[slot].astype(F32), i % chunks == 0, gact_v.at[slot], gg_v.at[slot],
                  start_v.at[slot], dt_v.at[slot], slope_v.at[slot], stepw_ref, skip_ref,
                  gvals_v.at[c, r], part_v.at[c, r], gstepw_ref, gsbias_ref, gskip_ref,
                  u_s, gy_s, gu_s, ah_s, bcoef_s, bt_s, hist_s, adj_a, harm_a, adj_b, harm_b, db_s, dc_s, carry_s, gd_s, rate_s, factor_s, kept_s, rank, n)
        late = min(3, chunks - 1)

        @pl.when((i % chunks == chunks - 1) & (r + 1 < rows))
        def _():
            send_row(r)

        @pl.when((i % chunks == late) & (r > 0))
        def _():
            sum_row(r - 1)

        if split:
            pl.when(i == 1)(trade.chip)
            pl.when(i == 5)(trade.spread)
            pl.when(i == 14)(trade.share)
        if extra:
            pl.when(i == 2)(chip_sum)
            pl.when(i == 8)(whole_sum)
        if inside:
            lo = jnp.where(edge, jnp.where(i == 4, 0, jnp.where(i == 9, 1, 2)), jnp.where(i == 9, 0, 1))
            hi = jnp.where(edge, lo + 1, jnp.where(i == 9, 1, jnp.where(i == 13, 3, 0)))

            @pl.when((i == 4) | (i == 9) | (i == 13))
            def _():
                for k in range(own_v.shape[0]):
                    pl.when(i == 4)(own_loads[k].wait)

                def one(k, _):
                    settle(k)
                    return 0
                lax.fori_loop(lo, hi, one, 0)
        return 0

    lax.fori_loop(0, count, scan, 0)
    send_row(rows - 1)

    def conv(i, _):
        c, r = where_of(i)

        @pl.when(i >= 2)
        def _():
            gci_out(i - 2).wait()

        conv_back_step(ci_ref.at[c, r], ci_ref.at[jnp.maximum(c - 1, 0), r], c == 0, i % chunks == 0, gvals_v.at[c, r], sel2_v.at[c, r],
                       taps_ref, cbias_ref, selw_ref, gci_v.at[i % 2], gtaps_ref, gcbias_ref, gselw_ref, ext_s, gext_s)
        gci_out(i).start()
        return 0

    for r in range(rows - 1):
        every_other(lambda s: landed_second(s, r).wait_recv())
    lax.fori_loop(0, count - chunks, conv, 0)
    sum_row(rows - 1)
    if inside:
        settle(zs - 1)
        red_ref[...] = own_v[z]
    if split:
        trade.pass_on()
    every_other(lambda s: landed_second(s, rows - 1).wait_recv())
    lax.fori_loop(count - chunks, count, conv, 0)
    picked, taps = gselw_ref.shape[0], gtaps_ref.shape[0]
    late_ref[0:picked, :] = gselw_ref[...].astype(BF16)
    late_ref[picked:picked + rank, :] = gstepw_ref[...].astype(BF16)
    late_ref[picked + rank:picked + rank + n, :] = (gd_s[...] * rate_s[...] * (1.0 / LOG2E)).astype(BF16)
    filler = jnp.zeros((13 - taps, gtaps_ref.shape[1]), F32)
    late_ref[picked + rank + n:, :] = jnp.concatenate([gtaps_ref[...], gsbias_ref[...], gskip_ref[...], gcbias_ref[...], filler], axis=0).astype(BF16)
    for i in range(max(0, count - 2), count):
        gci_out(i).wait()
    if split:
        trade.finish()
    for r in range(rows):
        every_other(lambda s: first(s, r).wait_send())
        every_other(lambda s: second(s, r).wait_send())
    if extra:
        to_core.wait_send()
        for j in range(1, xs):
            across(j).wait_send()
        back_in.wait_recv()
        back_out.wait_send()
    if inside:
        for i in range(zs):
            t = dest(i)
            for h in range(2):
                to_side(i, h).wait_send()

                @pl.when(t > z)
                def _():
                    climb(t, h).wait_send()

                @pl.when(t < z)
                def _():
                    sink(t, h).wait_send()


def backward(gg, gact, x, dt, slope, starts, sel, ci, stepw, decay, skip, taps, cbias, selw, mixed, ging, gout, copies, n):
    chunks, rows, length, width = ci.shape
    rank = stepw.shape[0]
    zs, ys = grid_of(chunks, copies)
    xs = max(1, copies // 2)
    wide = BLOCK * n
    inside = mixed is not None
    extra = copies % 2 == 0
    split = ging is not None
    sds = jax.ShapeDtypeStruct
    dma = pltpu.SemaphoreType.DMA
    vmem = pl.BlockSpec(memory_space=pltpu.VMEM)
    hbm = pl.BlockSpec(memory_space=pl.ANY)
    args = [gg, gact, x, dt, slope, starts, sel, ci, stepw, decay, skip, taps, cbias, selw]
    in_specs = [hbm] * 6 + [vmem] * 8
    out_specs = [hbm, vmem]
    out_shape = [sds(ci.shape, BF16), sds((selw.shape[0] + rank + n + 16, width), BF16)]
    tile, coef = (length, width), sel.shape
    scratch = [pltpu.VMEM((2,) + tile, F32), pltpu.VMEM((2,) + tile, F32), pltpu.VMEM((2,) + tile, BF16),
               pltpu.VMEM((2,) + tile, F32), pltpu.VMEM((2,) + tile, F32), pltpu.VMEM((2, n, width), F32),
               pltpu.VMEM((2,) + tile, BF16), pltpu.VMEM(ci.shape, F32),
               pltpu.VMEM(coef, BF16), pltpu.VMEM(coef, BF16), pltpu.VMEM(coef, BF16),
               pltpu.VMEM(tile, F32), pltpu.VMEM(tile, F32), pltpu.VMEM(tile, F32), pltpu.VMEM(tile, F32),
               pltpu.VMEM((length, wide), BF16), pltpu.VMEM((2 * n, length), F32), pltpu.VMEM((length * n, width), BF16),
               pltpu.VMEM((wide, width), BF16), pltpu.VMEM((wide, width), BF16), pltpu.VMEM((wide, width), BF16), pltpu.VMEM((wide, width), BF16),
               pltpu.VMEM((length, wide), F32), pltpu.VMEM((length, wide), F32),
               pltpu.VMEM((n, width), F32), pltpu.VMEM((n, width), F32), pltpu.VMEM((n, width), F32),
               pltpu.VMEM((length * n, width), F32), pltpu.VMEM((length * n, width), F32),
               pltpu.VMEM((rank, width), F32), pltpu.VMEM((1, width), F32), pltpu.VMEM((1, width), F32),
               pltpu.VMEM(taps.shape, F32), pltpu.VMEM((1, width), F32), pltpu.VMEM(selw.shape, F32),
               pltpu.VMEM((length + 8, width), F32), pltpu.VMEM((length + 8, width), F32),
               dma((6, 2)), dma((2,)), dma((chunks, rows)), dma((chunks, rows)), dma((chunks, rows)), dma((chunks, rows))]
    if inside:
        tokens, model = mixed.shape[1:]
        args.append(mixed)
        in_specs.append(hbm)
        out_specs.append(vmem)
        out_shape.append(sds((tokens, model), BF16))
        scratch += [pltpu.VMEM((zs, tokens, model), BF16), pltpu.VMEM((zs, tokens, model), BF16), pltpu.VMEM((zs + 1, tokens, model), BF16),
                    dma((zs,)), dma((zs, 2)), dma((zs, 2)), dma((zs, 2)), dma((zs, 2)), dma((zs + 1, 2))]
    if split:
        args.append(ging)
        in_specs.append(hbm)
        out_specs.append(hbm)
        out_shape.append(sds((copies * ging.shape[2], chunks * width), BF16))
    if extra:
        args.append(gout)
        in_specs.append(vmem)
        out_specs.append(vmem)
        out_shape.append(sds(gout.shape, BF16))
        part = (gout.shape[0] // 2, gout.shape[1])
        scratch += [pltpu.VMEM(part, BF16), pltpu.VMEM(part, BF16), pltpu.VMEM((xs,) + part, BF16),
                    dma(()), dma(()), dma((xs,)), dma((xs,)), dma(()), dma(())]
    if split:
        scratch += exchange_scratch(chunks, copies, ging.shape[2], width)
    return pl.pallas_call(
        functools.partial(backward_kernel, chunks=chunks, copies=copies, n=n, inside=inside, extra=extra, split=split),
        in_specs=in_specs,
        out_specs=out_specs,
        out_shape=out_shape,
        scratch_shapes=scratch,
        compiler_params=pltpu.CompilerParams(collective_id=2, has_side_effects=True, vmem_limit_bytes=63 * 1024 * 1024),
        name="backward",
    )(*args)


from jax.sharding import PartitionSpec as P


def local(hidden, grad_out, lengths, norm_gain, input_weight, conv_weight, conv_bias, select_weight,
          step_weight, step_bias, decay_log, skip_weight, output_weight):
    rows, length, model = hidden.shape
    chunks = lax.axis_size("seq")
    copies = lax.axis_size("dp")
    width = output_weight.shape[0]
    share = input_weight.shape[0]
    rank = step_weight.shape[0]
    n = decay_log.shape[0]
    tokens = chunks * rows * length
    here = lax.axis_index("seq")

    split = (share // copies) % 16 == 0 and copies % 2 == 0
    normed, ci, gate, w_all, gain_row = gather_project(
        hidden.reshape(rows * length, model), input_weight, norm_gain.astype(F32).reshape(1, share), chunks, copies, share, split)
    normed = normed.reshape(tokens, model)
    slots = here * length + lax.broadcasted_iota(jnp.int32, (rows, length), 1)
    valid = (slots < lengths[:, None]).astype(F32)[..., None]
    cotangent = grad_out.astype(F32) * valid
    shaped = lambda a: a.reshape(chunks, rows, length, a.shape[-1])
    ci, gate = shaped(ci), shaped(gate)
    bias_row = conv_bias.reshape(1, width)
    step_row = step_bias.reshape(1, width)
    skip_row = skip_weight.reshape(1, width)
    gm, sel, x, gated, gact, tail, dt, slope, starts, mixed = forward(
        ci, gate, cotangent.astype(BF16).reshape(rows * length, model), conv_weight, bias_row, select_weight,
        step_weight, step_row, decay_log, skip_row, output_weight, copies, n)
    gm = gm.reshape(tokens, model)
    gated2 = gated.reshape(tokens, width)
    gg = lax.dot_general(gm, output_weight, (((1,), (1,)), ((), ())), preferred_element_type=F32)
    ggate = (gg * tail.reshape(tokens, width).astype(F32)).astype(BF16)
    zs, ys = grid_of(chunks, copies)
    inside = ys == 2 and zs == 4
    source = hidden.astype(F32)
    tn = lambda a, b: lax.dot_general(a, b, (((0,), (0,)), ((), ())), preferred_element_type=F32)
    blocks = lambda g: tn(normed, g).astype(BF16).reshape(chunks, copies, share // copies, width)
    ging = blocks(ggate)
    gout = tn(gated2, gm).astype(BF16)
    flat = lambda a: a.reshape(chunks, rows * length, a.shape[-1])
    got = backward(shaped(gg), gact, x, dt, slope, starts, sel, ci, step_weight, decay_log, skip_row, conv_weight, bias_row, select_weight,
                   mixed if inside else None, ging if split else None, gout, copies, n)
    gci, late = got[:2]
    mixed = got[2].reshape(rows, length, model) if inside else lax.psum_scatter(shaped(mixed), "seq", scatter_dimension=0, tiled=False)
    gout = got[-1].astype(F32)
    output = ((source + mixed.astype(F32)) * valid).astype(BF16)
    tap_count = conv_weight.shape[0]
    done = scatter_sums(flat(gci), ggate.reshape(chunks, rows * length, width), w_all, late, flat(shaped(normed)), chunks, copies, split)
    scaled, late = done[:2]
    if split:
        gin = jnp.concatenate([done[2], got[-2]], axis=1).astype(F32)
    else:
        gin = jnp.stack([blocks(gci.reshape(tokens, width)), ging], axis=3)
        gin = lax.psum_scatter(gin, "dp", scatter_dimension=1, tiled=False)
        gin = lax.all_to_all(gin, "seq", split_axis=0, concat_axis=2, tiled=False)
        gin = lax.all_gather(gin.reshape(share // copies, 2 * chunks * width), "dp", axis=0, tiled=True).astype(F32)
    ggain = jnp.sum(gin * input_weight.astype(F32), axis=1) / norm_gain.astype(F32)
    scaled = scaled.reshape(rows, length, model).astype(F32) * gain_row
    inverse = lax.rsqrt(jnp.mean(source * source, axis=-1, keepdims=True) + EPSILON)
    ghidden = inverse * scaled - source * inverse ** 3 * jnp.mean(scaled * source, axis=-1, keepdims=True) + cotangent
    sizes = (select_weight.shape[0], rank, n, tap_count)
    ends = [sum(sizes[:k + 1]) for k in range(len(sizes))]
    gselw, gstepw, gdecay, gtaps = (late[e - k:e] for e, k in zip(ends, sizes))
    gstepb, gskip, gconvb = (late[ends[-1] + k] for k in range(3))
    return (output, ghidden, ggain, gin, gtaps, gconvb, gselw, gstepw, gstepb,
            gdecay, gskip, gout)


def solution(mesh):
    tok, vec, col, row = P("dp", "seq", None), P("seq"), P(None, "seq"), P("seq", None)
    return jax.shard_map(
        local,
        mesh=mesh,
        in_specs=(tok, tok, P("dp"), vec, row, col, vec, col, col, vec, col, vec, row),
        out_specs=(tok, tok, vec, row, col, vec, col, col, vec, col, vec, row),
        check_vma=False,
    )
```

```python
import functools
import jax
import jax.numpy as jnp
from jax import lax
from jax.experimental import pallas as pl
from jax.experimental.pallas import tpu as pltpu

BLOCK = 16
EPSILON = 1e-05
LOG2E = 1.4426950408889634
F32 = jnp.float32
BF16 = jnp.bfloat16


def inverse_of(whole):
    guess = pl.reciprocal(whole, approx=True)
    return guess * (2.0 - whole * guess)


def gates_of(pre):
    small = jnp.exp2(jnp.abs(pre) * -LOG2E)
    whole = 1.0 + small
    log_part = jnp.where(small < 1e-3, small * (1.0 - small * (0.5 - small * (1.0 / 3.0))), jnp.log(whole))
    return jnp.maximum(pre, 0.0) + log_part, jnp.where(pre >= 0.0, 1.0, small) * inverse_of(whole)


def sigmoid(v):
    return 0.5 + 0.5 * jnp.tanh(0.5 * v)


def nt_dot(a, b):
    return lax.dot_general(a, b, (((1,), (1,)), ((), ())), preferred_element_type=F32)


def lane_tiles(width):
    step = min(width, 512)
    return [slice(k, k + step) for k in range(0, width, step)]


def tile_matrix(n, wide):
    col = lax.broadcasted_iota(jnp.int32, (n, wide), 1)
    row = lax.broadcasted_iota(jnp.int32, (n, wide), 0)
    return (col % n == row).astype(F32)


def diagonal_mask(rows, n, wide):
    col = lax.broadcasted_iota(jnp.int32, (rows, wide), 1)
    row = lax.broadcasted_iota(jnp.int32, (rows, wide), 0)
    return col // n == row % BLOCK


def scan_step(selected, x, gate, fresh, stepw_ref, bias_ref, skip_ref, gated_ref, gact_ref, tail_ref, dt_ref, slope_ref,
              u_s, y_s, coef_s, bt_s, hist_a, hist_b, state_s, rate_s, rank, n):
    length = x.shape[0]
    wide = BLOCK * n
    state_s[...] = jnp.where(fresh, 0.0, state_s[...])
    low = selected[:rank].T.astype(BF16)
    pre = jnp.dot(low, stepw_ref[...], preferred_element_type=F32) + bias_ref[...]
    dt, slope = gates_of(pre)
    dt_ref[...] = dt
    slope_ref[...] = slope
    u_s[...] = dt * x
    bt_s[...] = selected[rank:]
    spread = jnp.dot(selected[rank:].T[:, n:], tile_matrix(n, wide), preferred_element_type=F32)
    coef_s[...] = jnp.where(diagonal_mask(length, n, wide), spread, 0.0).astype(BF16)
    blocks = length // BLOCK

    def finish(k, hist):
        rows = pl.ds(pl.multiple_of(k * BLOCK, BLOCK), BLOCK)
        y_s[rows, :] = jnp.dot(coef_s[rows, :], hist[...], preferred_element_type=F32)

    def block(k, state, hist):
        at = pl.multiple_of(k * BLOCK, BLOCK)
        bs = pltpu.roll(bt_s[0:n, :], length - at, 1)
        dts = dt_ref[pl.ds(at, BLOCK), :]
        us = u_s[pl.ds(at, BLOCK), :]
        rate = rate_s[...]
        for i in range(BLOCK):
            factor = jnp.exp2(dts[i:i + 1, :] * rate)
            state = factor * state + us[i:i + 1, :] * bs[:, i:i + 1]
            hist[i * n:(i + 1) * n, :] = state.astype(BF16)
        return state

    def pair(j, state):
        finish(jnp.maximum(2 * j - 1, 0), hist_b)
        state = block(2 * j, state, hist_a)
        finish(2 * j, hist_a)
        return block(2 * j + 1, state, hist_b)

    state_s[...] = lax.fori_loop(0, blocks // 2, pair, state_s[...])
    finish(blocks - 1, hist_b)
    ssm = y_s[...] + skip_ref[...] * x
    sg = sigmoid(gate)
    gact = gate * sg
    gact_ref[...] = gact
    tail_ref[...] = (ssm * sg * (1.0 + gate * (1.0 - sg))).astype(BF16)
    gated_ref[...] = (ssm * gact).astype(BF16)


def back_step(selected, x, fresh, gact_ref, gg_ref, start_ref, dt_ref, slope_ref, stepw_ref, skip_ref,
              gvals_ref, gsel_ref, gstepw_ref, gbias_ref, gskip_ref,
              u_s, gy_s, gu_s, ah_s, bcoef_s, bt_s, hist_s, adj_a, harm_a, adj_b, harm_b, db_s, dc_s, carry_s, gd_s, rate_s, factor_s, kept_s, rank, n):
    length = x.shape[0]
    wide = BLOCK * n
    blocks = length // BLOCK
    carry_s[...] = jnp.where(fresh, 0.0, carry_s[...])
    gg = gg_ref[...]
    gy = gg * gact_ref[...]
    gskip_ref[...] += jnp.sum(gy * x, axis=0, keepdims=True)
    gy_s[...] = gy
    dt = dt_ref[...]
    u_s[...] = dt * x
    bt_s[...] = selected[rank:]
    tiles = tile_matrix(n, wide)
    spread = jnp.dot(selected[rank:].T[:, :n], tiles, preferred_element_type=F32)
    bcoef_s[...] = jnp.where(diagonal_mask(length, n, wide), spread, 0.0).astype(BF16)
    keep = diagonal_mask(BLOCK, n, wide)
    ones = keep.astype(BF16)
    lanes = lane_tiles(x.shape[1])
    state_s = start_ref

    def steps(lane):
        def again(k, state):
            at = pl.multiple_of(k * BLOCK, BLOCK)
            bs = pltpu.roll(bt_s[0:n, :], length - at, 1)
            dts = dt_ref[pl.ds(at, BLOCK), lane]
            us = u_s[pl.ds(at, BLOCK), lane]
            rate = rate_s[:, lane]
            for i in range(BLOCK):
                here = pl.ds(pl.multiple_of((at + i) * n, n), n)
                factor = jnp.exp2(dts[i:i + 1, :] * rate)
                factor_s[here, lane] = factor
                old = factor * state
                kept_s[here, lane] = old
                state = old + us[i:i + 1, :] * bs[:, i:i + 1]
                hist_s[here, lane] = state.astype(BF16)
            return state

        lax.fori_loop(0, blocks, again, state_s[:, lane])

        def products(k, adj_s, harm_s):
            at = pl.multiple_of(k * BLOCK, BLOCK)
            rows = pl.ds(at, BLOCK)
            adj = adj_s[:, lane]
            gu_s[rows, lane] = jnp.dot(bcoef_s[rows, :], adj, preferred_element_type=F32)
            ah_s[rows, lane] = jnp.dot(ones, harm_s[:, lane], preferred_element_type=F32)
            db = jnp.where(keep, nt_dot(u_s[rows, lane].astype(BF16), adj), 0.0)
            states = hist_s[pl.ds(pl.multiple_of(at * n, n), wide), lane]
            dc = jnp.where(keep, nt_dot(gy_s[rows, lane].astype(BF16), states), 0.0)
            if lane.start == 0:
                db_s[rows, :] = db
                dc_s[rows, :] = dc
            else:
                db_s[rows, :] += db
                dc_s[rows, :] += dc

        def block(k, carry, adj_s, harm_s):
            at = pl.multiple_of(k * BLOCK, BLOCK)
            cs = pltpu.roll(bt_s[n:2 * n, :], length - at, 1)
            dts = dt_ref[pl.ds(at, BLOCK), lane]
            gys = gy_s[pl.ds(at, BLOCK), lane]
            rate = rate_s[:, lane]
            gd = gd_s[:, lane]
            for i in range(BLOCK - 1, -1, -1):
                here = pl.ds(pl.multiple_of((at + i) * n, n), n)
                g = cs[:, i:i + 1] * gys[i:i + 1, :] + carry
                adj_s[i * n:(i + 1) * n, lane] = g.astype(BF16)
                carry = factor_s[here, lane] * g
                h = g * kept_s[here, lane]
                harm_s[i * n:(i + 1) * n, lane] = (h * rate).astype(BF16)
                gd = gd + dts[i:i + 1, :] * h
            gd_s[:, lane] = gd
            return carry

        def pair(j, carry):
            k = blocks - 1 - 2 * j
            if lane.start == 0:
                products(jnp.minimum(k + 1, blocks - 1), adj_b, harm_b)
            else:
                @pl.when(j > 0)
                def _():
                    products(k + 1, adj_b, harm_b)
            carry = block(k, carry, adj_a, harm_a)
            products(k, adj_a, harm_a)
            return block(k - 1, carry, adj_b, harm_b)

        carry_s[:, lane] = lax.fori_loop(0, blocks // 2, pair, carry_s[:, lane])
        products(0, adj_b, harm_b)

    for lane in lanes:
        steps(lane)
    gu = gu_s[...]
    gpre = ((x * gu + ah_s[...] * (1.0 / LOG2E)) * slope_ref[...]).astype(BF16)
    gvals_ref[...] = (gy * skip_ref[...] + dt * gu).astype(gvals_ref.dtype)
    gbias_ref[...] += jnp.sum(gpre.astype(F32), axis=0, keepdims=True)
    gstepw_ref[...] += jnp.dot(selected[:rank].astype(BF16), gpre, preferred_element_type=F32)
    fold = lambda ref: nt_dot(tiles.astype(BF16), ref[...].astype(BF16))
    gsel_ref[0:rank, :] = nt_dot(stepw_ref[...], gpre).astype(BF16)
    gsel_ref[rank:rank + n, :] = fold(db_s).astype(BF16)
    gsel_ref[rank + n:rank + 2 * n, :] = fold(dc_s).astype(BF16)


def conv_step(ci, fresh, taps_ref, bias_ref, selw_ref, ext_s):
    length = ci.shape[0]
    tap_count = taps_ref.shape[0]
    ext_s[0:8, :] = jnp.where(fresh, 0.0, ext_s[length:length + 8, :])
    ext_s[8:, :] = ci.astype(F32)
    total = bias_ref[...].astype(F32)
    for k in range(tap_count):
        total = total + taps_ref[k:k + 1, :].astype(F32) * ext_s[pl.ds(8 - tap_count + 1 + k, length), :]
    x = (total * sigmoid(total)).astype(BF16)
    return x, nt_dot(selw_ref[...], x).astype(BF16)


def conv_back_step(ci_ref, prev_ref, first, fresh, gvals_ref, gsel_ref, taps_ref, bias_ref, selw_ref,
                   gci_ref, gtaps_ref, gbias_ref, gselw_ref, ext_s, gext_s):
    length = ci_ref.shape[0]
    tap_count = taps_ref.shape[0]
    gext_s[length:, :] = jnp.where(fresh, 0.0, gext_s[length:, :])
    ext_s[8:, :] = ci_ref[...].astype(F32)
    before = prev_ref[...][length - 16:, :].astype(F32)[8:, :]
    ext_s[0:8, :] = jnp.where(first, 0.0, before)
    total = bias_ref[...].astype(F32)
    for k in range(tap_count):
        total = total + taps_ref[k:k + 1, :].astype(F32) * ext_s[pl.ds(8 - tap_count + 1 + k, length), :]
    sg = sigmoid(total)
    x = (total * sg).astype(BF16)
    gsel = gsel_ref[...]
    gvals = gvals_ref[...] + jnp.dot(gsel.astype(F32).T.astype(BF16), selw_ref[...], preferred_element_type=F32)
    gconv = gvals * sg * (1.0 + total * (1.0 - sg))
    gbias_ref[...] += jnp.sum(gconv, axis=0, keepdims=True)
    for k in range(tap_count):
        gtaps_ref[k:k + 1, :] += jnp.sum(gconv * ext_s[pl.ds(8 - tap_count + 1 + k, length), :], axis=0, keepdims=True)
    gselw_ref[...] += jnp.dot(gsel, x, preferred_element_type=F32)
    gext_s[0:length, :] = gconv
    gci = jnp.zeros_like(gconv)
    for k in range(tap_count):
        gci = gci + taps_ref[k:k + 1, :].astype(F32) * gext_s[pl.ds(tap_count - 1 - k, length), :]
    gci_ref[...] = gci.astype(BF16)
    gext_s[length:, :] = gconv[0:8, :]


MESH = pl.DeviceIdType.MESH


def remote(src, dst, send, recv, device):
    return pltpu.make_async_remote_copy(src_ref=src, dst_ref=dst, send_sem=send, recv_sem=recv, device_id=device, device_id_type=MESH)


def grid_of(chunks, copies):
    deep = max(1, copies // 2)
    return (chunks // deep, deep) if chunks % deep == 0 else (chunks, 1)


def meet(chunks, copies):
    me, mine = lax.axis_index("seq"), lax.axis_index("dp")
    barrier = pltpu.get_barrier_semaphore()

    def greet(k, _):
        pl.semaphore_signal(barrier, inc=1, device_id={"seq": lax.rem(me + k, chunks)}, device_id_type=MESH)
        return 0

    def greet_copy(k, _):
        pl.semaphore_signal(barrier, inc=1, device_id={"dp": lax.rem(mine + k, copies)}, device_id_type=MESH)
        return 0

    lax.fori_loop(1, chunks, greet, 0)
    if copies > 1:
        lax.fori_loop(1, copies, greet_copy, 0)
    pl.semaphore_wait(barrier, chunks - 1 + max(copies - 1, 0))


def gather_project_kernel(hid_ref, wq_ref, gain_ref, n_ref, ci_ref, gate_ref, w_ref, row_ref,
                          hid_v, gain_v, w_v, n_v, ci_v, gate_v,
                          load_sem, out_sem, hrecv, hside, hup, hdown, hlend,
                          w1send, w1recv, w2recv, w2send, w3send, gsend, grecv, *, chunks, copies, share, split):
    zs, ys = grid_of(chunks, copies)
    xs = copies // 2
    me, mine = lax.axis_index("seq"), lax.axis_index("dp")
    z, y = me // ys, me % ys
    x, c = mine // 2, mine % 2
    tokens, model = hid_v.shape[1:]
    width = ci_v.shape[1]
    inner = chunks * width
    half = tokens // 2
    even = ys == 2 and zs % 2 == 0
    piece = share // (copies if split else 1)
    spot = mine if split else 0
    load = pltpu.make_async_copy(hid_ref, hid_v.at[me], load_sem)
    load.start()
    meet(chunks, copies)
    load.wait()

    def w_rows(s, d):
        return pl.ds(pl.multiple_of(s * share + d * piece, piece), piece)

    def w_first(s, part):
        src = wq_ref.at[pl.ds(pl.multiple_of(spot * piece, piece), piece), pl.ds(pl.multiple_of(part * inner + s * width, width), width)]
        return remote(src, w_v.at[w_rows(me, spot), pl.ds(part * width, width)], w1send.at[s, part], w1recv.at[me, part], {"seq": s})

    def w_landed(s, part):
        dst = w_v.at[w_rows(s, spot), pl.ds(part * width, width)]
        return remote(dst, dst, w1send.at[s, part], w1recv.at[s, part], {"seq": s})

    def w_own(part):
        src = wq_ref.at[pl.ds(pl.multiple_of(spot * piece, piece), piece), pl.ds(pl.multiple_of(part * inner + me * width, width), width)]
        return pltpu.make_async_copy(src, w_v.at[w_rows(me, spot), pl.ds(part * width, width)], out_sem.at[part])

    def every_other(fn):
        def one(k, _):
            fn(lax.rem(me + k, chunks))
            return 0
        lax.fori_loop(1, chunks, one, 0)

    def gain_to(s):
        return remote(gain_ref, gain_v.at[me], gsend.at[s], grecv.at[me], {"seq": s})

    def gain_from(s):
        return remote(gain_v.at[s], gain_v.at[s], gsend.at[s], grecv.at[s], {"seq": s})

    def send_first(s):
        gain_to(s).start()
        w_first(s, 0).start()
        w_first(s, 1).start()

    def block(o, yy, h):
        return hid_v.at[o * ys + yy, pl.ds(h * half, half)]

    def up(o, h):
        return remote(block(o, y, h), block(o, y, h), hup.at[o, h], hrecv.at[o * ys + y, h], {"seq": (z + 1) * ys + y})

    def down(o, h):
        return remote(block(o, y, h), block(o, y, h), hdown.at[o, h], hrecv.at[o * ys + y, h], {"seq": (z - 1) * ys + y})

    def side(o, j, h):
        other = lax.rem(y + j, ys)
        return remote(block(o, y, h), block(o, y, h), hside.at[o, j - 1, h], hrecv.at[o * ys + y, h], {"seq": z * ys + other})

    def landed(o, yy, h):
        return remote(block(o, yy, h), block(o, yy, h), hside.at[o, 0, h], hrecv.at[o * ys + yy, h], {"seq": lax.rem(me + 1, chunks)})

    def when(cond, fn):
        pl.when(cond)(fn)

    gain_own = pltpu.make_async_copy(gain_ref, gain_v.at[me], out_sem.at[2])
    gain_own.start()
    for part in range(2):
        w_own(part).start()
    for h in range(2):
        when(z + 1 < zs, lambda: up(z, h).start())
        when(z > 0, lambda: down(z, h).start())
        for j in range(1, ys):
            side(z, j, h).start()
    every_other(send_first)

    partner = z + 1 - 2 * (z % 2)

    def sides(o, h, act):
        if even and h == 1:
            when(o != partner, lambda: act(side(o, 1, h)))
        else:
            for j in range(1, ys):
                act(side(o, j, h))

    def lend():
        return remote(block(z, 1 - y, 1), block(z, 1 - y, 1), hlend, hrecv.at[z * ys + 1 - y, 1], {"seq": partner * ys + y})

    def lend_on():
        if even:
            landed(z, 1 - y, 1).wait_recv()
            lend().start()

    def relay(k):
        for h in range(2):
            @pl.when(z - k >= 0)
            def _():
                landed(z - k, y, h).wait_recv()
                when(z + 1 < zs, lambda: up(z - k, h).start())
                sides(z - k, h, lambda one: one.start())

            @pl.when(z + k < zs)
            def _():
                landed(z + k, y, h).wait_recv()
                when(z > 0, lambda: down(z + k, h).start())
                sides(z + k, h, lambda one: one.start())

    def shared(s, d, sems, k, device):
        return remote(w_v.at[w_rows(s, d)], w_v.at[w_rows(s, d)], sems.at[s, k], w2recv.at[s, d], device)

    def spread(s):
        for j in range(1, xs):
            shared(s, mine, w2send, j - 1, {"dp": lax.rem(x + j, xs) * 2 + c}).start()
        shared(s, mine, w3send, 0, {"dp": x * 2 + 1 - c}).start()

    gain_own.wait()
    for part in range(2):
        w_own(part).wait()
    if split:
        spread(me)

    def take_first(s):
        gain_from(s).wait_recv()
        for part in range(2):
            w_landed(s, part).wait_recv()
        if split:
            spread(s)

    if zs > 1:
        relay(1)
    every_other(take_first)

    def take_second(s, _):
        for j in range(1, xs):
            d = lax.rem(x + j, xs) * 2 + c
            shared(s, d, w2send, j - 1, {"dp": d}).wait_recv()
            shared(s, d, w3send, j, {"dp": x * 2 + 1 - c}).start()
        return 0

    def take_third(s, _):
        for j in range(xs):
            d = lax.rem(x + j, xs) * 2 + 1 - c
            shared(s, d, w2send, 0, {"dp": d}).wait_recv()
        return 0

    if zs > 2:
        relay(2)
    lend_on()
    if split:
        lax.fori_loop(0, chunks, take_second, 0)
    if split:
        lax.fori_loop(0, chunks, take_third, 0)

    row_ref[...] = jnp.concatenate([gain_v[s] for s in range(chunks)], axis=-1)
    w_out = pltpu.make_async_copy(w_v, w_ref, load_sem)
    w_out.start()
    steps = 4 if width >= 512 else 1
    tile = 2 * width // steps

    def project(at):
        def rows(i, _):
            sl = pl.ds(pl.multiple_of(i * 32, 32), 32)
            h = hid_v[at, sl, :].astype(F32)
            inverse = lax.rsqrt(jnp.mean(h * h, axis=-1, keepdims=True) + EPSILON)
            n_v[sl, :] = (h * inverse * row_ref[...]).astype(BF16)
            return 0
        lax.fori_loop(0, tokens // 32, rows, 0)
        n_out = pltpu.make_async_copy(n_v, n_ref.at[at], out_sem.at[0])
        n_out.start()

        def columns(i, _):
            sl = pl.ds(pl.multiple_of(i * tile, tile), tile)
            got = jnp.dot(n_v[...], w_v[:, sl], preferred_element_type=F32)
            if steps == 1:
                ci_v[...] = got[:, :width].astype(BF16)
                gate_v[...] = got[:, width:]
            else:
                @pl.when(i < steps // 2)
                def _():
                    ci_v[:, sl] = got.astype(BF16)

                @pl.when(i >= steps // 2)
                def _():
                    gate_v[:, pl.ds(pl.multiple_of(i * tile - width, tile), tile)] = got
            return 0
        lax.fori_loop(0, steps, columns, 0)
        ci_out = pltpu.make_async_copy(ci_v, ci_ref.at[at], out_sem.at[1])
        gate_out = pltpu.make_async_copy(gate_v, gate_ref.at[at], out_sem.at[2])
        ci_out.start()
        gate_out.start()
        n_out.wait()
        ci_out.wait()
        gate_out.wait()

    def work(first, last):
        def one(i, _):
            k0, j = i // (2 * ys), i % (2 * ys)
            lower, yy = j // ys, j % ys
            own = yy == y
            k = k0 - jnp.where(own, 0, 1)
            o = z + k * (2 * lower - 1)
            ok = (k >= 0) & (k < zs) & (o >= 0) & (o < zs) & ((lower == 0) | (k > 0))
            if even:
                ok = ok & (own | (o != partner))

            @pl.when(ok & jnp.logical_not(own))
            def _():
                landed(o, yy, 0).wait_recv()
                if even:
                    when(o != z, lambda: landed(o, yy, 1).wait_recv())
                else:
                    landed(o, yy, 1).wait_recv()

            @pl.when(ok)
            def _():
                project(o * ys + yy)
            return 0
        lax.fori_loop(first * 2 * ys, last * 2 * ys, one, 0)

    work(0, min(2, zs))

    def later(k, _):
        relay(k)
        work(k - 1, k)
        return 0

    lax.fori_loop(3, zs, later, 0)
    work(max(2, zs - 1), zs)
    work(zs, zs + 1)
    if even:
        for h in range(2):
            landed(partner, 1 - y, h).wait_recv()
        project(partner * ys + 1 - y)
    w_out.wait()

    def drain_first(s):
        gain_to(s).wait_send()
        for part in range(2):
            w_first(s, part).wait_send()

    every_other(drain_first)

    def drain_second(s, _):
        for j in range(1, xs):
            shared(s, mine, w2send, j - 1, {"dp": mine}).wait_send()
        for j in range(xs):
            shared(s, mine, w3send, j, {"dp": mine}).wait_send()
        return 0

    if split:
        lax.fori_loop(0, chunks, drain_second, 0)

    def drain(k, _):
        for h in range(2):
            @pl.when(z - k >= 0)
            def _():
                when(z + 1 < zs, lambda: up(z - k, h).wait_send())
                sides(z - k, h, lambda one: one.wait_send())

            @pl.when((z + k < zs) & (k > 0))
            def _():
                when(z > 0, lambda: down(z + k, h).wait_send())
                sides(z + k, h, lambda one: one.wait_send())
        return 0

    lax.fori_loop(0, zs, drain, 0)
    for h in range(2):
        when(z > 0, lambda: down(z, h).wait_send())
    if even:
        lend().wait_send()


def gather_project(hidden, wq, gain, chunks, copies, share, split):
    tokens, model = hidden.shape
    width = wq.shape[1] // 2 // chunks
    zs, ys = grid_of(chunks, copies)
    any_spec = pl.BlockSpec(memory_space=pl.ANY)
    sds = jax.ShapeDtypeStruct
    dma = pltpu.SemaphoreType.DMA
    return pl.pallas_call(
        functools.partial(gather_project_kernel, chunks=chunks, copies=copies, share=share, split=split),
        in_specs=[any_spec] * 3,
        out_specs=[any_spec] * 4 + [pl.BlockSpec(memory_space=pltpu.VMEM)],
        out_shape=[sds((chunks, tokens, model), BF16), sds((chunks, tokens, width), BF16),
                   sds((chunks, tokens, width), F32), sds((model, 2 * width), BF16), sds((1, model), F32)],
        scratch_shapes=[
            pltpu.VMEM((chunks, tokens, model), BF16), pltpu.VMEM((chunks, 1, share), F32), pltpu.VMEM((model, 2 * width), BF16),
            pltpu.VMEM((tokens, model), BF16), pltpu.VMEM((tokens, width), BF16), pltpu.VMEM((tokens, width), F32),
            dma(()), dma((3,)), dma((chunks, 2)), dma((zs, max(1, ys - 1), 2)), dma((zs, 2)), dma((zs, 2)), dma(()),
            dma((chunks, 2)), dma((chunks, 2)), dma((chunks, copies)), dma((chunks, max(1, copies // 2))), dma((chunks, max(1, copies // 2))),
            dma((chunks,)), dma((chunks,)),
        ],
        compiler_params=pltpu.CompilerParams(collective_id=0, has_side_effects=True, vmem_limit_bytes=60 * 1024 * 1024),
        name="gather_project",
    )(hidden, wq, gain)


SPLITS = (8, 14)


def forward_kernel(ci_ref, gate_ref, gm_ref, taps_ref, cbias_ref, selw_ref, stepw_ref, sbias_ref, decay_ref, skip_ref, wout_ref,
                   gmall_ref, sel_ref, x_ref, gated_ref, gact_ref, tail_ref, dt_ref, slope_ref, start_ref, mixed_ref,
                   gate_v, part_v, recv_v, x_v, gated_v, gact_v, tail_v, dt_v, slope_v, start_v,
                   mixed_v,
                   ext_s, u_s, y_s, coef_s, bt_s, hist_a, hist_b, state_s, rate_s,
                   load_sem, own_sem, out_sem, mixed_sem, grecv, gside, gup, gdown, glend, send1, recv1, send2, recv2, *, chunks, copies, n):
    zs, ys = grid_of(chunks, copies)
    me = lax.axis_index("seq")
    z, y = me // ys, me % ys
    tokens, model = gm_ref.shape
    rows, length, width = ci_ref.shape[1:]
    rank = stepw_ref.shape[0]
    half = tokens // 2
    even = ys == 2 and zs % 2 == 0
    load = pltpu.make_async_copy(gate_ref, gate_v, load_sem)
    load.start()
    own = pltpu.make_async_copy(gm_ref, gmall_ref.at[me], own_sem)
    own.start()
    meet(chunks, 1)

    def block(o, yy, h):
        return gmall_ref.at[o * ys + yy, pl.ds(h * half, half)]

    def source(o, h, k):
        return gm_ref.at[pl.ds(h * half, half)] if k is None else block(o, y, h)

    def up(o, h, k=0):
        return remote(source(o, h, k), block(o, y, h), gup.at[o, h], grecv.at[o * ys + y, h], {"seq": (z + 1) * ys + y})

    def down(o, h, k=0):
        return remote(source(o, h, k), block(o, y, h), gdown.at[o, h], grecv.at[o * ys + y, h], {"seq": (z - 1) * ys + y})

    def side(o, j, h, k=0):
        return remote(source(o, h, k), block(o, y, h), gside.at[o, j - 1, h], grecv.at[o * ys + y, h], {"seq": z * ys + lax.rem(y + j, ys)})

    def landed(o, yy, h):
        return remote(block(o, yy, h), block(o, yy, h), gside.at[o, 0, h], grecv.at[o * ys + yy, h], {"seq": lax.rem(me + 1, chunks)})

    def when(cond, fn):
        pl.when(cond)(fn)

    def first_sends(h):
        when(z + 1 < zs, lambda: up(z, h, None).start())
        when(z > 0, lambda: down(z, h, None).start())
        for j in range(1, ys):
            side(z, j, h, None).start()

    first_sends(0)

    partner = z + 1 - 2 * (z % 2)

    def sides(o, h, act):
        if even and h == 1:
            when(o != partner, lambda: act(side(o, 1, h)))
        else:
            for j in range(1, ys):
                act(side(o, j, h))

    def lend():
        return remote(block(z, 1 - y, 1), block(z, 1 - y, 1), glend, grecv.at[z * ys + 1 - y, 1], {"seq": partner * ys + y})

    def lend_on():
        if even:
            landed(z, 1 - y, 1).wait_recv()
            lend().start()

    def relay(k):
        for h in range(2):
            @pl.when(z - k >= 0)
            def _():
                landed(z - k, y, h).wait_recv()
                when(z + 1 < zs, lambda: up(z - k, h).start())
                sides(z - k, h, lambda one: one.start())

            @pl.when(z + k < zs)
            def _():
                landed(z + k, y, h).wait_recv()
                when(z > 0, lambda: down(z + k, h).start())
                sides(z + k, h, lambda one: one.start())

    rate_s[...] = -jnp.exp(decay_ref[...].astype(F32)) * LOG2E

    def conv(i, _):
        r, c = i // chunks, i % chunks
        x, part = conv_step(ci_ref[c, r], c == 0, taps_ref, cbias_ref, selw_ref, ext_s)
        x_v[c, r] = x
        part_v[c, r] = part
        return 0

    def first(s, r):
        return remote(part_v.at[s, r], recv_v.at[me, r], send1.at[s, r], recv1.at[me, r], {"seq": s})

    def landed_first(s, r):
        return remote(part_v.at[s, r], recv_v.at[s, r], send1.at[s, r], recv1.at[s, r], {"seq": s})

    def second(s, r):
        return remote(sel_ref.at[me, r], sel_ref.at[me, r], send2.at[s, r], recv2.at[me, r], {"seq": s})

    def landed_second(s, r):
        return remote(sel_ref.at[s, r], sel_ref.at[s, r], send2.at[s, r], recv2.at[s, r], {"seq": s})

    def every_other(fn):
        def one(k, _):
            fn(lax.rem(me + k, chunks))
            return 0
        lax.fori_loop(1, chunks, one, 0)

    for r in range(rows):
        lax.fori_loop(r * chunks, (r + 1) * chunks, conv, 0)
        every_other(lambda s: first(s, r).start())
        recv_v[me, r] = part_v[me, r]
        if r == 0:
            first_sends(1)
    x_out = pltpu.make_async_copy(x_v, x_ref, out_sem.at[0, 0])
    x_out.start()
    for r in range(rows):
        every_other(lambda s: landed_first(s, r).wait_recv())
        total = recv_v[0, r].astype(F32)
        for s in range(1, chunks):
            total = total + recv_v[s, r].astype(F32)
        sel_ref[me, r] = total.astype(BF16)
        every_other(lambda s: second(s, r).start())
    if zs > 1:
        relay(1)
    if zs <= 2:
        lend_on()
    load.wait()
    pairs = ((gated_v, gated_ref), (gact_v, gact_ref), (tail_v, tail_ref), (dt_v, dt_ref), (slope_v, slope_ref), (start_v, start_ref))

    def outs(c, r):
        return [pltpu.make_async_copy(src.at[c, r], dst.at[c, r], out_sem.at[1 + k, c * rows + r]) for k, (src, dst) in enumerate(pairs)]

    def scan(i, _):
        r, c = i // chunks, i % chunks

        @pl.when(c == 0)
        def _():
            every_other(lambda s: landed_second(s, r).wait_recv())

        start_v[c, r] = jnp.where(c == 0, 0.0, state_s[...])
        scan_step(sel_ref[c, r].astype(F32), x_v[c, r].astype(F32), gate_v[c, r], c == 0, stepw_ref, sbias_ref, skip_ref,
                  gated_v.at[c, r], gact_v.at[c, r], tail_v.at[c, r], dt_v.at[c, r], slope_v.at[c, r],
                  u_s, y_s, coef_s, bt_s, hist_a, hist_b, state_s, rate_s, rank, n)
        for one in outs(c, r):
            one.start()
        return 0

    count = rows * chunks
    at = 0
    for k in range(2, zs):
        cut = min(count, count * (SPLITS[k - 2] if zs == 4 else 16 * (k - 1) // zs) // 16)
        lax.fori_loop(at, cut, scan, 0)
        relay(k)
        if k == 2:
            lend_on()
        at = cut
    lax.fori_loop(at, count, scan, 0)

    tile = min(512, model)

    def mixed_out(s):
        return pltpu.make_async_copy(mixed_v.at[s % 2], mixed_ref.at[s], mixed_sem.at[s % 2])

    def mix(s, _):
        @pl.when(s >= 2)
        def _():
            mixed_out(s - 2).wait()

        lhs = gated_v[s].reshape(tokens, width)

        def one(i, _):
            sl = pl.ds(pl.multiple_of(i * tile, tile), tile)
            mixed_v[s % 2, :, sl] = jnp.dot(lhs, wout_ref[:, sl], preferred_element_type=F32).astype(BF16)
            return 0
        lax.fori_loop(0, model // tile, one, 0)
        mixed_out(s).start()
        return 0

    lax.fori_loop(0, chunks, mix, 0)
    for s in range(chunks - 2, chunks):
        mixed_out(s).wait()

    def others(o, _):
        for j in range(1, ys):
            landed(o, lax.rem(y + j, ys), 0).wait_recv()
            if even:
                when(o != z, lambda: landed(o, 1 - y, 1).wait_recv())
            else:
                landed(o, lax.rem(y + j, ys), 1).wait_recv()
        return 0

    lax.fori_loop(0, zs, others, 0)
    own.wait()
    x_out.wait()

    def settle(i, _):
        for one in outs(i // rows, i % rows):
            one.wait()
        return 0

    lax.fori_loop(0, count, settle, 0)
    for r in range(rows):
        every_other(lambda s: first(s, r).wait_send())
        every_other(lambda s: second(s, r).wait_send())

    def drain(k, _):
        for h in range(2):
            @pl.when(z - k >= 0)
            def _():
                when(z + 1 < zs, lambda: up(z - k, h).wait_send())
                sides(z - k, h, lambda one: one.wait_send())

            @pl.when((z + k < zs) & (k > 0))
            def _():
                when(z > 0, lambda: down(z + k, h).wait_send())
                sides(z + k, h, lambda one: one.wait_send())
        return 0

    lax.fori_loop(0, zs, drain, 0)
    for h in range(2):
        when(z > 0, lambda: down(z, h).wait_send())
    if even:
        lend().wait_send()


def forward(ci, gate, gm, taps, cbias, selw, stepw, sbias, decay, skip, wout, copies, n):
    chunks, rows, length, width = ci.shape
    tokens, model = gm.shape
    zs, ys = grid_of(chunks, copies)
    wide = BLOCK * n
    sds = jax.ShapeDtypeStruct
    dma = pltpu.SemaphoreType.DMA
    vmem = pl.BlockSpec(memory_space=pltpu.VMEM)
    hbm = pl.BlockSpec(memory_space=pl.ANY)
    coef = (chunks, rows, selw.shape[0], length)
    starts = (chunks, rows, n, width)
    full = ci.shape
    return pl.pallas_call(
        functools.partial(forward_kernel, chunks=chunks, copies=copies, n=n),
        in_specs=[vmem, hbm] + [vmem] * 9,
        out_specs=[hbm, vmem] + [hbm] * 8,
        out_shape=[sds((chunks, tokens, model), BF16), sds(coef, BF16), sds(full, BF16), sds(full, BF16), sds(full, F32), sds(full, BF16),
                   sds(full, F32), sds(full, F32), sds(starts, F32), sds((chunks, tokens, model), BF16)],
        scratch_shapes=[
            pltpu.VMEM(full, F32), pltpu.VMEM(coef, BF16), pltpu.VMEM(coef, BF16), pltpu.VMEM(full, BF16), pltpu.VMEM(full, BF16),
            pltpu.VMEM(full, F32), pltpu.VMEM(full, BF16), pltpu.VMEM(full, F32), pltpu.VMEM(full, F32), pltpu.VMEM(starts, F32),
            pltpu.VMEM((2, tokens, model), BF16),
            pltpu.VMEM((length + 8, width), F32), pltpu.VMEM((length, width), F32), pltpu.VMEM((length, width), F32),
            pltpu.VMEM((length, wide), BF16), pltpu.VMEM((2 * n, length), F32), pltpu.VMEM((wide, width), BF16), pltpu.VMEM((wide, width), BF16),
            pltpu.VMEM((n, width), F32), pltpu.VMEM((n, width), F32),
            dma(()), dma(()), dma((7, rows * chunks)), dma((2,)), dma((chunks, 2)), dma((zs, max(1, ys - 1), 2)), dma((zs, 2)), dma((zs, 2)), dma(()),
            dma((chunks, rows)), dma((chunks, rows)), dma((chunks, rows)), dma((chunks, rows)),
        ],
        compiler_params=pltpu.CompilerParams(collective_id=1, has_side_effects=True, vmem_limit_bytes=60 * 1024 * 1024),
        name="forward",
    )(ci, gate, gm, taps, cbias, selw, stepw, sbias, decay, skip, wout)


class Exchange:
    def __init__(self, gin, out, bufs, sems, chunks, copies):
        self.gin, self.out = gin, out
        self.g1, self.mine_v, self.g2, self.t_v, self.fin = bufs
        self.load, self.s1, self.r1, self.s2, self.r2, self.s3, self.r3, self.s4, self.r4 = sems
        self.chunks, self.xs = chunks, copies // 2
        self.me, self.mine = lax.axis_index("seq"), lax.axis_index("dp")
        self.x, self.c = self.mine // 2, self.mine % 2
        self.piece, self.width = self.t_v.shape[1:]

    def own(self, q):
        return pltpu.make_async_copy(self.gin.at[:, q * 2 + self.c], self.mine_v.at[q], self.load.at[q])

    def to_core(self, q):
        return remote(self.gin.at[:, q * 2 + 1 - self.c], self.g1.at[q], self.s1.at[q], self.r1.at[q], {"dp": self.x * 2 + 1 - self.c})

    def across(self, q):
        return remote(self.mine_v.at[q], self.g2.at[self.x], self.s2.at[q], self.r2.at[self.x], {"dp": q * 2 + self.c})

    def from_across(self, q):
        return remote(self.g2.at[q], self.g2.at[q], self.s2.at[q], self.r2.at[q], {"dp": q * 2 + self.c})

    def columns(self, s):
        return self.fin.at[:, pl.ds(pl.multiple_of(s * self.width, self.width), self.width)]

    def turn(self, s):
        return remote(self.t_v.at[s], self.columns(self.me), self.s3.at[s], self.r3.at[self.me], {"seq": s})

    def turned(self, s):
        return remote(self.columns(s), self.columns(s), self.s3.at[s], self.r3.at[s], {"seq": s})

    def rows_of(self, d):
        return self.out.at[pl.ds(pl.multiple_of(d * self.piece, self.piece), self.piece)]

    def share_to(self, k, d):
        return remote(self.fin, self.rows_of(self.mine), self.s4.at[k], self.r4.at[self.mine], {"dp": d})

    def hand_on(self, row, k):
        return remote(self.rows_of(row), self.rows_of(row), self.s4.at[k], self.r4.at[row], {"dp": self.x * 2 + 1 - self.c})

    def shared(self, d):
        return remote(self.rows_of(d), self.rows_of(d), self.s4.at[0], self.r4.at[d], {"dp": d})

    def keep(self):
        return pltpu.make_async_copy(self.fin, self.rows_of(self.mine), self.load.at[self.xs])

    def others(self, fn):
        def one(k, _):
            fn(lax.rem(self.me + k, self.chunks))
            return 0
        lax.fori_loop(1, self.chunks, one, 0)

    def column_peers(self):
        return [lax.rem(self.x + j, self.xs) * 2 + self.c for j in range(1, self.xs)]

    def begin(self):
        for q in range(self.xs):
            self.own(q).start()
            self.to_core(q).start()

    def chip(self):
        for q in range(self.xs):
            self.own(q).wait()
            self.to_core(q).wait_recv()

            def fold(s, _):
                self.mine_v[q, s] = (self.mine_v[q, s].astype(F32) + self.g1[q, s].astype(F32)).astype(BF16)
                return 0
            lax.fori_loop(0, self.chunks, fold, 0)
            pl.when(q != self.x)(lambda: self.across(q).start())

    def spread(self):
        for q in range(self.xs):
            pl.when(q != self.x)(lambda: self.from_across(q).wait_recv())

        def fold(s, _):
            total = self.mine_v[self.x, s].astype(F32)
            for j in range(1, self.xs):
                total = total + self.g2[lax.rem(self.x + j, self.xs), s].astype(F32)
            self.t_v[s] = total.astype(BF16)
            return 0
        lax.fori_loop(0, self.chunks, fold, 0)
        self.others(lambda s: self.turn(s).start())
        self.columns(self.me)[...] = self.t_v[self.me]

    def share(self):
        self.others(lambda s: self.turned(s).wait_recv())
        for j, d in enumerate(self.column_peers()):
            self.share_to(1 + j, d).start()
        self.share_to(0, self.x * 2 + 1 - self.c).start()
        self.keep().start()

    def pass_on(self):
        for j, d in enumerate(self.column_peers()):
            self.shared(d).wait_recv()
            self.hand_on(d, self.xs + j).start()

    def finish(self):
        self.keep().wait()
        for j in range(self.xs):
            self.shared(lax.rem(self.x + j, self.xs) * 2 + 1 - self.c).wait_recv()
        for q in range(self.xs):
            self.to_core(q).wait_send()
            pl.when(q != self.x)(lambda: self.across(q).wait_send())
        self.others(lambda s: self.turn(s).wait_send())
        for j in range(self.xs):
            self.share_to(j, self.mine).wait_send()
        for j, d in enumerate(self.column_peers()):
            self.hand_on(d, self.xs + j).wait_send()


def exchange_scratch(chunks, copies, piece, width):
    xs = copies // 2
    dma = pltpu.SemaphoreType.DMA
    slab = (chunks, piece, width)
    bufs = [pltpu.VMEM((xs,) + slab, BF16), pltpu.VMEM((xs,) + slab, BF16), pltpu.VMEM((xs,) + slab, BF16), pltpu.VMEM(slab, BF16),
            pltpu.VMEM((piece, chunks * width), BF16)]
    return bufs + [dma((xs + 1,)), dma((xs,)), dma((xs,)), dma((xs,)), dma((xs,)), dma((chunks,)), dma((chunks,)), dma((2 * xs,)), dma((copies,))]


def order_of(zs):
    return [sorted(range(zs), key=lambda t: (-abs(t - z), t)) for z in range(zs)]


def scatter_kernel(*refs, chunks, copies, split):
    gc_ref, gg_ref, w_ref, late_ref = refs[:4]
    norm_ref = refs[4] if split else None
    refs = refs[4 + split:]
    red_ref, sum_ref = refs[:2]
    all_ref = refs[2] if split else None
    refs = refs[2 + split:]
    (ysend_v, yrecv_v, own_v, zrecv_v, lend_v, late_v, w_v, load_sem,
     ysend, yrecv, zup, zdown, zrecv, lend_sem, lsend, lrecv) = refs[:16]
    if split:
        gin_v, norm_v, norm_sem = refs[16:19]
        trade = Exchange(gin_v, all_ref, refs[19:24], refs[24:33], chunks, copies)
    zs, ys = grid_of(chunks, copies)
    xs = copies // 2
    me, mine = lax.axis_index("seq"), lax.axis_index("dp")
    z, y = me // ys, me % ys
    x, c = mine // 2, mine % 2
    tokens, width = gc_ref.shape[1:]
    model = w_ref.shape[0]
    half = tokens // 2
    tile = min(256, model)
    tables = order_of(zs)
    partner = z + 1 - 2 * (z % 2)

    def dest(i):
        got = 0
        for k in range(zs):
            got = got + jnp.where(z == k, tables[k][i], 0)
        return got

    w_in = pltpu.make_async_copy(w_ref, w_v, load_sem.at[0])
    w_in.start()

    def norm_in(s):
        cols = pl.ds(pl.multiple_of(s * norm_v.shape[-1], norm_v.shape[-1]), norm_v.shape[-1])
        return pltpu.make_async_copy(norm_ref.at[:, :, cols], norm_v.at[s % 2], norm_sem.at[s % 2])

    if split:
        norm_in(0).start()
    meet(chunks, copies)

    def late_to(d):
        return remote(late_ref, late_v.at[mine], lsend.at[d], lrecv.at[mine], {"dp": d})

    def late_from(d):
        return remote(late_v.at[d], late_v.at[d], lsend.at[d], lrecv.at[d], {"dp": d})

    def every_copy(fn):
        def one(k, _):
            fn(lax.rem(mine + k, copies))
            return 0
        lax.fori_loop(1, copies, one, 0)

    w_in.wait()

    def partial(s, out, at):
        def one(i, _):
            sl = pl.ds(pl.multiple_of(i * tile, tile), tile)
            got = nt_dot(gc_ref[s], w_v[sl, :width]) + nt_dot(gg_ref[s], w_v[sl, width:])
            out[at, :, sl] = got.astype(BF16)
            return 0
        lax.fori_loop(0, model // tile, one, 0)

    def to_side(i, j, h):
        rows = pl.ds(h * half, half)
        k = i * (ys - 1) + j - 1
        return remote(ysend_v.at[k % ysend_v.shape[0], rows], yrecv_v.at[k, rows], ysend.at[k, h], yrecv.at[k, h], {"seq": z * ys + lax.rem(y + j, ys)})

    slots = ysend_v.shape[0]
    even = False

    def lend(i):
        return remote(ysend_v.at[i, pl.ds(half, half)], lend_v, lend_sem.at[0], lend_sem.at[1], {"seq": partner * ys + y})

    def send_side(i, j, h):
        if not even or h == 0:
            to_side(i, j, h).start()
            return

        @pl.when(dest(i) != partner)
        def _():
            if i == zs - 1:
                lend(i).wait_recv()

                def one(r, _):
                    sl = pl.ds(pl.multiple_of(half + r * 32, 32), 32)
                    ysend_v[i, sl, :] = (ysend_v[i, sl, :].astype(F32) + lend_v[pl.ds(pl.multiple_of(r * 32, 32), 32), :].astype(F32)).astype(BF16)
                    return 0
                lax.fori_loop(0, half // 32, one, 0)
            to_side(i, j, h).start()

    def if_sent(i, h, fn):
        if even and h == 1:
            pl.when(dest(i) != partner)(fn)
        else:
            fn()

    ahead = 2 if slots == zs * (ys - 1) else zs
    def outgoing(i):
        for j in range(1, ys):
            k = i * (ys - 1) + j - 1
            if k >= slots:
                for h in range(2):
                    to_side((k - slots) // (ys - 1), (k - slots) % (ys - 1) + 1, h).wait_send()
            partial(dest(i) * ys + lax.rem(y + j, ys), ysend_v, k % slots)
            if i < ahead:
                for h in range(2):
                    send_side(i, j, h)
            if even:
                pl.when(dest(i) == partner)(lambda: lend(i).start())

    if split:
        for i in range(min(2, zs)):
            outgoing(i)

        def weights(s, _):
            @pl.when(s + 1 < chunks)
            def _():
                norm_in(s + 1).start()

            norm_in(s).wait()
            n_all = norm_v[s % 2].reshape(chunks * tokens, norm_v.shape[-1])
            got = lax.dot_general(n_all, gc_ref[...].reshape(chunks * tokens, width), (((0,), (0,)), ((), ())), preferred_element_type=F32)
            gin_v[s] = got.astype(BF16).reshape(gin_v.shape[1:])
            return 0

        lax.fori_loop(0, chunks, weights, 0)
        trade.begin()

    for i in range(min(2, zs) if split else 0, zs):
        outgoing(i)
    if split:
        trade.chip()
    every_copy(lambda d: late_to(d).start())

    def arrived(i, j, h):
        rows = pl.ds(h * half, half)
        k = i * (ys - 1) + j - 1
        return remote(yrecv_v.at[k, rows], yrecv_v.at[k, rows], ysend.at[k, h], yrecv.at[k, h], {"seq": z * ys + lax.rem(y + j, ys)})

    def climb(t, h):
        rows = pl.ds(h * half, half)
        return remote(own_v.at[t, rows], zrecv_v.at[t, rows], zup.at[t, h], zrecv.at[t, h], {"seq": (z + 1) * ys + y})

    def sink(t, h):
        rows = pl.ds(h * half, half)
        slot = jnp.where(t == z - 1, zs, t)
        return remote(own_v.at[t, rows], zrecv_v.at[slot, rows], zdown.at[t, h], zrecv.at[slot, h], {"seq": (z - 1) * ys + y})

    def from_z(slot, h):
        rows = pl.ds(h * half, half)
        return remote(zrecv_v.at[slot, rows], zrecv_v.at[slot, rows], zup.at[0, h], zrecv.at[slot, h], {"seq": lax.rem(me + 1, chunks)})

    def accumulate(t, h, read):
        def one(r, _):
            sl = pl.ds(pl.multiple_of(h * half + r * 32, 32), 32)
            own_v[t, sl, :] = (own_v[t, sl, :].astype(F32) + read(sl)).astype(BF16)
            return 0
        lax.fori_loop(0, half // 32, one, 0)

    for i in range(zs):
        t = dest(i)
        partial(t * ys + y, own_v, t)
        for h in range(2):
            for j in range(1, ys):
                if_sent(i, h, lambda: arrived(i, ys - j, h).wait_recv())

            def side_sum(sl):
                total = yrecv_v[i * (ys - 1), sl, :].astype(F32)
                for j in range(2, ys):
                    total = total + yrecv_v[i * (ys - 1) + j - 1, sl, :].astype(F32)
                return total

            if ys > 1:
                if_sent(i, h, lambda: accumulate(t, h, side_sum))

            @pl.when(((t > z) & (z > 0)) | ((t == z) & (z > 0)))
            def _():
                from_z(t, h).wait_recv()
                accumulate(t, h, lambda sl: zrecv_v[t, sl, :].astype(F32))

            @pl.when((t < z) & (z + 1 < zs))
            def _():
                from_z(t, h).wait_recv()
                accumulate(t, h, lambda sl: zrecv_v[t, sl, :].astype(F32))

            @pl.when((t == z) & (z + 1 < zs))
            def _():
                from_z(zs, h).wait_recv()
                accumulate(t, h, lambda sl: zrecv_v[zs, sl, :].astype(F32))

            @pl.when(t > z)
            def _():
                climb(t, h).start()

            @pl.when(t < z)
            def _():
                sink(t, h).start()
        if split and i == 0:
            trade.spread()
        if split and i == min(1, zs - 1):
            trade.share()
        if i + ahead < zs:
            for j in range(1, ys):
                for h in range(2):
                    send_side(i + ahead, j, h)

    red_ref[...] = own_v[z]
    every_copy(lambda d: late_from(d).wait_recv())
    total = late_ref[...].astype(F32)
    for k in range(1, copies):
        total = total + late_v[lax.rem(mine + k, copies)].astype(F32)
    sum_ref[...] = total
    if split:
        trade.pass_on()
        trade.finish()

    every_copy(lambda d: late_to(d).wait_send())
    count = zs * (ys - 1)
    for k in range(max(0, count - slots), count):
        for h in range(2):
            if_sent(k // (ys - 1), h, lambda: to_side(k // (ys - 1), k % (ys - 1) + 1, h).wait_send())
    if even:
        lend(0).wait_send()
    for i in range(zs):
        t = dest(i)
        for h in range(2):
            @pl.when(t > z)
            def _():
                climb(t, h).wait_send()

            @pl.when(t < z)
            def _():
                sink(t, h).wait_send()


def scatter_sums(gc, gg, w_all, late, normed, chunks, copies, split):
    tokens, width = gc.shape[1:]
    model = w_all.shape[0]
    zs, ys = grid_of(chunks, copies)
    xs = max(1, copies // 2)
    others = max(1, zs * (ys - 1))
    slots = min(others, 4)
    any_spec = pl.BlockSpec(memory_space=pl.ANY)
    vmem = pl.BlockSpec(memory_space=pltpu.VMEM)
    sds = jax.ShapeDtypeStruct
    dma = pltpu.SemaphoreType.DMA
    args = [gc, gg, w_all, late]
    in_specs = [vmem, vmem, any_spec, vmem]
    out_specs = [vmem, vmem]
    out_shape = [sds((tokens, model), BF16), sds(late.shape, F32)]
    scratch = [pltpu.VMEM((slots, tokens, model), BF16), pltpu.VMEM((others, tokens, model), BF16),
               pltpu.VMEM((zs, tokens, model), BF16), pltpu.VMEM((zs + 1, tokens, model), BF16), pltpu.VMEM((tokens // 2, model), BF16),
               pltpu.VMEM((copies,) + late.shape, BF16), pltpu.VMEM(w_all.shape, BF16)]
    sems = [dma((1,)), dma((others, 2)), dma((others, 2)), dma((zs, 2)), dma((zs, 2)), dma((zs + 1, 2)), dma((2,)), dma((copies,)), dma((copies,))]
    if split:
        share = model // chunks
        piece = share // copies
        args.append(normed)
        in_specs.append(any_spec)
        out_specs.append(any_spec)
        out_shape.append(sds((share, chunks * width), BF16))
        sems += [pltpu.VMEM((chunks, copies, piece, width), BF16), pltpu.VMEM((2, chunks, tokens, share), BF16), dma((2,))]
        sems += exchange_scratch(chunks, copies, piece, width)
    return pl.pallas_call(
        functools.partial(scatter_kernel, chunks=chunks, copies=copies, split=split),
        in_specs=in_specs,
        out_specs=out_specs,
        out_shape=out_shape,
        scratch_shapes=scratch + sems,
        compiler_params=pltpu.CompilerParams(collective_id=3, has_side_effects=True, vmem_limit_bytes=62 * 1024 * 1024),
        name="scatter_sums",
    )(*args)
def backward_kernel(*refs, chunks, copies, n, inside, extra, split):
    ins = 14 + (1 if inside else 0) + (1 if split else 0) + (1 if extra else 0)
    (gg_ref, gact_ref, x_ref, dt_ref, slope_ref, start_ref, sel_ref, ci_ref, stepw_ref, decay_ref, skip_ref,
     taps_ref, cbias_ref, selw_ref) = refs[:14]
    mixed_ref = refs[14] if inside else None
    gin_ref = refs[ins - 1 - extra] if split else None
    gout_ref = refs[ins - 1] if extra else None
    outs = 2 + (1 if inside else 0) + (1 if split else 0) + (1 if extra else 0)
    gci_ref, late_ref = refs[ins:ins + 2]
    red_ref = refs[ins + 2] if inside else None
    all_ref = refs[ins + outs - 1 - extra] if split else None
    gsum_ref = refs[ins + outs - 1] if extra else None
    refs = refs[ins + outs:]
    (gg_v, gact_v, x_v, dt_v, slope_v, start_v, gci_v, gvals_v, part_v, recv_v, sel2_v,
     u_s, gy_s, gu_s, ah_s, bcoef_s, bt_s, hist_s, adj_a, harm_a, adj_b, harm_b, db_s, dc_s, carry_s, gd_s, rate_s, factor_s, kept_s,
     gstepw_ref, gsbias_ref, gskip_ref, gtaps_ref, gcbias_ref, gselw_ref,
     ext_s, gext_s, in_sem, gci_sem, send1, recv1, send2, recv2) = refs[:43]
    refs = refs[43:]
    if inside:
        own_v, yrecv_v, zrecv_v, own_sem, ysend, yrecv, zup, zdown, zrecv = refs[:9]
        refs = refs[9:]
    if extra:
        core_v, half_v, far_v, esend, erecv, asend, arecv, bsend, brecv = refs[:9]
        refs = refs[9:]
    if split:
        trade = Exchange(gin_ref, all_ref, refs[:5], refs[5:14], chunks, copies)
    zs, ys = grid_of(chunks, copies)
    xs = copies // 2
    me, mine = lax.axis_index("seq"), lax.axis_index("dp")
    z, y = me // ys, me % ys
    xd, cd = mine // 2, mine % 2
    rows = sel_ref.shape[1]
    rank = stepw_ref.shape[0]
    count = rows * chunks

    def where_of(i):
        return chunks - 1 - i % chunks, i // chunks

    streams = ((gg_ref, gg_v), (gact_ref, gact_v), (x_ref, x_v), (dt_ref, dt_v), (slope_ref, slope_v), (start_ref, start_v))

    def fetch(i):
        c, r = where_of(i)
        return [pltpu.make_async_copy(src.at[c, r], dst.at[i % 2], in_sem.at[k, i % 2]) for k, (src, dst) in enumerate(streams)]

    for one in fetch(0):
        one.start()
    if inside:
        tokens, model = red_ref.shape
        half = tokens // 2
        own_loads = [pltpu.make_async_copy(mixed_ref.at[t * ys + y], own_v.at[t], own_sem.at[t]) for t in range(zs)]
        for one in own_loads:
            one.start()
    meet(chunks, copies if extra else 1)

    if split:
        trade.begin()

    if inside:
        tables = order_of(zs)

        def dest(i):
            got = 0
            for k in range(zs):
                for q in range(zs):
                    got = got + jnp.where((z == k) & (i == q), tables[k][q], 0)
            return got

        def part_rows(h):
            return pl.ds(h * half, half)

        def to_side(i, h):
            return remote(mixed_ref.at[dest(i) * ys + 1 - y, part_rows(h)], yrecv_v.at[i, part_rows(h)], ysend.at[i, h], yrecv.at[i, h], {"seq": z * ys + 1 - y})

        def arrived(i, h):
            return remote(yrecv_v.at[i, part_rows(h)], yrecv_v.at[i, part_rows(h)], ysend.at[i, h], yrecv.at[i, h], {"seq": z * ys + 1 - y})

        def climb(t, h):
            return remote(own_v.at[t, part_rows(h)], zrecv_v.at[t, part_rows(h)], zup.at[t, h], zrecv.at[t, h], {"seq": (z + 1) * ys + y})

        def sink(t, h):
            slot = jnp.where(t == z - 1, zs, t)
            return remote(own_v.at[t, part_rows(h)], zrecv_v.at[slot, part_rows(h)], zdown.at[t, h], zrecv.at[slot, h], {"seq": (z - 1) * ys + y})

        def from_z(slot, h):
            return remote(zrecv_v.at[slot, part_rows(h)], zrecv_v.at[slot, part_rows(h)], zup.at[0, h], zrecv.at[slot, h], {"seq": lax.rem(me + 1, chunks)})

        def accumulate(t, h, buf, slot):
            def one(r, _):
                sl = pl.ds(pl.multiple_of(h * half + r * 32, 32), 32)
                own_v[t, sl, :] = own_v[t, sl, :] + buf[slot, sl, :]
                return 0
            lax.fori_loop(0, half // 32, one, 0)

        def settle(i):
            t = dest(i)
            for h in range(2):
                arrived(i, h).wait_recv()
                accumulate(t, h, yrecv_v, i)

                @pl.when((t >= z) & (z > 0))
                def _():
                    from_z(t, h).wait_recv()
                    accumulate(t, h, zrecv_v, t)

                @pl.when((t < z) & (z + 1 < zs))
                def _():
                    from_z(t, h).wait_recv()
                    accumulate(t, h, zrecv_v, t)

                @pl.when((t == z) & (z + 1 < zs))
                def _():
                    from_z(zs, h).wait_recv()
                    accumulate(t, h, zrecv_v, zs)

                @pl.when(t > z)
                def _():
                    climb(t, h).start()

                @pl.when(t < z)
                def _():
                    sink(t, h).start()

            @pl.when(i + 2 < zs)
            def _():
                for h in range(2):
                    to_side(i + 2, h).start()

        for i in range(2):
            for h in range(2):
                to_side(i, h).start()
        edge = (z == 0) | (z == zs - 1)

    if extra:
        grows = gout_ref.shape[0] // 2

        def part_of(core):
            return pl.ds(pl.multiple_of(core * grows, grows), grows)

        to_core = remote(gout_ref.at[part_of(1 - cd)], core_v, esend, erecv, {"dp": xd * 2 + 1 - cd})

        def across(j):
            return remote(half_v, far_v.at[xd], asend.at[j], arecv.at[xd], {"dp": lax.rem(xd + j, xs) * 2 + cd})

        def from_across(j):
            q = lax.rem(xd + j, xs)
            return remote(far_v.at[q], far_v.at[q], asend.at[j], arecv.at[q], {"dp": q * 2 + cd})

        back_out = remote(gsum_ref.at[part_of(cd)], gsum_ref.at[part_of(cd)], bsend, brecv, {"dp": xd * 2 + 1 - cd})
        back_in = remote(gsum_ref.at[part_of(1 - cd)], gsum_ref.at[part_of(1 - cd)], bsend, brecv, {"dp": xd * 2 + 1 - cd})
        to_core.start()

        def by_rows(fn):
            def one(i, _):
                fn(pl.ds(pl.multiple_of(i * 16, 16), 16), pl.ds(pl.multiple_of(cd * grows + i * 16, 16), 16))
                return 0
            lax.fori_loop(0, grows // 16, one, 0)

        def chip_sum():
            to_core.wait_recv()

            def fold(at, full):
                half_v[at, :] = (gout_ref[full, :].astype(F32) + core_v[at, :].astype(F32)).astype(BF16)
            by_rows(fold)
            for j in range(1, xs):
                across(j).start()

        def whole_sum():
            for j in range(1, xs):
                from_across(j).wait_recv()

            def fold(at, full):
                total = half_v[at, :].astype(F32)
                for j in range(1, xs):
                    total = total + far_v[lax.rem(xd + j, xs), at, :].astype(F32)
                gsum_ref[full, :] = total.astype(BF16)
            by_rows(fold)
            back_out.start()

    def first(s, r):
        return remote(part_v.at[s, r], recv_v.at[me, r], send1.at[s, r], recv1.at[me, r], {"seq": s})

    def landed_first(s, r):
        return remote(part_v.at[s, r], recv_v.at[s, r], send1.at[s, r], recv1.at[s, r], {"seq": s})

    def second(s, r):
        return remote(sel2_v.at[me, r], sel2_v.at[me, r], send2.at[s, r], recv2.at[me, r], {"seq": s})

    def landed_second(s, r):
        return remote(sel2_v.at[s, r], sel2_v.at[s, r], send2.at[s, r], recv2.at[s, r], {"seq": s})

    def every_other(fn):
        def one(k, _):
            fn(lax.rem(me + k, chunks))
            return 0
        lax.fori_loop(1, chunks, one, 0)

    def send_row(r):
        every_other(lambda s: first(s, r).start())
        recv_v[me, r] = part_v[me, r]

    def sum_row(r):
        every_other(lambda s: landed_first(s, r).wait_recv())
        total = recv_v[0, r].astype(F32)
        for s in range(1, chunks):
            total = total + recv_v[s, r].astype(F32)
        sel2_v[me, r] = total.astype(BF16)
        every_other(lambda s: second(s, r).start())

    for ref in (gstepw_ref, gsbias_ref, gskip_ref, gd_s, gtaps_ref, gcbias_ref, gselw_ref):
        ref[...] = jnp.zeros_like(ref)
    rate_s[...] = -jnp.exp(decay_ref[...].astype(F32)) * LOG2E

    def gci_out(i):
        c, r = where_of(i)
        return pltpu.make_async_copy(gci_v.at[i % 2], gci_ref.at[c, r], gci_sem.at[i % 2])

    def scan(i, _):
        c, r = where_of(i)
        slot = i % 2

        @pl.when(i + 1 < count)
        def _():
            for one in fetch(i + 1):
                one.start()

        for one in fetch(i):
            one.wait()
        back_step(sel_ref[c, r].astype(F32), x_v[slot].astype(F32), i % chunks == 0, gact_v.at[slot], gg_v.at[slot],
                  start_v.at[slot], dt_v.at[slot], slope_v.at[slot], stepw_ref, skip_ref,
                  gvals_v.at[c, r], part_v.at[c, r], gstepw_ref, gsbias_ref, gskip_ref,
                  u_s, gy_s, gu_s, ah_s, bcoef_s, bt_s, hist_s, adj_a, harm_a, adj_b, harm_b, db_s, dc_s, carry_s, gd_s, rate_s, factor_s, kept_s, rank, n)
        late = min(3, chunks - 1)

        @pl.when((i % chunks == chunks - 1) & (r + 1 < rows))
        def _():
            send_row(r)

        @pl.when((i % chunks == late) & (r > 0))
        def _():
            sum_row(r - 1)

        if split:
            pl.when(i == 1)(trade.chip)
            pl.when(i == 5)(trade.spread)
            pl.when(i == 14)(trade.share)
        if extra:
            pl.when(i == 2)(chip_sum)
            pl.when(i == 8)(whole_sum)
        if inside:
            lo = jnp.where(edge, jnp.where(i == 4, 0, jnp.where(i == 9, 1, 2)), jnp.where(i == 9, 0, 1))
            hi = jnp.where(edge, lo + 1, jnp.where(i == 9, 1, jnp.where(i == 13, 3, 0)))

            @pl.when((i == 4) | (i == 9) | (i == 13))
            def _():
                for k in range(own_v.shape[0]):
                    pl.when(i == 4)(own_loads[k].wait)

                def one(k, _):
                    settle(k)
                    return 0
                lax.fori_loop(lo, hi, one, 0)
        return 0

    lax.fori_loop(0, count, scan, 0)
    send_row(rows - 1)

    def conv(i, _):
        c, r = where_of(i)

        @pl.when(i >= 2)
        def _():
            gci_out(i - 2).wait()

        conv_back_step(ci_ref.at[c, r], ci_ref.at[jnp.maximum(c - 1, 0), r], c == 0, i % chunks == 0, gvals_v.at[c, r], sel2_v.at[c, r],
                       taps_ref, cbias_ref, selw_ref, gci_v.at[i % 2], gtaps_ref, gcbias_ref, gselw_ref, ext_s, gext_s)
        gci_out(i).start()
        return 0

    for r in range(rows - 1):
        every_other(lambda s: landed_second(s, r).wait_recv())
    lax.fori_loop(0, count - chunks, conv, 0)
    sum_row(rows - 1)
    if inside:
        settle(zs - 1)
        red_ref[...] = own_v[z]
    if split:
        trade.pass_on()
    every_other(lambda s: landed_second(s, rows - 1).wait_recv())
    lax.fori_loop(count - chunks, count, conv, 0)
    picked, taps = gselw_ref.shape[0], gtaps_ref.shape[0]
    late_ref[0:picked, :] = gselw_ref[...].astype(BF16)
    late_ref[picked:picked + rank, :] = gstepw_ref[...].astype(BF16)
    late_ref[picked + rank:picked + rank + n, :] = (gd_s[...] * rate_s[...] * (1.0 / LOG2E)).astype(BF16)
    filler = jnp.zeros((13 - taps, gtaps_ref.shape[1]), F32)
    late_ref[picked + rank + n:, :] = jnp.concatenate([gtaps_ref[...], gsbias_ref[...], gskip_ref[...], gcbias_ref[...], filler], axis=0).astype(BF16)
    for i in range(max(0, count - 2), count):
        gci_out(i).wait()
    if split:
        trade.finish()
    for r in range(rows):
        every_other(lambda s: first(s, r).wait_send())
        every_other(lambda s: second(s, r).wait_send())
    if extra:
        to_core.wait_send()
        for j in range(1, xs):
            across(j).wait_send()
        back_in.wait_recv()
        back_out.wait_send()
    if inside:
        for i in range(zs):
            t = dest(i)
            for h in range(2):
                to_side(i, h).wait_send()

                @pl.when(t > z)
                def _():
                    climb(t, h).wait_send()

                @pl.when(t < z)
                def _():
                    sink(t, h).wait_send()


def backward(gg, gact, x, dt, slope, starts, sel, ci, stepw, decay, skip, taps, cbias, selw, mixed, ging, gout, copies, n):
    chunks, rows, length, width = ci.shape
    rank = stepw.shape[0]
    zs, ys = grid_of(chunks, copies)
    xs = max(1, copies // 2)
    wide = BLOCK * n
    inside = mixed is not None
    extra = copies % 2 == 0
    split = ging is not None
    sds = jax.ShapeDtypeStruct
    dma = pltpu.SemaphoreType.DMA
    vmem = pl.BlockSpec(memory_space=pltpu.VMEM)
    hbm = pl.BlockSpec(memory_space=pl.ANY)
    args = [gg, gact, x, dt, slope, starts, sel, ci, stepw, decay, skip, taps, cbias, selw]
    in_specs = [hbm] * 6 + [vmem] * 8
    out_specs = [hbm, vmem]
    out_shape = [sds(ci.shape, BF16), sds((selw.shape[0] + rank + n + 16, width), BF16)]
    tile, coef = (length, width), sel.shape
    scratch = [pltpu.VMEM((2,) + tile, F32), pltpu.VMEM((2,) + tile, F32), pltpu.VMEM((2,) + tile, BF16),
               pltpu.VMEM((2,) + tile, F32), pltpu.VMEM((2,) + tile, F32), pltpu.VMEM((2, n, width), F32),
               pltpu.VMEM((2,) + tile, BF16), pltpu.VMEM(ci.shape, F32),
               pltpu.VMEM(coef, BF16), pltpu.VMEM(coef, BF16), pltpu.VMEM(coef, BF16),
               pltpu.VMEM(tile, F32), pltpu.VMEM(tile, F32), pltpu.VMEM(tile, F32), pltpu.VMEM(tile, F32),
               pltpu.VMEM((length, wide), BF16), pltpu.VMEM((2 * n, length), F32), pltpu.VMEM((length * n, width), BF16),
               pltpu.VMEM((wide, width), BF16), pltpu.VMEM((wide, width), BF16), pltpu.VMEM((wide, width), BF16), pltpu.VMEM((wide, width), BF16),
               pltpu.VMEM((length, wide), F32), pltpu.VMEM((length, wide), F32),
               pltpu.VMEM((n, width), F32), pltpu.VMEM((n, width), F32), pltpu.VMEM((n, width), F32),
               pltpu.VMEM((length * n, width), F32), pltpu.VMEM((length * n, width), F32),
               pltpu.VMEM((rank, width), F32), pltpu.VMEM((1, width), F32), pltpu.VMEM((1, width), F32),
               pltpu.VMEM(taps.shape, F32), pltpu.VMEM((1, width), F32), pltpu.VMEM(selw.shape, F32),
               pltpu.VMEM((length + 8, width), F32), pltpu.VMEM((length + 8, width), F32),
               dma((6, 2)), dma((2,)), dma((chunks, rows)), dma((chunks, rows)), dma((chunks, rows)), dma((chunks, rows))]
    if inside:
        tokens, model = mixed.shape[1:]
        args.append(mixed)
        in_specs.append(hbm)
        out_specs.append(vmem)
        out_shape.append(sds((tokens, model), BF16))
        scratch += [pltpu.VMEM((zs, tokens, model), BF16), pltpu.VMEM((zs, tokens, model), BF16), pltpu.VMEM((zs + 1, tokens, model), BF16),
                    dma((zs,)), dma((zs, 2)), dma((zs, 2)), dma((zs, 2)), dma((zs, 2)), dma((zs + 1, 2))]
    if split:
        args.append(ging)
        in_specs.append(hbm)
        out_specs.append(hbm)
        out_shape.append(sds((copies * ging.shape[2], chunks * width), BF16))
    if extra:
        args.append(gout)
        in_specs.append(vmem)
        out_specs.append(vmem)
        out_shape.append(sds(gout.shape, BF16))
        part = (gout.shape[0] // 2, gout.shape[1])
        scratch += [pltpu.VMEM(part, BF16), pltpu.VMEM(part, BF16), pltpu.VMEM((xs,) + part, BF16),
                    dma(()), dma(()), dma((xs,)), dma((xs,)), dma(()), dma(())]
    if split:
        scratch += exchange_scratch(chunks, copies, ging.shape[2], width)
    return pl.pallas_call(
        functools.partial(backward_kernel, chunks=chunks, copies=copies, n=n, inside=inside, extra=extra, split=split),
        in_specs=in_specs,
        out_specs=out_specs,
        out_shape=out_shape,
        scratch_shapes=scratch,
        compiler_params=pltpu.CompilerParams(collective_id=2, has_side_effects=True, vmem_limit_bytes=63 * 1024 * 1024),
        name="backward",
    )(*args)


from jax.sharding import PartitionSpec as P


def local(hidden, grad_out, lengths, norm_gain, input_weight, conv_weight, conv_bias, select_weight,
          step_weight, step_bias, decay_log, skip_weight, output_weight):
    rows, length, model = hidden.shape
    chunks = lax.axis_size("seq")
    copies = lax.axis_size("dp")
    width = output_weight.shape[0]
    share = input_weight.shape[0]
    rank = step_weight.shape[0]
    n = decay_log.shape[0]
    tokens = chunks * rows * length
    here = lax.axis_index("seq")

    split = (share // copies) % 16 == 0 and copies % 2 == 0
    normed, ci, gate, w_all, gain_row = gather_project(
        hidden.reshape(rows * length, model), input_weight, norm_gain.astype(F32).reshape(1, share), chunks, copies, share, split)
    normed = normed.reshape(tokens, model)
    slots = here * length + lax.broadcasted_iota(jnp.int32, (rows, length), 1)
    valid = (slots < lengths[:, None]).astype(F32)[..., None]
    cotangent = grad_out.astype(F32) * valid
    shaped = lambda a: a.reshape(chunks, rows, length, a.shape[-1])
    ci, gate = shaped(ci), shaped(gate)
    bias_row = conv_bias.reshape(1, width)
    step_row = step_bias.reshape(1, width)
    skip_row = skip_weight.reshape(1, width)
    gm, sel, x, gated, gact, tail, dt, slope, starts, mixed = forward(
        ci, gate, cotangent.astype(BF16).reshape(rows * length, model), conv_weight, bias_row, select_weight,
        step_weight, step_row, decay_log, skip_row, output_weight, copies, n)
    gm = gm.reshape(tokens, model)
    gated2 = gated.reshape(tokens, width)
    gg = lax.dot_general(gm, output_weight, (((1,), (1,)), ((), ())), preferred_element_type=F32)
    ggate = (gg * tail.reshape(tokens, width).astype(F32)).astype(BF16)
    zs, ys = grid_of(chunks, copies)
    inside = ys == 2 and zs == 4
    source = hidden.astype(F32)
    tn = lambda a, b: lax.dot_general(a, b, (((0,), (0,)), ((), ())), preferred_element_type=F32)
    blocks = lambda g: tn(normed, g).astype(BF16).reshape(chunks, copies, share // copies, width)
    ging = blocks(ggate)
    gout = tn(gated2, gm).astype(BF16)
    flat = lambda a: a.reshape(chunks, rows * length, a.shape[-1])
    got = backward(shaped(gg), gact, x, dt, slope, starts, sel, ci, step_weight, decay_log, skip_row, conv_weight, bias_row, select_weight,
                   mixed if inside else None, ging if split else None, gout, copies, n)
    gci, late = got[:2]
    mixed = got[2].reshape(rows, length, model) if inside else lax.psum_scatter(shaped(mixed), "seq", scatter_dimension=0, tiled=False)
    gout = got[-1].astype(F32)
    output = ((source + mixed.astype(F32)) * valid).astype(BF16)
    tap_count = conv_weight.shape[0]
    done = scatter_sums(flat(gci), ggate.reshape(chunks, rows * length, width), w_all, late, flat(shaped(normed)), chunks, copies, split)
    scaled, late = done[:2]
    if split:
        gin = jnp.concatenate([done[2], got[-2]], axis=1).astype(F32)
    else:
        gin = jnp.stack([blocks(gci.reshape(tokens, width)), ging], axis=3)
        gin = lax.psum_scatter(gin, "dp", scatter_dimension=1, tiled=False)
        gin = lax.all_to_all(gin, "seq", split_axis=0, concat_axis=2, tiled=False)
        gin = lax.all_gather(gin.reshape(share // copies, 2 * chunks * width), "dp", axis=0, tiled=True).astype(F32)
    ggain = jnp.sum(gin * input_weight.astype(F32), axis=1) / norm_gain.astype(F32)
    scaled = scaled.reshape(rows, length, model).astype(F32) * gain_row
    inverse = lax.rsqrt(jnp.mean(source * source, axis=-1, keepdims=True) + EPSILON)
    ghidden = inverse * scaled - source * inverse ** 3 * jnp.mean(scaled * source, axis=-1, keepdims=True) + cotangent
    sizes = (select_weight.shape[0], rank, n, tap_count)
    ends = [sum(sizes[:k + 1]) for k in range(len(sizes))]
    gselw, gstepw, gdecay, gtaps = (late[e - k:e] for e, k in zip(ends, sizes))
    gstepb, gskip, gconvb = (late[ends[-1] + k] for k in range(3))
    return (output, ghidden, ggain, gin, gtaps, gconvb, gselw, gstepw, gstepb,
            gdecay, gskip, gout)


def solution(mesh):
    tok, vec, col, row = P("dp", "seq", None), P("seq"), P(None, "seq"), P("seq", None)
    return jax.shard_map(
        local,
        mesh=mesh,
        in_specs=(tok, tok, P("dp"), vec, row, col, vec, col, col, vec, col, vec, row),
        out_specs=(tok, tok, vec, row, col, vec, col, col, vec, col, vec, row),
        check_vma=False,
    )
```
